32 devices in a mesh: dp: 4 (over y, core), cp: 8 (over z, x).
Axes of the slice: x: 2, y: 2, z: 4, core: 2. Of those that a mesh axis runs over, the one named last changes fastest.
Arguments:
- tokens: bfloat16 [8192, 1600], P(('dp', 'cp')), may hold values from -6 to 6
- params: bfloat16 [19456, 1600], P(('dp', 'cp')), as said below
- out_grad: bfloat16 [8192, 1600], P(('dp', 'cp')), may hold values from -6 to 6
- lengths: int32 [4, 2], P('dp'), may hold values from 1024 to 1024, as said below
Outputs:
- output: bfloat16 [8192, 1600], P(('dp', 'cp'))
- input_grad: bfloat16 [8192, 1600], P(('dp', 'cp'))
- param_grad: float32 [19456, 1600], P(('dp', 'cp'))
The draws below stay inside these ranges and needn't reach their ends.
Inputs may be any that keep to these rules, and one draw needn't show every extreme that they name: Rows of params past the used ones are never read. Multiples of 128; a group's lengths sum to 2048; one of them is 1024 and one 1024.
All inputs are finite; a program needn't handle non-finite values.
Results may differ from the reference program's by a relative error of at most 0.028.
Values may be sent and summed in bfloat16 or wider, within the bound.
A program may use at most 832 MiB of HBM per device.

```python
import jax
import jax.numpy as jnp
from jax import lax

D = 1600
HEADS = 25
FF = 6400
HEAD_DIM = 64
TILE = 128
MIN_LEN = 1024
TOK_DEV = 256
GROUP = 2048
TOKENS = 8192
SEQS = 2
LONGEST = 1024
REACH = 4
ROWS = 19456
N_DP = 4


def draw_params(key, part):
    keys = jax.random.split(key, 2)
    noise = jax.random.normal(keys[0], (ROWS, D), jnp.float32)
    uniform_draw = jax.random.uniform(keys[1], (ROWS, D), jnp.float32, -1.0, 1.0)
    row_index = jnp.arange(ROWS, dtype=jnp.int32)[:, None]
    vec_start = 4 * D + 2 * FF
    offset = row_index - vec_start
    row_scale = jnp.where(row_index < 3 * D, D ** (-0.5), jnp.where(row_index < 4 * D, 3.0 * D ** (-0.5), jnp.where(row_index < 4 * D + FF, D ** (-0.5), jnp.where(row_index < vec_start, 1.5 * FF ** (-0.5), 0.4))))
    values = noise * row_scale
    is_gain = (offset == 0) | (offset == 5)
    values = jnp.where(is_gain, 1.0 + 0.45 * uniform_draw, values)
    return values.astype(jnp.bfloat16)


def draw_lengths(key, part):
    tile_units = (GROUP - LONGEST - (SEQS - 1) * MIN_LEN) // TILE
    others = SEQS - 2

    def one_group(sub_key):
        key_order, key_moves, key_final = jax.random.split(sub_key, 3)
        chosen = jnp.array([LONGEST, MIN_LEN], jnp.int32)
        if others > 0:
            share_base = tile_units // others
            remainder = tile_units - share_base * others
            ranking = jax.random.permutation(key_order, others)
            extras = share_base + (ranking < remainder).astype(jnp.int32)
            shifted = jax.random.randint(key_moves, (others,), 0, share_base + 1)
            extras = extras - shifted + jnp.roll(shifted, 1)
            chosen = jnp.concatenate([chosen, (MIN_LEN + TILE * extras).astype(jnp.int32)])
        return chosen[jax.random.permutation(key_final, SEQS)]
    return jax.vmap(one_group)(jax.random.split(key, N_DP))


def level_of(rng, dims, cuts, low, top_value):
    level = 1.0
    for axis_at, blocks in cuts:
        steps = jax.random.uniform(jax.random.fold_in(jax.random.fold_in(rng, 6), axis_at), (blocks,), jnp.float32, low / len(cuts), top_value / len(cuts))
        level = level * jnp.repeat(jnp.exp(steps), dims[axis_at] // blocks).reshape((-1,) + (1,) * (len(dims) - 1 - axis_at))
    return level


def scatter_about(stream_key, dims, width, reach, shards=(), held_as=jnp.bfloat16):
    entries = width * jax.random.normal(stream_key, dims, jnp.float32)
    if shards:
        entries = entries * level_of(stream_key, dims, shards, -0.22, 0.18)
    return jnp.clip(entries, -reach, reach).astype(held_as)


def setup_inputs(seed: int = 0) -> dict:
    arg_keys = jax.random.split(jax.random.key(seed), 5)
    tokens = scatter_about(arg_keys[0], (TOKENS, D), 1.0, 6.0, ((0, 32),))
    params = draw_params(jax.random.fold_in(arg_keys[4], 71), 0)
    out_grad = scatter_about(arg_keys[2], (TOKENS, D), 1.0, 6.0, ((0, 32),))
    lengths = draw_lengths(jax.random.fold_in(arg_keys[4], 71), 0)
    return {"tokens": tokens, "params": params, "out_grad": out_grad, "lengths": lengths}


@jax.custom_vjp
def low(v):
    return lax.optimization_barrier(v.astype(jnp.bfloat16)).astype(jnp.float32)

@jax.custom_vjp
def low_back(v):
    return v

def low_keep(v):
    return (low(v), None)

def low_pass(kept, grad):
    return (grad,)

def back_keep(v):
    return (v, None)

def back_low(kept, grad):
    return (low(grad),)
low.defvjp(low_keep, low_pass)
low_back.defvjp(back_keep, back_low)
EPSILON = 1e-05
MASKED = -1e+30
GELU_SCALE = 0.7978845608028654
HIGHEST = lax.Precision.HIGHEST

def layer_norm(values, gain_row, bias_row):
    centre = values - lax.optimization_barrier(jnp.mean(values, axis=-1, keepdims=True))
    spread = lax.optimization_barrier(jnp.mean(centre * centre, axis=-1, keepdims=True))
    return centre * lax.rsqrt(spread + EPSILON) * gain_row + bias_row

def gelu_tanh(values):
    return 0.5 * values * (1.0 + jnp.tanh(GELU_SCALE * (values + 0.044715 * values * values * values)))

def segment_of(position, seq_ends):
    return lax.optimization_barrier(jnp.sum((position[:, None] >= seq_ends[None, :]).astype(jnp.int32), axis=1))

def attend(queries, key_rows, value_rows, lengths_row):
    seq_ends = jnp.cumsum(lengths_row).astype(jnp.int32)
    front_pad = REACH * TOK_DEV
    window = front_pad + TOK_DEV
    segment = segment_of(jnp.arange(GROUP, dtype=jnp.int32), seq_ends)
    padded_seg = jnp.concatenate([jnp.full((front_pad,), -1, jnp.int32), segment])
    key_pad = jnp.pad(key_rows, ((front_pad, 0), (0, 0), (0, 0)))
    value_pad = jnp.pad(value_rows, ((front_pad, 0), (0, 0), (0, 0)))
    score_scale = HEAD_DIM ** (-0.5)

    def one_block(block_index):
        first_row = (block_index * TOK_DEV).astype(jnp.int32)
        query_blk = lax.dynamic_slice_in_dim(queries, first_row, TOK_DEV, 0)
        key_blk = lax.dynamic_slice_in_dim(key_pad, first_row, window, 0)
        value_blk = lax.dynamic_slice_in_dim(value_pad, first_row, window, 0)
        query_seg = lax.dynamic_slice_in_dim(segment, first_row, TOK_DEV, 0)
        key_seg = lax.dynamic_slice_in_dim(padded_seg, first_row, window, 0)
        query_pos = first_row + jnp.arange(TOK_DEV, dtype=jnp.int32)
        key_pos = first_row - front_pad + jnp.arange(window, dtype=jnp.int32)
        allowed = (key_seg[None, :] == query_seg[:, None]) & (key_pos[None, :] <= query_pos[:, None])
        scores = low_back(jnp.einsum('qhd,khd->hqk', query_blk, key_blk, precision=HIGHEST) * score_scale)
        scores = jnp.where(allowed[None], scores, MASKED)
        row_top = lax.optimization_barrier(jnp.max(scores, axis=-1, keepdims=True))
        log_total = row_top + jnp.log(lax.optimization_barrier(jnp.sum(jnp.exp(scores - row_top), axis=-1, keepdims=True)))
        weights = low(jnp.exp(scores - log_total))
        return jnp.einsum('hqk,khd->qhd', weights, value_blk, precision=HIGHEST)
    mixed = lax.map(jax.checkpoint(one_block), jnp.arange(GROUP // TOK_DEV, dtype=jnp.int32))
    return mixed.reshape(GROUP, D)

def group_forward(inputs, flat_table, lengths_row):
    out_end = 4 * D
    fc_end = out_end + FF
    proj_end = fc_end + FF
    vec_end = proj_end + 8
    w_attn = flat_table[0:3 * D]
    w_out = flat_table[3 * D:out_end]
    w_fc = flat_table[out_end:fc_end]
    w_proj = flat_table[fc_end:proj_end]
    vectors = flat_table[proj_end:vec_end]
    fc_bias = flat_table[vec_end:vec_end + FF // D].reshape(FF)
    act_one = low(layer_norm(inputs, vectors[0], vectors[1]))
    qkv_bias = jnp.concatenate([vectors[2], jnp.zeros_like(vectors[2]), vectors[3]])
    qkv = low(low_back(jnp.dot(act_one, w_attn.T, precision=HIGHEST) + qkv_bias))
    queries = qkv[:, :D].reshape(GROUP, HEADS, HEAD_DIM)
    key_rows = qkv[:, D:2 * D].reshape(GROUP, HEADS, HEAD_DIM)
    value_rows = qkv[:, 2 * D:].reshape(GROUP, HEADS, HEAD_DIM)
    mixed = low(low_back(attend(queries, key_rows, value_rows, lengths_row)))
    attn_out = low_back(jnp.dot(mixed, w_out.T, precision=HIGHEST) + vectors[4])
    residual = inputs + attn_out
    act_two = low(layer_norm(residual, vectors[5], vectors[6]))
    pre_act = low_back(jnp.dot(act_two, w_fc.T, precision=HIGHEST) + fc_bias)
    act_hidden = low(gelu_tanh(pre_act))
    return residual + jnp.dot(act_hidden, w_proj, precision=HIGHEST) + vectors[7]

def reference(tokens, params, out_grad, lengths):
    weights = params.astype(jnp.float32)
    inputs = tokens.astype(jnp.float32).reshape(N_DP, GROUP, D)
    cotangent = out_grad.astype(jnp.float32).reshape(N_DP, GROUP, D)

    def one_group(summed_grads, group_data):
        group_in, group_cot, group_len = group_data
        result, pullback = jax.vjp(lambda values, flat_table: group_forward(values, flat_table, group_len), group_in, weights)
        input_back, table_back = pullback(group_cot)
        return (summed_grads + table_back, (result, input_back))
    summed_grads, (results, input_backs) = lax.scan(one_group, jnp.zeros_like(weights), (inputs, cotangent, lengths))
    return (results.reshape(TOKENS, D).astype(jnp.bfloat16), input_backs.reshape(TOKENS, D).astype(jnp.bfloat16), summed_grads)
```

```python
import functools

import jax
import jax.numpy as jnp
from jax import lax
from jax.experimental import pallas as pl
from jax.experimental.pallas import tpu as pltpu
from jax.sharding import PartitionSpec as P

HEADS = 25
FF = 6400
HEAD_DIM = 64
TILE = 128
MIN_LEN = 1024
MAX_LEN = 4096


EPSILON = 1e-05
MASKED = -1e30
GELU_SCALE = 0.7978845608028654


def from_behind(value, axis, by):
    length = lax.axis_size(axis)
    pairs = [(i, i + by) for i in range(length) if 0 <= i + by < length]
    return lax.ppermute(value, axis, pairs)


def layer_norm(values, gain_row, bias_row):
    centre = values - jnp.mean(values, axis=-1, keepdims=True)
    spread = jnp.mean(centre * centre, axis=-1, keepdims=True)
    return centre * lax.rsqrt(spread + EPSILON) * gain_row + bias_row


def gelu_tanh(values):
    return (
        0.5 * values * (1.0 + jnp.tanh(GELU_SCALE * (values + 0.044715 * values * values * values)))
    )


def segment_of(position, seq_ends):
    return jnp.sum((position[:, None] >= seq_ends[None, :]).astype(jnp.int32), axis=1)


def unpack(gathered, model_width, hidden):
    out_end = 4 * model_width
    fc_end = out_end + hidden
    proj_end = fc_end + hidden
    vec_end = proj_end + 8
    return (
        gathered[0 : 3 * model_width],
        gathered[3 * model_width : out_end],
        gathered[out_end:fc_end],
        gathered[fc_end:proj_end],
        gathered[proj_end:vec_end].astype(jnp.float32),
        gathered[vec_end : vec_end + hidden // model_width].astype(jnp.float32).reshape(hidden),
    )


def matmul_nt(left_mat, right_mat):
    return lax.dot_general(
        left_mat, right_mat, (((1,), (1,)), ((), ())), preferred_element_type=jnp.float32
    )


def matmul_tn(left_mat, right_mat):
    return lax.dot_general(
        left_mat, right_mat, (((0,), (0,)), ((), ())), preferred_element_type=jnp.float32
    )


def matmul_nn(left_mat, right_mat):
    return jnp.dot(left_mat, right_mat, preferred_element_type=jnp.float32)


def per_device_general(tokens, params, out_grad, lengths):
    tok_rows, model_width = tokens.shape
    hidden = FF
    head_count = HEADS
    head_size = HEAD_DIM
    cp_count = lax.axis_size("cp")
    group_rows = tok_rows * cp_count
    seq_count = lengths.shape[1]
    longest = min(MAX_LEN, group_rows - (seq_count - 1) * MIN_LEN)
    reach_back = min(cp_count - 1, (longest + tok_rows - TILE - 1) // tok_rows)
    pair_count = (reach_back + 2) // 2
    score_scale = head_size ** (-0.5)
    gathered = lax.all_gather(params, ("dp", "cp"), axis=0, tiled=True)
    w_attn, w_out, w_fc, w_proj, vectors, fc_bias = unpack(gathered, model_width, hidden)
    inputs = tokens.astype(jnp.float32)
    act_one = layer_norm(inputs, vectors[0], vectors[1]).astype(jnp.bfloat16)
    qkv_bias = jnp.concatenate([vectors[2], jnp.zeros_like(vectors[2]), vectors[3]])
    qkv = (matmul_nt(act_one, w_attn) + qkv_bias).astype(jnp.bfloat16)
    queries = qkv[:, :model_width].reshape(tok_rows, head_count, head_size)
    key_value = qkv[:, model_width:]
    device = lax.axis_index("cp")
    seq_ends = jnp.cumsum(lengths[0])
    query_pos = device * tok_rows + jnp.arange(tok_rows, dtype=jnp.int32)
    query_seg = segment_of(query_pos, seq_ends)
    store = jnp.zeros((2 * pair_count, tok_rows, 2 * model_width), jnp.bfloat16)
    store = store.at[0].set(key_value)

    def fetch(step_index, state_pair):
        moving, held_rows = state_pair
        moving = from_behind(moving, "cp", 1)
        return (moving, lax.dynamic_update_index_in_dim(held_rows, moving, step_index, 0))

    _, store = lax.fori_loop(1, reach_back + 1, fetch, (key_value, store))

    def pair_mask(pair_index):
        owners = 2 * pair_index + jnp.arange(2, dtype=jnp.int32)
        key_pos = (
            (device - owners)[:, None] * tok_rows + jnp.arange(tok_rows, dtype=jnp.int32)[None, :]
        ).reshape(2 * tok_rows)
        usable = jnp.broadcast_to((owners <= reach_back)[:, None], (2, tok_rows)).reshape(
            2 * tok_rows
        ) & (key_pos >= 0)
        key_seg = segment_of(key_pos, seq_ends)
        return (
            (key_seg[None, :] == query_seg[:, None])
            & (key_pos[None, :] <= query_pos[:, None])
            & usable[None, :]
        )

    def pair_rows(pair_index):
        block_rows = lax.dynamic_slice_in_dim(store, 2 * pair_index, 2, 0).reshape(
            2 * tok_rows, 2 * model_width
        )
        return (
            block_rows[:, :model_width].reshape(2 * tok_rows, head_count, head_size),
            block_rows[:, model_width:].reshape(2 * tok_rows, head_count, head_size),
        )

    def pair_scores(key_rows, allowed):
        raw_scores = (
            jnp.einsum("qhd,khd->hqk", queries, key_rows, preferred_element_type=jnp.float32)
            * score_scale
        )
        return jnp.where(allowed[None], raw_scores, MASKED)

    def visit(work):

        def step_pair(pair_index, running):
            allowed = pair_mask(pair_index)
            result = work(pair_index, allowed, running)
            return result

        return step_pair

    def add_total(pair_index, allowed, running):
        row_top, summed = running
        key_rows, _ = pair_rows(pair_index)
        scores = pair_scores(key_rows, allowed)
        new_top = jnp.maximum(row_top, jnp.max(scores, axis=-1, keepdims=True))
        summed = summed * jnp.exp(row_top - new_top) + jnp.sum(
            jnp.exp(scores - new_top), axis=-1, keepdims=True
        )
        return (new_top, summed)

    start_top = jnp.full((head_count, tok_rows, 1), MASKED, jnp.float32)
    start_sum = jnp.zeros((head_count, tok_rows, 1), jnp.float32)
    row_top, summed = lax.fori_loop(0, pair_count, visit(add_total), (start_top, start_sum))
    log_total = row_top + jnp.log(summed)

    def add_mix(pair_index, allowed, running):
        key_rows, value_rows = pair_rows(pair_index)
        prob_rows = jnp.exp(pair_scores(key_rows, allowed) - log_total).astype(jnp.bfloat16)
        return running + jnp.einsum(
            "hqk,khd->qhd", prob_rows, value_rows, preferred_element_type=jnp.float32
        )

    mixed_full = lax.fori_loop(
        0, pair_count, visit(add_mix), jnp.zeros((tok_rows, head_count, head_size), jnp.float32)
    )
    mixed = mixed_full.reshape(tok_rows, model_width).astype(jnp.bfloat16)
    attn_out = matmul_nt(mixed, w_out) + vectors[4]
    residual = inputs + attn_out
    act_two = layer_norm(residual, vectors[5], vectors[6]).astype(jnp.bfloat16)
    pre_act = matmul_nt(act_two, w_fc) + fc_bias
    act_hidden = gelu_tanh(pre_act).astype(jnp.bfloat16)
    output = (residual + matmul_nn(act_hidden, w_proj) + vectors[7]).astype(jnp.bfloat16)
    gathered = lax.all_gather(params, ("dp", "cp"), axis=0, tiled=True)
    w_attn, w_out, w_fc, w_proj, vectors, fc_bias = unpack(gathered, model_width, hidden)
    grad_out_f = out_grad.astype(jnp.float32)
    grad_hidden = matmul_nt(out_grad, w_proj)
    _, pull_gelu = jax.vjp(gelu_tanh, pre_act)
    grad_fc = pull_gelu(grad_hidden)[0].astype(jnp.bfloat16)
    grad_act_two = matmul_nn(grad_fc, w_fc)
    _, pull_two = jax.vjp(layer_norm, residual, vectors[5], vectors[6])
    grad_res_norm, grad_gain_two, grad_bias_two = pull_two(grad_act_two)
    grad_res = grad_out_f + grad_res_norm
    grad_attn = grad_res.astype(jnp.bfloat16)
    grad_mix = (
        matmul_nn(grad_attn, w_out).astype(jnp.bfloat16).reshape(tok_rows, head_count, head_size)
    )
    grad_dot = jnp.transpose(jnp.sum(grad_mix.astype(jnp.float32) * mixed_full, axis=-1), (1, 0))[
        :, :, None
    ]

    def add_grads(pair_index, allowed, running):
        grad_query, grad_store = running
        key_rows, value_rows = pair_rows(pair_index)
        prob_rows = jnp.exp(pair_scores(key_rows, allowed) - log_total)
        grad_probs = jnp.einsum(
            "qhd,khd->hqk", grad_mix, value_rows, preferred_element_type=jnp.float32
        )
        grad_scores = (prob_rows * (grad_probs - grad_dot)).astype(jnp.bfloat16)
        grad_query = (
            grad_query
            + jnp.einsum("hqk,khd->qhd", grad_scores, key_rows, preferred_element_type=jnp.float32)
            * score_scale
        )
        grad_keys = (
            jnp.einsum("hqk,qhd->khd", grad_scores, queries, preferred_element_type=jnp.float32)
            * score_scale
        )
        grad_values = jnp.einsum(
            "hqk,qhd->khd",
            prob_rows.astype(jnp.bfloat16),
            grad_mix,
            preferred_element_type=jnp.float32,
        )
        pair_grad = jnp.concatenate(
            [
                grad_keys.reshape(2 * tok_rows, model_width),
                grad_values.reshape(2 * tok_rows, model_width),
            ],
            axis=1,
        )
        pair_grad = pair_grad.reshape(2, tok_rows, 2 * model_width)
        grad_store = lax.dynamic_update_slice_in_dim(grad_store, pair_grad, 2 * pair_index, 0)
        return (grad_query, grad_store)

    start_query = jnp.zeros((tok_rows, head_count, head_size), jnp.float32)
    start_store = jnp.zeros((2 * pair_count, tok_rows, 2 * model_width), jnp.float32)
    grad_query, grad_store = lax.fori_loop(
        0, pair_count, visit(add_grads), (start_query, start_store)
    )

    def send_back(step_index, moving):
        moving = moving + lax.dynamic_index_in_dim(
            grad_store, reach_back - step_index, 0, keepdims=False
        )
        return from_behind(moving.astype(jnp.bfloat16), "cp", -1).astype(moving.dtype)

    returned = lax.fori_loop(
        0, reach_back, send_back, jnp.zeros((tok_rows, 2 * model_width), jnp.float32)
    )
    grad_kv = returned + grad_store[0]
    grad_qkv = jnp.concatenate([grad_query.reshape(tok_rows, model_width), grad_kv], axis=1).astype(
        jnp.bfloat16
    )
    grad_qkv_f = grad_qkv.astype(jnp.float32)
    grad_act_one = matmul_nn(grad_qkv, w_attn)
    _, pull_one = jax.vjp(layer_norm, inputs, vectors[0], vectors[1])
    grad_in_norm, grad_gain_one, grad_bias_one = pull_one(grad_act_one)
    input_grad = (grad_res + grad_in_norm).astype(jnp.bfloat16)
    grad_vectors = jnp.stack(
        [
            grad_gain_one,
            grad_bias_one,
            jnp.sum(grad_qkv_f[:, :model_width], axis=0),
            jnp.sum(grad_qkv_f[:, 2 * model_width :], axis=0),
            jnp.sum(grad_attn.astype(jnp.float32), axis=0),
            grad_gain_two,
            grad_bias_two,
            jnp.sum(grad_out_f, axis=0),
        ]
    )
    grad_fc_bias = jnp.sum(grad_fc.astype(jnp.float32), axis=0).reshape(
        hidden // model_width, model_width
    )
    used_rows = 4 * model_width + 2 * hidden + 8 + hidden // model_width
    total_rows = gathered.shape[0]
    local_grad = jnp.concatenate(
        [
            matmul_tn(grad_qkv, act_one),
            matmul_tn(grad_attn, mixed),
            matmul_tn(grad_fc, act_two),
            matmul_tn(act_hidden, out_grad),
            grad_vectors,
            grad_fc_bias,
            jnp.zeros((total_rows - used_rows, model_width), jnp.float32),
        ],
        axis=0,
    )
    dp_count = lax.axis_size("dp")
    device_count = dp_count * cp_count
    share_rows = total_rows // device_count
    spread_rows = local_grad.reshape(device_count, 1, share_rows, model_width)
    received = lax.all_to_all(
        spread_rows.astype(jnp.bfloat16), ("dp", "cp"), split_axis=0, concat_axis=1, tiled=True
    ).astype(spread_rows.dtype)
    param_grad = jnp.sum(received, axis=1).reshape(share_rows, model_width)
    return (output, input_grad, param_grad)


MESH = pl.DeviceIdType.MESH
GRAIN = 8
NT = (((1,), (1,)), ((), ()))
TN = (((0,), (0,)), ((), ()))


def dot_nt(a, b):
    return lax.dot_general(a, b, NT, preferred_element_type=jnp.float32)


def dot_tn(a, b):
    return lax.dot_general(a, b, TN, preferred_element_type=jnp.float32)


def dot_nn(a, b):
    return jnp.dot(a, b, preferred_element_type=jnp.float32)


def flat_id(y, c, z, x):
    return ((y * 2 + c) * 4 + z) * 2 + x


def permute(value, move):
    pairs = []
    for y in range(2):
        for c in range(2):
            for z in range(4):
                for x in range(2):
                    to = move(y, c, z, x)
                    if to is not None:
                        pairs.append((flat_id(y, c, z, x), flat_id(*to)))
    return lax.ppermute(value, ("dp", "cp"), pairs)


def over_x(value):
    return permute(value, lambda y, c, z, x: (y, c, z, 1 - x))


def over_c(value):
    return permute(value, lambda y, c, z, x: (y, 1 - c, z, x))


def over_cx(value):
    return permute(value, lambda y, c, z, x: (y, 1 - c, z, 1 - x))


def over_y(value):
    return permute(value, lambda y, c, z, x: (1 - y, c, z, x))


def over_z(value, by):
    return permute(value, lambda y, c, z, x: (y, c, (z + by) % 4, x))


class Sizes:
    def __init__(self, width, hidden, heads, head_size, rows):
        self.width = width
        self.hidden = hidden
        self.heads = heads
        self.head_size = head_size
        self.quarter_heads = -(-heads // 4)
        self.part = self.quarter_heads * head_size
        self.part_grains = self.part // GRAIN
        self.width_grains = width // GRAIN
        self.spill = 4 * self.part_grains - self.width_grains
        self.qkv = 3 * self.part_grains // 8
        self.out = self.part_grains // 8
        self.mlp = hidden // 4 // 8 // GRAIN
        self.block = rows // GRAIN
        self.out_start = 3 * self.width_grains
        self.fc_start = 4 * self.width_grains
        self.proj_start = self.fc_start + hidden // GRAIN
        self.vec_start = self.proj_start + hidden // GRAIN
        self.vec = 2
        self.used = self.vec_start + self.vec


def my_place():
    dp = lax.axis_index("dp")
    cp = lax.axis_index("cp")
    return dp // 2, dp % 2, cp // 2, cp % 2


def spread_kernel(sz, p_ref, qkv_ref, out_ref, fc_ref, proj_ref, vec_ref, send_sems, recv_sems):
    y, c, z, x = my_place()
    me = flat_id(y, c, z, x)

    def place_of(quarter, share):
        return (share // 4) * 2 + quarter // 2, (share % 4) * 2 + quarter % 2

    def send(grain, ref, slot, dp, cp, sem, recv):
        mine = dp * 8 + cp == me

        @pl.when(mine)
        def _():
            pltpu.make_async_copy(p_ref.at[grain], ref.at[slot], recv).start()

        @pl.when(jnp.logical_not(mine))
        def _():
            copy = pltpu.make_async_remote_copy(
                src_ref=p_ref.at[grain],
                dst_ref=ref.at[slot],
                send_sem=sem,
                recv_sem=recv,
                device_id=(dp, cp),
                device_id_type=MESH,
            )
            copy.start()

    def each(grain, act):
        table = me * sz.block + grain

        def headed(base, parts, ref, recv, share_size):
            offset = table - base
            part = offset // sz.width_grains
            local = offset % sz.width_grains

            def one(quarter, inner, sem):
                spot = part * sz.part_grains + inner
                dp, cp = place_of(quarter, spot // share_size)
                act(grain, ref, spot % share_size, dp, cp, sem, recv)

            @pl.when(jnp.logical_and(offset >= 0, offset < parts * sz.width_grains))
            def _():
                one(local // sz.part_grains, local % sz.part_grains, send_sems.at[grain])

                @pl.when(local < sz.spill)
                def _():
                    one(3, sz.part_grains - sz.spill + local, send_sems.at[sz.block + grain])

        headed(0, 3, qkv_ref, recv_sems.at[0], sz.qkv)
        headed(sz.out_start, 1, out_ref, recv_sems.at[1], sz.out)

        def plain(base, ref, recv):
            offset = table - base

            @pl.when(jnp.logical_and(offset >= 0, offset < 32 * sz.mlp))
            def _():
                dp, cp = place_of(offset // (8 * sz.mlp), (offset // sz.mlp) % 8)
                act(grain, ref, offset % sz.mlp, dp, cp, send_sems.at[grain], recv)

        plain(sz.fc_start, fc_ref, recv_sems.at[2])
        plain(sz.proj_start, proj_ref, recv_sems.at[3])

    def start(grain, _):
        each(grain, send)
        return 0

    lax.fori_loop(0, sz.block, start, 0)

    owner = sz.vec_start // sz.block
    spot = sz.vec_start % sz.block

    @pl.when(me == owner)
    def _():
        def to(device, _):
            @pl.when(device != me)
            def _():
                pltpu.make_async_remote_copy(
                    src_ref=p_ref.at[pl.ds(spot, sz.vec)],
                    dst_ref=vec_ref,
                    send_sem=send_sems.at[2 * sz.block + device],
                    recv_sem=recv_sems.at[4],
                    device_id=(device // 8, device % 8),
                    device_id_type=MESH,
                ).start()

            return 0

        lax.fori_loop(0, 32, to, 0)
        pltpu.make_async_copy(p_ref.at[pl.ds(spot, sz.vec)], vec_ref, recv_sems.at[4]).start()

    def sent(grain, ref, slot, dp, cp, sem, recv):
        @pl.when(dp * 8 + cp != me)
        def _():
            pltpu.make_async_copy(p_ref.at[grain], p_ref.at[grain], sem).wait()

    def finish(grain, _):
        each(grain, sent)
        return 0

    lax.fori_loop(0, sz.block, finish, 0)

    @pl.when(me == owner)
    def _():
        def to(device, _):
            @pl.when(device != me)
            def _():
                pltpu.make_async_copy(vec_ref, vec_ref, send_sems.at[2 * sz.block + device]).wait()

            return 0

        lax.fori_loop(0, 32, to, 0)

    for index, ref in enumerate((qkv_ref, out_ref, fc_ref, proj_ref, vec_ref)):
        pltpu.make_async_copy(ref, ref, recv_sems.at[index]).wait()


def spread(sz, table):
    width = table.shape[-1]
    hbm = pl.BlockSpec(memory_space=pl.ANY)

    def like(grains):
        return jax.ShapeDtypeStruct((grains, GRAIN, width), table.dtype)

    return pl.pallas_call(
        functools.partial(spread_kernel, sz),
        out_shape=(like(sz.qkv), like(sz.out), like(sz.mlp), like(sz.mlp), like(sz.vec)),
        in_specs=[hbm],
        out_specs=[hbm] * 5,
        scratch_shapes=[
            pltpu.SemaphoreType.DMA((2 * sz.block + 32,)),
            pltpu.SemaphoreType.DMA((5,)),
        ],
        compiler_params=pltpu.CompilerParams(has_side_effects=True),
        name="spread",
    )(table)


def collect_kernel(sz, qkv_ref, out_ref, fc_ref, proj_ref, g_ref, send_sems, recv_sem):
    y, c, z, x = my_place()
    me = flat_id(y, c, z, x)
    quarter = c * 2 + x
    share = y * 4 + z

    def send(ref, slot, table, sem):
        dest = table // sz.block
        mine = dest == me

        @pl.when(mine)
        def _():
            pltpu.make_async_copy(ref.at[slot], g_ref.at[table % sz.block], recv_sem).start()

        @pl.when(jnp.logical_not(mine))
        def _():
            pltpu.make_async_remote_copy(
                src_ref=ref.at[slot],
                dst_ref=g_ref.at[table % sz.block],
                send_sem=sem,
                recv_sem=recv_sem,
                device_id=(dest // 8, dest % 8),
                device_id_type=MESH,
            ).start()

    def sent(ref, slot, table, sem):
        @pl.when(table // sz.block != me)
        def _():
            pltpu.make_async_copy(ref.at[slot], ref.at[slot], sem).wait()

    def run(act):
        def headed(ref, size, base, first_sem):
            def one(slot, _):
                spot = share * size + slot
                part = spot // sz.part_grains
                local = quarter * sz.part_grains + spot % sz.part_grains

                @pl.when(local < sz.width_grains)
                def _():
                    act(ref, slot, base + part * sz.width_grains + local, send_sems.at[first_sem + slot])

                return 0

            lax.fori_loop(0, size, one, 0)

        def plain(ref, base, first_sem):
            def one(slot, _):
                table = base + (quarter * 8 + share) * sz.mlp + slot
                act(ref, slot, table, send_sems.at[first_sem + slot])
                return 0

            lax.fori_loop(0, sz.mlp, one, 0)

        headed(qkv_ref, sz.qkv, 0, 0)
        headed(out_ref, sz.out, sz.out_start, sz.qkv)
        plain(fc_ref, sz.fc_start, sz.qkv + sz.out)
        plain(proj_ref, sz.proj_start, sz.qkv + sz.out + sz.mlp)

    run(send)
    run(sent)
    last = sz.vec_start // sz.block

    @pl.when(me == last)
    def _():
        view = g_ref.at[pl.ds(0, sz.vec_start % sz.block)]
        pltpu.make_async_copy(view, view, recv_sem).wait()

    @pl.when(me != last)
    def _():
        pltpu.make_async_copy(g_ref, g_ref, recv_sem).wait()


def collect(sz, qkv, out, fc, proj):
    hbm = pl.BlockSpec(memory_space=pl.ANY)
    return pl.pallas_call(
        functools.partial(collect_kernel, sz),
        out_shape=jax.ShapeDtypeStruct((sz.block, GRAIN, qkv.shape[-1]), qkv.dtype),
        in_specs=[hbm] * 4,
        out_specs=hbm,
        scratch_shapes=[
            pltpu.SemaphoreType.DMA((sz.qkv + sz.out + 2 * sz.mlp,)),
            pltpu.SemaphoreType.DMA,
        ],
        compiler_params=pltpu.CompilerParams(has_side_effects=True),
        name="collect",
    )(qkv, out, fc, proj)


def attend_kernel(heads, size, odd_ref, qkv_ref, before_ref, mix_ref, lse_ref):
    part = heads * size
    rows = qkv_ref.shape[0]
    blk = 128
    scale = size**-0.5
    lane = lax.broadcasted_iota(jnp.int32, (blk, rows), 1)
    line = lax.broadcasted_iota(jnp.int32, (blk, rows), 0)

    def block(index, _):
        first = pl.multiple_of(index * blk, blk)
        allowed = lane <= line + first

        def one(with_before):
            for h in range(heads):
                cols = slice(h * size, (h + 1) * size)
                keys = slice(part + h * size, part + (h + 1) * size)
                vals = slice(2 * part + h * size, 2 * part + (h + 1) * size)
                vals_b = slice(part + h * size, part + (h + 1) * size)
                q = qkv_ref[pl.ds(first, blk), cols]
                s = dot_nt(q, qkv_ref[:, keys]) * scale
                s = jnp.where(allowed, s, MASKED)
                top = jnp.max(s, axis=-1, keepdims=True)
                if with_before:
                    s_b = dot_nt(q, before_ref[:, cols]) * scale
                    top = jnp.maximum(top, jnp.max(s_b, axis=-1, keepdims=True))
                    p_b = jnp.exp(s_b - top)
                p = jnp.exp(s - top)
                total = jnp.sum(p, axis=-1, keepdims=True)
                mix = dot_nn(p.astype(jnp.bfloat16), qkv_ref[:, vals])
                if with_before:
                    total = total + jnp.sum(p_b, axis=-1, keepdims=True)
                    mix = mix + dot_nn(p_b.astype(jnp.bfloat16), before_ref[:, vals_b])
                mix_ref[pl.ds(first, blk), cols] = mix / total
                lse_ref[pl.ds(first, blk), h : h + 1] = top + jnp.log(total)

        @pl.when(odd_ref[0] == 1)
        def _():
            one(True)

        @pl.when(odd_ref[0] == 0)
        def _():
            one(False)

        return 0

    lax.fori_loop(0, rows // blk, block, 0)


def attend(sz, odd, qkv, before):
    rows = qkv.shape[0] // 2
    return pl.pallas_call(
        functools.partial(attend_kernel, sz.quarter_heads, sz.head_size),
        grid_spec=pltpu.PrefetchScalarGridSpec(
            num_scalar_prefetch=1,
            grid=(2,),
            in_specs=[
                pl.BlockSpec((rows, 3 * sz.part), lambda g, odd: (g, 0)),
                pl.BlockSpec((rows, 2 * sz.part), lambda g, odd: (g, 0)),
            ],
            out_specs=[
                pl.BlockSpec((rows, sz.part), lambda g, odd: (g, 0)),
                pl.BlockSpec((rows, 8), lambda g, odd: (g, 0)),
            ],
        ),
        out_shape=(
            jax.ShapeDtypeStruct((2 * rows, sz.part), jnp.float32),
            jax.ShapeDtypeStruct((2 * rows, 8), jnp.float32),
        ),
        cost_estimate=pl.CostEstimate(
            flops=2 * 2 * 2 * rows * 2 * rows * sz.part,
            bytes_accessed=20 * rows * sz.part,
            transcendentals=4 * rows * rows * sz.quarter_heads,
        ),
        compiler_params=pltpu.CompilerParams(vmem_limit_bytes=40 << 20),
        name="attend",
    )(odd, qkv, before)


def attend_back_kernel(heads, size, own, flag_ref, qkv_ref, kv_ref, do_ref, mix_ref, lse_ref, seed_ref, dq_ref, dkv_ref):
    part = heads * size
    rows = qkv_ref.shape[0]
    blk = 128
    scale = size**-0.5
    lane = lax.broadcasted_iota(jnp.int32, (blk, rows), 1)
    line = lax.broadcasted_iota(jnp.int32, (blk, rows), 0)
    key_start = part if own else 0

    def work():
        dkv_ref[...] = jnp.zeros_like(dkv_ref)

        def block(index, _):
            first = pl.multiple_of(index * blk, blk)
            if own:
                allowed = lane <= line + first
            for h in range(heads):
                cols = slice(h * size, (h + 1) * size)
                keys = slice(key_start + h * size, key_start + (h + 1) * size)
                vals = slice(key_start + part + h * size, key_start + part + (h + 1) * size)
                out_vals = slice(part + h * size, part + (h + 1) * size)
                q = qkv_ref[pl.ds(first, blk), cols]
                k = kv_ref[:, keys]
                do = do_ref[pl.ds(first, blk), cols]
                s = dot_nt(q, k) * scale
                p = jnp.exp(s - lse_ref[pl.ds(first, blk), h : h + 1])
                if own:
                    p = jnp.where(allowed, p, 0.0)
                dp = dot_nt(do, kv_ref[:, vals])
                delta = jnp.sum(
                    do.astype(jnp.float32) * mix_ref[pl.ds(first, blk), cols], axis=-1, keepdims=True
                )
                ds = (p * (dp - delta)).astype(jnp.bfloat16)
                dq = dot_nn(ds, k) * scale
                if own:
                    dq = dq + seed_ref[pl.ds(first, blk), cols]
                dq_ref[pl.ds(first, blk), cols] = dq.astype(dq_ref.dtype)
                dkv_ref[:, cols] += dot_tn(ds, q) * scale
                dkv_ref[:, out_vals] += dot_tn(p.astype(jnp.bfloat16), do)
            return 0

        lax.fori_loop(0, rows // blk, block, 0)

    if own:
        work()
    else:

        @pl.when(flag_ref[0] == 1)
        def _():
            work()

        @pl.when(flag_ref[0] == 0)
        def _():
            dq_ref[...] = jnp.zeros_like(dq_ref)
            dkv_ref[...] = jnp.zeros_like(dkv_ref)


def attend_back(sz, own, odd, qkv, kv, grad_mix, mix, lse, seed):
    rows = qkv.shape[0] // 2
    part = sz.part

    def rows_of(width):
        return pl.BlockSpec((rows, width), lambda g, odd: (g, 0))

    return pl.pallas_call(
        functools.partial(attend_back_kernel, sz.quarter_heads, sz.head_size, own),
        grid_spec=pltpu.PrefetchScalarGridSpec(
            num_scalar_prefetch=1,
            grid=(2,),
            in_specs=[
                rows_of(3 * part),
                rows_of(3 * part if own else 2 * part),
                rows_of(part),
                rows_of(part),
                rows_of(8),
                rows_of(part) if own else pl.BlockSpec((8, 128), lambda g, odd: (0, 0)),
            ],
            out_specs=[rows_of(part), rows_of(2 * part)],
        ),
        out_shape=(
            jax.ShapeDtypeStruct((2 * rows, part), jnp.bfloat16 if own else jnp.float32),
            jax.ShapeDtypeStruct((2 * rows, 2 * part), jnp.float32),
        ),
        cost_estimate=pl.CostEstimate(
            flops=5 * 2 * 2 * rows * rows * part,
            bytes_accessed=40 * rows * part,
            transcendentals=2 * rows * rows * sz.quarter_heads,
        ),
        compiler_params=pltpu.CompilerParams(vmem_limit_bytes=48 << 20),
        name="attend_back_own" if own else "attend_back_before",
    )(odd, qkv, kv, grad_mix, mix, lse, seed)


def norm_parts(values):
    mean = jnp.mean(values, axis=-1, keepdims=True)
    centre = values - mean
    rs = lax.rsqrt(jnp.mean(centre * centre, axis=-1, keepdims=True) + EPSILON)
    return centre * rs, rs


def norm_back(normed, rs, grad, gain):
    e = grad * gain
    return rs * (
        e
        - jnp.mean(e, axis=-1, keepdims=True)
        - normed * jnp.mean(e * normed, axis=-1, keepdims=True)
    )


def per_device_quad(tokens, params, out_grad, lengths):
    rows, width = tokens.shape
    hidden = FF
    sz = Sizes(width, hidden, HEADS, HEAD_DIM, params.shape[0])
    y, c, z, x = my_place()
    quarter = c * 2 + x
    bf16, f32 = jnp.bfloat16, jnp.float32

    def pick(value, index):
        return lax.dynamic_index_in_dim(value, index, 0, keepdims=False)

    def put(value, update, index):
        return lax.dynamic_update_slice_in_dim(value, update[None], index, 0)

    def both(mine, other, index):
        first = jnp.where(index == 0, mine, other)
        second = jnp.where(index == 0, other, mine)
        return jnp.stack([first, second])

    def quad_gather(value):
        pair = both(value, over_x(value), x)
        return both(pair, over_c(pair), c)

    def quad_sum(partial):
        sent = pick(partial, 1 - c).astype(bf16)
        summed = pick(partial, c) + over_c(sent).astype(f32)
        sent = pick(summed, 1 - x).astype(bf16)
        return pick(summed, x) + over_x(sent).astype(f32)

    def quad_exchange(value):
        got = jnp.zeros_like(value)
        got = put(got, pick(value, quarter), quarter)
        got = put(got, over_x(pick(value, quarter ^ 1)), quarter ^ 1)
        got = put(got, over_c(pick(value, quarter ^ 2)), quarter ^ 2)
        return put(got, over_cx(pick(value, quarter ^ 3)), quarter ^ 3)

    def gather_relative(share):
        half = jnp.concatenate([share] + [over_z(share, d) for d in (1, 2, 3)])
        return jnp.concatenate([half, over_y(half)])

    def gather_ordered(share):
        half = jnp.zeros((4,) + share.shape, share.dtype)
        half = put(half, share, z)
        for d in (1, 2, 3):
            half = put(half, over_z(share, d), (z - d) % 4)
        full = both(half, over_y(half), y)
        return full.reshape((8 * share.shape[0],) + share.shape[1:])

    def reduce_relative(left, right):
        half = left.shape[1] // 2
        sent = dot_tn(left[:, half:], right).astype(bf16)
        kept = dot_tn(left[:, :half], right)
        summed = kept.reshape(4, half // 4, -1) + over_y(sent).astype(f32).reshape(4, half // 4, -1)
        total = summed[0]
        for d in (1, 2, 3):
            total = total + over_z(summed[d].astype(bf16), -d).astype(f32)
        return total

    def reduce_ordered(kept, sent):
        summed = kept + over_y(sent.astype(bf16)).astype(f32)
        summed = summed.reshape(4, summed.shape[0] // 4, -1)
        total = pick(summed, z)
        for d in (1, 2, 3):
            total = total + over_z(pick(summed, (z + d) % 4).astype(bf16), d).astype(f32)
        return total

    tok_all = quad_gather(tokens)
    cot_all = quad_gather(out_grad).reshape(4 * rows, width)
    s_qkv, s_out, s_fc, s_proj, vec = spread(sz, params.reshape(sz.block, GRAIN, width))
    flat = lambda value: value.reshape(-1, width)
    vectors = flat(vec).astype(f32)
    fc_bias = vectors[8 : 8 + hidden // width].reshape(hidden)
    w_qkv = gather_ordered(flat(s_qkv))
    w_out = quad_gather(gather_ordered(flat(s_out))).reshape(-1, width)[:width]
    w_fc = gather_relative(flat(s_fc))
    w_proj = gather_relative(flat(s_proj))

    normed_all, _ = norm_parts(tok_all.astype(f32))
    act_one = (normed_all * vectors[0] + vectors[1]).astype(bf16).reshape(4 * rows, width)

    def quarter_of(vector):
        padded = jnp.pad(vector, (0, 4 * sz.part - width))
        return lax.dynamic_slice_in_dim(padded, quarter * sz.part, sz.part, 0)

    qkv_bias = jnp.concatenate(
        [quarter_of(vectors[2]), jnp.zeros((sz.part,), f32), quarter_of(vectors[3])]
    )
    qkv = (dot_nt(act_one, w_qkv) + qkv_bias).astype(bf16)
    kv = qkv[:, sz.part :]
    before = permute(kv, lambda py, pc, pz, px: (py, pc, pz + 1, px) if pz % 2 == 0 else None)
    odd = (z % 2).astype(jnp.int32).reshape(1)
    mix, lse = attend(sz, odd, qkv, before)
    mixed = quad_exchange(mix.astype(bf16).reshape(4, rows, sz.part))
    mixed = jnp.transpose(mixed, (1, 0, 2)).reshape(rows, 4 * sz.part)[:, :width]
    inputs = tokens.astype(f32)
    residual = inputs + (dot_nt(mixed, w_out) + vectors[4])
    normed_two, rs_two = norm_parts(residual)
    act_two = quad_gather((normed_two * vectors[5] + vectors[6]).astype(bf16)).reshape(4 * rows, width)
    bias_rel = lax.dynamic_index_in_dim(fc_bias.reshape(4, 2, 4, hidden // 32), quarter, 0, keepdims=False)
    bias_rel = jnp.where(y == 0, bias_rel, bias_rel[::-1])
    bias_rel = jnp.stack([lax.dynamic_index_in_dim(bias_rel, (z - d) % 4, 1, keepdims=False) for d in range(4)], 1)
    pre_act = dot_nt(act_two, w_fc) + bias_rel.reshape(hidden // 4)
    act_hidden, pull_gelu = jax.vjp(gelu_tanh, pre_act)
    act_hidden = act_hidden.astype(bf16)
    g_proj = reduce_relative(act_hidden, cot_all)
    partial_out = dot_nn(act_hidden, w_proj).reshape(2, 2, rows, width)
    output = (residual + quad_sum(partial_out) + vectors[7]).astype(bf16)

    cot = out_grad.astype(f32)
    grad_fc = pull_gelu(dot_nt(cot_all, w_proj))[0].astype(bf16)
    grad_two = quad_sum(dot_nn(grad_fc, w_fc).reshape(2, 2, rows, width))
    g_fc = reduce_relative(grad_fc, act_two)
    grad_res = cot + norm_back(normed_two, rs_two, grad_two, vectors[5])
    grad_attn = grad_res.astype(bf16)
    grad_mix = dot_nn(grad_attn, w_out).astype(bf16)
    grad_mix = jnp.pad(grad_mix, ((0, 0), (0, 4 * sz.part - width)))
    grad_mix = jnp.transpose(grad_mix.reshape(rows, 4, sz.part), (1, 0, 2))
    grad_mix = quad_exchange(grad_mix).reshape(4 * rows, sz.part)
    seed = jnp.zeros((8, 128), f32)
    dq_before, dkv_before = attend_back(sz, False, odd, qkv, before, grad_mix, mix, lse, seed)
    returned = permute(
        dkv_before.astype(bf16), lambda py, pc, pz, px: (py, pc, pz - 1, px) if pz % 2 == 1 else None
    )
    dq, dkv = attend_back(sz, True, odd, qkv, qkv, grad_mix, mix, lse, dq_before)
    grad_qkv = jnp.concatenate([dq, (dkv + returned.astype(f32)).astype(bf16)], axis=1)
    grad_one = quad_sum(dot_nn(grad_qkv, w_qkv).reshape(2, 2, rows, width))

    half = 3 * sz.part // 2
    halves = [grad_qkv[:, :half], grad_qkv[:, half:]]
    mine = jnp.where(y == 0, halves[0], halves[1])
    other = jnp.where(y == 0, halves[1], halves[0])
    g_qkv = reduce_ordered(dot_tn(mine, act_one), dot_tn(other, act_one))

    g_out = jnp.pad(dot_tn(grad_attn, mixed), ((0, 4 * sz.part - width), (0, 0))).reshape(2, 2, sz.part, width)
    g_out = quad_sum(g_out).reshape(2, sz.part // 2, width)
    g_out = reduce_ordered(pick(g_out, y), pick(g_out, 1 - y))

    normed_one, rs_one = norm_parts(inputs)
    input_grad = (grad_res + norm_back(normed_one, rs_one, grad_one, vectors[0])).astype(bf16)

    def placed(vector):
        spot = lax.dynamic_update_slice_in_dim(jnp.zeros((4 * sz.part,), f32), vector, quarter * sz.part, 0)
        return spot[:width]

    sums = jnp.sum(grad_qkv.astype(f32), axis=0)
    bias_sum = jnp.sum(grad_fc.astype(f32), axis=0).reshape(2, 4, hidden // 32)
    ordered = jnp.stack([lax.dynamic_index_in_dim(bias_sum, (z - k) % 4, 1, keepdims=False) for k in range(4)], 1)
    ordered = jnp.where(y == 0, ordered, ordered[::-1]).reshape(1, hidden // 4)
    fc_rows = lax.dynamic_update_slice_in_dim(jnp.zeros((4, hidden // 4), f32), ordered, quarter, 0)
    grad_vectors = jnp.concatenate(
        [
            jnp.stack(
                [
                    jnp.sum(grad_one * normed_one, axis=0),
                    jnp.sum(grad_one, axis=0),
                    placed(sums[: sz.part]),
                    placed(sums[2 * sz.part :]),
                    jnp.sum(grad_attn.astype(f32), axis=0),
                    jnp.sum(grad_two * normed_two, axis=0),
                    jnp.sum(grad_two, axis=0),
                    jnp.sum(cot, axis=0),
                ]
            ),
            fc_rows.reshape(hidden // width, width),
        ]
    )
    grad_vectors = lax.psum(grad_vectors, ("dp", "cp"))

    grains = lambda value: value.astype(bf16).reshape(-1, GRAIN, width)
    table = collect(sz, grains(g_qkv), grains(g_out), grains(g_fc), grains(g_proj))
    table = table.reshape(sz.block * GRAIN, width).astype(f32)
    used = (sz.vec_start % sz.block) * GRAIN
    tail = jnp.concatenate(
        [grad_vectors, jnp.zeros((sz.block * GRAIN - used - grad_vectors.shape[0], width), f32)]
    )
    last = flat_id(y, c, z, x) == sz.vec_start // sz.block
    tail = jnp.where(last, tail, table[used:])
    param_grad = jnp.concatenate([table[:used], tail])
    return (output, input_grad, param_grad)


def fits_quad(mesh, tokens, params, lengths):
    dp, cp = mesh.shape["dp"], mesh.shape["cp"]
    rows = tokens.shape[0] // (dp * cp)
    width = tokens.shape[1]
    blocks = params.shape[0] // (dp * cp)
    return (
        (dp, cp) == (4, 8)
        and lengths.shape[1] == 2
        and rows * cp == lengths.shape[1] * MIN_LEN
        and rows % 128 == 0
        and blocks % GRAIN == 0
        and (HEADS, HEAD_DIM, FF, width) == (25, 64, 6400, 1600)
    )


def solution(mesh):
    in_specs = (P(("dp", "cp"), None), P(("dp", "cp"), None), P(("dp", "cp"), None), P("dp", None))
    out_specs = (P(("dp", "cp"), None), P(("dp", "cp"), None), P(("dp", "cp"), None))

    def step(tokens, params, out_grad, lengths):
        body = per_device_quad if fits_quad(mesh, tokens, params, lengths) else per_device_general
        return jax.shard_map(
            body, mesh=mesh, in_specs=in_specs, out_specs=out_specs, check_vma=False
        )(tokens, params, out_grad, lengths)

    return step
```

```python
import functools

import jax
import jax.numpy as jnp
from jax import lax
from jax.experimental import pallas as pl
from jax.experimental.pallas import tpu as pltpu
from jax.sharding import PartitionSpec as P

HEADS = 25
FF = 6400
HEAD_DIM = 64
TILE = 128
MIN_LEN = 1024
MAX_LEN = 4096


EPSILON = 1e-05
MASKED = -1e30
GELU_SCALE = 0.7978845608028654


def from_behind(value, axis, by):
    length = lax.axis_size(axis)
    pairs = [(i, i + by) for i in range(length) if 0 <= i + by < length]
    return lax.ppermute(value, axis, pairs)


def layer_norm(values, gain_row, bias_row):
    centre = values - jnp.mean(values, axis=-1, keepdims=True)
    spread = jnp.mean(centre * centre, axis=-1, keepdims=True)
    return centre * lax.rsqrt(spread + EPSILON) * gain_row + bias_row


def gelu_tanh(values):
    return (
        0.5 * values * (1.0 + jnp.tanh(GELU_SCALE * (values + 0.044715 * values * values * values)))
    )


def segment_of(position, seq_ends):
    return jnp.sum((position[:, None] >= seq_ends[None, :]).astype(jnp.int32), axis=1)


def unpack(gathered, model_width, hidden):
    out_end = 4 * model_width
    fc_end = out_end + hidden
    proj_end = fc_end + hidden
    vec_end = proj_end + 8
    return (
        gathered[0 : 3 * model_width],
        gathered[3 * model_width : out_end],
        gathered[out_end:fc_end],
        gathered[fc_end:proj_end],
        gathered[proj_end:vec_end].astype(jnp.float32),
        gathered[vec_end : vec_end + hidden // model_width].astype(jnp.float32).reshape(hidden),
    )


def matmul_nt(left_mat, right_mat):
    return lax.dot_general(
        left_mat, right_mat, (((1,), (1,)), ((), ())), preferred_element_type=jnp.float32
    )


def matmul_tn(left_mat, right_mat):
    return lax.dot_general(
        left_mat, right_mat, (((0,), (0,)), ((), ())), preferred_element_type=jnp.float32
    )


def matmul_nn(left_mat, right_mat):
    return jnp.dot(left_mat, right_mat, preferred_element_type=jnp.float32)


def per_device_general(tokens, params, out_grad, lengths):
    tok_rows, model_width = tokens.shape
    hidden = FF
    head_count = HEADS
    head_size = HEAD_DIM
    cp_count = lax.axis_size("cp")
    group_rows = tok_rows * cp_count
    seq_count = lengths.shape[1]
    longest = min(MAX_LEN, group_rows - (seq_count - 1) * MIN_LEN)
    reach_back = min(cp_count - 1, (longest + tok_rows - TILE - 1) // tok_rows)
    pair_count = (reach_back + 2) // 2
    score_scale = head_size ** (-0.5)
    gathered = lax.all_gather(params, ("dp", "cp"), axis=0, tiled=True)
    w_attn, w_out, w_fc, w_proj, vectors, fc_bias = unpack(gathered, model_width, hidden)
    inputs = tokens.astype(jnp.float32)
    act_one = layer_norm(inputs, vectors[0], vectors[1]).astype(jnp.bfloat16)
    qkv_bias = jnp.concatenate([vectors[2], jnp.zeros_like(vectors[2]), vectors[3]])
    qkv = (matmul_nt(act_one, w_attn) + qkv_bias).astype(jnp.bfloat16)
    queries = qkv[:, :model_width].reshape(tok_rows, head_count, head_size)
    key_value = qkv[:, model_width:]
    device = lax.axis_index("cp")
    seq_ends = jnp.cumsum(lengths[0])
    query_pos = device * tok_rows + jnp.arange(tok_rows, dtype=jnp.int32)
    query_seg = segment_of(query_pos, seq_ends)
    store = jnp.zeros((2 * pair_count, tok_rows, 2 * model_width), jnp.bfloat16)
    store = store.at[0].set(key_value)

    def fetch(step_index, state_pair):
        moving, held_rows = state_pair
        moving = from_behind(moving, "cp", 1)
        return (moving, lax.dynamic_update_index_in_dim(held_rows, moving, step_index, 0))

    _, store = lax.fori_loop(1, reach_back + 1, fetch, (key_value, store))

    def pair_mask(pair_index):
        owners = 2 * pair_index + jnp.arange(2, dtype=jnp.int32)
        key_pos = (
            (device - owners)[:, None] * tok_rows + jnp.arange(tok_rows, dtype=jnp.int32)[None, :]
        ).reshape(2 * tok_rows)
        usable = jnp.broadcast_to((owners <= reach_back)[:, None], (2, tok_rows)).reshape(
            2 * tok_rows
        ) & (key_pos >= 0)
        key_seg = segment_of(key_pos, seq_ends)
        return (
            (key_seg[None, :] == query_seg[:, None])
            & (key_pos[None, :] <= query_pos[:, None])
            & usable[None, :]
        )

    def pair_rows(pair_index):
        block_rows = lax.dynamic_slice_in_dim(store, 2 * pair_index, 2, 0).reshape(
            2 * tok_rows, 2 * model_width
        )
        return (
            block_rows[:, :model_width].reshape(2 * tok_rows, head_count, head_size),
            block_rows[:, model_width:].reshape(2 * tok_rows, head_count, head_size),
        )

    def pair_scores(key_rows, allowed):
        raw_scores = (
            jnp.einsum("qhd,khd->hqk", queries, key_rows, preferred_element_type=jnp.float32)
            * score_scale
        )
        return jnp.where(allowed[None], raw_scores, MASKED)

    def visit(work):

        def step_pair(pair_index, running):
            allowed = pair_mask(pair_index)
            result = work(pair_index, allowed, running)
            return result

        return step_pair

    def add_total(pair_index, allowed, running):
        row_top, summed = running
        key_rows, _ = pair_rows(pair_index)
        scores = pair_scores(key_rows, allowed)
        new_top = jnp.maximum(row_top, jnp.max(scores, axis=-1, keepdims=True))
        summed = summed * jnp.exp(row_top - new_top) + jnp.sum(
            jnp.exp(scores - new_top), axis=-1, keepdims=True
        )
        return (new_top, summed)

    start_top = jnp.full((head_count, tok_rows, 1), MASKED, jnp.float32)
    start_sum = jnp.zeros((head_count, tok_rows, 1), jnp.float32)
    row_top, summed = lax.fori_loop(0, pair_count, visit(add_total), (start_top, start_sum))
    log_total = row_top + jnp.log(summed)

    def add_mix(pair_index, allowed, running):
        key_rows, value_rows = pair_rows(pair_index)
        prob_rows = jnp.exp(pair_scores(key_rows, allowed) - log_total).astype(jnp.bfloat16)
        return running + jnp.einsum(
            "hqk,khd->qhd", prob_rows, value_rows, preferred_element_type=jnp.float32
        )

    mixed_full = lax.fori_loop(
        0, pair_count, visit(add_mix), jnp.zeros((tok_rows, head_count, head_size), jnp.float32)
    )
    mixed = mixed_full.reshape(tok_rows, model_width).astype(jnp.bfloat16)
    attn_out = matmul_nt(mixed, w_out) + vectors[4]
    residual = inputs + attn_out
    act_two = layer_norm(residual, vectors[5], vectors[6]).astype(jnp.bfloat16)
    pre_act = matmul_nt(act_two, w_fc) + fc_bias
    act_hidden = gelu_tanh(pre_act).astype(jnp.bfloat16)
    output = (residual + matmul_nn(act_hidden, w_proj) + vectors[7]).astype(jnp.bfloat16)
    gathered = lax.all_gather(params, ("dp", "cp"), axis=0, tiled=True)
    w_attn, w_out, w_fc, w_proj, vectors, fc_bias = unpack(gathered, model_width, hidden)
    grad_out_f = out_grad.astype(jnp.float32)
    grad_hidden = matmul_nt(out_grad, w_proj)
    _, pull_gelu = jax.vjp(gelu_tanh, pre_act)
    grad_fc = pull_gelu(grad_hidden)[0].astype(jnp.bfloat16)
    grad_act_two = matmul_nn(grad_fc, w_fc)
    _, pull_two = jax.vjp(layer_norm, residual, vectors[5], vectors[6])
    grad_res_norm, grad_gain_two, grad_bias_two = pull_two(grad_act_two)
    grad_res = grad_out_f + grad_res_norm
    grad_attn = grad_res.astype(jnp.bfloat16)
    grad_mix = (
        matmul_nn(grad_attn, w_out).astype(jnp.bfloat16).reshape(tok_rows, head_count, head_size)
    )
    grad_dot = jnp.transpose(jnp.sum(grad_mix.astype(jnp.float32) * mixed_full, axis=-1), (1, 0))[
        :, :, None
    ]

    def add_grads(pair_index, allowed, running):
        grad_query, grad_store = running
        key_rows, value_rows = pair_rows(pair_index)
        prob_rows = jnp.exp(pair_scores(key_rows, allowed) - log_total)
        grad_probs = jnp.einsum(
            "qhd,khd->hqk", grad_mix, value_rows, preferred_element_type=jnp.float32
        )
        grad_scores = (prob_rows * (grad_probs - grad_dot)).astype(jnp.bfloat16)
        grad_query = (
            grad_query
            + jnp.einsum("hqk,khd->qhd", grad_scores, key_rows, preferred_element_type=jnp.float32)
            * score_scale
        )
        grad_keys = (
            jnp.einsum("hqk,qhd->khd", grad_scores, queries, preferred_element_type=jnp.float32)
            * score_scale
        )
        grad_values = jnp.einsum(
            "hqk,qhd->khd",
            prob_rows.astype(jnp.bfloat16),
            grad_mix,
            preferred_element_type=jnp.float32,
        )
        pair_grad = jnp.concatenate(
            [
                grad_keys.reshape(2 * tok_rows, model_width),
                grad_values.reshape(2 * tok_rows, model_width),
            ],
            axis=1,
        )
        pair_grad = pair_grad.reshape(2, tok_rows, 2 * model_width)
        grad_store = lax.dynamic_update_slice_in_dim(grad_store, pair_grad, 2 * pair_index, 0)
        return (grad_query, grad_store)

    start_query = jnp.zeros((tok_rows, head_count, head_size), jnp.float32)
    start_store = jnp.zeros((2 * pair_count, tok_rows, 2 * model_width), jnp.float32)
    grad_query, grad_store = lax.fori_loop(
        0, pair_count, visit(add_grads), (start_query, start_store)
    )

    def send_back(step_index, moving):
        moving = moving + lax.dynamic_index_in_dim(
            grad_store, reach_back - step_index, 0, keepdims=False
        )
        return from_behind(moving.astype(jnp.bfloat16), "cp", -1).astype(moving.dtype)

    returned = lax.fori_loop(
        0, reach_back, send_back, jnp.zeros((tok_rows, 2 * model_width), jnp.float32)
    )
    grad_kv = returned + grad_store[0]
    grad_qkv = jnp.concatenate([grad_query.reshape(tok_rows, model_width), grad_kv], axis=1).astype(
        jnp.bfloat16
    )
    grad_qkv_f = grad_qkv.astype(jnp.float32)
    grad_act_one = matmul_nn(grad_qkv, w_attn)
    _, pull_one = jax.vjp(layer_norm, inputs, vectors[0], vectors[1])
    grad_in_norm, grad_gain_one, grad_bias_one = pull_one(grad_act_one)
    input_grad = (grad_res + grad_in_norm).astype(jnp.bfloat16)
    grad_vectors = jnp.stack(
        [
            grad_gain_one,
            grad_bias_one,
            jnp.sum(grad_qkv_f[:, :model_width], axis=0),
            jnp.sum(grad_qkv_f[:, 2 * model_width :], axis=0),
            jnp.sum(grad_attn.astype(jnp.float32), axis=0),
            grad_gain_two,
            grad_bias_two,
            jnp.sum(grad_out_f, axis=0),
        ]
    )
    grad_fc_bias = jnp.sum(grad_fc.astype(jnp.float32), axis=0).reshape(
        hidden // model_width, model_width
    )
    used_rows = 4 * model_width + 2 * hidden + 8 + hidden // model_width
    total_rows = gathered.shape[0]
    local_grad = jnp.concatenate(
        [
            matmul_tn(grad_qkv, act_one),
            matmul_tn(grad_attn, mixed),
            matmul_tn(grad_fc, act_two),
            matmul_tn(act_hidden, out_grad),
            grad_vectors,
            grad_fc_bias,
            jnp.zeros((total_rows - used_rows, model_width), jnp.float32),
        ],
        axis=0,
    )
    dp_count = lax.axis_size("dp")
    device_count = dp_count * cp_count
    share_rows = total_rows // device_count
    spread_rows = local_grad.reshape(device_count, 1, share_rows, model_width)
    received = lax.all_to_all(
        spread_rows.astype(jnp.bfloat16), ("dp", "cp"), split_axis=0, concat_axis=1, tiled=True
    ).astype(spread_rows.dtype)
    param_grad = jnp.sum(received, axis=1).reshape(share_rows, model_width)
    return (output, input_grad, param_grad)


MESH = pl.DeviceIdType.MESH
GRAIN = 8
NT = (((1,), (1,)), ((), ()))
TN = (((0,), (0,)), ((), ()))


def dot_nt(a, b):
    return lax.dot_general(a, b, NT, preferred_element_type=jnp.float32)


def dot_tn(a, b):
    return lax.dot_general(a, b, TN, preferred_element_type=jnp.float32)


def dot_nn(a, b):
    return jnp.dot(a, b, preferred_element_type=jnp.float32)


def flat_id(y, c, z, x):
    return ((y * 2 + c) * 4 + z) * 2 + x


def permute(value, move):
    pairs = []
    for y in range(2):
        for c in range(2):
            for z in range(4):
                for x in range(2):
                    to = move(y, c, z, x)
                    if to is not None:
                        pairs.append((flat_id(y, c, z, x), flat_id(*to)))
    return lax.ppermute(value, ("dp", "cp"), pairs)


def over_y(value):
    return permute(value, lambda y, c, z, x: (1 - y, c, z, x))


def over_z(value, by):
    return permute(value, lambda y, c, z, x: (y, c, (z + by) % 4, x))


class Sizes:
    def __init__(self, width, hidden, heads, head_size, rows):
        self.width = width
        self.hidden = hidden
        self.heads = heads
        self.head_size = head_size
        self.quarter_heads = -(-heads // 4)
        self.part = self.quarter_heads * head_size
        self.part_grains = self.part // GRAIN
        self.width_grains = width // GRAIN
        self.spill = 4 * self.part_grains - self.width_grains
        self.qkv = 3 * self.part_grains // 8
        self.out = self.part_grains // 8
        self.mlp = hidden // 4 // 8 // GRAIN
        self.block = rows // GRAIN
        self.out_start = 3 * self.width_grains
        self.fc_start = 4 * self.width_grains
        self.proj_start = self.fc_start + hidden // GRAIN
        self.vec_start = self.proj_start + hidden // GRAIN
        self.vec = 2
        self.used = self.vec_start + self.vec


def my_place():
    dp = lax.axis_index("dp")
    cp = lax.axis_index("cp")
    return dp // 2, dp % 2, cp // 2, cp % 2


def place_of(quarter, share):
    return (share // 4) * 2 + quarter // 2, (share % 4) * 2 + quarter % 2


class Wires:
    def __init__(self, send_sems, recv_sems):
        self.send_sems = send_sems
        self.recv_sems = recv_sems
        self.count = 0

    def to(self, src, dst, dp, cp):
        index = self.count
        self.count += 1
        return pltpu.make_async_remote_copy(
            src_ref=src,
            dst_ref=dst,
            send_sem=self.send_sems.at[index],
            recv_sem=self.recv_sems.at[index],
            device_id=(dp, cp),
            device_id_type=MESH,
        )


class PlaceGather:
    def __init__(self, wires, full):
        self.wires = wires
        self.full = full
        self.dp, self.cp = lax.axis_index("dp"), lax.axis_index("cp")
        self.y, self.z, self.x = self.dp // 2, self.cp // 2, self.cp % 2
        self.started = []

    def send(self, slot, dp, cp):
        view = self.full.at[slot]
        copy = self.wires.to(view, view, dp, cp)
        copy.start()
        self.started.append(copy)
        return copy

    def start(self):
        mine = self.y * 4 + self.z
        self.along = []
        for d in (1, 3, 2):
            self.along.append((d, self.send(mine, self.dp, ((self.z + d) % 4) * 2 + self.x)))
        self.over = [self.send(mine, (self.dp + 2) % 4, self.cp)]

    def forward(self):
        for d, copy in self.along:
            copy.wait_recv()
            self.over.append(self.send(self.y * 4 + (self.z - d + 4) % 4, (self.dp + 2) % 4, self.cp))

    def finish(self):
        for copy in self.over:
            copy.wait_recv()
        for copy in self.started:
            copy.wait_send()


class QuadGather:
    def __init__(self, wires, block, full, local_sem):
        self.wires = wires
        self.block = block
        self.full = full
        self.dp, self.cp = lax.axis_index("dp"), lax.axis_index("cp")
        self.c, self.x = self.dp % 2, self.cp % 2
        self.over_x = (self.dp, self.cp + 1 - 2 * self.x)
        self.over_c = (self.dp + 1 - 2 * self.c, self.cp)
        self.local_sem = local_sem

    def start(self):
        spot = self.full.at[self.c, self.x]
        self.by_x = self.wires.to(self.block, spot, *self.over_x)
        self.by_c = self.wires.to(self.block, spot, *self.over_c)
        self.by_x.start()
        self.by_c.start()
        self.local = pltpu.make_async_copy(self.block, spot, self.local_sem)
        self.local.start()

    def forward(self):
        self.by_x.wait_recv()
        spot = self.full.at[self.c, 1 - self.x]
        self.pass_on = self.wires.to(spot, spot, *self.over_c)
        self.pass_on.start()

    def finish(self):
        self.by_c.wait_recv()
        self.pass_on.wait_recv()
        self.by_x.wait_send()
        self.by_c.wait_send()
        self.pass_on.wait_send()
        self.local.wait()


def open_kernel(
    sz, p_ref, tok_ref, cot_ref, qkv_ref, out_ref, fc_ref, proj_ref, vec_ref, tok_all, cot_all,
    spread_sems, kind_sems, send_sems, recv_sems, local_sems,
):
    y, c, z, x = my_place()
    me = flat_id(y, c, z, x)
    wires = Wires(send_sems, recv_sems)
    tok = QuadGather(wires, tok_ref, tok_all, local_sems.at[0])
    cot = QuadGather(wires, cot_ref, cot_all, local_sems.at[1])

    def send(grain, ref, slot, quarter, share, sem, recv):
        dp, cp = place_of(quarter, share)
        mine = dp * 8 + cp == me

        @pl.when(mine)
        def _():
            pltpu.make_async_copy(p_ref.at[grain], ref.at[share, slot], recv).start()

        @pl.when(jnp.logical_not(mine))
        def _():
            pltpu.make_async_remote_copy(
                src_ref=p_ref.at[grain],
                dst_ref=ref.at[share, slot],
                send_sem=sem,
                recv_sem=recv,
                device_id=(dp, cp),
                device_id_type=MESH,
            ).start()

    def sent(grain, ref, slot, quarter, share, sem, recv):
        dp, cp = place_of(quarter, share)

        @pl.when(dp * 8 + cp != me)
        def _():
            pltpu.make_async_copy(p_ref.at[grain], p_ref.at[grain], sem).wait()

    def headed(act, grain, base, parts, ref, recv, share_size):
        offset = me * sz.block + grain - base
        part = offset // sz.width_grains
        local = offset % sz.width_grains

        def one(quarter, inner, sem):
            spot = part * sz.part_grains + inner
            act(grain, ref, spot % share_size, quarter, spot // share_size, sem, recv)

        @pl.when(jnp.logical_and(offset >= 0, offset < parts * sz.width_grains))
        def _():
            one(local // sz.part_grains, local % sz.part_grains, spread_sems.at[grain])

            @pl.when(local < sz.spill)
            def _():
                one(3, sz.part_grains - sz.spill + local, spread_sems.at[sz.block + grain])

    def plain(act, grain, base, ref, recv):
        offset = me * sz.block + grain - base

        @pl.when(jnp.logical_and(offset >= 0, offset < 32 * sz.mlp))
        def _():
            act(
                grain, ref, offset % sz.mlp, offset // (8 * sz.mlp), (offset // sz.mlp) % 8,
                spread_sems.at[grain], recv,
            )

    def heads(act):
        def one(grain, _):
            headed(act, grain, 0, 3, qkv_ref, kind_sems.at[0], sz.qkv)
            return 0

        lax.fori_loop(0, sz.block, one, 0)

    def others(act):
        def one(grain, _):
            headed(act, grain, sz.out_start, 1, out_ref, kind_sems.at[1], sz.out)
            plain(act, grain, sz.fc_start, fc_ref, kind_sems.at[2])
            plain(act, grain, sz.proj_start, proj_ref, kind_sems.at[3])
            return 0

        lax.fori_loop(0, sz.block, one, 0)

    owner = sz.vec_start // sz.block
    spot = sz.vec_start % sz.block

    def vector_sends(act):
        @pl.when(me == owner)
        def _():
            def to(device, _):
                @pl.when(device != me)
                def _():
                    act(
                        pltpu.make_async_remote_copy(
                            src_ref=p_ref.at[pl.ds(spot, sz.vec)],
                            dst_ref=vec_ref,
                            send_sem=spread_sems.at[2 * sz.block + device],
                            recv_sem=kind_sems.at[4],
                            device_id=(device // 8, device % 8),
                            device_id_type=MESH,
                        )
                    )

                return 0

            lax.fori_loop(0, 32, to, 0)

    heads(send)
    tok.start()
    cot.start()
    mine = y * 4 + z
    pltpu.make_async_copy(qkv_ref.at[mine], qkv_ref.at[mine], kind_sems.at[0]).wait()
    weights = PlaceGather(wires, qkv_ref)
    weights.start()
    others(send)
    vector_sends(lambda copy: copy.start())

    @pl.when(me == owner)
    def _():
        pltpu.make_async_copy(p_ref.at[pl.ds(spot, sz.vec)], vec_ref, kind_sems.at[4]).start()

    weights.forward()
    tok.forward()
    cot.forward()
    heads(sent)
    others(sent)
    vector_sends(lambda copy: copy.wait_send())
    for index, ref in enumerate((out_ref, fc_ref, proj_ref)):
        pltpu.make_async_copy(ref.at[mine], ref.at[mine], kind_sems.at[index + 1]).wait()
    pltpu.make_async_copy(vec_ref, vec_ref, kind_sems.at[4]).wait()
    tok.finish()
    cot.finish()
    weights.finish()


HBM = pl.BlockSpec(memory_space=pl.ANY)
VMEM = pl.BlockSpec(memory_space=pltpu.VMEM)
REMOTE = pltpu.CompilerParams(has_side_effects=True)


def wire_sems(count):
    return [pltpu.SemaphoreType.DMA((count,)), pltpu.SemaphoreType.DMA((count,))]


def open_call(sz, table, tokens, cotangent):
    rows, width = tokens.shape

    def like(*shape):
        return jax.ShapeDtypeStruct(shape + (width,), table.dtype)

    return pl.pallas_call(
        functools.partial(open_kernel, sz),
        out_shape=(
            like(8, sz.qkv, GRAIN),
            like(8, sz.out, GRAIN),
            like(8, sz.mlp, GRAIN),
            like(8, sz.mlp, GRAIN),
            like(sz.vec, GRAIN),
            like(2, 2, rows),
            like(2, 2, rows),
        ),
        in_specs=[HBM, VMEM, VMEM],
        out_specs=[HBM] * 7,
        scratch_shapes=[
            pltpu.SemaphoreType.DMA((2 * sz.block + 32,)),
            pltpu.SemaphoreType.DMA((5,)),
            *wire_sems(13),
            pltpu.SemaphoreType.DMA((2,)),
        ],
        compiler_params=REMOTE,
        name="open",
    )(table, tokens, cotangent)


def keys_kernel(kv_ref, out_in, fc_in, before_ref, out_ref, fc_ref, out_all, send_sems, recv_sems, local_sem):
    y, c, z, x = my_place()
    dp, cp = lax.axis_index("dp"), lax.axis_index("cp")
    wires = Wires(send_sems, recv_sems)
    keys = wires.to(kv_ref, before_ref, dp, (cp + 2) % 8)

    @pl.when(z % 2 == 0)
    def _():
        keys.start()

    first = PlaceGather(wires, out_ref)
    second = PlaceGather(wires, fc_ref)
    first.start()
    second.start()
    first.forward()
    first.finish()
    quad = QuadGather(wires, out_ref, out_all, local_sem)
    quad.start()

    @pl.when(z % 2 == 1)
    def _():
        keys.wait_recv()

    second.forward()
    quad.forward()
    second.finish()
    quad.finish()

    @pl.when(z % 2 == 0)
    def _():
        keys.wait_send()


def keys_call(kv, w_out, w_fc):
    def like(value, *lead):
        return jax.ShapeDtypeStruct(lead + value.shape, value.dtype)

    return pl.pallas_call(
        keys_kernel,
        out_shape=(like(kv), like(w_out), like(w_fc), like(w_out, 2, 2)),
        in_specs=[HBM] * 3,
        out_specs=[HBM] * 4,
        input_output_aliases={1: 1, 2: 2},
        scratch_shapes=[*wire_sems(18), pltpu.SemaphoreType.DMA],
        compiler_params=REMOTE,
        name="keys",
    )(kv, w_out, w_fc)


def acts_kernel(act_ref, proj_in, act_all, proj_ref, send_sems, recv_sems, local_sem):
    wires = Wires(send_sems, recv_sems)
    quad = QuadGather(wires, act_ref, act_all, local_sem)
    places = PlaceGather(wires, proj_ref)
    quad.start()
    places.start()
    quad.forward()
    places.forward()
    quad.finish()
    places.finish()


def acts_call(act, w_proj):
    return pl.pallas_call(
        acts_kernel,
        out_shape=(
            jax.ShapeDtypeStruct((2, 2) + act.shape, act.dtype),
            jax.ShapeDtypeStruct(w_proj.shape, w_proj.dtype),
        ),
        in_specs=[VMEM, HBM],
        out_specs=[HBM] * 2,
        input_output_aliases={1: 1},
        scratch_shapes=[*wire_sems(10), pltpu.SemaphoreType.DMA],
        compiler_params=REMOTE,
        name="acts",
    )(act, w_proj)


def swap_kernel(in_ref, out_ref, send_sems, recv_sems, local_sem):
    y, c, z, x = my_place()
    wires = Wires(send_sems, recv_sems)
    mine = c * 2 + x
    copies = []
    for dc, dx in ((1, 1), (0, 1), (1, 0)):
        tc = c + dc * (1 - 2 * c)
        tx = x + dx * (1 - 2 * x)
        copies.append(wires.to(in_ref.at[tc * 2 + tx], out_ref.at[mine], y * 2 + tc, z * 2 + tx))
    for copy in copies:
        copy.start()
    local = pltpu.make_async_copy(in_ref.at[mine], out_ref.at[mine], local_sem)
    local.start()
    for copy in copies:
        copy.wait_recv()
    for copy in copies:
        copy.wait_send()
    local.wait()


def swap_call(value):
    return pl.pallas_call(
        swap_kernel,
        out_shape=jax.ShapeDtypeStruct(value.shape, value.dtype),
        in_specs=[VMEM],
        out_specs=VMEM,
        scratch_shapes=[*wire_sems(3), pltpu.SemaphoreType.DMA],
        compiler_params=REMOTE,
        name="swap",
    )(value)


def quad_sum_kernel(in_ref, out_ref, got_c, stage, got_x, send_sems, recv_sems):
    y, c, z, x = my_place()
    dp, cp = lax.axis_index("dp"), lax.axis_index("cp")
    wires = Wires(send_sems, recv_sems)
    by_c = wires.to(in_ref.at[1 - c], got_c, dp + 1 - 2 * c, cp)
    by_x = wires.to(stage, got_x, dp, cp + 1 - 2 * x)
    by_c.start()
    by_c.wait_recv()
    rows = out_ref.shape[0]
    step = 32

    def to_send(index, _):
        span = pl.ds(pl.multiple_of(index * step, step), step)
        stage[span, :] = (
            in_ref[c, 1 - x, span, :].astype(jnp.float32) + got_c[1 - x, span, :].astype(jnp.float32)
        ).astype(stage.dtype)
        return 0

    lax.fori_loop(0, rows // step, to_send, 0)
    by_x.start()

    def to_keep(index, _):
        span = pl.ds(pl.multiple_of(index * step, step), step)
        out_ref[span, :] = in_ref[c, x, span, :].astype(jnp.float32) + got_c[x, span, :].astype(jnp.float32)
        return 0

    lax.fori_loop(0, rows // step, to_keep, 0)
    by_x.wait_recv()

    def to_add(index, _):
        span = pl.ds(pl.multiple_of(index * step, step), step)
        out_ref[span, :] += got_x[span, :].astype(jnp.float32)
        return 0

    lax.fori_loop(0, rows // step, to_add, 0)
    by_c.wait_send()
    by_x.wait_send()


def quad_sum(partial):
    rows, width = partial.shape[2:]
    return pl.pallas_call(
        quad_sum_kernel,
        out_shape=jax.ShapeDtypeStruct((rows, width), jnp.float32),
        in_specs=[VMEM],
        out_specs=VMEM,
        scratch_shapes=[
            pltpu.VMEM((2, rows, width), partial.dtype),
            pltpu.VMEM((rows, width), partial.dtype),
            pltpu.VMEM((rows, width), partial.dtype),
            *wire_sems(2),
        ],
        compiler_params=REMOTE,
        name="quad_sum",
    )(partial)


def collect_kernel(sz, qkv_ref, out_ref, fc_ref, proj_ref, vec_ref, g_ref, vecs_ref, send_sems, recv_sem, vec_sems):
    y, c, z, x = my_place()
    me = flat_id(y, c, z, x)
    quarter = c * 2 + x
    share = y * 4 + z

    def send(ref, slot, table, sem):
        dest = table // sz.block
        mine = dest == me

        @pl.when(mine)
        def _():
            pltpu.make_async_copy(ref.at[slot], g_ref.at[table % sz.block], recv_sem).start()

        @pl.when(jnp.logical_not(mine))
        def _():
            pltpu.make_async_remote_copy(
                src_ref=ref.at[slot],
                dst_ref=g_ref.at[table % sz.block],
                send_sem=sem,
                recv_sem=recv_sem,
                device_id=(dest // 8, dest % 8),
                device_id_type=MESH,
            ).start()

    def sent(ref, slot, table, sem):
        @pl.when(table // sz.block != me)
        def _():
            pltpu.make_async_copy(ref.at[slot], ref.at[slot], sem).wait()

    def run(act):
        def headed(ref, size, base, first_sem):
            def one(slot, _):
                spot = share * size + slot
                part = spot // sz.part_grains
                local = quarter * sz.part_grains + spot % sz.part_grains

                @pl.when(local < sz.width_grains)
                def _():
                    act(ref, slot, base + part * sz.width_grains + local, send_sems.at[first_sem + slot])

                return 0

            lax.fori_loop(0, size, one, 0)

        def plain(ref, base, first_sem):
            def one(slot, _):
                table = base + (quarter * 8 + share) * sz.mlp + slot
                act(ref, slot, table, send_sems.at[first_sem + slot])
                return 0

            lax.fori_loop(0, sz.mlp, one, 0)

        headed(qkv_ref, sz.qkv, 0, 0)
        headed(out_ref, sz.out, sz.out_start, sz.qkv)
        plain(fc_ref, sz.fc_start, sz.qkv + sz.out)
        plain(proj_ref, sz.proj_start, sz.qkv + sz.out + sz.mlp)

    last = sz.vec_start // sz.block
    vec_copy = pltpu.make_async_remote_copy(
        src_ref=vec_ref,
        dst_ref=vecs_ref.at[me],
        send_sem=vec_sems.at[0],
        recv_sem=vec_sems.at[1],
        device_id=(last // 8, last % 8),
        device_id_type=MESH,
    )

    @pl.when(me != last)
    def _():
        vec_copy.start()

    @pl.when(me == last)
    def _():
        pltpu.make_async_copy(vec_ref, vecs_ref.at[me], vec_sems.at[1]).start()

    run(send)
    run(sent)

    @pl.when(me != last)
    def _():
        vec_copy.wait_send()

    @pl.when(me == last)
    def _():
        view = g_ref.at[pl.ds(0, sz.vec_start % sz.block)]
        pltpu.make_async_copy(view, view, recv_sem).wait()
        pltpu.make_async_copy(vecs_ref, vecs_ref, vec_sems.at[1]).wait()

    @pl.when(me != last)
    def _():
        pltpu.make_async_copy(g_ref, g_ref, recv_sem).wait()


def collect(sz, qkv, out, fc, proj, vectors):
    width = qkv.shape[-1]
    return pl.pallas_call(
        functools.partial(collect_kernel, sz),
        out_shape=(
            jax.ShapeDtypeStruct((sz.block, GRAIN, width), qkv.dtype),
            jax.ShapeDtypeStruct((32,) + vectors.shape, vectors.dtype),
        ),
        in_specs=[HBM] * 5,
        out_specs=[HBM] * 2,
        scratch_shapes=[
            pltpu.SemaphoreType.DMA((sz.qkv + sz.out + 2 * sz.mlp,)),
            pltpu.SemaphoreType.DMA,
            pltpu.SemaphoreType.DMA((2,)),
        ],
        compiler_params=REMOTE,
        name="collect",
    )(qkv, out, fc, proj, vectors)


def attend_kernel(heads, size, odd_ref, q_ref, kv_ref, before_ref, mix_ref, lse_ref):
    part = heads * size
    rows = q_ref.shape[0]
    blk = 128
    scale = size**-0.5
    lane = lax.broadcasted_iota(jnp.int32, (blk, rows), 1)
    line = lax.broadcasted_iota(jnp.int32, (blk, rows), 0)

    def block(index, _):
        first = pl.multiple_of(index * blk, blk)
        allowed = lane <= line + first

        def one(with_before):
            for h in range(heads):
                cols = slice(h * size, (h + 1) * size)
                vals = slice(part + h * size, part + (h + 1) * size)
                q = q_ref[pl.ds(first, blk), cols]
                s = dot_nt(q, kv_ref[:, cols]) * scale
                s = jnp.where(allowed, s, MASKED)
                top = jnp.max(s, axis=-1, keepdims=True)
                if with_before:
                    s_b = dot_nt(q, before_ref[:, cols]) * scale
                    top = jnp.maximum(top, jnp.max(s_b, axis=-1, keepdims=True))
                    p_b = jnp.exp(s_b - top)
                p = jnp.exp(s - top)
                total = jnp.sum(p, axis=-1, keepdims=True)
                mix = dot_nn(p.astype(jnp.bfloat16), kv_ref[:, vals])
                if with_before:
                    total = total + jnp.sum(p_b, axis=-1, keepdims=True)
                    mix = mix + dot_nn(p_b.astype(jnp.bfloat16), before_ref[:, vals])
                mix_ref[pl.ds(first, blk), cols] = mix / total
                lse_ref[pl.ds(first, blk), h : h + 1] = top + jnp.log(total)

        @pl.when(odd_ref[0] == 1)
        def _():
            one(True)

        @pl.when(odd_ref[0] == 0)
        def _():
            one(False)

        return 0

    lax.fori_loop(0, rows // blk, block, 0)


def attend(sz, odd, q, kv, before):
    rows = q.shape[0] // 2
    return pl.pallas_call(
        functools.partial(attend_kernel, sz.quarter_heads, sz.head_size),
        grid_spec=pltpu.PrefetchScalarGridSpec(
            num_scalar_prefetch=1,
            grid=(2,),
            in_specs=[
                pl.BlockSpec((rows, sz.part), lambda g, odd: (g, 0)),
                pl.BlockSpec((rows, 2 * sz.part), lambda g, odd: (g, 0)),
                pl.BlockSpec((rows, 2 * sz.part), lambda g, odd: (g, 0)),
            ],
            out_specs=[
                pl.BlockSpec((rows, sz.part), lambda g, odd: (g, 0)),
                pl.BlockSpec((rows, 8), lambda g, odd: (g, 0)),
            ],
        ),
        out_shape=(
            jax.ShapeDtypeStruct((2 * rows, sz.part), jnp.float32),
            jax.ShapeDtypeStruct((2 * rows, 8), jnp.float32),
        ),
        cost_estimate=pl.CostEstimate(
            flops=2 * 2 * 2 * rows * 2 * rows * sz.part,
            bytes_accessed=20 * rows * sz.part,
            transcendentals=4 * rows * rows * sz.quarter_heads,
        ),
        compiler_params=pltpu.CompilerParams(vmem_limit_bytes=40 << 20),
        name="attend",
    )(odd, q, kv, before)


def attend_back_kernel(heads, size, own, flag_ref, q_ref, kv_ref, do_ref, mix_ref, lse_ref, seed_ref, dq_ref, dkv_ref):
    part = heads * size
    rows = q_ref.shape[0]
    blk = 128
    scale = size**-0.5
    lane = lax.broadcasted_iota(jnp.int32, (blk, rows), 1)
    line = lax.broadcasted_iota(jnp.int32, (blk, rows), 0)

    def work():
        dkv_ref[...] = jnp.zeros_like(dkv_ref)

        def block(index, _):
            first = pl.multiple_of(index * blk, blk)
            if own:
                allowed = lane <= line + first
            for h in range(heads):
                cols = slice(h * size, (h + 1) * size)
                vals = slice(part + h * size, part + (h + 1) * size)
                q = q_ref[pl.ds(first, blk), cols]
                k = kv_ref[:, cols]
                do = do_ref[pl.ds(first, blk), cols]
                s = dot_nt(q, k) * scale
                p = jnp.exp(s - lse_ref[pl.ds(first, blk), h : h + 1])
                if own:
                    p = jnp.where(allowed, p, 0.0)
                dp = dot_nt(do, kv_ref[:, vals])
                delta = jnp.sum(
                    do.astype(jnp.float32) * mix_ref[pl.ds(first, blk), cols], axis=-1, keepdims=True
                )
                ds = (p * (dp - delta)).astype(jnp.bfloat16)
                dq = dot_nn(ds, k) * scale
                if own:
                    dq = dq + seed_ref[pl.ds(first, blk), cols]
                dq_ref[pl.ds(first, blk), cols] = dq.astype(dq_ref.dtype)
                dkv_ref[:, cols] += dot_tn(ds, q) * scale
                dkv_ref[:, vals] += dot_tn(p.astype(jnp.bfloat16), do)
            return 0

        lax.fori_loop(0, rows // blk, block, 0)

    if own:
        work()
    else:

        @pl.when(flag_ref[0] == 1)
        def _():
            work()

        @pl.when(flag_ref[0] == 0)
        def _():
            dq_ref[...] = jnp.zeros_like(dq_ref)
            dkv_ref[...] = jnp.zeros_like(dkv_ref)


def attend_back(sz, own, odd, q, kv, grad_mix, mix, lse, seed):
    rows = q.shape[0] // 2
    part = sz.part

    def rows_of(width):
        return pl.BlockSpec((rows, width), lambda g, odd: (g, 0))

    return pl.pallas_call(
        functools.partial(attend_back_kernel, sz.quarter_heads, sz.head_size, own),
        grid_spec=pltpu.PrefetchScalarGridSpec(
            num_scalar_prefetch=1,
            grid=(2,),
            in_specs=[
                rows_of(part),
                rows_of(2 * part),
                rows_of(part),
                rows_of(part),
                rows_of(8),
                rows_of(part) if own else pl.BlockSpec((8, 128), lambda g, odd: (0, 0)),
            ],
            out_specs=[rows_of(part), rows_of(2 * part)],
        ),
        out_shape=(
            jax.ShapeDtypeStruct((2 * rows, part), jnp.bfloat16 if own else jnp.float32),
            jax.ShapeDtypeStruct((2 * rows, 2 * part), jnp.float32),
        ),
        cost_estimate=pl.CostEstimate(
            flops=5 * 2 * 2 * rows * rows * part,
            bytes_accessed=40 * rows * part,
            transcendentals=2 * rows * rows * sz.quarter_heads,
        ),
        compiler_params=pltpu.CompilerParams(vmem_limit_bytes=48 << 20),
        name="attend_back_own" if own else "attend_back_before",
    )(odd, q, kv, grad_mix, mix, lse, seed)


def norm_parts(values):
    mean = jnp.mean(values, axis=-1, keepdims=True)
    centre = values - mean
    rs = lax.rsqrt(jnp.mean(centre * centre, axis=-1, keepdims=True) + EPSILON)
    return centre * rs, rs


def norm_back(normed, rs, grad, gain):
    e = grad * gain
    return rs * (
        e
        - jnp.mean(e, axis=-1, keepdims=True)
        - normed * jnp.mean(e * normed, axis=-1, keepdims=True)
    )


def per_device_quad(tokens, params, out_grad, lengths):
    rows, width = tokens.shape
    hidden = FF
    sz = Sizes(width, hidden, HEADS, HEAD_DIM, params.shape[0])
    y, c, z, x = my_place()
    quarter = c * 2 + x
    bf16, f32 = jnp.bfloat16, jnp.float32

    def pick(value, index):
        return lax.dynamic_index_in_dim(value, index, 0, keepdims=False)

    def reduce_ordered(kept, sent):
        summed = kept + over_y(sent.astype(bf16)).astype(f32)
        summed = summed.reshape(4, summed.shape[0] // 4, -1)
        total = pick(summed, z)
        for d in (1, 2, 3):
            total = total + over_z(pick(summed, (z + d) % 4).astype(bf16), d).astype(f32)
        return total

    def halves_of(value):
        half = value.shape[1] // 2
        first, second = value[:, :half], value[:, half:]
        return jnp.where(y == 0, first, second), jnp.where(y == 0, second, first)

    def reduce_places(left, right):
        mine, other = halves_of(left)
        return reduce_ordered(dot_tn(mine, right), dot_tn(other, right))

    w_qkv, w_out, w_fc, w_proj, vec, tok_all, cot_all = open_call(
        sz, params.reshape(sz.block, GRAIN, width), tokens, out_grad
    )
    flat = lambda value: value.reshape(-1, width)
    vectors = flat(vec).astype(f32)
    fc_bias = vectors[8 : 8 + hidden // width].reshape(hidden)
    w_qkv, cot_all = flat(w_qkv), flat(cot_all)
    normed_all, _ = norm_parts(flat(tok_all).astype(f32))
    act_one = (normed_all * vectors[0] + vectors[1]).astype(bf16)

    def quarter_of(vector):
        padded = jnp.pad(vector, (0, 4 * sz.part - width))
        return lax.dynamic_slice_in_dim(padded, quarter * sz.part, sz.part, 0)

    kv_bias = jnp.concatenate([jnp.zeros((sz.part,), f32), quarter_of(vectors[3])])
    kv = (dot_nt(act_one, w_qkv[sz.part :]) + kv_bias).astype(bf16)
    q = (dot_nt(act_one, w_qkv[: sz.part]) + quarter_of(vectors[2])).astype(bf16)
    before, _, w_fc, w_out = keys_call(kv, w_out, w_fc)
    w_fc, w_out = flat(w_fc), flat(w_out)[:width]
    odd = (z % 2).astype(jnp.int32).reshape(1)
    mix, lse = attend(sz, odd, q, kv, before)
    mixed = swap_call(mix.astype(bf16).reshape(4, rows, sz.part))
    mixed = jnp.transpose(mixed, (1, 0, 2)).reshape(rows, 4 * sz.part)[:, :width]
    inputs = tokens.astype(f32)
    residual = inputs + (dot_nt(mixed, w_out) + vectors[4])
    normed_two, rs_two = norm_parts(residual)
    act_two, w_proj = acts_call((normed_two * vectors[5] + vectors[6]).astype(bf16), w_proj)
    act_two, w_proj = flat(act_two), flat(w_proj)
    bias = lax.dynamic_slice_in_dim(fc_bias, quarter * (hidden // 4), hidden // 4, 0)
    pre_act = dot_nt(act_two, w_fc) + bias
    act_hidden, pull_gelu = jax.vjp(gelu_tanh, pre_act)
    act_hidden = act_hidden.astype(bf16)
    g_proj = reduce_places(act_hidden, cot_all)
    grad_fc = pull_gelu(dot_nt(cot_all, w_proj))[0].astype(bf16)
    grad_two = quad_sum(dot_nn(grad_fc, w_fc).astype(bf16).reshape(2, 2, rows, width))
    g_fc = reduce_places(grad_fc, act_two)

    cot = out_grad.astype(f32)
    grad_res = cot + norm_back(normed_two, rs_two, grad_two, vectors[5])
    grad_attn = grad_res.astype(bf16)
    grad_mix = dot_nn(grad_attn, w_out).astype(bf16)
    grad_mix = jnp.pad(grad_mix, ((0, 0), (0, 4 * sz.part - width)))
    grad_mix = jnp.transpose(grad_mix.reshape(rows, 4, sz.part), (1, 0, 2))
    grad_mix = swap_call(grad_mix).reshape(4 * rows, sz.part)
    seed = jnp.zeros((8, 128), f32)
    dq_before, dkv_before = attend_back(sz, False, odd, q, before, grad_mix, mix, lse, seed)
    returned = permute(
        dkv_before.astype(bf16), lambda py, pc, pz, px: (py, pc, pz - 1, px) if pz % 2 == 1 else None
    )
    partial_out = dot_nn(act_hidden, w_proj).astype(bf16).reshape(2, 2, rows, width)
    output = (residual + quad_sum(partial_out) + vectors[7]).astype(bf16)
    dq, dkv = attend_back(sz, True, odd, q, kv, grad_mix, mix, lse, dq_before)
    grad_qkv = jnp.concatenate([dq, (dkv + returned.astype(f32)).astype(bf16)], axis=1)
    g_qkv = reduce_places(grad_qkv, act_one)
    grad_one = quad_sum(dot_nn(grad_qkv, w_qkv).astype(bf16).reshape(2, 2, rows, width))

    g_out = jnp.pad(dot_tn(grad_attn, mixed).astype(bf16), ((0, 4 * sz.part - width), (0, 0)))
    g_out = quad_sum(g_out.reshape(2, 2, sz.part, width)).reshape(2, sz.part // 2, width)
    g_out = reduce_ordered(pick(g_out, y), pick(g_out, 1 - y))

    normed_one, rs_one = norm_parts(inputs)
    input_grad = (grad_res + norm_back(normed_one, rs_one, grad_one, vectors[0])).astype(bf16)

    def placed(vector):
        spot = lax.dynamic_update_slice_in_dim(jnp.zeros((4 * sz.part,), f32), vector, quarter * sz.part, 0)
        return spot[:width]

    sums = jnp.sum(grad_qkv.astype(f32), axis=0)
    bias_sum = jnp.sum(grad_fc.astype(f32), axis=0).reshape(1, hidden // 4)
    fc_rows = lax.dynamic_update_slice_in_dim(jnp.zeros((4, hidden // 4), f32), bias_sum, quarter, 0)
    grad_vectors = jnp.concatenate(
        [
            jnp.stack(
                [
                    jnp.sum(grad_one * normed_one, axis=0),
                    jnp.sum(grad_one, axis=0),
                    placed(sums[: sz.part]),
                    placed(sums[2 * sz.part :]),
                    jnp.sum(grad_attn.astype(f32), axis=0),
                    jnp.sum(grad_two * normed_two, axis=0),
                    jnp.sum(grad_two, axis=0),
                    jnp.sum(cot, axis=0),
                ]
            ),
            fc_rows.reshape(hidden // width, width),
        ]
    )
    count = grad_vectors.shape[0]
    grad_vectors = jnp.pad(grad_vectors, ((0, sz.vec * GRAIN - count), (0, 0)))
    grains = lambda value: value.astype(bf16).reshape(-1, GRAIN, width)
    table, all_vectors = collect(
        sz, grains(g_qkv), grains(g_out), grains(g_fc), grains(g_proj), grad_vectors.reshape(sz.vec, GRAIN, width)
    )
    grad_vectors = jnp.sum(all_vectors.reshape(32, sz.vec * GRAIN, width), axis=0)[:count]
    table = table.reshape(sz.block * GRAIN, width).astype(f32)
    used = (sz.vec_start % sz.block) * GRAIN
    tail = jnp.concatenate(
        [grad_vectors, jnp.zeros((sz.block * GRAIN - used - grad_vectors.shape[0], width), f32)]
    )
    last = flat_id(y, c, z, x) == sz.vec_start // sz.block
    tail = jnp.where(last, tail, table[used:])
    param_grad = jnp.concatenate([table[:used], tail])
    return (output, input_grad, param_grad)


def fits_quad(mesh, tokens, params, lengths):
    dp, cp = mesh.shape["dp"], mesh.shape["cp"]
    rows = tokens.shape[0] // (dp * cp)
    width = tokens.shape[1]
    blocks = params.shape[0] // (dp * cp)
    return (
        (dp, cp) == (4, 8)
        and lengths.shape[1] == 2
        and rows * cp == lengths.shape[1] * MIN_LEN
        and rows % 128 == 0
        and blocks % GRAIN == 0
        and (HEADS, HEAD_DIM, FF, width) == (25, 64, 6400, 1600)
    )


def solution(mesh):
    in_specs = (P(("dp", "cp"), None), P(("dp", "cp"), None), P(("dp", "cp"), None), P("dp", None))
    out_specs = (P(("dp", "cp"), None), P(("dp", "cp"), None), P(("dp", "cp"), None))

    def step(tokens, params, out_grad, lengths):
        body = per_device_quad if fits_quad(mesh, tokens, params, lengths) else per_device_general
        return jax.shard_map(
            body, mesh=mesh, in_specs=in_specs, out_specs=out_specs, check_vma=False
        )(tokens, params, out_grad, lengths)

    return step
```

```python
import functools

import jax
import jax.numpy as jnp
from jax import lax
from jax.experimental import pallas as pl
from jax.experimental.pallas import tpu as pltpu
from jax.sharding import PartitionSpec as P


HEADS = 25
FF = 6400
HEAD_DIM = 64
TILE = 128
MIN_LEN = 1024
MAX_LEN = 4096


EPSILON = 1e-05
MASKED = -1e30
GELU_SCALE = 0.7978845608028654


def from_behind(value, axis, by):
    length = lax.axis_size(axis)
    pairs = [(i, i + by) for i in range(length) if 0 <= i + by < length]
    return lax.ppermute(value, axis, pairs)


def layer_norm(values, gain_row, bias_row):
    centre = values - jnp.mean(values, axis=-1, keepdims=True)
    spread = jnp.mean(centre * centre, axis=-1, keepdims=True)
    return centre * lax.rsqrt(spread + EPSILON) * gain_row + bias_row


def gelu_tanh(values):
    return (
        0.5 * values * (1.0 + jnp.tanh(GELU_SCALE * (values + 0.044715 * values * values * values)))
    )


def segment_of(position, seq_ends):
    return jnp.sum((position[:, None] >= seq_ends[None, :]).astype(jnp.int32), axis=1)


def unpack(gathered, model_width, hidden):
    out_end = 4 * model_width
    fc_end = out_end + hidden
    proj_end = fc_end + hidden
    vec_end = proj_end + 8
    return (
        gathered[0 : 3 * model_width],
        gathered[3 * model_width : out_end],
        gathered[out_end:fc_end],
        gathered[fc_end:proj_end],
        gathered[proj_end:vec_end].astype(jnp.float32),
        gathered[vec_end : vec_end + hidden // model_width].astype(jnp.float32).reshape(hidden),
    )


def matmul_nt(left_mat, right_mat):
    return lax.dot_general(
        left_mat, right_mat, (((1,), (1,)), ((), ())), preferred_element_type=jnp.float32
    )


def matmul_tn(left_mat, right_mat):
    return lax.dot_general(
        left_mat, right_mat, (((0,), (0,)), ((), ())), preferred_element_type=jnp.float32
    )


def matmul_nn(left_mat, right_mat):
    return jnp.dot(left_mat, right_mat, preferred_element_type=jnp.float32)


def per_device_general(tokens, params, out_grad, lengths):
    tok_rows, model_width = tokens.shape
    hidden = FF
    head_count = HEADS
    head_size = HEAD_DIM
    cp_count = lax.axis_size("cp")
    group_rows = tok_rows * cp_count
    seq_count = lengths.shape[1]
    longest = min(MAX_LEN, group_rows - (seq_count - 1) * MIN_LEN)
    reach_back = min(cp_count - 1, (longest + tok_rows - TILE - 1) // tok_rows)
    pair_count = (reach_back + 2) // 2
    score_scale = head_size ** (-0.5)
    gathered = lax.all_gather(params, ("dp", "cp"), axis=0, tiled=True)
    w_attn, w_out, w_fc, w_proj, vectors, fc_bias = unpack(gathered, model_width, hidden)
    inputs = tokens.astype(jnp.float32)
    act_one = layer_norm(inputs, vectors[0], vectors[1]).astype(jnp.bfloat16)
    qkv_bias = jnp.concatenate([vectors[2], jnp.zeros_like(vectors[2]), vectors[3]])
    qkv = (matmul_nt(act_one, w_attn) + qkv_bias).astype(jnp.bfloat16)
    queries = qkv[:, :model_width].reshape(tok_rows, head_count, head_size)
    key_value = qkv[:, model_width:]
    device = lax.axis_index("cp")
    seq_ends = jnp.cumsum(lengths[0])
    query_pos = device * tok_rows + jnp.arange(tok_rows, dtype=jnp.int32)
    query_seg = segment_of(query_pos, seq_ends)
    store = jnp.zeros((2 * pair_count, tok_rows, 2 * model_width), jnp.bfloat16)
    store = store.at[0].set(key_value)

    def fetch(step_index, state_pair):
        moving, held_rows = state_pair
        moving = from_behind(moving, "cp", 1)
        return (moving, lax.dynamic_update_index_in_dim(held_rows, moving, step_index, 0))

    _, store = lax.fori_loop(1, reach_back + 1, fetch, (key_value, store))

    def pair_mask(pair_index):
        owners = 2 * pair_index + jnp.arange(2, dtype=jnp.int32)
        key_pos = (
            (device - owners)[:, None] * tok_rows + jnp.arange(tok_rows, dtype=jnp.int32)[None, :]
        ).reshape(2 * tok_rows)
        usable = jnp.broadcast_to((owners <= reach_back)[:, None], (2, tok_rows)).reshape(
            2 * tok_rows
        ) & (key_pos >= 0)
        key_seg = segment_of(key_pos, seq_ends)
        return (
            (key_seg[None, :] == query_seg[:, None])
            & (key_pos[None, :] <= query_pos[:, None])
            & usable[None, :]
        )

    def pair_rows(pair_index):
        block_rows = lax.dynamic_slice_in_dim(store, 2 * pair_index, 2, 0).reshape(
            2 * tok_rows, 2 * model_width
        )
        return (
            block_rows[:, :model_width].reshape(2 * tok_rows, head_count, head_size),
            block_rows[:, model_width:].reshape(2 * tok_rows, head_count, head_size),
        )

    def pair_scores(key_rows, allowed):
        raw_scores = (
            jnp.einsum("qhd,khd->hqk", queries, key_rows, preferred_element_type=jnp.float32)
            * score_scale
        )
        return jnp.where(allowed[None], raw_scores, MASKED)

    def visit(work):

        def step_pair(pair_index, running):
            allowed = pair_mask(pair_index)
            result = work(pair_index, allowed, running)
            return result

        return step_pair

    def add_total(pair_index, allowed, running):
        row_top, summed = running
        key_rows, _ = pair_rows(pair_index)
        scores = pair_scores(key_rows, allowed)
        new_top = jnp.maximum(row_top, jnp.max(scores, axis=-1, keepdims=True))
        summed = summed * jnp.exp(row_top - new_top) + jnp.sum(
            jnp.exp(scores - new_top), axis=-1, keepdims=True
        )
        return (new_top, summed)

    start_top = jnp.full((head_count, tok_rows, 1), MASKED, jnp.float32)
    start_sum = jnp.zeros((head_count, tok_rows, 1), jnp.float32)
    row_top, summed = lax.fori_loop(0, pair_count, visit(add_total), (start_top, start_sum))
    log_total = row_top + jnp.log(summed)

    def add_mix(pair_index, allowed, running):
        key_rows, value_rows = pair_rows(pair_index)
        prob_rows = jnp.exp(pair_scores(key_rows, allowed) - log_total).astype(jnp.bfloat16)
        return running + jnp.einsum(
            "hqk,khd->qhd", prob_rows, value_rows, preferred_element_type=jnp.float32
        )

    mixed_full = lax.fori_loop(
        0, pair_count, visit(add_mix), jnp.zeros((tok_rows, head_count, head_size), jnp.float32)
    )
    mixed = mixed_full.reshape(tok_rows, model_width).astype(jnp.bfloat16)
    attn_out = matmul_nt(mixed, w_out) + vectors[4]
    residual = inputs + attn_out
    act_two = layer_norm(residual, vectors[5], vectors[6]).astype(jnp.bfloat16)
    pre_act = matmul_nt(act_two, w_fc) + fc_bias
    act_hidden = gelu_tanh(pre_act).astype(jnp.bfloat16)
    output = (residual + matmul_nn(act_hidden, w_proj) + vectors[7]).astype(jnp.bfloat16)
    gathered = lax.all_gather(params, ("dp", "cp"), axis=0, tiled=True)
    w_attn, w_out, w_fc, w_proj, vectors, fc_bias = unpack(gathered, model_width, hidden)
    grad_out_f = out_grad.astype(jnp.float32)
    grad_hidden = matmul_nt(out_grad, w_proj)
    _, pull_gelu = jax.vjp(gelu_tanh, pre_act)
    grad_fc = pull_gelu(grad_hidden)[0].astype(jnp.bfloat16)
    grad_act_two = matmul_nn(grad_fc, w_fc)
    _, pull_two = jax.vjp(layer_norm, residual, vectors[5], vectors[6])
    grad_res_norm, grad_gain_two, grad_bias_two = pull_two(grad_act_two)
    grad_res = grad_out_f + grad_res_norm
    grad_attn = grad_res.astype(jnp.bfloat16)
    grad_mix = (
        matmul_nn(grad_attn, w_out).astype(jnp.bfloat16).reshape(tok_rows, head_count, head_size)
    )
    grad_dot = jnp.transpose(jnp.sum(grad_mix.astype(jnp.float32) * mixed_full, axis=-1), (1, 0))[
        :, :, None
    ]

    def add_grads(pair_index, allowed, running):
        grad_query, grad_store = running
        key_rows, value_rows = pair_rows(pair_index)
        prob_rows = jnp.exp(pair_scores(key_rows, allowed) - log_total)
        grad_probs = jnp.einsum(
            "qhd,khd->hqk", grad_mix, value_rows, preferred_element_type=jnp.float32
        )
        grad_scores = (prob_rows * (grad_probs - grad_dot)).astype(jnp.bfloat16)
        grad_query = (
            grad_query
            + jnp.einsum("hqk,khd->qhd", grad_scores, key_rows, preferred_element_type=jnp.float32)
            * score_scale
        )
        grad_keys = (
            jnp.einsum("hqk,qhd->khd", grad_scores, queries, preferred_element_type=jnp.float32)
            * score_scale
        )
        grad_values = jnp.einsum(
            "hqk,qhd->khd",
            prob_rows.astype(jnp.bfloat16),
            grad_mix,
            preferred_element_type=jnp.float32,
        )
        pair_grad = jnp.concatenate(
            [
                grad_keys.reshape(2 * tok_rows, model_width),
                grad_values.reshape(2 * tok_rows, model_width),
            ],
            axis=1,
        )
        pair_grad = pair_grad.reshape(2, tok_rows, 2 * model_width)
        grad_store = lax.dynamic_update_slice_in_dim(grad_store, pair_grad, 2 * pair_index, 0)
        return (grad_query, grad_store)

    start_query = jnp.zeros((tok_rows, head_count, head_size), jnp.float32)
    start_store = jnp.zeros((2 * pair_count, tok_rows, 2 * model_width), jnp.float32)
    grad_query, grad_store = lax.fori_loop(
        0, pair_count, visit(add_grads), (start_query, start_store)
    )

    def send_back(step_index, moving):
        moving = moving + lax.dynamic_index_in_dim(
            grad_store, reach_back - step_index, 0, keepdims=False
        )
        return from_behind(moving.astype(jnp.bfloat16), "cp", -1).astype(moving.dtype)

    returned = lax.fori_loop(
        0, reach_back, send_back, jnp.zeros((tok_rows, 2 * model_width), jnp.float32)
    )
    grad_kv = returned + grad_store[0]
    grad_qkv = jnp.concatenate([grad_query.reshape(tok_rows, model_width), grad_kv], axis=1).astype(
        jnp.bfloat16
    )
    grad_qkv_f = grad_qkv.astype(jnp.float32)
    grad_act_one = matmul_nn(grad_qkv, w_attn)
    _, pull_one = jax.vjp(layer_norm, inputs, vectors[0], vectors[1])
    grad_in_norm, grad_gain_one, grad_bias_one = pull_one(grad_act_one)
    input_grad = (grad_res + grad_in_norm).astype(jnp.bfloat16)
    grad_vectors = jnp.stack(
        [
            grad_gain_one,
            grad_bias_one,
            jnp.sum(grad_qkv_f[:, :model_width], axis=0),
            jnp.sum(grad_qkv_f[:, 2 * model_width :], axis=0),
            jnp.sum(grad_attn.astype(jnp.float32), axis=0),
            grad_gain_two,
            grad_bias_two,
            jnp.sum(grad_out_f, axis=0),
        ]
    )
    grad_fc_bias = jnp.sum(grad_fc.astype(jnp.float32), axis=0).reshape(
        hidden // model_width, model_width
    )
    used_rows = 4 * model_width + 2 * hidden + 8 + hidden // model_width
    total_rows = gathered.shape[0]
    local_grad = jnp.concatenate(
        [
            matmul_tn(grad_qkv, act_one),
            matmul_tn(grad_attn, mixed),
            matmul_tn(grad_fc, act_two),
            matmul_tn(act_hidden, out_grad),
            grad_vectors,
            grad_fc_bias,
            jnp.zeros((total_rows - used_rows, model_width), jnp.float32),
        ],
        axis=0,
    )
    dp_count = lax.axis_size("dp")
    device_count = dp_count * cp_count
    share_rows = total_rows // device_count
    spread_rows = local_grad.reshape(device_count, 1, share_rows, model_width)
    received = lax.all_to_all(
        spread_rows.astype(jnp.bfloat16), ("dp", "cp"), split_axis=0, concat_axis=1, tiled=True
    ).astype(spread_rows.dtype)
    param_grad = jnp.sum(received, axis=1).reshape(share_rows, model_width)
    return (output, input_grad, param_grad)


MESH = pl.DeviceIdType.MESH
GRAIN = 8
NT = (((1,), (1,)), ((), ()))
TN = (((0,), (0,)), ((), ()))


def dot_nt(a, b):
    return lax.dot_general(a, b, NT, preferred_element_type=jnp.float32)


def dot_tn(a, b):
    return lax.dot_general(a, b, TN, preferred_element_type=jnp.float32)


def dot_nn(a, b):
    return jnp.dot(a, b, preferred_element_type=jnp.float32)


def flat_id(y, c, z, x):
    return ((y * 2 + c) * 4 + z) * 2 + x


def permute(value, move):
    pairs = []
    for y in range(2):
        for c in range(2):
            for z in range(4):
                for x in range(2):
                    to = move(y, c, z, x)
                    if to is not None:
                        pairs.append((flat_id(y, c, z, x), flat_id(*to)))
    return lax.ppermute(value, ("dp", "cp"), pairs)


def over_y(value):
    return permute(value, lambda y, c, z, x: (1 - y, c, z, x))


def over_z(value, by):
    return permute(value, lambda y, c, z, x: (y, c, (z + by) % 4, x))


class Sizes:
    def __init__(self, width, hidden, heads, head_size, rows):
        self.head_size = head_size
        self.quarter_heads = -(-heads // 4)
        self.part = self.quarter_heads * head_size
        self.part_grains = self.part // GRAIN
        self.width_grains = width // GRAIN
        self.spill = 4 * self.part_grains - self.width_grains
        self.qkv = 3 * self.part_grains // 8
        self.out = self.part_grains // 8
        self.mlp = hidden // 4 // 8 // GRAIN
        self.block = rows // GRAIN
        self.out_start = 3 * self.width_grains
        self.fc_start = 4 * self.width_grains
        self.proj_start = self.fc_start + hidden // GRAIN
        self.vec_start = self.proj_start + hidden // GRAIN
        self.vec = 2


def my_place():
    dp = lax.axis_index("dp")
    cp = lax.axis_index("cp")
    return dp // 2, dp % 2, cp // 2, cp % 2


def place_of(quarter, share):
    return (share // 4) * 2 + quarter // 2, (share % 4) * 2 + quarter % 2


class Wires:
    def __init__(self, send_sems, recv_sems):
        self.send_sems = send_sems
        self.recv_sems = recv_sems
        self.count = 0

    def to(self, src, dst, dp, cp):
        index = self.count
        self.count += 1
        return pltpu.make_async_remote_copy(
            src_ref=src,
            dst_ref=dst,
            send_sem=self.send_sems.at[index],
            recv_sem=self.recv_sems.at[index],
            device_id=(dp, cp),
            device_id_type=MESH,
        )


class PlaceGather:
    def __init__(self, wires, full):
        self.wires = wires
        self.full = full
        self.dp, self.cp = lax.axis_index("dp"), lax.axis_index("cp")
        self.y, self.z, self.x = self.dp // 2, self.cp // 2, self.cp % 2
        self.started = []

    def send(self, slot, dp, cp):
        view = self.full.at[slot]
        copy = self.wires.to(view, view, dp, cp)
        copy.start()
        self.started.append(copy)
        return copy

    def start(self):
        mine = self.y * 4 + self.z
        self.along = []
        for d in (1, 3, 2):
            self.along.append((d, self.send(mine, self.dp, ((self.z + d) % 4) * 2 + self.x)))
        self.over = [self.send(mine, (self.dp + 2) % 4, self.cp)]

    def forward(self):
        for d, copy in self.along:
            copy.wait_recv()
            self.over.append(self.send(self.y * 4 + (self.z - d + 4) % 4, (self.dp + 2) % 4, self.cp))

    def finish(self):
        for copy in self.over:
            copy.wait_recv()
        for copy in self.started:
            copy.wait_send()


class QuadGather:
    def __init__(self, wires, block, full, local_sem):
        self.wires = wires
        self.block = block
        self.full = full
        self.dp, self.cp = lax.axis_index("dp"), lax.axis_index("cp")
        self.c, self.x = self.dp % 2, self.cp % 2
        self.over_x = (self.dp, self.cp + 1 - 2 * self.x)
        self.over_c = (self.dp + 1 - 2 * self.c, self.cp)
        self.local_sem = local_sem

    def start(self):
        spot = self.full.at[self.c, self.x]
        self.by_x = self.wires.to(self.block, spot, *self.over_x)
        self.by_c = self.wires.to(self.block, spot, *self.over_c)
        self.by_x.start()
        self.by_c.start()
        self.local = pltpu.make_async_copy(self.block, spot, self.local_sem)
        self.local.start()

    def forward(self):
        self.by_x.wait_recv()
        spot = self.full.at[self.c, 1 - self.x]
        self.pass_on = self.wires.to(spot, spot, *self.over_c)
        self.pass_on.start()

    def finish(self):
        self.by_c.wait_recv()
        self.pass_on.wait_recv()
        self.by_x.wait_send()
        self.by_c.wait_send()
        self.pass_on.wait_send()
        self.local.wait()


def open_kernel(
    sz, p_ref, tok_ref, cot_ref, qkv_ref, out_ref, fc_ref, proj_ref, vec_ref, tok_all, cot_all,
    spread_sems, kind_sems, send_sems, recv_sems, local_sems,
):
    y, c, z, x = my_place()
    me = flat_id(y, c, z, x)
    wires = Wires(send_sems, recv_sems)
    tok = QuadGather(wires, tok_ref, tok_all, local_sems.at[0])
    cot = QuadGather(wires, cot_ref, cot_all, local_sems.at[1])

    def send(grain, ref, slot, quarter, share, sem, recv):
        dp, cp = place_of(quarter, share)
        mine = dp * 8 + cp == me

        @pl.when(mine)
        def _():
            pltpu.make_async_copy(p_ref.at[grain], ref.at[share, slot], recv).start()

        @pl.when(jnp.logical_not(mine))
        def _():
            pltpu.make_async_remote_copy(
                src_ref=p_ref.at[grain],
                dst_ref=ref.at[share, slot],
                send_sem=sem,
                recv_sem=recv,
                device_id=(dp, cp),
                device_id_type=MESH,
            ).start()

    def sent(grain, ref, slot, quarter, share, sem, recv):
        dp, cp = place_of(quarter, share)

        @pl.when(dp * 8 + cp != me)
        def _():
            pltpu.make_async_copy(p_ref.at[grain], p_ref.at[grain], sem).wait()

    def headed(act, grain, base, parts, ref, recv, share_size):
        offset = me * sz.block + grain - base
        part = offset // sz.width_grains
        local = offset % sz.width_grains

        def one(quarter, inner, sem):
            spot = part * sz.part_grains + inner
            act(grain, ref, spot % share_size, quarter, spot // share_size, sem, recv)

        @pl.when(jnp.logical_and(offset >= 0, offset < parts * sz.width_grains))
        def _():
            one(local // sz.part_grains, local % sz.part_grains, spread_sems.at[grain])

            @pl.when(local < sz.spill)
            def _():
                one(3, sz.part_grains - sz.spill + local, spread_sems.at[sz.block + grain])

    def plain(act, grain, base, ref, recv):
        offset = me * sz.block + grain - base

        @pl.when(jnp.logical_and(offset >= 0, offset < 32 * sz.mlp))
        def _():
            act(
                grain, ref, offset % sz.mlp, offset // (8 * sz.mlp), (offset // sz.mlp) % 8,
                spread_sems.at[grain], recv,
            )

    def heads(act):
        def one(grain, _):
            headed(act, grain, 0, 3, qkv_ref, kind_sems.at[0], sz.qkv)
            return 0

        lax.fori_loop(0, sz.block, one, 0)

    def others(act):
        def one(grain, _):
            headed(act, grain, sz.out_start, 1, out_ref, kind_sems.at[1], sz.out)
            plain(act, grain, sz.fc_start, fc_ref, kind_sems.at[2])
            plain(act, grain, sz.proj_start, proj_ref, kind_sems.at[3])
            return 0

        lax.fori_loop(0, sz.block, one, 0)

    owner = sz.vec_start // sz.block
    spot = sz.vec_start % sz.block

    def vector_sends(act):
        @pl.when(me == owner)
        def _():
            def to(device, _):
                @pl.when(device != me)
                def _():
                    act(
                        pltpu.make_async_remote_copy(
                            src_ref=p_ref.at[pl.ds(spot, sz.vec)],
                            dst_ref=vec_ref,
                            send_sem=spread_sems.at[2 * sz.block + device],
                            recv_sem=kind_sems.at[4],
                            device_id=(device // 8, device % 8),
                            device_id_type=MESH,
                        )
                    )

                return 0

            lax.fori_loop(0, 32, to, 0)

    heads(send)
    tok.start()
    cot.start()
    mine = y * 4 + z
    pltpu.make_async_copy(qkv_ref.at[mine], qkv_ref.at[mine], kind_sems.at[0]).wait()
    weights = PlaceGather(wires, qkv_ref)
    weights.start()
    others(send)
    vector_sends(lambda copy: copy.start())

    @pl.when(me == owner)
    def _():
        pltpu.make_async_copy(p_ref.at[pl.ds(spot, sz.vec)], vec_ref, kind_sems.at[4]).start()

    weights.forward()
    tok.forward()
    cot.forward()
    heads(sent)
    others(sent)
    vector_sends(lambda copy: copy.wait_send())
    for index, ref in enumerate((out_ref, fc_ref, proj_ref)):
        pltpu.make_async_copy(ref.at[mine], ref.at[mine], kind_sems.at[index + 1]).wait()
    pltpu.make_async_copy(vec_ref, vec_ref, kind_sems.at[4]).wait()
    tok.finish()
    cot.finish()
    weights.finish()


HBM = pl.BlockSpec(memory_space=pl.ANY)
VMEM = pl.BlockSpec(memory_space=pltpu.VMEM)
REMOTE = pltpu.CompilerParams(has_side_effects=True)


def remote_params(ident=None, vmem=None):
    return pltpu.CompilerParams(has_side_effects=True, collective_id=ident, vmem_limit_bytes=vmem)


def greet(partners):
    barrier = pltpu.get_barrier_semaphore()
    for dp, cp in partners:
        pl.semaphore_signal(barrier, inc=1, device_id=(dp, cp), device_id_type=MESH)
    pl.semaphore_wait(barrier, len(partners))


def cost(us):
    return pl.CostEstimate(flops=0, bytes_accessed=int(us * 3.0e6), transcendentals=0)


def wire_sems(count):
    return [pltpu.SemaphoreType.DMA((count,)), pltpu.SemaphoreType.DMA((count,))]


def open_call(sz, table, tokens, cotangent):
    rows, width = tokens.shape

    def like(*shape):
        return jax.ShapeDtypeStruct(shape + (width,), table.dtype)

    return pl.pallas_call(
        functools.partial(open_kernel, sz),
        out_shape=(
            like(8, sz.qkv, GRAIN),
            like(8, sz.out, GRAIN),
            like(8, sz.mlp, GRAIN),
            like(8, sz.mlp, GRAIN),
            like(sz.vec, GRAIN),
            like(2, 2, rows),
            like(2, 2, rows),
        ),
        in_specs=[HBM, VMEM, VMEM],
        out_specs=[HBM] * 7,
        scratch_shapes=[
            pltpu.SemaphoreType.DMA((2 * sz.block + 32,)),
            pltpu.SemaphoreType.DMA((5,)),
            *wire_sems(13),
            pltpu.SemaphoreType.DMA((2,)),
        ],
        compiler_params=REMOTE,
        name="open",
    )(table, tokens, cotangent)


def keys_kernel(kv_ref, out_in, fc_in, before_ref, out_ref, fc_ref, out_all, send_sems, recv_sems, local_sem):
    _, _, z, _ = my_place()
    dp, cp = lax.axis_index("dp"), lax.axis_index("cp")
    wires = Wires(send_sems, recv_sems)
    keys = wires.to(kv_ref, before_ref, dp, (cp + 2) % 8)

    @pl.when(z % 2 == 0)
    def _():
        keys.start()

    first = PlaceGather(wires, out_ref)
    second = PlaceGather(wires, fc_ref)
    first.start()
    second.start()
    first.forward()
    first.finish()
    quad = QuadGather(wires, out_ref, out_all, local_sem)
    quad.start()

    @pl.when(z % 2 == 1)
    def _():
        keys.wait_recv()

    second.forward()
    quad.forward()
    second.finish()
    quad.finish()

    @pl.when(z % 2 == 0)
    def _():
        keys.wait_send()


def keys_call(kv, w_out, w_fc):
    def like(value, *lead):
        return jax.ShapeDtypeStruct(lead + value.shape, value.dtype)

    return pl.pallas_call(
        keys_kernel,
        out_shape=(like(kv), like(w_out), like(w_fc), like(w_out, 2, 2)),
        in_specs=[HBM] * 3,
        out_specs=[HBM] * 4,
        input_output_aliases={1: 1, 2: 2},
        scratch_shapes=[*wire_sems(18), pltpu.SemaphoreType.DMA],
        compiler_params=REMOTE,
        name="keys",
    )(kv, w_out, w_fc)


def acts_kernel(act_ref, proj_in, act_all, proj_ref, send_sems, recv_sems, local_sem):
    wires = Wires(send_sems, recv_sems)
    quad = QuadGather(wires, act_ref, act_all, local_sem)
    places = PlaceGather(wires, proj_ref)
    quad.start()
    places.start()
    quad.forward()
    places.forward()
    quad.finish()
    places.finish()


def acts_call(act, w_proj):
    return pl.pallas_call(
        acts_kernel,
        out_shape=(
            jax.ShapeDtypeStruct((2, 2) + act.shape, act.dtype),
            jax.ShapeDtypeStruct(w_proj.shape, w_proj.dtype),
        ),
        in_specs=[VMEM, HBM],
        out_specs=[HBM] * 2,
        input_output_aliases={1: 1},
        scratch_shapes=[*wire_sems(10), pltpu.SemaphoreType.DMA],
        compiler_params=REMOTE,
        name="acts",
    )(act, w_proj)


def swap_kernel(in_ref, out_ref, send_sems, recv_sems, local_sem):
    y, c, z, x = my_place()
    wires = Wires(send_sems, recv_sems)
    mine = c * 2 + x
    others = [(1 - c, 1 - x), (c, 1 - x), (1 - c, x)]
    greet([(y * 2 + tc, z * 2 + tx) for tc, tx in others])
    copies = []
    for tc, tx in others:
        copies.append(wires.to(in_ref.at[tc * 2 + tx], out_ref.at[mine], y * 2 + tc, z * 2 + tx))
    for copy in copies:
        copy.start()
    local = pltpu.make_async_copy(in_ref.at[mine], out_ref.at[mine], local_sem)
    local.start()
    for copy in copies:
        copy.wait_recv()
    for copy in copies:
        copy.wait_send()
    local.wait()


def swap_call(value, ident):
    return pl.pallas_call(
        swap_kernel,
        out_shape=jax.ShapeDtypeStruct(value.shape, value.dtype),
        in_specs=[VMEM],
        out_specs=VMEM,
        scratch_shapes=[*wire_sems(3), pltpu.SemaphoreType.DMA],
        compiler_params=remote_params(ident),
        cost_estimate=cost(20),
        name="swap",
    )(value)


class QuadSum:
    step = 32

    def __init__(self, in_ref, out_ref, got_c, stage, got_x, send_sems, recv_sems):
        self.y, self.c, self.z, self.x = my_place()
        dp, cp = lax.axis_index("dp"), lax.axis_index("cp")
        wires = Wires(send_sems, recv_sems)
        self.in_ref, self.out_ref, self.got_c, self.stage, self.got_x = in_ref, out_ref, got_c, stage, got_x
        self.partners = [(dp + 1 - 2 * self.c, cp), (dp, cp + 1 - 2 * self.x)]
        self.by_c = wires.to(in_ref.at[1 - self.c], got_c, *self.partners[0])
        self.by_x = wires.to(stage, got_x, *self.partners[1])

    def each(self, act):
        def one(index, _):
            act(pl.ds(pl.multiple_of(index * self.step, self.step), self.step))
            return 0

        lax.fori_loop(0, self.out_ref.shape[0] // self.step, one, 0)

    def start(self):
        greet(self.partners)
        self.by_c.start()

    def middle(self):
        c, x = self.c, self.x
        self.by_c.wait_recv()

        def to_send(span):
            self.stage[span, :] = (
                self.in_ref[c, 1 - x, span, :].astype(jnp.float32) + self.got_c[1 - x, span, :].astype(jnp.float32)
            ).astype(self.stage.dtype)

        self.each(to_send)
        self.by_x.start()

    def finish(self):
        c, x = self.c, self.x
        self.by_x.wait_recv()

        def to_add(span):
            self.out_ref[span, :] = (
                self.in_ref[c, x, span, :].astype(jnp.float32)
                + self.got_c[x, span, :].astype(jnp.float32)
                + self.got_x[span, :].astype(jnp.float32)
            )

        self.each(to_add)
        self.by_c.wait_send()
        self.by_x.wait_send()


def quad_sum_kernel(*refs):
    quad = QuadSum(*refs)
    quad.start()
    quad.middle()
    quad.finish()


def quad_scratch(partial):
    rows, width = partial.shape[2:]
    return [
        pltpu.VMEM((2, rows, width), partial.dtype),
        pltpu.VMEM((rows, width), partial.dtype),
        pltpu.VMEM((rows, width), partial.dtype),
        *wire_sems(2),
    ]


def quad_sum(partial, ident):
    return pl.pallas_call(
        quad_sum_kernel,
        out_shape=jax.ShapeDtypeStruct(partial.shape[2:], jnp.float32),
        in_specs=[VMEM],
        out_specs=VMEM,
        scratch_shapes=quad_scratch(partial),
        compiler_params=remote_params(ident),
        cost_estimate=cost(30),
        name="quad_sum",
    )(partial)


def collect_kernel(sz, qkv_ref, out_ref, fc_ref, proj_ref, vec_ref, g_ref, vecs_ref, send_sems, recv_sem, vec_sems):
    y, c, z, x = my_place()
    me = flat_id(y, c, z, x)
    quarter = c * 2 + x
    share = y * 4 + z

    def send(ref, slot, table, sem):
        dest = table // sz.block
        mine = dest == me

        @pl.when(mine)
        def _():
            pltpu.make_async_copy(ref.at[slot], g_ref.at[table % sz.block], recv_sem).start()

        @pl.when(jnp.logical_not(mine))
        def _():
            pltpu.make_async_remote_copy(
                src_ref=ref.at[slot],
                dst_ref=g_ref.at[table % sz.block],
                send_sem=sem,
                recv_sem=recv_sem,
                device_id=(dest // 8, dest % 8),
                device_id_type=MESH,
            ).start()

    def sent(ref, slot, table, sem):
        @pl.when(table // sz.block != me)
        def _():
            pltpu.make_async_copy(ref.at[slot], ref.at[slot], sem).wait()

    def run(act):
        def headed(ref, size, base, first_sem):
            def one(slot, _):
                spot = share * size + slot
                part = spot // sz.part_grains
                local = quarter * sz.part_grains + spot % sz.part_grains

                @pl.when(local < sz.width_grains)
                def _():
                    act(ref, slot, base + part * sz.width_grains + local, send_sems.at[first_sem + slot])

                return 0

            lax.fori_loop(0, size, one, 0)

        def plain(ref, base, first_sem):
            def one(slot, _):
                table = base + (quarter * 8 + share) * sz.mlp + slot
                act(ref, slot, table, send_sems.at[first_sem + slot])
                return 0

            lax.fori_loop(0, sz.mlp, one, 0)

        headed(qkv_ref, sz.qkv, 0, 0)
        headed(out_ref, sz.out, sz.out_start, sz.qkv)
        plain(fc_ref, sz.fc_start, sz.qkv + sz.out)
        plain(proj_ref, sz.proj_start, sz.qkv + sz.out + sz.mlp)

    last = sz.vec_start // sz.block
    vec_copy = pltpu.make_async_remote_copy(
        src_ref=vec_ref,
        dst_ref=vecs_ref.at[me],
        send_sem=vec_sems.at[0],
        recv_sem=vec_sems.at[1],
        device_id=(last // 8, last % 8),
        device_id_type=MESH,
    )

    @pl.when(me != last)
    def _():
        vec_copy.start()

    @pl.when(me == last)
    def _():
        pltpu.make_async_copy(vec_ref, vecs_ref.at[me], vec_sems.at[1]).start()

    run(send)
    run(sent)

    @pl.when(me != last)
    def _():
        vec_copy.wait_send()

    @pl.when(me == last)
    def _():
        view = g_ref.at[pl.ds(0, sz.vec_start % sz.block)]
        pltpu.make_async_copy(view, view, recv_sem).wait()
        pltpu.make_async_copy(vecs_ref, vecs_ref, vec_sems.at[1]).wait()

    @pl.when(me != last)
    def _():
        pltpu.make_async_copy(g_ref, g_ref, recv_sem).wait()


def collect(sz, qkv, out, fc, proj, vectors):
    width = qkv.shape[-1]
    return pl.pallas_call(
        functools.partial(collect_kernel, sz),
        out_shape=(
            jax.ShapeDtypeStruct((sz.block, GRAIN, width), qkv.dtype),
            jax.ShapeDtypeStruct((32,) + vectors.shape, vectors.dtype),
        ),
        in_specs=[HBM] * 5,
        out_specs=[HBM] * 2,
        scratch_shapes=[
            pltpu.SemaphoreType.DMA((sz.qkv + sz.out + 2 * sz.mlp,)),
            pltpu.SemaphoreType.DMA,
            pltpu.SemaphoreType.DMA((2,)),
        ],
        compiler_params=REMOTE,
        name="collect",
    )(qkv, out, fc, proj, vectors)


def attend_kernel(heads, size, odd_ref, q_ref, kv_ref, before_ref, mix_ref, lse_ref):
    part = heads * size
    rows = q_ref.shape[0]
    blk = 128
    scale = size**-0.5
    lane = lax.broadcasted_iota(jnp.int32, (blk, rows), 1)
    line = lax.broadcasted_iota(jnp.int32, (blk, rows), 0)

    def block(index, _):
        first = pl.multiple_of(index * blk, blk)
        allowed = lane <= line + first

        def one(with_before):
            for h in range(heads):
                cols = slice(h * size, (h + 1) * size)
                vals = slice(part + h * size, part + (h + 1) * size)
                q = q_ref[pl.ds(first, blk), cols]
                s = dot_nt(q, kv_ref[:, cols]) * scale
                s = jnp.where(allowed, s, MASKED)
                top = jnp.max(s, axis=-1, keepdims=True)
                if with_before:
                    s_b = dot_nt(q, before_ref[:, cols]) * scale
                    top = jnp.maximum(top, jnp.max(s_b, axis=-1, keepdims=True))
                    p_b = jnp.exp(s_b - top)
                p = jnp.exp(s - top)
                total = jnp.sum(p, axis=-1, keepdims=True)
                mix = dot_nn(p.astype(jnp.bfloat16), kv_ref[:, vals])
                if with_before:
                    total = total + jnp.sum(p_b, axis=-1, keepdims=True)
                    mix = mix + dot_nn(p_b.astype(jnp.bfloat16), before_ref[:, vals])
                mix_ref[pl.ds(first, blk), cols] = mix / total
                lse_ref[pl.ds(first, blk), h : h + 1] = top + jnp.log(total)

        @pl.when(odd_ref[0] == 1)
        def _():
            one(True)

        @pl.when(odd_ref[0] == 0)
        def _():
            one(False)

        return 0

    lax.fori_loop(0, rows // blk, block, 0)


def attend(sz, odd, q, kv, before):
    rows = q.shape[0] // 2
    return pl.pallas_call(
        functools.partial(attend_kernel, sz.quarter_heads, sz.head_size),
        grid_spec=pltpu.PrefetchScalarGridSpec(
            num_scalar_prefetch=1,
            grid=(2,),
            in_specs=[
                pl.BlockSpec((rows, sz.part), lambda g, odd: (g, 0)),
                pl.BlockSpec((rows, 2 * sz.part), lambda g, odd: (g, 0)),
                pl.BlockSpec((rows, 2 * sz.part), lambda g, odd: (g, 0)),
            ],
            out_specs=[
                pl.BlockSpec((rows, sz.part), lambda g, odd: (g, 0)),
                pl.BlockSpec((rows, 8), lambda g, odd: (g, 0)),
            ],
        ),
        out_shape=(
            jax.ShapeDtypeStruct((2 * rows, sz.part), jnp.float32),
            jax.ShapeDtypeStruct((2 * rows, 8), jnp.float32),
        ),
        cost_estimate=pl.CostEstimate(
            flops=2 * 2 * 2 * rows * 2 * rows * sz.part,
            bytes_accessed=20 * rows * sz.part,
            transcendentals=4 * rows * rows * sz.quarter_heads,
        ),
        compiler_params=pltpu.CompilerParams(vmem_limit_bytes=40 << 20),
        name="attend",
    )(odd, q, kv, before)


def attend_back_kernel(heads, size, own, *refs):
    if own:
        q_ref, kv_ref, do_ref, mix_ref, lse_ref, seed_ref, term_ref, dq_ref, dkv_ref, sum_ref = refs[:10]
    else:
        q_ref, kv_ref, do_ref, mix_ref, lse_ref, term_ref, dq_ref, dkv_ref, sum_ref = refs[:9]
    quad = QuadSum(term_ref, sum_ref, *refs[-5:])
    quad.start()
    _, _, z, _ = my_place()
    part = heads * size
    rows = q_ref.shape[0] // 2
    blk = 128
    scale = size**-0.5
    lane = lax.broadcasted_iota(jnp.int32, (blk, rows), 1)
    line = lax.broadcasted_iota(jnp.int32, (blk, rows), 0)

    def group(start):
        keys_at = slice(start, start + rows)

        def block(index, _):
            first = pl.multiple_of(index * blk, blk)
            here = pl.ds(pl.multiple_of(start + first, blk), blk)
            if own:
                allowed = lane <= line + first
            for h in range(heads):
                cols = slice(h * size, (h + 1) * size)
                vals = slice(part + h * size, part + (h + 1) * size)
                q = q_ref[here, cols]
                k = kv_ref[keys_at, cols]
                do = do_ref[here, cols]
                s = dot_nt(q, k) * scale
                p = jnp.exp(s - lse_ref[here, h : h + 1])
                if own:
                    p = jnp.where(allowed, p, 0.0)
                dp = dot_nt(do, kv_ref[keys_at, vals])
                delta = jnp.sum(do.astype(jnp.float32) * mix_ref[here, cols], axis=-1, keepdims=True)
                ds = (p * (dp - delta)).astype(jnp.bfloat16)
                dq = dot_nn(ds, k) * scale
                if own:
                    dq = dq + seed_ref[here, cols]
                dq_ref[here, cols] = dq.astype(dq_ref.dtype)
                dkv_ref[keys_at, cols] += dot_tn(ds, q) * scale
                dkv_ref[keys_at, vals] += dot_tn(p.astype(jnp.bfloat16), do)
            return 0

        lax.fori_loop(0, rows // blk, block, 0)

    dkv_ref[...] = jnp.zeros_like(dkv_ref)
    if own:
        group(0)
        quad.middle()
        group(rows)
        quad.finish()
    else:
        odd = z % 2 == 1

        @pl.when(odd)
        def _():
            group(0)

        quad.middle()

        @pl.when(odd)
        def _():
            group(rows)

        @pl.when(jnp.logical_not(odd))
        def _():
            dq_ref[...] = jnp.zeros_like(dq_ref)

        quad.finish()


def attend_back(sz, own, q, kv, grad_mix, mix, lse, seed, term, ident):
    operands = [q, kv, grad_mix, mix, lse] + ([seed] if own else []) + [term]
    return pl.pallas_call(
        functools.partial(attend_back_kernel, sz.quarter_heads, sz.head_size, own),
        out_shape=(
            jax.ShapeDtypeStruct(q.shape, jnp.bfloat16 if own else jnp.float32),
            jax.ShapeDtypeStruct(kv.shape, jnp.float32),
            jax.ShapeDtypeStruct(term.shape[2:], jnp.float32),
        ),
        in_specs=[VMEM] * len(operands),
        out_specs=[VMEM] * 3,
        scratch_shapes=quad_scratch(term),
        cost_estimate=cost(35),
        compiler_params=remote_params(ident, 56 << 20),
        name="attend_back_own" if own else "attend_back_before",
    )(*operands)


def norm_parts(values):
    mean = jnp.mean(values, axis=-1, keepdims=True)
    centre = values - mean
    rs = lax.rsqrt(jnp.mean(centre * centre, axis=-1, keepdims=True) + EPSILON)
    return centre * rs, rs


def norm_back(normed, rs, grad, gain):
    e = grad * gain
    return rs * (
        e
        - jnp.mean(e, axis=-1, keepdims=True)
        - normed * jnp.mean(e * normed, axis=-1, keepdims=True)
    )


def per_device_quad(tokens, params, out_grad, lengths):
    rows, width = tokens.shape
    hidden = FF
    sz = Sizes(width, hidden, HEADS, HEAD_DIM, params.shape[0])
    y, c, z, x = my_place()
    quarter = c * 2 + x
    bf16, f32 = jnp.bfloat16, jnp.float32

    def pick(value, index):
        return lax.dynamic_index_in_dim(value, index, 0, keepdims=False)

    def halves_of(value):
        half = value.shape[1] // 2
        first, second = value[:, :half], value[:, half:]
        return jnp.where(y == 0, first, second), jnp.where(y == 0, second, first)

    def to_other_y(sent):
        return over_y(sent.astype(bf16))

    def to_places(kept, got):
        summed = kept + got.astype(f32)
        summed = summed.reshape(4, summed.shape[0] // 4, -1)
        total = pick(summed, z)
        for d in (1, 2, 3):
            got = over_z(pick(summed, (z + d) % 4).astype(bf16), d)
            total = total + got.astype(f32)
        return total

    w_qkv, w_out, w_fc, w_proj, vec, tok_all, cot_all = open_call(
        sz, params.reshape(sz.block, GRAIN, width), tokens, out_grad
    )
    flat = lambda value: value.reshape(-1, width)
    vectors = flat(vec).astype(f32)
    fc_bias = vectors[8 : 8 + hidden // width].reshape(hidden)
    w_qkv, cot_all = flat(w_qkv), flat(cot_all)
    normed_all, _ = norm_parts(flat(tok_all).astype(f32))
    act_one = (normed_all * vectors[0] + vectors[1]).astype(bf16)

    def quarter_of(vector):
        padded = jnp.pad(vector, (0, 4 * sz.part - width))
        return lax.dynamic_slice_in_dim(padded, quarter * sz.part, sz.part, 0)

    kv_bias = jnp.concatenate([jnp.zeros((sz.part,), f32), quarter_of(vectors[3])])
    kv = (dot_nt(act_one, w_qkv[sz.part :]) + kv_bias).astype(bf16)
    q = (dot_nt(act_one, w_qkv[: sz.part]) + quarter_of(vectors[2])).astype(bf16)
    before, _, w_fc, w_out = keys_call(kv, w_out, w_fc)
    w_fc, w_out = flat(w_fc), flat(w_out)[:width]
    odd = (z % 2).astype(jnp.int32).reshape(1)
    mix, lse = attend(sz, odd, q, kv, before)
    mixed = swap_call(mix.astype(bf16).reshape(4, rows, sz.part), 1)
    mixed = jnp.transpose(mixed, (1, 0, 2)).reshape(rows, 4 * sz.part)[:, :width]
    inputs = tokens.astype(f32)
    residual = inputs + (dot_nt(mixed, w_out) + vectors[4])
    normed_two, rs_two = norm_parts(residual)
    act_two, w_proj = acts_call((normed_two * vectors[5] + vectors[6]).astype(bf16), w_proj)
    act_two, w_proj = flat(act_two), flat(w_proj)
    bias = lax.dynamic_slice_in_dim(fc_bias, quarter * (hidden // 4), hidden // 4, 0)
    pre_act = dot_nt(act_two, w_fc) + bias
    act_hidden, pull_gelu = jax.vjp(gelu_tanh, pre_act)
    act_hidden = act_hidden.astype(bf16)
    hid_mine, hid_other = halves_of(act_hidden)
    got_proj = to_other_y(dot_tn(hid_other, cot_all))
    grad_fc = pull_gelu(dot_nt(cot_all, w_proj))[0].astype(bf16)
    fc_mine, fc_other = halves_of(grad_fc)
    got_fc = to_other_y(dot_tn(fc_other, act_two))
    grad_two = quad_sum(dot_nn(grad_fc, w_fc).astype(bf16).reshape(2, 2, rows, width), 2)

    cot = out_grad.astype(f32)
    grad_res = cot + norm_back(normed_two, rs_two, grad_two, vectors[5])
    grad_attn = grad_res.astype(bf16)
    grad_mix = dot_nn(grad_attn, w_out).astype(bf16)
    grad_mix = jnp.pad(grad_mix, ((0, 0), (0, 4 * sz.part - width)))
    grad_mix = jnp.transpose(grad_mix.reshape(rows, 4, sz.part), (1, 0, 2))
    grad_mix = swap_call(grad_mix, 3).reshape(4 * rows, sz.part)
    g_proj = to_places(dot_tn(hid_mine, cot_all), got_proj)
    g_out = jnp.pad(dot_tn(grad_attn, mixed).astype(bf16), ((0, 4 * sz.part - width), (0, 0)))
    dq_before, dkv_before, g_out = attend_back(
        sz, False, q, before, grad_mix, mix, lse, None, g_out.reshape(2, 2, sz.part, width), 4
    )
    returned = permute(
        dkv_before.astype(bf16), lambda py, pc, pz, px: (py, pc, pz - 1, px) if pz % 2 == 1 else None
    )
    g_fc = to_places(dot_tn(fc_mine, act_two), got_fc)
    g_out = g_out.reshape(2, sz.part // 2, width)
    got_out = to_other_y(pick(g_out, 1 - y))
    partial_out = dot_nn(act_hidden, w_proj).astype(bf16).reshape(2, 2, rows, width)
    dq, dkv, out_sum = attend_back(sz, True, q, kv, grad_mix, mix, lse, dq_before, partial_out, 5)
    output = (residual + out_sum + vectors[7]).astype(bf16)
    grad_qkv = jnp.concatenate([dq, (dkv + returned.astype(f32)).astype(bf16)], axis=1)
    qkv_mine, qkv_other = halves_of(grad_qkv)
    got_qkv = to_other_y(dot_tn(qkv_other, act_one))
    grad_one = quad_sum(dot_nn(grad_qkv, w_qkv).astype(bf16).reshape(2, 2, rows, width), 6)
    g_out = to_places(pick(g_out, y), got_out)
    g_qkv = to_places(dot_tn(qkv_mine, act_one), got_qkv)

    normed_one, rs_one = norm_parts(inputs)
    input_grad = (grad_res + norm_back(normed_one, rs_one, grad_one, vectors[0])).astype(bf16)

    def placed(vector):
        spot = lax.dynamic_update_slice_in_dim(jnp.zeros((4 * sz.part,), f32), vector, quarter * sz.part, 0)
        return spot[:width]

    sums = jnp.sum(grad_qkv.astype(f32), axis=0)
    bias_sum = jnp.sum(grad_fc.astype(f32), axis=0).reshape(1, hidden // 4)
    fc_rows = lax.dynamic_update_slice_in_dim(jnp.zeros((4, hidden // 4), f32), bias_sum, quarter, 0)
    grad_vectors = jnp.concatenate(
        [
            jnp.stack(
                [
                    jnp.sum(grad_one * normed_one, axis=0),
                    jnp.sum(grad_one, axis=0),
                    placed(sums[: sz.part]),
                    placed(sums[2 * sz.part :]),
                    jnp.sum(grad_attn.astype(f32), axis=0),
                    jnp.sum(grad_two * normed_two, axis=0),
                    jnp.sum(grad_two, axis=0),
                    jnp.sum(cot, axis=0),
                ]
            ),
            fc_rows.reshape(hidden // width, width),
        ]
    )
    count = grad_vectors.shape[0]
    grad_vectors = jnp.pad(grad_vectors, ((0, sz.vec * GRAIN - count), (0, 0)))
    grains = lambda value: value.astype(bf16).reshape(-1, GRAIN, width)
    table, all_vectors = collect(
        sz, grains(g_qkv), grains(g_out), grains(g_fc), grains(g_proj), grad_vectors.reshape(sz.vec, GRAIN, width)
    )
    grad_vectors = jnp.sum(all_vectors.reshape(32, sz.vec * GRAIN, width), axis=0)[:count]
    table = table.reshape(sz.block * GRAIN, width).astype(f32)
    used = (sz.vec_start % sz.block) * GRAIN
    tail = jnp.concatenate(
        [grad_vectors, jnp.zeros((sz.block * GRAIN - used - grad_vectors.shape[0], width), f32)]
    )
    last = flat_id(y, c, z, x) == sz.vec_start // sz.block
    tail = jnp.where(last, tail, table[used:])
    param_grad = jnp.concatenate([table[:used], tail])
    return (output, input_grad, param_grad)


def fits_quad(mesh, tokens, params, lengths):
    dp, cp = mesh.shape["dp"], mesh.shape["cp"]
    rows = tokens.shape[0] // (dp * cp)
    width = tokens.shape[1]
    blocks = params.shape[0] // (dp * cp)
    return (
        (dp, cp) == (4, 8)
        and lengths.shape[1] == 2
        and rows * cp == lengths.shape[1] * MIN_LEN
        and rows % 128 == 0
        and blocks % GRAIN == 0
        and (HEADS, HEAD_DIM, FF, width) == (25, 64, 6400, 1600)
    )


def solution(mesh):
    in_specs = (P(("dp", "cp"), None), P(("dp", "cp"), None), P(("dp", "cp"), None), P("dp", None))
    out_specs = (P(("dp", "cp"), None), P(("dp", "cp"), None), P(("dp", "cp"), None))

    def step(tokens, params, out_grad, lengths):
        body = per_device_quad if fits_quad(mesh, tokens, params, lengths) else per_device_general

        return jax.shard_map(
            body, mesh=mesh, in_specs=in_specs, out_specs=out_specs, check_vma=False
        )(tokens, params, out_grad, lengths)

    return step
```

```python
import functools

import jax
import jax.numpy as jnp
from jax import lax
from jax.experimental import pallas as pl
from jax.experimental.layout import Layout, with_layout_constraint
from jax.experimental.pallas import tpu as pltpu
from jax.sharding import PartitionSpec as P


HEADS = 25
FF = 6400
HEAD_DIM = 64
TILE = 128
MIN_LEN = 1024
MAX_LEN = 4096


EPSILON = 1e-05
MASKED = -1e30
GELU_SCALE = 0.7978845608028654


def from_behind(value, axis, by):
    length = lax.axis_size(axis)
    pairs = [(i, i + by) for i in range(length) if 0 <= i + by < length]
    return lax.ppermute(value, axis, pairs)


def layer_norm(values, gain_row, bias_row):
    centre = values - jnp.mean(values, axis=-1, keepdims=True)
    spread = jnp.mean(centre * centre, axis=-1, keepdims=True)
    return centre * lax.rsqrt(spread + EPSILON) * gain_row + bias_row


def gelu_tanh(values):
    return (
        0.5 * values * (1.0 + jnp.tanh(GELU_SCALE * (values + 0.044715 * values * values * values)))
    )


def segment_of(position, seq_ends):
    return jnp.sum((position[:, None] >= seq_ends[None, :]).astype(jnp.int32), axis=1)


def unpack(gathered, model_width, hidden):
    out_end = 4 * model_width
    fc_end = out_end + hidden
    proj_end = fc_end + hidden
    vec_end = proj_end + 8
    return (
        gathered[0 : 3 * model_width],
        gathered[3 * model_width : out_end],
        gathered[out_end:fc_end],
        gathered[fc_end:proj_end],
        gathered[proj_end:vec_end].astype(jnp.float32),
        gathered[vec_end : vec_end + hidden // model_width].astype(jnp.float32).reshape(hidden),
    )


def matmul_nt(left_mat, right_mat):
    return lax.dot_general(
        left_mat, right_mat, (((1,), (1,)), ((), ())), preferred_element_type=jnp.float32
    )


def matmul_tn(left_mat, right_mat):
    return lax.dot_general(
        left_mat, right_mat, (((0,), (0,)), ((), ())), preferred_element_type=jnp.float32
    )


def matmul_nn(left_mat, right_mat):
    return jnp.dot(left_mat, right_mat, preferred_element_type=jnp.float32)


def per_device_general(tokens, params, out_grad, lengths):
    tok_rows, model_width = tokens.shape
    hidden = FF
    head_count = HEADS
    head_size = HEAD_DIM
    cp_count = lax.axis_size("cp")
    group_rows = tok_rows * cp_count
    seq_count = lengths.shape[1]
    longest = min(MAX_LEN, group_rows - (seq_count - 1) * MIN_LEN)
    reach_back = min(cp_count - 1, (longest + tok_rows - TILE - 1) // tok_rows)
    pair_count = (reach_back + 2) // 2
    score_scale = head_size ** (-0.5)
    gathered = lax.all_gather(params, ("dp", "cp"), axis=0, tiled=True)
    w_attn, w_out, w_fc, w_proj, vectors, fc_bias = unpack(gathered, model_width, hidden)
    inputs = tokens.astype(jnp.float32)
    act_one = layer_norm(inputs, vectors[0], vectors[1]).astype(jnp.bfloat16)
    qkv_bias = jnp.concatenate([vectors[2], jnp.zeros_like(vectors[2]), vectors[3]])
    qkv = (matmul_nt(act_one, w_attn) + qkv_bias).astype(jnp.bfloat16)
    queries = qkv[:, :model_width].reshape(tok_rows, head_count, head_size)
    key_value = qkv[:, model_width:]
    device = lax.axis_index("cp")
    seq_ends = jnp.cumsum(lengths[0])
    query_pos = device * tok_rows + jnp.arange(tok_rows, dtype=jnp.int32)
    query_seg = segment_of(query_pos, seq_ends)
    store = jnp.zeros((2 * pair_count, tok_rows, 2 * model_width), jnp.bfloat16)
    store = store.at[0].set(key_value)

    def fetch(step_index, state_pair):
        moving, held_rows = state_pair
        moving = from_behind(moving, "cp", 1)
        return (moving, lax.dynamic_update_index_in_dim(held_rows, moving, step_index, 0))

    _, store = lax.fori_loop(1, reach_back + 1, fetch, (key_value, store))

    def pair_mask(pair_index):
        owners = 2 * pair_index + jnp.arange(2, dtype=jnp.int32)
        key_pos = (
            (device - owners)[:, None] * tok_rows + jnp.arange(tok_rows, dtype=jnp.int32)[None, :]
        ).reshape(2 * tok_rows)
        usable = jnp.broadcast_to((owners <= reach_back)[:, None], (2, tok_rows)).reshape(
            2 * tok_rows
        ) & (key_pos >= 0)
        key_seg = segment_of(key_pos, seq_ends)
        return (
            (key_seg[None, :] == query_seg[:, None])
            & (key_pos[None, :] <= query_pos[:, None])
            & usable[None, :]
        )

    def pair_rows(pair_index):
        block_rows = lax.dynamic_slice_in_dim(store, 2 * pair_index, 2, 0).reshape(
            2 * tok_rows, 2 * model_width
        )
        return (
            block_rows[:, :model_width].reshape(2 * tok_rows, head_count, head_size),
            block_rows[:, model_width:].reshape(2 * tok_rows, head_count, head_size),
        )

    def pair_scores(key_rows, allowed):
        raw_scores = (
            jnp.einsum("qhd,khd->hqk", queries, key_rows, preferred_element_type=jnp.float32)
            * score_scale
        )
        return jnp.where(allowed[None], raw_scores, MASKED)

    def visit(work):

        def step_pair(pair_index, running):
            allowed = pair_mask(pair_index)
            result = work(pair_index, allowed, running)
            return result

        return step_pair

    def add_total(pair_index, allowed, running):
        row_top, summed = running
        key_rows, _ = pair_rows(pair_index)
        scores = pair_scores(key_rows, allowed)
        new_top = jnp.maximum(row_top, jnp.max(scores, axis=-1, keepdims=True))
        summed = summed * jnp.exp(row_top - new_top) + jnp.sum(
            jnp.exp(scores - new_top), axis=-1, keepdims=True
        )
        return (new_top, summed)

    start_top = jnp.full((head_count, tok_rows, 1), MASKED, jnp.float32)
    start_sum = jnp.zeros((head_count, tok_rows, 1), jnp.float32)
    row_top, summed = lax.fori_loop(0, pair_count, visit(add_total), (start_top, start_sum))
    log_total = row_top + jnp.log(summed)

    def add_mix(pair_index, allowed, running):
        key_rows, value_rows = pair_rows(pair_index)
        prob_rows = jnp.exp(pair_scores(key_rows, allowed) - log_total).astype(jnp.bfloat16)
        return running + jnp.einsum(
            "hqk,khd->qhd", prob_rows, value_rows, preferred_element_type=jnp.float32
        )

    mixed_full = lax.fori_loop(
        0, pair_count, visit(add_mix), jnp.zeros((tok_rows, head_count, head_size), jnp.float32)
    )
    mixed = mixed_full.reshape(tok_rows, model_width).astype(jnp.bfloat16)
    attn_out = matmul_nt(mixed, w_out) + vectors[4]
    residual = inputs + attn_out
    act_two = layer_norm(residual, vectors[5], vectors[6]).astype(jnp.bfloat16)
    pre_act = matmul_nt(act_two, w_fc) + fc_bias
    act_hidden = gelu_tanh(pre_act).astype(jnp.bfloat16)
    output = (residual + matmul_nn(act_hidden, w_proj) + vectors[7]).astype(jnp.bfloat16)
    gathered = lax.all_gather(params, ("dp", "cp"), axis=0, tiled=True)
    w_attn, w_out, w_fc, w_proj, vectors, fc_bias = unpack(gathered, model_width, hidden)
    grad_out_f = out_grad.astype(jnp.float32)
    grad_hidden = matmul_nt(out_grad, w_proj)
    _, pull_gelu = jax.vjp(gelu_tanh, pre_act)
    grad_fc = pull_gelu(grad_hidden)[0].astype(jnp.bfloat16)
    grad_act_two = matmul_nn(grad_fc, w_fc)
    _, pull_two = jax.vjp(layer_norm, residual, vectors[5], vectors[6])
    grad_res_norm, grad_gain_two, grad_bias_two = pull_two(grad_act_two)
    grad_res = grad_out_f + grad_res_norm
    grad_attn = grad_res.astype(jnp.bfloat16)
    grad_mix = (
        matmul_nn(grad_attn, w_out).astype(jnp.bfloat16).reshape(tok_rows, head_count, head_size)
    )
    grad_dot = jnp.transpose(jnp.sum(grad_mix.astype(jnp.float32) * mixed_full, axis=-1), (1, 0))[
        :, :, None
    ]

    def add_grads(pair_index, allowed, running):
        grad_query, grad_store = running
        key_rows, value_rows = pair_rows(pair_index)
        prob_rows = jnp.exp(pair_scores(key_rows, allowed) - log_total)
        grad_probs = jnp.einsum(
            "qhd,khd->hqk", grad_mix, value_rows, preferred_element_type=jnp.float32
        )
        grad_scores = (prob_rows * (grad_probs - grad_dot)).astype(jnp.bfloat16)
        grad_query = (
            grad_query
            + jnp.einsum("hqk,khd->qhd", grad_scores, key_rows, preferred_element_type=jnp.float32)
            * score_scale
        )
        grad_keys = (
            jnp.einsum("hqk,qhd->khd", grad_scores, queries, preferred_element_type=jnp.float32)
            * score_scale
        )
        grad_values = jnp.einsum(
            "hqk,qhd->khd",
            prob_rows.astype(jnp.bfloat16),
            grad_mix,
            preferred_element_type=jnp.float32,
        )
        pair_grad = jnp.concatenate(
            [
                grad_keys.reshape(2 * tok_rows, model_width),
                grad_values.reshape(2 * tok_rows, model_width),
            ],
            axis=1,
        )
        pair_grad = pair_grad.reshape(2, tok_rows, 2 * model_width)
        grad_store = lax.dynamic_update_slice_in_dim(grad_store, pair_grad, 2 * pair_index, 0)
        return (grad_query, grad_store)

    start_query = jnp.zeros((tok_rows, head_count, head_size), jnp.float32)
    start_store = jnp.zeros((2 * pair_count, tok_rows, 2 * model_width), jnp.float32)
    grad_query, grad_store = lax.fori_loop(
        0, pair_count, visit(add_grads), (start_query, start_store)
    )

    def send_back(step_index, moving):
        moving = moving + lax.dynamic_index_in_dim(
            grad_store, reach_back - step_index, 0, keepdims=False
        )
        return from_behind(moving.astype(jnp.bfloat16), "cp", -1).astype(moving.dtype)

    returned = lax.fori_loop(
        0, reach_back, send_back, jnp.zeros((tok_rows, 2 * model_width), jnp.float32)
    )
    grad_kv = returned + grad_store[0]
    grad_qkv = jnp.concatenate([grad_query.reshape(tok_rows, model_width), grad_kv], axis=1).astype(
        jnp.bfloat16
    )
    grad_qkv_f = grad_qkv.astype(jnp.float32)
    grad_act_one = matmul_nn(grad_qkv, w_attn)
    _, pull_one = jax.vjp(layer_norm, inputs, vectors[0], vectors[1])
    grad_in_norm, grad_gain_one, grad_bias_one = pull_one(grad_act_one)
    input_grad = (grad_res + grad_in_norm).astype(jnp.bfloat16)
    grad_vectors = jnp.stack(
        [
            grad_gain_one,
            grad_bias_one,
            jnp.sum(grad_qkv_f[:, :model_width], axis=0),
            jnp.sum(grad_qkv_f[:, 2 * model_width :], axis=0),
            jnp.sum(grad_attn.astype(jnp.float32), axis=0),
            grad_gain_two,
            grad_bias_two,
            jnp.sum(grad_out_f, axis=0),
        ]
    )
    grad_fc_bias = jnp.sum(grad_fc.astype(jnp.float32), axis=0).reshape(
        hidden // model_width, model_width
    )
    used_rows = 4 * model_width + 2 * hidden + 8 + hidden // model_width
    total_rows = gathered.shape[0]
    local_grad = jnp.concatenate(
        [
            matmul_tn(grad_qkv, act_one),
            matmul_tn(grad_attn, mixed),
            matmul_tn(grad_fc, act_two),
            matmul_tn(act_hidden, out_grad),
            grad_vectors,
            grad_fc_bias,
            jnp.zeros((total_rows - used_rows, model_width), jnp.float32),
        ],
        axis=0,
    )
    dp_count = lax.axis_size("dp")
    device_count = dp_count * cp_count
    share_rows = total_rows // device_count
    spread_rows = local_grad.reshape(device_count, 1, share_rows, model_width)
    received = lax.all_to_all(
        spread_rows.astype(jnp.bfloat16), ("dp", "cp"), split_axis=0, concat_axis=1, tiled=True
    ).astype(spread_rows.dtype)
    param_grad = jnp.sum(received, axis=1).reshape(share_rows, model_width)
    return (output, input_grad, param_grad)


MESH = pl.DeviceIdType.MESH
GRAIN = 8
NT = (((1,), (1,)), ((), ()))
TN = (((0,), (0,)), ((), ()))


def dot_nt(a, b):
    return lax.dot_general(a, b, NT, preferred_element_type=jnp.float32)


def dot_tn(a, b):
    return lax.dot_general(a, b, TN, preferred_element_type=jnp.float32)


def dot_nn(a, b):
    return jnp.dot(a, b, preferred_element_type=jnp.float32)


def flat_id(y, c, z, x):
    return ((y * 2 + c) * 4 + z) * 2 + x


def permute(value, move):
    pairs = []
    for y in range(2):
        for c in range(2):
            for z in range(4):
                for x in range(2):
                    to = move(y, c, z, x)
                    if to is not None:
                        pairs.append((flat_id(y, c, z, x), flat_id(*to)))
    return lax.ppermute(value, ("dp", "cp"), pairs)


def over_y(value):
    return permute(value, lambda y, c, z, x: (1 - y, c, z, x))


def over_z(value, by):
    return permute(value, lambda y, c, z, x: (y, c, (z + by) % 4, x))


class Sizes:
    def __init__(self, width, hidden, heads, head_size, rows):
        self.head_size = head_size
        self.quarter_heads = -(-heads // 4)
        self.part = self.quarter_heads * head_size
        self.part_grains = self.part // GRAIN
        self.width_grains = width // GRAIN
        self.spill = 4 * self.part_grains - self.width_grains
        self.qkv = 3 * self.part_grains // 8
        self.out = self.part_grains // 8
        self.mlp = hidden // 4 // 8 // GRAIN
        self.block = rows // GRAIN
        self.out_start = 3 * self.width_grains
        self.fc_start = 4 * self.width_grains
        self.proj_start = self.fc_start + hidden // GRAIN
        self.vec_start = self.proj_start + hidden // GRAIN
        self.vec = 2


def my_place():
    dp = lax.axis_index("dp")
    cp = lax.axis_index("cp")
    return dp // 2, dp % 2, cp // 2, cp % 2


def place_of(quarter, share):
    return (share // 4) * 2 + quarter // 2, (share % 4) * 2 + quarter % 2


class Wires:
    def __init__(self, send_sems, recv_sems):
        self.send_sems = send_sems
        self.recv_sems = recv_sems
        self.count = 0

    def to(self, src, dst, dp, cp):
        index = self.count
        self.count += 1
        return pltpu.make_async_remote_copy(
            src_ref=src,
            dst_ref=dst,
            send_sem=self.send_sems.at[index],
            recv_sem=self.recv_sems.at[index],
            device_id=(dp, cp),
            device_id_type=MESH,
        )


class PlaceGather:
    def __init__(self, wires, full):
        self.wires = wires
        self.full = full
        self.dp, self.cp = lax.axis_index("dp"), lax.axis_index("cp")
        self.y, self.z, self.x = self.dp // 2, self.cp // 2, self.cp % 2
        self.started = []

    def send(self, slot, dp, cp):
        view = self.full.at[slot]
        copy = self.wires.to(view, view, dp, cp)
        copy.start()
        self.started.append(copy)
        return copy

    def partners(self):
        along = [(self.dp, ((self.z + d) % 4) * 2 + self.x) for d in (1, 2, 3)]
        return along + [((self.dp + 2) % 4, self.cp)]

    def start_over(self):
        self.over = [self.send(self.y * 4 + self.z, (self.dp + 2) % 4, self.cp)]

    def start(self, over=True):
        mine = self.y * 4 + self.z
        self.along = []
        for d in (1, 3, 2):
            self.along.append((d, self.send(mine, self.dp, ((self.z + d) % 4) * 2 + self.x)))
        self.over = []
        if over:
            self.start_over()

    def forward(self):
        for d, copy in self.along:
            copy.wait_recv()
            self.over.append(self.send(self.y * 4 + (self.z - d + 4) % 4, (self.dp + 2) % 4, self.cp))

    def finish(self):
        for copy in self.over:
            copy.wait_recv()
        for copy in self.started:
            copy.wait_send()


class QuadGather:
    def __init__(self, wires, block, full, local_sem):
        self.wires = wires
        self.block = block
        self.full = full
        self.dp, self.cp = lax.axis_index("dp"), lax.axis_index("cp")
        self.c, self.x = self.dp % 2, self.cp % 2
        self.over_x = (self.dp, self.cp + 1 - 2 * self.x)
        self.over_c = (self.dp + 1 - 2 * self.c, self.cp)
        self.local_sem = local_sem

    def start(self):
        spot = self.full.at[self.c, self.x]
        self.by_x = self.wires.to(self.block, spot, *self.over_x)
        self.by_c = self.wires.to(self.block, spot, *self.over_c)
        self.by_x.start()
        self.by_c.start()
        self.local = pltpu.make_async_copy(self.block, spot, self.local_sem)
        self.local.start()

    def forward(self):
        self.by_x.wait_recv()
        spot = self.full.at[self.c, 1 - self.x]
        self.pass_on = self.wires.to(spot, spot, *self.over_c)
        self.pass_on.start()

    def finish(self):
        self.by_c.wait_recv()
        self.pass_on.wait_recv()
        self.by_x.wait_send()
        self.by_c.wait_send()
        self.pass_on.wait_send()
        self.local.wait()


def open_kernel(
    sz, p_ref, tok_ref, cot_ref, qkv_ref, out_ref, fc_ref, proj_ref, vec_ref, tok_all, cot_all,
    spread_sems, kind_sems, send_sems, recv_sems, local_sems,
):
    y, c, z, x = my_place()
    me = flat_id(y, c, z, x)
    wires = Wires(send_sems, recv_sems)
    tok = QuadGather(wires, tok_ref, tok_all, local_sems.at[0])
    cot = QuadGather(wires, cot_ref, cot_all, local_sems.at[1])

    def send(grain, ref, slot, quarter, share, sem, recv):
        dp, cp = place_of(quarter, share)
        mine = dp * 8 + cp == me

        @pl.when(mine)
        def _():
            pltpu.make_async_copy(p_ref.at[grain], ref.at[share, slot], recv).start()

        @pl.when(jnp.logical_not(mine))
        def _():
            pltpu.make_async_remote_copy(
                src_ref=p_ref.at[grain],
                dst_ref=ref.at[share, slot],
                send_sem=sem,
                recv_sem=recv,
                device_id=(dp, cp),
                device_id_type=MESH,
            ).start()

    def sent(grain, ref, slot, quarter, share, sem, recv):
        dp, cp = place_of(quarter, share)

        @pl.when(dp * 8 + cp != me)
        def _():
            pltpu.make_async_copy(p_ref.at[grain], p_ref.at[grain], sem).wait()

    def headed(act, grain, base, parts, ref, recv, share_size):
        offset = me * sz.block + grain - base
        part = offset // sz.width_grains
        local = offset % sz.width_grains

        def one(quarter, inner, sem):
            spot = part * sz.part_grains + inner
            act(grain, ref, spot % share_size, quarter, spot // share_size, sem, recv)

        @pl.when(jnp.logical_and(offset >= 0, offset < parts * sz.width_grains))
        def _():
            one(local // sz.part_grains, local % sz.part_grains, spread_sems.at[grain])

            @pl.when(local < sz.spill)
            def _():
                one(3, sz.part_grains - sz.spill + local, spread_sems.at[sz.block + grain])

    def plain(act, grain, base, ref, recv):
        offset = me * sz.block + grain - base

        @pl.when(jnp.logical_and(offset >= 0, offset < 32 * sz.mlp))
        def _():
            act(
                grain, ref, offset % sz.mlp, offset // (8 * sz.mlp), (offset // sz.mlp) % 8,
                spread_sems.at[grain], recv,
            )

    def heads(act):
        def one(grain, _):
            headed(act, grain, 0, 3, qkv_ref, kind_sems.at[0], sz.qkv)
            return 0

        lax.fori_loop(0, sz.block, one, 0)

    def others(act):
        def one(grain, _):
            headed(act, grain, sz.out_start, 1, out_ref, kind_sems.at[1], sz.out)
            plain(act, grain, sz.fc_start, fc_ref, kind_sems.at[2])
            plain(act, grain, sz.proj_start, proj_ref, kind_sems.at[3])
            return 0

        lax.fori_loop(0, sz.block, one, 0)

    owner = sz.vec_start // sz.block
    spot = sz.vec_start % sz.block

    def vector_sends(act):
        @pl.when(me == owner)
        def _():
            def to(device, _):
                @pl.when(device != me)
                def _():
                    act(
                        pltpu.make_async_remote_copy(
                            src_ref=p_ref.at[pl.ds(spot, sz.vec)],
                            dst_ref=vec_ref,
                            send_sem=spread_sems.at[2 * sz.block + device],
                            recv_sem=kind_sems.at[4],
                            device_id=(device // 8, device % 8),
                            device_id_type=MESH,
                        )
                    )

                return 0

            lax.fori_loop(0, 32, to, 0)

    heads(send)
    tok.start()
    cot.start()
    mine = y * 4 + z
    pltpu.make_async_copy(qkv_ref.at[mine], qkv_ref.at[mine], kind_sems.at[0]).wait()
    weights = PlaceGather(wires, qkv_ref)
    weights.start()
    others(send)
    vector_sends(lambda copy: copy.start())

    @pl.when(me == owner)
    def _():
        pltpu.make_async_copy(p_ref.at[pl.ds(spot, sz.vec)], vec_ref, kind_sems.at[4]).start()

    weights.forward()
    tok.forward()
    cot.forward()
    heads(sent)
    others(sent)
    vector_sends(lambda copy: copy.wait_send())
    for index, ref in enumerate((out_ref, fc_ref, proj_ref)):
        pltpu.make_async_copy(ref.at[mine], ref.at[mine], kind_sems.at[index + 1]).wait()
    pltpu.make_async_copy(vec_ref, vec_ref, kind_sems.at[4]).wait()
    tok.finish()
    cot.finish()
    weights.finish()


HBM = pl.BlockSpec(memory_space=pl.ANY)
VMEM = pl.BlockSpec(memory_space=pltpu.VMEM)
REMOTE = pltpu.CompilerParams(has_side_effects=True)


def remote_params(ident=None, vmem=None):
    return pltpu.CompilerParams(has_side_effects=True, collective_id=ident, vmem_limit_bytes=vmem)


def greet(partners):
    barrier = pltpu.get_barrier_semaphore()
    for dp, cp in partners:
        pl.semaphore_signal(barrier, inc=1, device_id=(dp, cp), device_id_type=MESH)
    pl.semaphore_wait(barrier, len(partners))


def cost(us):
    return pl.CostEstimate(flops=0, bytes_accessed=int(us * 3.0e6), transcendentals=0)


def wire_sems(count):
    return [pltpu.SemaphoreType.DMA((count,)), pltpu.SemaphoreType.DMA((count,))]


def open_call(sz, table, tokens, cotangent):
    rows, width = tokens.shape

    def like(*shape):
        return jax.ShapeDtypeStruct(shape + (width,), table.dtype)

    return pl.pallas_call(
        functools.partial(open_kernel, sz),
        out_shape=(
            like(8, sz.qkv, GRAIN),
            like(8, sz.out, GRAIN),
            like(8, sz.mlp, GRAIN),
            like(8, sz.mlp, GRAIN),
            like(sz.vec, GRAIN),
            like(2, 2, rows),
            like(2, 2, rows),
        ),
        in_specs=[HBM, VMEM, VMEM],
        out_specs=[HBM] * 7,
        scratch_shapes=[
            pltpu.SemaphoreType.DMA((2 * sz.block + 32,)),
            pltpu.SemaphoreType.DMA((5,)),
            *wire_sems(13),
            pltpu.SemaphoreType.DMA((2,)),
        ],
        compiler_params=REMOTE,
        name="open",
    )(table, tokens, cotangent)


def forward_kernel(
    heads, size, q_ref, kv_ref, out_in, fc_in, proj_in,
    mix_ref, lse_ref, before_ref, mixed_ref, out_ref, fc_ref, proj_ref, out_all,
    stage, send_sems, recv_sems, local_sems,
):
    y, c, z, x = my_place()
    dp, cp = lax.axis_index("dp"), lax.axis_index("cp")
    wires = Wires(send_sems, recv_sems)
    part = heads * size
    rows = q_ref.shape[0] // 2
    blk = 128
    scale = size**-0.5
    odd = z % 2 == 1
    w_out, w_fc, w_proj = [PlaceGather(wires, ref) for ref in (out_ref, fc_ref, proj_ref)]
    others = [(c, 1 - x), (1 - c, x), (1 - c, 1 - x)]
    quad = [(y * 2 + tc, z * 2 + tx) for tc, tx in others]
    greet(w_out.partners() + quad)
    keys = wires.to(kv_ref, before_ref, dp, (cp + 2) % 8)

    @pl.when(jnp.logical_not(odd))
    def _():
        keys.start()

    w_out.start()
    w_fc.start()

    def own(group, _):
        start = group * rows
        for i in range(rows // blk):
            here = pl.ds(pl.multiple_of(start + i * blk, blk), blk)
            seen = (i + 1) * blk
            keys_at = pl.ds(pl.multiple_of(start, rows), seen)
            lane = lax.broadcasted_iota(jnp.int32, (blk, seen), 1)
            line = lax.broadcasted_iota(jnp.int32, (blk, seen), 0)
            allowed = lane <= line + i * blk
            for h in range(heads):
                cols = slice(h * size, (h + 1) * size)
                vals = slice(part + h * size, part + (h + 1) * size)
                s = dot_nt(q_ref[here, cols], kv_ref[keys_at, cols]) * scale
                s = jnp.where(allowed, s, MASKED)
                top = jnp.max(s, axis=-1, keepdims=True)
                p = jnp.exp(s - top)
                total = jnp.sum(p, axis=-1, keepdims=True)
                mix_ref[here, cols] = dot_nn(p.astype(jnp.bfloat16), kv_ref[keys_at, vals]) / total
                lse_ref[here, h : h + 1] = top + jnp.log(total)
        return 0

    lax.fori_loop(0, 2, own, 0)
    w_out.forward()

    def add_before(index, _):
        here = pl.ds(pl.multiple_of(index * blk, blk), blk)
        keys_at = pl.ds(pl.multiple_of((index * blk) // rows * rows, rows), rows)
        for h in range(heads):
            cols = slice(h * size, (h + 1) * size)
            vals = slice(part + h * size, part + (h + 1) * size)
            s = dot_nt(q_ref[here, cols], before_ref[keys_at, cols]) * scale
            lse = lse_ref[here, h : h + 1]
            top = jnp.maximum(lse, jnp.max(s, axis=-1, keepdims=True))
            p = jnp.exp(s - top)
            kept = jnp.exp(lse - top)
            total = kept + jnp.sum(p, axis=-1, keepdims=True)
            mix = mix_ref[here, cols] * kept + dot_nn(p.astype(jnp.bfloat16), before_ref[keys_at, vals])
            mix_ref[here, cols] = mix / total
            lse_ref[here, h : h + 1] = top + jnp.log(total)
        return 0

    w_out.finish()
    whole = QuadGather(wires, out_ref, out_all, local_sems.at[0])
    whole.start()

    @pl.when(odd)
    def _():
        keys.wait_recv()
        lax.fori_loop(0, 2 * rows // blk, add_before, 0)

    def round_off(index, _):
        here = pl.ds(pl.multiple_of(index * blk, blk), blk)
        stage[here, :] = mix_ref[here, :].astype(stage.dtype)
        return 0

    lax.fori_loop(0, 2 * rows // blk, round_off, 0)
    w_proj.start_over()
    mine = c * 2 + x
    each = rows // 2
    swaps = []
    for (tc, tx), (tdp, tcp) in zip(others, quad):
        block = stage.at[pl.ds(pl.multiple_of((tc * 2 + tx) * each, each), each)]
        swaps.append(wires.to(block, mixed_ref.at[mine], tdp, tcp))
    for copy in swaps:
        copy.start()
    local = pltpu.make_async_copy(
        stage.at[pl.ds(pl.multiple_of(mine * each, each), each)], mixed_ref.at[mine], local_sems.at[1]
    )
    local.start()
    w_fc.forward()
    whole.forward()
    for copy in swaps:
        copy.wait_recv()
    whole.finish()
    w_fc.finish()
    w_proj.over[0].wait_recv()
    w_proj.over[0].wait_send()
    for copy in swaps:
        copy.wait_send()
    local.wait()

    @pl.when(jnp.logical_not(odd))
    def _():
        keys.wait_send()


def forward_call(sz, q, kv, w_out, w_fc, w_proj):
    part = sz.part
    rows = q.shape[0]

    def like(value, *lead):
        return jax.ShapeDtypeStruct(lead + value.shape, value.dtype)

    return pl.pallas_call(
        functools.partial(forward_kernel, sz.quarter_heads, sz.head_size),
        out_shape=(
            jax.ShapeDtypeStruct((rows, part), jnp.float32),
            jax.ShapeDtypeStruct((rows, 8), jnp.float32),
            like(kv),
            jax.ShapeDtypeStruct((4, rows // 4, part), jnp.bfloat16),
            like(w_out),
            like(w_fc),
            like(w_proj),
            like(w_out, 2, 2),
        ),
        in_specs=[VMEM, VMEM, HBM, HBM, HBM],
        out_specs=[VMEM] * 4 + [HBM] * 4,
        input_output_aliases={2: 4, 3: 5, 4: 6},
        scratch_shapes=[
            pltpu.VMEM((rows, part), jnp.bfloat16),
            *wire_sems(22),
            pltpu.SemaphoreType.DMA((2,)),
        ],
        cost_estimate=cost(120),
        compiler_params=remote_params(1, 56 << 20),
        name="forward",
    )(q, kv, w_out, w_fc, w_proj)


def acts_kernel(act_ref, proj_in, act_all, proj_ref, send_sems, recv_sems, local_sem):
    wires = Wires(send_sems, recv_sems)
    quad = QuadGather(wires, act_ref, act_all, local_sem)
    places = PlaceGather(wires, proj_ref)
    greet(places.partners() + [quad.over_x, quad.over_c])
    quad.start()
    places.start(False)
    quad.forward()
    places.forward()
    quad.finish()
    places.finish()


def acts_call(act, w_proj):
    return pl.pallas_call(
        acts_kernel,
        out_shape=(
            jax.ShapeDtypeStruct((2, 2) + act.shape, act.dtype),
            jax.ShapeDtypeStruct(w_proj.shape, w_proj.dtype),
        ),
        in_specs=[VMEM, HBM],
        out_specs=[HBM] * 2,
        input_output_aliases={1: 1},
        scratch_shapes=[*wire_sems(9), pltpu.SemaphoreType.DMA],
        cost_estimate=cost(60),
        compiler_params=remote_params(2),
        name="acts",
    )(act, w_proj)


def swap_kernel(in_ref, out_ref, send_sems, recv_sems, local_sem):
    y, c, z, x = my_place()
    wires = Wires(send_sems, recv_sems)
    mine = c * 2 + x
    others = [(1 - c, 1 - x), (c, 1 - x), (1 - c, x)]
    greet([(y * 2 + tc, z * 2 + tx) for tc, tx in others])
    copies = []
    for tc, tx in others:
        copies.append(wires.to(in_ref.at[tc * 2 + tx], out_ref.at[mine], y * 2 + tc, z * 2 + tx))
    for copy in copies:
        copy.start()
    local = pltpu.make_async_copy(in_ref.at[mine], out_ref.at[mine], local_sem)
    local.start()
    for copy in copies:
        copy.wait_recv()
    for copy in copies:
        copy.wait_send()
    local.wait()


def swap_call(value, ident):
    return pl.pallas_call(
        swap_kernel,
        out_shape=jax.ShapeDtypeStruct(value.shape, value.dtype),
        in_specs=[VMEM],
        out_specs=VMEM,
        scratch_shapes=[*wire_sems(3), pltpu.SemaphoreType.DMA],
        compiler_params=remote_params(ident),
        cost_estimate=cost(20),
        name="swap",
    )(value)


class QuadSum:
    step = 32

    def __init__(self, in_ref, out_ref, got_c, stage, got_x, send_sems, recv_sems):
        self.y, self.c, self.z, self.x = my_place()
        dp, cp = lax.axis_index("dp"), lax.axis_index("cp")
        wires = Wires(send_sems, recv_sems)
        self.in_ref, self.out_ref, self.got_c, self.stage, self.got_x = in_ref, out_ref, got_c, stage, got_x
        self.partners = [(dp + 1 - 2 * self.c, cp), (dp, cp + 1 - 2 * self.x)]
        self.by_c = wires.to(in_ref.at[1 - self.c], got_c, *self.partners[0])
        self.by_x = wires.to(stage, got_x, *self.partners[1])

    def each(self, act):
        def one(index, _):
            act(pl.ds(pl.multiple_of(index * self.step, self.step), self.step))
            return 0

        lax.fori_loop(0, self.out_ref.shape[0] // self.step, one, 0)

    def start(self):
        greet(self.partners)
        self.by_c.start()

    def middle(self):
        c, x = self.c, self.x
        self.by_c.wait_recv()

        def to_send(span):
            self.stage[span, :] = (
                self.in_ref[c, 1 - x, span, :].astype(jnp.float32) + self.got_c[1 - x, span, :].astype(jnp.float32)
            ).astype(self.stage.dtype)

        self.each(to_send)
        self.by_x.start()

    def finish(self):
        c, x = self.c, self.x
        self.by_x.wait_recv()

        def to_add(span):
            self.out_ref[span, :] = (
                self.in_ref[c, x, span, :].astype(jnp.float32)
                + self.got_c[x, span, :].astype(jnp.float32)
                + self.got_x[span, :].astype(jnp.float32)
            )

        self.each(to_add)
        self.by_c.wait_send()
        self.by_x.wait_send()


def quad_sum_kernel(*refs):
    quad = QuadSum(*refs)
    quad.start()
    quad.middle()
    quad.finish()


def quad_scratch(partial):
    rows, width = partial.shape[2:]
    return [
        pltpu.VMEM((2, rows, width), partial.dtype),
        pltpu.VMEM((rows, width), partial.dtype),
        pltpu.VMEM((rows, width), partial.dtype),
        *wire_sems(2),
    ]


def quad_sum(partial, ident):
    return pl.pallas_call(
        quad_sum_kernel,
        out_shape=jax.ShapeDtypeStruct(partial.shape[2:], jnp.float32),
        in_specs=[VMEM],
        out_specs=VMEM,
        scratch_shapes=quad_scratch(partial),
        compiler_params=remote_params(ident),
        cost_estimate=cost(30),
        name="quad_sum",
    )(partial)


def collect_kernel(sz, qkv_ref, out_ref, fc_ref, proj_ref, vec_ref, g_ref, vecs_ref, send_sems, recv_sem, vec_sems):
    y, c, z, x = my_place()
    me = flat_id(y, c, z, x)
    quarter = c * 2 + x
    share = y * 4 + z

    def send(ref, slot, table, sem):
        dest = table // sz.block
        mine = dest == me

        @pl.when(mine)
        def _():
            pltpu.make_async_copy(ref.at[slot], g_ref.at[table % sz.block], recv_sem).start()

        @pl.when(jnp.logical_not(mine))
        def _():
            pltpu.make_async_remote_copy(
                src_ref=ref.at[slot],
                dst_ref=g_ref.at[table % sz.block],
                send_sem=sem,
                recv_sem=recv_sem,
                device_id=(dest // 8, dest % 8),
                device_id_type=MESH,
            ).start()

    def sent(ref, slot, table, sem):
        @pl.when(table // sz.block != me)
        def _():
            pltpu.make_async_copy(ref.at[slot], ref.at[slot], sem).wait()

    def run(act):
        def headed(ref, size, base, first_sem):
            def one(slot, _):
                spot = share * size + slot
                part = spot // sz.part_grains
                local = quarter * sz.part_grains + spot % sz.part_grains

                @pl.when(local < sz.width_grains)
                def _():
                    act(ref, slot, base + part * sz.width_grains + local, send_sems.at[first_sem + slot])

                return 0

            lax.fori_loop(0, size, one, 0)

        def plain(ref, base, first_sem):
            def one(slot, _):
                table = base + (quarter * 8 + share) * sz.mlp + slot
                act(ref, slot, table, send_sems.at[first_sem + slot])
                return 0

            lax.fori_loop(0, sz.mlp, one, 0)

        headed(qkv_ref, sz.qkv, 0, 0)
        headed(out_ref, sz.out, sz.out_start, sz.qkv)
        plain(fc_ref, sz.fc_start, sz.qkv + sz.out)
        plain(proj_ref, sz.proj_start, sz.qkv + sz.out + sz.mlp)

    last = sz.vec_start // sz.block
    vec_copy = pltpu.make_async_remote_copy(
        src_ref=vec_ref,
        dst_ref=vecs_ref.at[me],
        send_sem=vec_sems.at[0],
        recv_sem=vec_sems.at[1],
        device_id=(last // 8, last % 8),
        device_id_type=MESH,
    )

    @pl.when(me != last)
    def _():
        vec_copy.start()

    @pl.when(me == last)
    def _():
        pltpu.make_async_copy(vec_ref, vecs_ref.at[me], vec_sems.at[1]).start()

    run(send)
    run(sent)

    @pl.when(me != last)
    def _():
        vec_copy.wait_send()

    @pl.when(me == last)
    def _():
        view = g_ref.at[pl.ds(0, sz.vec_start % sz.block)]
        pltpu.make_async_copy(view, view, recv_sem).wait()
        pltpu.make_async_copy(vecs_ref, vecs_ref, vec_sems.at[1]).wait()

    @pl.when(me != last)
    def _():
        pltpu.make_async_copy(g_ref, g_ref, recv_sem).wait()


def collect(sz, qkv, out, fc, proj, vectors):
    width = qkv.shape[-1]
    return pl.pallas_call(
        functools.partial(collect_kernel, sz),
        out_shape=(
            jax.ShapeDtypeStruct((sz.block, GRAIN, width), qkv.dtype),
            jax.ShapeDtypeStruct((32,) + vectors.shape, vectors.dtype),
        ),
        in_specs=[HBM] * 5,
        out_specs=[HBM] * 2,
        scratch_shapes=[
            pltpu.SemaphoreType.DMA((sz.qkv + sz.out + 2 * sz.mlp,)),
            pltpu.SemaphoreType.DMA,
            pltpu.SemaphoreType.DMA((2,)),
        ],
        compiler_params=REMOTE,
        name="collect",
    )(qkv, out, fc, proj, vectors)


def attend_back_kernel(heads, size, own, *refs):
    if own:
        q_ref, kv_ref, do_ref, mix_ref, lse_ref, seed_ref, term_ref, dq_ref, dkv_ref, sum_ref = refs[:10]
    else:
        q_ref, kv_ref, do_ref, mix_ref, lse_ref, term_ref, dq_ref, dkv_ref, sum_ref = refs[:9]
    quad = QuadSum(term_ref, sum_ref, *refs[-5:])
    quad.start()
    _, _, z, _ = my_place()
    part = heads * size
    rows = q_ref.shape[0] // 2
    blk = 128
    scale = size**-0.5

    def visit(here, start, seen, allowed):
        keys_at = pl.ds(start, seen)
        for h in range(heads):
            cols = slice(h * size, (h + 1) * size)
            vals = slice(part + h * size, part + (h + 1) * size)
            q = q_ref[here, cols]
            k = kv_ref[keys_at, cols]
            do = do_ref[here, cols]
            s = dot_nt(q, k) * scale
            p = jnp.exp(s - lse_ref[here, h : h + 1])
            if own:
                p = jnp.where(allowed, p, 0.0)
            dp = dot_nt(do, kv_ref[keys_at, vals])
            delta = jnp.sum(do.astype(jnp.float32) * mix_ref[here, cols], axis=-1, keepdims=True)
            ds = (p * (dp - delta)).astype(jnp.bfloat16)
            dq = dot_nn(ds, k) * scale
            if own:
                dq = dq + seed_ref[here, cols]
            dq_ref[here, cols] = dq.astype(dq_ref.dtype)
            dkv_ref[keys_at, cols] += dot_tn(ds, q) * scale
            dkv_ref[keys_at, vals] += dot_tn(p.astype(jnp.bfloat16), do)

    def group(index):
        start = pl.multiple_of(index * rows, rows)
        if not own:

            def block(i, _):
                visit(pl.ds(pl.multiple_of(start + i * blk, blk), blk), start, rows, None)
                return 0

            lax.fori_loop(0, rows // blk, block, 0)
            return
        for i in range(rows // blk):
            seen = (i + 1) * blk
            lane = lax.broadcasted_iota(jnp.int32, (blk, seen), 1)
            line = lax.broadcasted_iota(jnp.int32, (blk, seen), 0)
            visit(pl.ds(pl.multiple_of(start + i * blk, blk), blk), start, seen, lane <= line + i * blk)

    def clear(index, _):
        here = pl.ds(pl.multiple_of(index * blk, blk), blk)
        dkv_ref[here, :] = jnp.zeros((blk, dkv_ref.shape[1]), dkv_ref.dtype)
        if not own:
            dq_ref[here, :] = jnp.zeros((blk, dq_ref.shape[1]), dq_ref.dtype)
        return 0

    lax.fori_loop(0, 2 * rows // blk, clear, 0)

    def one(index, _):
        if own:
            group(index)
        else:

            @pl.when(z % 2 == 1)
            def _():
                group(index)

        @pl.when(index == 0)
        def _():
            quad.middle()

        return 0

    lax.fori_loop(0, 2, one, 0)
    quad.finish()


def attend_back(sz, own, q, kv, grad_mix, mix, lse, seed, term, ident):
    operands = [q, kv, grad_mix, mix, lse] + ([seed] if own else []) + [term]
    return pl.pallas_call(
        functools.partial(attend_back_kernel, sz.quarter_heads, sz.head_size, own),
        out_shape=(
            jax.ShapeDtypeStruct(q.shape, jnp.bfloat16 if own else jnp.float32),
            jax.ShapeDtypeStruct(kv.shape, jnp.float32),
            jax.ShapeDtypeStruct(term.shape[2:], jnp.float32),
        ),
        in_specs=[VMEM] * len(operands),
        out_specs=[VMEM] * 3,
        scratch_shapes=quad_scratch(term),
        cost_estimate=cost(35),
        compiler_params=remote_params(ident, 56 << 20),
        name="attend_back_own" if own else "attend_back_before",
    )(*operands)


def rowwise(value):
    return with_layout_constraint(value, Layout(major_to_minor=(0, 1)))


def norm_parts(values):
    mean = jnp.mean(values, axis=-1, keepdims=True)
    centre = values - mean
    rs = lax.rsqrt(jnp.mean(centre * centre, axis=-1, keepdims=True) + EPSILON)
    return centre * rs, rs


def norm_back(normed, rs, grad, gain):
    e = grad * gain
    return rs * (
        e
        - jnp.mean(e, axis=-1, keepdims=True)
        - normed * jnp.mean(e * normed, axis=-1, keepdims=True)
    )


def per_device_quad(tokens, params, out_grad, lengths):
    rows, width = tokens.shape
    hidden = FF
    sz = Sizes(width, hidden, HEADS, HEAD_DIM, params.shape[0])
    y, c, z, x = my_place()
    quarter = c * 2 + x
    bf16, f32 = jnp.bfloat16, jnp.float32

    def pick(value, index):
        return lax.dynamic_index_in_dim(value, index, 0, keepdims=False)

    def halves_of(value):
        half = value.shape[1] // 2
        first, second = value[:, :half], value[:, half:]
        return jnp.where(y == 0, first, second), jnp.where(y == 0, second, first)

    def to_other_y(sent):
        return over_y(sent.astype(bf16))

    def to_places(kept, got):
        summed = kept + got.astype(f32)
        summed = summed.reshape(4, summed.shape[0] // 4, -1)
        total = pick(summed, z)
        for d in (1, 2, 3):
            got = over_z(pick(summed, (z + d) % 4).astype(bf16), d)
            total = total + got.astype(f32)
        return total

    w_qkv, w_out, w_fc, w_proj, vec, tok_all, cot_all = open_call(
        sz, params.reshape(sz.block, GRAIN, width), tokens, out_grad
    )
    flat = lambda value: value.reshape(-1, width)
    vectors = flat(vec).astype(f32)
    fc_bias = vectors[8 : 8 + hidden // width].reshape(hidden)
    w_qkv, cot_all = flat(w_qkv), flat(cot_all)
    normed_all, _ = norm_parts(flat(tok_all).astype(f32))
    act_one = (normed_all * vectors[0] + vectors[1]).astype(bf16)

    def quarter_of(vector):
        padded = jnp.pad(vector, (0, 4 * sz.part - width))
        return lax.dynamic_slice_in_dim(padded, quarter * sz.part, sz.part, 0)

    kv_bias = jnp.concatenate([jnp.zeros((sz.part,), f32), quarter_of(vectors[3])])
    kv = (dot_nt(act_one, w_qkv[sz.part :]) + kv_bias).astype(bf16)
    q = (dot_nt(act_one, w_qkv[: sz.part]) + quarter_of(vectors[2])).astype(bf16)
    mix, lse, before, mixed, _, w_fc, w_proj, w_out = forward_call(sz, q, kv, w_out, w_fc, w_proj)
    w_fc, w_out = flat(w_fc), flat(w_out)[:width]
    mixed = jnp.transpose(mixed, (1, 0, 2)).reshape(rows, 4 * sz.part)[:, :width]
    inputs = tokens.astype(f32)
    residual = inputs + (dot_nt(mixed, w_out) + vectors[4])
    normed_two, rs_two = norm_parts(residual)
    act_two, w_proj = acts_call((normed_two * vectors[5] + vectors[6]).astype(bf16), w_proj)
    act_two, w_proj = flat(act_two), flat(w_proj)
    bias = lax.dynamic_slice_in_dim(fc_bias, quarter * (hidden // 4), hidden // 4, 0)
    pre_act = dot_nt(act_two, w_fc) + bias
    act_hidden, pull_gelu = jax.vjp(gelu_tanh, pre_act)
    act_hidden = act_hidden.astype(bf16)
    hid_mine, hid_other = halves_of(act_hidden)
    got_proj = to_other_y(dot_tn(hid_other, cot_all))
    grad_fc = pull_gelu(dot_nt(cot_all, w_proj))[0].astype(bf16)
    fc_mine, fc_other = halves_of(grad_fc)
    got_fc = to_other_y(dot_tn(fc_other, act_two))
    grad_two = quad_sum(rowwise(dot_nn(grad_fc, w_fc).astype(bf16)).reshape(2, 2, rows, width), 7)

    cot = out_grad.astype(f32)
    grad_res = cot + norm_back(normed_two, rs_two, grad_two, vectors[5])
    grad_attn = grad_res.astype(bf16)
    grad_mix = dot_nn(grad_attn, w_out).astype(bf16)
    grad_mix = jnp.pad(grad_mix, ((0, 0), (0, 4 * sz.part - width)))
    grad_mix = jnp.transpose(grad_mix.reshape(rows, 4, sz.part), (1, 0, 2))
    grad_mix = swap_call(grad_mix, 3).reshape(4 * rows, sz.part)
    g_proj = to_places(dot_tn(hid_mine, cot_all), got_proj)
    partial_out = rowwise(dot_nn(act_hidden, w_proj).astype(bf16)).reshape(2, 2, rows, width)
    dq_before, dkv_before, out_sum = attend_back(
        sz, False, q, before, grad_mix, mix, lse, None, partial_out, 4
    )
    output = (residual + out_sum + vectors[7]).astype(bf16)
    returned = permute(
        dkv_before.astype(bf16), lambda py, pc, pz, px: (py, pc, pz - 1, px) if pz % 2 == 1 else None
    )
    g_fc = to_places(dot_tn(fc_mine, act_two), got_fc)
    g_out = rowwise(dot_tn(jnp.pad(grad_attn, ((0, 0), (0, 4 * sz.part - width))), mixed).astype(bf16))
    dq, dkv, g_out = attend_back(
        sz, True, q, kv, grad_mix, mix, lse, dq_before, g_out.reshape(2, 2, sz.part, width), 5
    )
    g_out = g_out.reshape(2, sz.part // 2, width)
    got_out = to_other_y(pick(g_out, 1 - y))
    grad_qkv = jnp.concatenate([dq, (dkv + returned.astype(f32)).astype(bf16)], axis=1)
    qkv_mine, qkv_other = halves_of(grad_qkv)
    got_qkv = to_other_y(dot_tn(qkv_other, act_one))
    grad_one = quad_sum(rowwise(dot_nn(grad_qkv, w_qkv).astype(bf16)).reshape(2, 2, rows, width), 6)
    g_out = to_places(pick(g_out, y), got_out)
    g_qkv = to_places(dot_tn(qkv_mine, act_one), got_qkv)

    normed_one, rs_one = norm_parts(inputs)
    input_grad = (grad_res + norm_back(normed_one, rs_one, grad_one, vectors[0])).astype(bf16)

    def placed(vector):
        spot = lax.dynamic_update_slice_in_dim(jnp.zeros((4 * sz.part,), f32), vector, quarter * sz.part, 0)
        return spot[:width]

    sums = jnp.sum(grad_qkv.astype(f32), axis=0)
    bias_sum = jnp.sum(grad_fc.astype(f32), axis=0).reshape(1, hidden // 4)
    fc_rows = lax.dynamic_update_slice_in_dim(jnp.zeros((4, hidden // 4), f32), bias_sum, quarter, 0)
    grad_vectors = jnp.concatenate(
        [
            jnp.stack(
                [
                    jnp.sum(grad_one * normed_one, axis=0),
                    jnp.sum(grad_one, axis=0),
                    placed(sums[: sz.part]),
                    placed(sums[2 * sz.part :]),
                    jnp.sum(grad_attn.astype(f32), axis=0),
                    jnp.sum(grad_two * normed_two, axis=0),
                    jnp.sum(grad_two, axis=0),
                    jnp.sum(cot, axis=0),
                ]
            ),
            fc_rows.reshape(hidden // width, width),
        ]
    )
    count = grad_vectors.shape[0]
    grad_vectors = jnp.pad(grad_vectors, ((0, sz.vec * GRAIN - count), (0, 0)))
    grains = lambda value: value.astype(bf16).reshape(-1, GRAIN, width)
    table, all_vectors = collect(
        sz, grains(g_qkv), grains(g_out), grains(g_fc), grains(g_proj), grad_vectors.reshape(sz.vec, GRAIN, width)
    )
    grad_vectors = jnp.sum(all_vectors.reshape(32, sz.vec * GRAIN, width), axis=0)[:count]
    table = table.reshape(sz.block * GRAIN, width).astype(f32)
    used = (sz.vec_start % sz.block) * GRAIN
    tail = jnp.concatenate(
        [grad_vectors, jnp.zeros((sz.block * GRAIN - used - grad_vectors.shape[0], width), f32)]
    )
    last = flat_id(y, c, z, x) == sz.vec_start // sz.block
    tail = jnp.where(last, tail, table[used:])
    param_grad = jnp.concatenate([table[:used], tail])
    return (output, input_grad, param_grad)


def fits_quad(mesh, tokens, params, lengths):
    dp, cp = mesh.shape["dp"], mesh.shape["cp"]
    rows = tokens.shape[0] // (dp * cp)
    width = tokens.shape[1]
    blocks = params.shape[0] // (dp * cp)
    return (
        (dp, cp) == (4, 8)
        and lengths.shape[1] == 2
        and rows * cp == lengths.shape[1] * MIN_LEN
        and rows % 128 == 0
        and blocks % GRAIN == 0
        and (HEADS, HEAD_DIM, FF, width) == (25, 64, 6400, 1600)
    )


def solution(mesh):
    in_specs = (P(("dp", "cp"), None), P(("dp", "cp"), None), P(("dp", "cp"), None), P("dp", None))
    out_specs = (P(("dp", "cp"), None), P(("dp", "cp"), None), P(("dp", "cp"), None))

    def step(tokens, params, out_grad, lengths):
        body = per_device_quad if fits_quad(mesh, tokens, params, lengths) else per_device_general

        return jax.shard_map(
            body, mesh=mesh, in_specs=in_specs, out_specs=out_specs, check_vma=False
        )(tokens, params, out_grad, lengths)

    return step
```

```python
import functools

import jax
import jax.numpy as jnp
from jax import lax
from jax.experimental import pallas as pl
from jax.experimental.layout import Layout, with_layout_constraint
from jax.experimental.pallas import tpu as pltpu
from jax.sharding import PartitionSpec as P


HEADS = 25
FF = 6400
HEAD_DIM = 64
TILE = 128
MIN_LEN = 1024
MAX_LEN = 4096


EPSILON = 1e-05
MASKED = -1e30
GELU_SCALE = 0.7978845608028654


def from_behind(value, axis, by):
    length = lax.axis_size(axis)
    pairs = [(i, i + by) for i in range(length) if 0 <= i + by < length]
    return lax.ppermute(value, axis, pairs)


def layer_norm(values, gain_row, bias_row):
    centre = values - jnp.mean(values, axis=-1, keepdims=True)
    spread = jnp.mean(centre * centre, axis=-1, keepdims=True)
    return centre * lax.rsqrt(spread + EPSILON) * gain_row + bias_row


def gelu_tanh(values):
    return (
        0.5 * values * (1.0 + jnp.tanh(GELU_SCALE * (values + 0.044715 * values * values * values)))
    )


def segment_of(position, seq_ends):
    return jnp.sum((position[:, None] >= seq_ends[None, :]).astype(jnp.int32), axis=1)


def unpack(gathered, model_width, hidden):
    out_end = 4 * model_width
    fc_end = out_end + hidden
    proj_end = fc_end + hidden
    vec_end = proj_end + 8
    return (
        gathered[0 : 3 * model_width],
        gathered[3 * model_width : out_end],
        gathered[out_end:fc_end],
        gathered[fc_end:proj_end],
        gathered[proj_end:vec_end].astype(jnp.float32),
        gathered[vec_end : vec_end + hidden // model_width].astype(jnp.float32).reshape(hidden),
    )


def matmul_nt(left_mat, right_mat):
    return lax.dot_general(
        left_mat, right_mat, (((1,), (1,)), ((), ())), preferred_element_type=jnp.float32
    )


def matmul_tn(left_mat, right_mat):
    return lax.dot_general(
        left_mat, right_mat, (((0,), (0,)), ((), ())), preferred_element_type=jnp.float32
    )


def matmul_nn(left_mat, right_mat):
    return jnp.dot(left_mat, right_mat, preferred_element_type=jnp.float32)


def per_device_general(tokens, params, out_grad, lengths):
    tok_rows, model_width = tokens.shape
    hidden = FF
    head_count = HEADS
    head_size = HEAD_DIM
    cp_count = lax.axis_size("cp")
    group_rows = tok_rows * cp_count
    seq_count = lengths.shape[1]
    longest = min(MAX_LEN, group_rows - (seq_count - 1) * MIN_LEN)
    reach_back = min(cp_count - 1, (longest + tok_rows - TILE - 1) // tok_rows)
    pair_count = (reach_back + 2) // 2
    score_scale = head_size ** (-0.5)
    gathered = lax.all_gather(params, ("dp", "cp"), axis=0, tiled=True)
    w_attn, w_out, w_fc, w_proj, vectors, fc_bias = unpack(gathered, model_width, hidden)
    inputs = tokens.astype(jnp.float32)
    act_one = layer_norm(inputs, vectors[0], vectors[1]).astype(jnp.bfloat16)
    qkv_bias = jnp.concatenate([vectors[2], jnp.zeros_like(vectors[2]), vectors[3]])
    qkv = (matmul_nt(act_one, w_attn) + qkv_bias).astype(jnp.bfloat16)
    queries = qkv[:, :model_width].reshape(tok_rows, head_count, head_size)
    key_value = qkv[:, model_width:]
    device = lax.axis_index("cp")
    seq_ends = jnp.cumsum(lengths[0])
    query_pos = device * tok_rows + jnp.arange(tok_rows, dtype=jnp.int32)
    query_seg = segment_of(query_pos, seq_ends)
    store = jnp.zeros((2 * pair_count, tok_rows, 2 * model_width), jnp.bfloat16)
    store = store.at[0].set(key_value)

    def fetch(step_index, state_pair):
        moving, held_rows = state_pair
        moving = from_behind(moving, "cp", 1)
        return (moving, lax.dynamic_update_index_in_dim(held_rows, moving, step_index, 0))

    _, store = lax.fori_loop(1, reach_back + 1, fetch, (key_value, store))

    def pair_mask(pair_index):
        owners = 2 * pair_index + jnp.arange(2, dtype=jnp.int32)
        key_pos = (
            (device - owners)[:, None] * tok_rows + jnp.arange(tok_rows, dtype=jnp.int32)[None, :]
        ).reshape(2 * tok_rows)
        usable = jnp.broadcast_to((owners <= reach_back)[:, None], (2, tok_rows)).reshape(
            2 * tok_rows
        ) & (key_pos >= 0)
        key_seg = segment_of(key_pos, seq_ends)
        return (
            (key_seg[None, :] == query_seg[:, None])
            & (key_pos[None, :] <= query_pos[:, None])
            & usable[None, :]
        )

    def pair_rows(pair_index):
        block_rows = lax.dynamic_slice_in_dim(store, 2 * pair_index, 2, 0).reshape(
            2 * tok_rows, 2 * model_width
        )
        return (
            block_rows[:, :model_width].reshape(2 * tok_rows, head_count, head_size),
            block_rows[:, model_width:].reshape(2 * tok_rows, head_count, head_size),
        )

    def pair_scores(key_rows, allowed):
        raw_scores = (
            jnp.einsum("qhd,khd->hqk", queries, key_rows, preferred_element_type=jnp.float32)
            * score_scale
        )
        return jnp.where(allowed[None], raw_scores, MASKED)

    def visit(work):

        def step_pair(pair_index, running):
            allowed = pair_mask(pair_index)
            result = work(pair_index, allowed, running)
            return result

        return step_pair

    def add_total(pair_index, allowed, running):
        row_top, summed = running
        key_rows, _ = pair_rows(pair_index)
        scores = pair_scores(key_rows, allowed)
        new_top = jnp.maximum(row_top, jnp.max(scores, axis=-1, keepdims=True))
        summed = summed * jnp.exp(row_top - new_top) + jnp.sum(
            jnp.exp(scores - new_top), axis=-1, keepdims=True
        )
        return (new_top, summed)

    start_top = jnp.full((head_count, tok_rows, 1), MASKED, jnp.float32)
    start_sum = jnp.zeros((head_count, tok_rows, 1), jnp.float32)
    row_top, summed = lax.fori_loop(0, pair_count, visit(add_total), (start_top, start_sum))
    log_total = row_top + jnp.log(summed)

    def add_mix(pair_index, allowed, running):
        key_rows, value_rows = pair_rows(pair_index)
        prob_rows = jnp.exp(pair_scores(key_rows, allowed) - log_total).astype(jnp.bfloat16)
        return running + jnp.einsum(
            "hqk,khd->qhd", prob_rows, value_rows, preferred_element_type=jnp.float32
        )

    mixed_full = lax.fori_loop(
        0, pair_count, visit(add_mix), jnp.zeros((tok_rows, head_count, head_size), jnp.float32)
    )
    mixed = mixed_full.reshape(tok_rows, model_width).astype(jnp.bfloat16)
    attn_out = matmul_nt(mixed, w_out) + vectors[4]
    residual = inputs + attn_out
    act_two = layer_norm(residual, vectors[5], vectors[6]).astype(jnp.bfloat16)
    pre_act = matmul_nt(act_two, w_fc) + fc_bias
    act_hidden = gelu_tanh(pre_act).astype(jnp.bfloat16)
    output = (residual + matmul_nn(act_hidden, w_proj) + vectors[7]).astype(jnp.bfloat16)
    gathered = lax.all_gather(params, ("dp", "cp"), axis=0, tiled=True)
    w_attn, w_out, w_fc, w_proj, vectors, fc_bias = unpack(gathered, model_width, hidden)
    grad_out_f = out_grad.astype(jnp.float32)
    grad_hidden = matmul_nt(out_grad, w_proj)
    _, pull_gelu = jax.vjp(gelu_tanh, pre_act)
    grad_fc = pull_gelu(grad_hidden)[0].astype(jnp.bfloat16)
    grad_act_two = matmul_nn(grad_fc, w_fc)
    _, pull_two = jax.vjp(layer_norm, residual, vectors[5], vectors[6])
    grad_res_norm, grad_gain_two, grad_bias_two = pull_two(grad_act_two)
    grad_res = grad_out_f + grad_res_norm
    grad_attn = grad_res.astype(jnp.bfloat16)
    grad_mix = (
        matmul_nn(grad_attn, w_out).astype(jnp.bfloat16).reshape(tok_rows, head_count, head_size)
    )
    grad_dot = jnp.transpose(jnp.sum(grad_mix.astype(jnp.float32) * mixed_full, axis=-1), (1, 0))[
        :, :, None
    ]

    def add_grads(pair_index, allowed, running):
        grad_query, grad_store = running
        key_rows, value_rows = pair_rows(pair_index)
        prob_rows = jnp.exp(pair_scores(key_rows, allowed) - log_total)
        grad_probs = jnp.einsum(
            "qhd,khd->hqk", grad_mix, value_rows, preferred_element_type=jnp.float32
        )
        grad_scores = (prob_rows * (grad_probs - grad_dot)).astype(jnp.bfloat16)
        grad_query = (
            grad_query
            + jnp.einsum("hqk,khd->qhd", grad_scores, key_rows, preferred_element_type=jnp.float32)
            * score_scale
        )
        grad_keys = (
            jnp.einsum("hqk,qhd->khd", grad_scores, queries, preferred_element_type=jnp.float32)
            * score_scale
        )
        grad_values = jnp.einsum(
            "hqk,qhd->khd",
            prob_rows.astype(jnp.bfloat16),
            grad_mix,
            preferred_element_type=jnp.float32,
        )
        pair_grad = jnp.concatenate(
            [
                grad_keys.reshape(2 * tok_rows, model_width),
                grad_values.reshape(2 * tok_rows, model_width),
            ],
            axis=1,
        )
        pair_grad = pair_grad.reshape(2, tok_rows, 2 * model_width)
        grad_store = lax.dynamic_update_slice_in_dim(grad_store, pair_grad, 2 * pair_index, 0)
        return (grad_query, grad_store)

    start_query = jnp.zeros((tok_rows, head_count, head_size), jnp.float32)
    start_store = jnp.zeros((2 * pair_count, tok_rows, 2 * model_width), jnp.float32)
    grad_query, grad_store = lax.fori_loop(
        0, pair_count, visit(add_grads), (start_query, start_store)
    )

    def send_back(step_index, moving):
        moving = moving + lax.dynamic_index_in_dim(
            grad_store, reach_back - step_index, 0, keepdims=False
        )
        return from_behind(moving.astype(jnp.bfloat16), "cp", -1).astype(moving.dtype)

    returned = lax.fori_loop(
        0, reach_back, send_back, jnp.zeros((tok_rows, 2 * model_width), jnp.float32)
    )
    grad_kv = returned + grad_store[0]
    grad_qkv = jnp.concatenate([grad_query.reshape(tok_rows, model_width), grad_kv], axis=1).astype(
        jnp.bfloat16
    )
    grad_qkv_f = grad_qkv.astype(jnp.float32)
    grad_act_one = matmul_nn(grad_qkv, w_attn)
    _, pull_one = jax.vjp(layer_norm, inputs, vectors[0], vectors[1])
    grad_in_norm, grad_gain_one, grad_bias_one = pull_one(grad_act_one)
    input_grad = (grad_res + grad_in_norm).astype(jnp.bfloat16)
    grad_vectors = jnp.stack(
        [
            grad_gain_one,
            grad_bias_one,
            jnp.sum(grad_qkv_f[:, :model_width], axis=0),
            jnp.sum(grad_qkv_f[:, 2 * model_width :], axis=0),
            jnp.sum(grad_attn.astype(jnp.float32), axis=0),
            grad_gain_two,
            grad_bias_two,
            jnp.sum(grad_out_f, axis=0),
        ]
    )
    grad_fc_bias = jnp.sum(grad_fc.astype(jnp.float32), axis=0).reshape(
        hidden // model_width, model_width
    )
    used_rows = 4 * model_width + 2 * hidden + 8 + hidden // model_width
    total_rows = gathered.shape[0]
    local_grad = jnp.concatenate(
        [
            matmul_tn(grad_qkv, act_one),
            matmul_tn(grad_attn, mixed),
            matmul_tn(grad_fc, act_two),
            matmul_tn(act_hidden, out_grad),
            grad_vectors,
            grad_fc_bias,
            jnp.zeros((total_rows - used_rows, model_width), jnp.float32),
        ],
        axis=0,
    )
    dp_count = lax.axis_size("dp")
    device_count = dp_count * cp_count
    share_rows = total_rows // device_count
    spread_rows = local_grad.reshape(device_count, 1, share_rows, model_width)
    received = lax.all_to_all(
        spread_rows.astype(jnp.bfloat16), ("dp", "cp"), split_axis=0, concat_axis=1, tiled=True
    ).astype(spread_rows.dtype)
    param_grad = jnp.sum(received, axis=1).reshape(share_rows, model_width)
    return (output, input_grad, param_grad)


MESH = pl.DeviceIdType.MESH
GRAIN = 8
NT = (((1,), (1,)), ((), ()))
TN = (((0,), (0,)), ((), ()))


def dot_nt(a, b):
    return lax.dot_general(a, b, NT, preferred_element_type=jnp.float32)


def dot_tn(a, b):
    return lax.dot_general(a, b, TN, preferred_element_type=jnp.float32)


def dot_nn(a, b):
    return jnp.dot(a, b, preferred_element_type=jnp.float32)


def flat_id(y, c, z, x):
    return ((y * 2 + c) * 4 + z) * 2 + x


def permute(value, move):
    pairs = []
    for y in range(2):
        for c in range(2):
            for z in range(4):
                for x in range(2):
                    to = move(y, c, z, x)
                    if to is not None:
                        pairs.append((flat_id(y, c, z, x), flat_id(*to)))
    return lax.ppermute(value, ("dp", "cp"), pairs)


def over_y(value):
    return permute(value, lambda y, c, z, x: (1 - y, c, z, x))


def over_z(value, by):
    return permute(value, lambda y, c, z, x: (y, c, (z + by) % 4, x))


class Sizes:
    def __init__(self, width, hidden, heads, head_size, rows):
        self.heads = heads
        self.head_size = head_size
        self.quarter_heads = -(-heads // 4)
        self.part = self.quarter_heads * head_size
        self.part_grains = self.part // GRAIN
        self.width_grains = width // GRAIN
        self.spill = 4 * self.part_grains - self.width_grains
        self.qkv = 3 * self.part_grains // 8
        self.out = self.part_grains // 8
        self.mlp = hidden // 4 // 8 // GRAIN
        self.block = rows // GRAIN
        self.out_start = 3 * self.width_grains
        self.fc_start = 4 * self.width_grains
        self.proj_start = self.fc_start + hidden // GRAIN
        self.vec_start = self.proj_start + hidden // GRAIN
        self.vec = 2
        self.head_grains = head_size // GRAIN
        self.fc_turn = self.turn(self.fc_start)
        self.proj_turn = self.turn(self.proj_start)

    def turn(self, start):
        return start // (2 * self.block) % 4


def spot_of_range(r):
    y = r // 6 + (r % 2) * ((r // 3) % 2)
    u = (r - (r + 5) // 8 - (r + 3) // 8) % 4
    return y, u


def range_of_spot(y, u):
    first = u + u // 3
    second = (1 - u // 2) * (u + 6) + (u // 2) * (2 * u - 1)
    return (1 - y) * first + y * second


RANGES = (0, 1, 2, 4, 6, 7, 3, 5)
SPOTS = (0, 1, 2, 6, 3, 7, 4, 5)


def slot_qkv(y, z):
    return 2 * z + y


def slot_out(y, z):
    return 4 * y + z


def slot_turned(turn):
    return lambda y, z: 4 * y + (z + 4 - turn) % 4


def my_place():
    dp = lax.axis_index("dp")
    cp = lax.axis_index("cp")
    return dp // 2, dp % 2, cp // 2, cp % 2


def device_of(quarter, y, z):
    return y * 2 + quarter // 2, z * 2 + quarter % 2


class Wires:
    def __init__(self, send_sems, recv_sems):
        self.send_sems = send_sems
        self.recv_sems = recv_sems
        self.count = 0

    def to(self, src, dst, dp, cp):
        index = self.count
        self.count += 1
        return pltpu.make_async_remote_copy(
            src_ref=src,
            dst_ref=dst,
            send_sem=self.send_sems.at[index],
            recv_sem=self.recv_sems.at[index],
            device_id=(dp, cp),
            device_id_type=MESH,
        )


class PlaceGather:
    def __init__(self, wires, full, slot):
        self.wires = wires
        self.full = full
        self.slot = slot
        self.dp, self.cp = lax.axis_index("dp"), lax.axis_index("cp")
        self.y, self.z, self.x = self.dp // 2, self.cp // 2, self.cp % 2
        self.started = []

    def send(self, slot, dp, cp):
        view = self.full.at[slot]
        copy = self.wires.to(view, view, dp, cp)
        copy.start()
        self.started.append(copy)
        return copy

    def partners(self):
        along = [(self.dp, ((self.z + d) % 4) * 2 + self.x) for d in (1, 2, 3)]
        return along + [((self.dp + 2) % 4, self.cp)]

    def start_over(self):
        self.over = [self.send(self.slot(self.y, self.z), (self.dp + 2) % 4, self.cp)]

    def start(self, over=True):
        mine = self.slot(self.y, self.z)
        self.along = []
        for d in (1, 3, 2):
            self.along.append((d, self.send(mine, self.dp, ((self.z + d) % 4) * 2 + self.x)))
        self.over = []
        if over:
            self.start_over()

    def forward(self):
        for d, copy in self.along:
            copy.wait_recv()
            self.over.append(self.send(self.slot(self.y, (self.z - d + 4) % 4), (self.dp + 2) % 4, self.cp))

    def finish(self):
        for copy in self.over:
            copy.wait_recv()
        for copy in self.started:
            copy.wait_send()


class QuadGather:
    def __init__(self, wires, block, full, local_sem):
        self.wires = wires
        self.block = block
        self.full = full
        self.dp, self.cp = lax.axis_index("dp"), lax.axis_index("cp")
        self.c, self.x = self.dp % 2, self.cp % 2
        self.over_x = (self.dp, self.cp + 1 - 2 * self.x)
        self.over_c = (self.dp + 1 - 2 * self.c, self.cp)
        self.local_sem = local_sem

    def start(self):
        spot = self.full.at[self.c, self.x]
        self.by_x = self.wires.to(self.block, spot, *self.over_x)
        self.by_c = self.wires.to(self.block, spot, *self.over_c)
        self.by_x.start()
        self.by_c.start()
        self.local = pltpu.make_async_copy(self.block, spot, self.local_sem)
        self.local.start()

    def forward(self):
        self.by_x.wait_recv()
        spot = self.full.at[self.c, 1 - self.x]
        self.pass_on = self.wires.to(spot, spot, *self.over_c)
        self.pass_on.start()

    def finish(self):
        self.by_c.wait_recv()
        self.pass_on.wait_recv()
        self.by_x.wait_send()
        self.by_c.wait_send()
        self.pass_on.wait_send()
        self.local.wait()


def open_kernel(
    sz, p_ref, tok_ref, cot_ref, qkv_ref, out_ref, fc_ref, proj_ref, vec_ref, tok_all, cot_all,
    spread_sems, kind_sems, send_sems, recv_sems, local_sems,
):
    y, c, z, x = my_place()
    me = flat_id(y, c, z, x)
    wires = Wires(send_sems, recv_sems)
    tok = QuadGather(wires, tok_ref, tok_all, local_sems.at[0])
    cot = QuadGather(wires, cot_ref, cot_all, local_sems.at[1])

    def send(grain, ref, spot, slot, quarter, py, pz, sem, recv):
        dp, cp = device_of(quarter, py, pz)
        mine = dp * 8 + cp == me

        @pl.when(mine)
        def _():
            pltpu.make_async_copy(p_ref.at[grain], ref.at[spot, slot], recv).start()

        @pl.when(jnp.logical_not(mine))
        def _():
            pltpu.make_async_remote_copy(
                src_ref=p_ref.at[grain],
                dst_ref=ref.at[spot, slot],
                send_sem=sem,
                recv_sem=recv,
                device_id=(dp, cp),
                device_id_type=MESH,
            ).start()

    def sent(grain, ref, spot, slot, quarter, py, pz, sem, recv):
        dp, cp = device_of(quarter, py, pz)

        @pl.when(dp * 8 + cp != me)
        def _():
            pltpu.make_async_copy(p_ref.at[grain], p_ref.at[grain], sem).wait()

    def headed(act, grain):
        table = me * sz.block + grain
        part = table // sz.width_grains
        inner = table % sz.width_grains
        head = inner // sz.head_grains
        rest = inner % sz.head_grains

        def one(quarter, sem):
            local = part * sz.part_grains + (head // 4) * sz.head_grains + rest
            spot = local // sz.qkv
            act(grain, qkv_ref, spot, local % sz.qkv, quarter, spot % 2, spot // 2, sem, kind_sems.at[0])

        @pl.when(table < sz.out_start)
        def _():
            one(head % 4, spread_sems.at[grain])

            @pl.when(head == sz.heads - 1)
            def _():
                for quarter in range(1, 4):
                    one(quarter, spread_sems.at[sz.block + (quarter - 1) * sz.head_grains + rest])

    def outward(act, grain):
        local = me * sz.block + grain - sz.out_start

        def one(quarter, inner, sem):
            spot = inner // sz.out
            act(grain, out_ref, spot, inner % sz.out, quarter, spot // 4, spot % 4, sem, kind_sems.at[1])

        @pl.when(jnp.logical_and(local >= 0, local < sz.width_grains))
        def _():
            one(local // sz.part_grains, local % sz.part_grains, spread_sems.at[grain])

            @pl.when(local < sz.spill)
            def _():
                one(3, sz.part_grains - sz.spill + local, spread_sems.at[sz.block + 3 * sz.head_grains + local])

    def plain(act, grain, base, turn, ref, recv):
        offset = me * sz.block + grain - base

        @pl.when(jnp.logical_and(offset >= 0, offset < 32 * sz.mlp))
        def _():
            local = offset // 4
            py, u = spot_of_range(local // sz.mlp)
            act(
                grain, ref, py * 4 + u, local % sz.mlp, offset % 4, py, (u + turn) % 4,
                spread_sems.at[grain], recv,
            )

    def heads(act):
        def one(grain, _):
            headed(act, grain)
            return 0

        lax.fori_loop(0, sz.block, one, 0)

    def others(act):
        def one(grain, _):
            outward(act, grain)
            plain(act, grain, sz.fc_start, sz.fc_turn, fc_ref, kind_sems.at[2])
            plain(act, grain, sz.proj_start, sz.proj_turn, proj_ref, kind_sems.at[3])
            return 0

        lax.fori_loop(0, sz.block, one, 0)

    owner = sz.vec_start // sz.block
    spot = sz.vec_start % sz.block

    def vector_sends(act):
        @pl.when(me == owner)
        def _():
            def to(device, _):
                @pl.when(device != me)
                def _():
                    act(
                        pltpu.make_async_remote_copy(
                            src_ref=p_ref.at[pl.ds(spot, sz.vec)],
                            dst_ref=vec_ref,
                            send_sem=spread_sems.at[sz.block + 3 * sz.head_grains + sz.spill + device],
                            recv_sem=kind_sems.at[4],
                            device_id=(device // 8, device % 8),
                            device_id_type=MESH,
                        )
                    )

                return 0

            lax.fori_loop(0, 32, to, 0)

    heads(send)
    tok.start()
    mine = slot_qkv(y, z)
    pltpu.make_async_copy(qkv_ref.at[mine], qkv_ref.at[mine], kind_sems.at[0]).wait()
    weights = PlaceGather(wires, qkv_ref, slot_qkv)
    weights.start()
    vector_sends(lambda copy: copy.start())

    @pl.when(me == owner)
    def _():
        pltpu.make_async_copy(p_ref.at[pl.ds(spot, sz.vec)], vec_ref, kind_sems.at[4]).start()

    others(send)
    cot.start()
    weights.forward()
    tok.forward()
    cot.forward()
    heads(sent)
    others(sent)
    vector_sends(lambda copy: copy.wait_send())
    for index, (ref, slot) in enumerate(
        ((out_ref, slot_out), (fc_ref, slot_turned(sz.fc_turn)), (proj_ref, slot_turned(sz.proj_turn)))
    ):
        view = ref.at[slot(y, z)]
        pltpu.make_async_copy(view, view, kind_sems.at[index + 1]).wait()
    pltpu.make_async_copy(vec_ref, vec_ref, kind_sems.at[4]).wait()
    tok.finish()
    cot.finish()
    weights.finish()


HBM = pl.BlockSpec(memory_space=pl.ANY)
VMEM = pl.BlockSpec(memory_space=pltpu.VMEM)
REMOTE = pltpu.CompilerParams(has_side_effects=True)


def remote_params(ident=None, vmem=None):
    return pltpu.CompilerParams(has_side_effects=True, collective_id=ident, vmem_limit_bytes=vmem)


def greet(partners):
    barrier = pltpu.get_barrier_semaphore()
    for dp, cp in partners:
        pl.semaphore_signal(barrier, inc=1, device_id=(dp, cp), device_id_type=MESH)
    pl.semaphore_wait(barrier, len(partners))


def cost(us):
    return pl.CostEstimate(flops=0, bytes_accessed=int(us * 3.0e6), transcendentals=0)


def wire_sems(count):
    return [pltpu.SemaphoreType.DMA((count,)), pltpu.SemaphoreType.DMA((count,))]


def open_call(sz, table, tokens, cotangent):
    rows, width = tokens.shape

    def like(*shape):
        return jax.ShapeDtypeStruct(shape + (width,), table.dtype)

    return pl.pallas_call(
        functools.partial(open_kernel, sz),
        out_shape=(
            like(8, sz.qkv, GRAIN),
            like(8, sz.out, GRAIN),
            like(8, sz.mlp, GRAIN),
            like(8, sz.mlp, GRAIN),
            like(sz.vec, GRAIN),
            like(2, 2, rows),
            like(2, 2, rows),
        ),
        in_specs=[HBM, VMEM, VMEM],
        out_specs=[HBM] * 7,
        scratch_shapes=[
            pltpu.SemaphoreType.DMA((sz.block + 3 * sz.head_grains + sz.spill + 32,)),
            pltpu.SemaphoreType.DMA((5,)),
            *wire_sems(13),
            pltpu.SemaphoreType.DMA((2,)),
        ],
        compiler_params=REMOTE,
        name="open",
    )(table, tokens, cotangent)


def forward_kernel(
    heads, size, fc_turn, proj_turn, q_ref, kv_ref, out_in, fc_in, proj_in,
    mix_ref, lse_ref, before_ref, mixed_ref, out_ref, fc_ref, proj_ref, out_all,
    stage, send_sems, recv_sems, local_sems,
):
    y, c, z, x = my_place()
    dp, cp = lax.axis_index("dp"), lax.axis_index("cp")
    wires = Wires(send_sems, recv_sems)
    part = heads * size
    rows = q_ref.shape[0] // 2
    blk = 128
    scale = size**-0.5
    odd = z % 2 == 1
    w_out = PlaceGather(wires, out_ref, slot_out)
    w_fc = PlaceGather(wires, fc_ref, slot_turned(fc_turn))
    w_proj = PlaceGather(wires, proj_ref, slot_turned(proj_turn))
    others = [(c, 1 - x), (1 - c, x), (1 - c, 1 - x)]
    quad = [(y * 2 + tc, z * 2 + tx) for tc, tx in others]
    greet(w_out.partners() + quad)
    keys = wires.to(kv_ref, before_ref, dp, (cp + 2) % 8)

    @pl.when(jnp.logical_not(odd))
    def _():
        keys.start()

    w_out.start()
    w_fc.start()

    def own(group, _):
        start = group * rows
        for i in range(rows // blk):
            here = pl.ds(pl.multiple_of(start + i * blk, blk), blk)
            seen = (i + 1) * blk
            keys_at = pl.ds(pl.multiple_of(start, rows), seen)
            lane = lax.broadcasted_iota(jnp.int32, (blk, seen), 1)
            line = lax.broadcasted_iota(jnp.int32, (blk, seen), 0)
            allowed = lane <= line + i * blk
            for h in range(heads):
                cols = slice(h * size, (h + 1) * size)
                vals = slice(part + h * size, part + (h + 1) * size)
                s = dot_nt(q_ref[here, cols], kv_ref[keys_at, cols]) * scale
                s = jnp.where(allowed, s, MASKED)
                top = jnp.max(s, axis=-1, keepdims=True)
                p = jnp.exp(s - top)
                total = jnp.sum(p, axis=-1, keepdims=True)
                mix_ref[here, cols] = dot_nn(p.astype(jnp.bfloat16), kv_ref[keys_at, vals]) / total
                lse_ref[here, h : h + 1] = top + jnp.log(total)
        return 0

    lax.fori_loop(0, 2, own, 0)
    w_out.forward()

    def add_before(index, _):
        here = pl.ds(pl.multiple_of(index * blk, blk), blk)
        keys_at = pl.ds(pl.multiple_of((index * blk) // rows * rows, rows), rows)
        for h in range(heads):
            cols = slice(h * size, (h + 1) * size)
            vals = slice(part + h * size, part + (h + 1) * size)
            s = dot_nt(q_ref[here, cols], before_ref[keys_at, cols]) * scale
            lse = lse_ref[here, h : h + 1]
            top = jnp.maximum(lse, jnp.max(s, axis=-1, keepdims=True))
            p = jnp.exp(s - top)
            kept = jnp.exp(lse - top)
            total = kept + jnp.sum(p, axis=-1, keepdims=True)
            mix = mix_ref[here, cols] * kept + dot_nn(p.astype(jnp.bfloat16), before_ref[keys_at, vals])
            mix_ref[here, cols] = mix / total
            lse_ref[here, h : h + 1] = top + jnp.log(total)
        return 0

    w_out.finish()
    whole = QuadGather(wires, out_ref, out_all, local_sems.at[0])
    whole.start()

    @pl.when(odd)
    def _():
        keys.wait_recv()
        lax.fori_loop(0, 2 * rows // blk, add_before, 0)

    def round_off(index, _):
        here = pl.ds(pl.multiple_of(index * blk, blk), blk)
        stage[here, :] = mix_ref[here, :].astype(stage.dtype)
        return 0

    lax.fori_loop(0, 2 * rows // blk, round_off, 0)
    w_proj.start_over()
    mine = c * 2 + x
    each = rows // 2
    swaps = []
    for (tc, tx), (tdp, tcp) in zip(others, quad):
        block = stage.at[pl.ds(pl.multiple_of((tc * 2 + tx) * each, each), each)]
        swaps.append(wires.to(block, mixed_ref.at[mine], tdp, tcp))
    for copy in swaps:
        copy.start()
    local = pltpu.make_async_copy(
        stage.at[pl.ds(pl.multiple_of(mine * each, each), each)], mixed_ref.at[mine], local_sems.at[1]
    )
    local.start()
    w_fc.forward()
    whole.forward()
    for copy in swaps:
        copy.wait_recv()
    whole.finish()
    w_fc.finish()
    w_proj.over[0].wait_recv()
    w_proj.over[0].wait_send()
    for copy in swaps:
        copy.wait_send()
    local.wait()

    @pl.when(jnp.logical_not(odd))
    def _():
        keys.wait_send()


def forward_call(sz, q, kv, w_out, w_fc, w_proj):
    part = sz.part
    rows = q.shape[0]

    def like(value, *lead):
        return jax.ShapeDtypeStruct(lead + value.shape, value.dtype)

    return pl.pallas_call(
        functools.partial(forward_kernel, sz.quarter_heads, sz.head_size, sz.fc_turn, sz.proj_turn),
        out_shape=(
            jax.ShapeDtypeStruct((rows, part), jnp.float32),
            jax.ShapeDtypeStruct((rows, 8), jnp.float32),
            like(kv),
            jax.ShapeDtypeStruct((4, rows // 4, part), jnp.bfloat16),
            like(w_out),
            like(w_fc),
            like(w_proj),
            like(w_out, 2, 2),
        ),
        in_specs=[VMEM, VMEM, HBM, HBM, HBM],
        out_specs=[VMEM] * 4 + [HBM] * 4,
        input_output_aliases={2: 4, 3: 5, 4: 6},
        scratch_shapes=[
            pltpu.VMEM((rows, part), jnp.bfloat16),
            *wire_sems(22),
            pltpu.SemaphoreType.DMA((2,)),
        ],
        cost_estimate=cost(120),
        compiler_params=remote_params(1, 56 << 20),
        name="forward",
    )(q, kv, w_out, w_fc, w_proj)


def acts_kernel(proj_turn, act_ref, proj_in, act_all, proj_ref, send_sems, recv_sems, local_sem):
    wires = Wires(send_sems, recv_sems)
    quad = QuadGather(wires, act_ref, act_all, local_sem)
    places = PlaceGather(wires, proj_ref, slot_turned(proj_turn))
    greet(places.partners() + [quad.over_x, quad.over_c])
    quad.start()
    places.start(False)
    quad.forward()
    places.forward()
    quad.finish()
    places.finish()


def acts_call(sz, act, w_proj):
    return pl.pallas_call(
        functools.partial(acts_kernel, sz.proj_turn),
        out_shape=(
            jax.ShapeDtypeStruct((2, 2) + act.shape, act.dtype),
            jax.ShapeDtypeStruct(w_proj.shape, w_proj.dtype),
        ),
        in_specs=[VMEM, HBM],
        out_specs=[HBM] * 2,
        input_output_aliases={1: 1},
        scratch_shapes=[*wire_sems(9), pltpu.SemaphoreType.DMA],
        cost_estimate=cost(60),
        compiler_params=remote_params(2),
        name="acts",
    )(act, w_proj)


def swap_kernel(in_ref, out_ref, send_sems, recv_sems, local_sem):
    y, c, z, x = my_place()
    wires = Wires(send_sems, recv_sems)
    mine = c * 2 + x
    others = [(1 - c, 1 - x), (c, 1 - x), (1 - c, x)]
    greet([(y * 2 + tc, z * 2 + tx) for tc, tx in others])
    copies = []
    for tc, tx in others:
        copies.append(wires.to(in_ref.at[tc * 2 + tx], out_ref.at[mine], y * 2 + tc, z * 2 + tx))
    for copy in copies:
        copy.start()
    local = pltpu.make_async_copy(in_ref.at[mine], out_ref.at[mine], local_sem)
    local.start()
    for copy in copies:
        copy.wait_recv()
    for copy in copies:
        copy.wait_send()
    local.wait()


def swap_call(value, ident):
    return pl.pallas_call(
        swap_kernel,
        out_shape=jax.ShapeDtypeStruct(value.shape, value.dtype),
        in_specs=[VMEM],
        out_specs=VMEM,
        scratch_shapes=[*wire_sems(3), pltpu.SemaphoreType.DMA],
        compiler_params=remote_params(ident),
        cost_estimate=cost(20),
        name="swap",
    )(value)


class QuadSum:
    step = 32

    def __init__(self, in_ref, out_ref, got_c, stage, got_x, send_sems, recv_sems):
        self.y, self.c, self.z, self.x = my_place()
        dp, cp = lax.axis_index("dp"), lax.axis_index("cp")
        wires = Wires(send_sems, recv_sems)
        self.in_ref, self.out_ref, self.got_c, self.stage, self.got_x = in_ref, out_ref, got_c, stage, got_x
        self.partners = [(dp + 1 - 2 * self.c, cp), (dp, cp + 1 - 2 * self.x)]
        self.by_c = wires.to(in_ref.at[1 - self.c], got_c, *self.partners[0])
        self.by_x = wires.to(stage, got_x, *self.partners[1])

    def each(self, act):
        def one(index, _):
            act(pl.ds(pl.multiple_of(index * self.step, self.step), self.step))
            return 0

        lax.fori_loop(0, self.out_ref.shape[0] // self.step, one, 0)

    def start(self):
        greet(self.partners)
        self.by_c.start()

    def middle(self):
        c, x = self.c, self.x
        self.by_c.wait_recv()

        def to_send(span):
            self.stage[span, :] = (
                self.in_ref[c, 1 - x, span, :].astype(jnp.float32) + self.got_c[1 - x, span, :].astype(jnp.float32)
            ).astype(self.stage.dtype)

        self.each(to_send)
        self.by_x.start()

    def finish(self):
        c, x = self.c, self.x
        self.by_x.wait_recv()

        def to_add(span):
            self.out_ref[span, :] = (
                self.in_ref[c, x, span, :].astype(jnp.float32)
                + self.got_c[x, span, :].astype(jnp.float32)
                + self.got_x[span, :].astype(jnp.float32)
            )

        self.each(to_add)
        self.by_c.wait_send()
        self.by_x.wait_send()


def quad_sum_kernel(*refs):
    quad = QuadSum(*refs)
    quad.start()
    quad.middle()
    quad.finish()


def quad_scratch(partial):
    rows, width = partial.shape[2:]
    return [
        pltpu.VMEM((2, rows, width), partial.dtype),
        pltpu.VMEM((rows, width), partial.dtype),
        pltpu.VMEM((rows, width), partial.dtype),
        *wire_sems(2),
    ]


def quad_sum(partial, ident):
    return pl.pallas_call(
        quad_sum_kernel,
        out_shape=jax.ShapeDtypeStruct(partial.shape[2:], jnp.float32),
        in_specs=[VMEM],
        out_specs=VMEM,
        scratch_shapes=quad_scratch(partial),
        compiler_params=remote_params(ident),
        cost_estimate=cost(30),
        name="quad_sum",
    )(partial)


def collect_kernel(sz, qkv_ref, out_ref, fc_ref, proj_ref, vec_ref, g_ref, vecs_ref, send_sems, recv_sem, vec_sems):
    y, c, z, x = my_place()
    me = flat_id(y, c, z, x)
    quarter = c * 2 + x

    def send(ref, slot, table, sem):
        dest = table // sz.block
        mine = dest == me

        @pl.when(mine)
        def _():
            pltpu.make_async_copy(ref.at[slot], g_ref.at[table % sz.block], recv_sem).start()

        @pl.when(jnp.logical_not(mine))
        def _():
            pltpu.make_async_remote_copy(
                src_ref=ref.at[slot],
                dst_ref=g_ref.at[table % sz.block],
                send_sem=sem,
                recv_sem=recv_sem,
                device_id=(dest // 8, dest % 8),
                device_id_type=MESH,
            ).start()

    def sent(ref, slot, table, sem):
        @pl.when(table // sz.block != me)
        def _():
            pltpu.make_async_copy(ref.at[slot], ref.at[slot], sem).wait()

    def run(act):
        def heads(slot, _):
            local = slot_qkv(y, z) * sz.qkv + slot
            inner = local % sz.part_grains
            head = 4 * (inner // sz.head_grains) + quarter

            @pl.when(head < sz.heads)
            def _():
                table = (local // sz.part_grains) * sz.width_grains + head * sz.head_grains + inner % sz.head_grains
                act(qkv_ref, slot, table, send_sems.at[slot])

            return 0

        lax.fori_loop(0, sz.qkv, heads, 0)

        def outward(slot, _):
            local = quarter * sz.part_grains + slot_out(y, z) * sz.out + slot

            @pl.when(local < sz.width_grains)
            def _():
                act(out_ref, slot, sz.out_start + local, send_sems.at[sz.qkv + slot])

            return 0

        lax.fori_loop(0, sz.out, outward, 0)

        def plain(ref, base, turn, first_sem):
            r = range_of_spot(y, (z + 4 - turn) % 4)

            def one(slot, _):
                table = base + 4 * (r * sz.mlp + slot) + quarter
                act(ref, slot, table, send_sems.at[first_sem + slot])
                return 0

            lax.fori_loop(0, sz.mlp, one, 0)

        plain(fc_ref, sz.fc_start, sz.fc_turn, sz.qkv + sz.out)
        plain(proj_ref, sz.proj_start, sz.proj_turn, sz.qkv + sz.out + sz.mlp)

    last = sz.vec_start // sz.block
    vec_copy = pltpu.make_async_remote_copy(
        src_ref=vec_ref,
        dst_ref=vecs_ref.at[me],
        send_sem=vec_sems.at[0],
        recv_sem=vec_sems.at[1],
        device_id=(last // 8, last % 8),
        device_id_type=MESH,
    )

    @pl.when(me != last)
    def _():
        vec_copy.start()

    @pl.when(me == last)
    def _():
        pltpu.make_async_copy(vec_ref, vecs_ref.at[me], vec_sems.at[1]).start()

    run(send)
    run(sent)

    @pl.when(me != last)
    def _():
        vec_copy.wait_send()

    @pl.when(me == last)
    def _():
        view = g_ref.at[pl.ds(0, sz.vec_start % sz.block)]
        pltpu.make_async_copy(view, view, recv_sem).wait()
        pltpu.make_async_copy(vecs_ref, vecs_ref, vec_sems.at[1]).wait()

    @pl.when(me != last)
    def _():
        pltpu.make_async_copy(g_ref, g_ref, recv_sem).wait()


def collect(sz, qkv, out, fc, proj, vectors):
    width = qkv.shape[-1]
    return pl.pallas_call(
        functools.partial(collect_kernel, sz),
        out_shape=(
            jax.ShapeDtypeStruct((sz.block, GRAIN, width), qkv.dtype),
            jax.ShapeDtypeStruct((32,) + vectors.shape, vectors.dtype),
        ),
        in_specs=[HBM] * 5,
        out_specs=[HBM] * 2,
        scratch_shapes=[
            pltpu.SemaphoreType.DMA((sz.qkv + sz.out + 2 * sz.mlp,)),
            pltpu.SemaphoreType.DMA,
            pltpu.SemaphoreType.DMA((2,)),
        ],
        compiler_params=REMOTE,
        name="collect",
    )(qkv, out, fc, proj, vectors)


def attend_back_kernel(heads, size, own, *refs):
    if own:
        q_ref, kv_ref, do_ref, mix_ref, lse_ref, seed_ref, term_ref, dq_ref, dkv_ref, sum_ref = refs[:10]
    else:
        q_ref, kv_ref, do_ref, mix_ref, lse_ref, term_ref, dq_ref, dkv_ref, sum_ref = refs[:9]
    quad = QuadSum(term_ref, sum_ref, *refs[-5:])
    quad.start()
    _, _, z, _ = my_place()
    part = heads * size
    rows = q_ref.shape[0] // 2
    blk = 128
    scale = size**-0.5

    def visit(here, start, seen, allowed):
        keys_at = pl.ds(start, seen)
        for h in range(heads):
            cols = slice(h * size, (h + 1) * size)
            vals = slice(part + h * size, part + (h + 1) * size)
            q = q_ref[here, cols]
            k = kv_ref[keys_at, cols]
            do = do_ref[here, cols]
            s = dot_nt(q, k) * scale
            p = jnp.exp(s - lse_ref[here, h : h + 1])
            if own:
                p = jnp.where(allowed, p, 0.0)
            dp = dot_nt(do, kv_ref[keys_at, vals])
            delta = jnp.sum(do.astype(jnp.float32) * mix_ref[here, cols], axis=-1, keepdims=True)
            ds = (p * (dp - delta)).astype(jnp.bfloat16)
            dq = dot_nn(ds, k) * scale
            if own:
                dq = dq + seed_ref[here, cols]
            dq_ref[here, cols] = dq.astype(dq_ref.dtype)
            dkv_ref[keys_at, cols] += dot_tn(ds, q) * scale
            dkv_ref[keys_at, vals] += dot_tn(p.astype(jnp.bfloat16), do)

    def group(index):
        start = pl.multiple_of(index * rows, rows)
        if not own:

            def block(i, _):
                visit(pl.ds(pl.multiple_of(start + i * blk, blk), blk), start, rows, None)
                return 0

            lax.fori_loop(0, rows // blk, block, 0)
            return
        for i in range(rows // blk):
            seen = (i + 1) * blk
            lane = lax.broadcasted_iota(jnp.int32, (blk, seen), 1)
            line = lax.broadcasted_iota(jnp.int32, (blk, seen), 0)
            visit(pl.ds(pl.multiple_of(start + i * blk, blk), blk), start, seen, lane <= line + i * blk)

    def clear(index, _):
        here = pl.ds(pl.multiple_of(index * blk, blk), blk)
        dkv_ref[here, :] = jnp.zeros((blk, dkv_ref.shape[1]), dkv_ref.dtype)
        if not own:
            dq_ref[here, :] = jnp.zeros((blk, dq_ref.shape[1]), dq_ref.dtype)
        return 0

    lax.fori_loop(0, 2 * rows // blk, clear, 0)

    def one(index, _):
        if own:
            group(index)
        else:

            @pl.when(z % 2 == 1)
            def _():
                group(index)

        @pl.when(index == 0)
        def _():
            quad.middle()

        return 0

    lax.fori_loop(0, 2, one, 0)
    quad.finish()


def attend_back(sz, own, q, kv, grad_mix, mix, lse, seed, term, ident):
    operands = [q, kv, grad_mix, mix, lse] + ([seed] if own else []) + [term]
    return pl.pallas_call(
        functools.partial(attend_back_kernel, sz.quarter_heads, sz.head_size, own),
        out_shape=(
            jax.ShapeDtypeStruct(q.shape, jnp.bfloat16 if own else jnp.float32),
            jax.ShapeDtypeStruct(kv.shape, jnp.float32),
            jax.ShapeDtypeStruct(term.shape[2:], jnp.float32),
        ),
        in_specs=[VMEM] * len(operands),
        out_specs=[VMEM] * 3,
        scratch_shapes=quad_scratch(term),
        cost_estimate=cost(35),
        compiler_params=remote_params(ident, 56 << 20),
        name="attend_back_own" if own else "attend_back_before",
    )(*operands)


def rowwise(value):
    return with_layout_constraint(value, Layout(major_to_minor=(0, 1)))


def norm_parts(values):
    mean = jnp.mean(values, axis=-1, keepdims=True)
    centre = values - mean
    rs = lax.rsqrt(jnp.mean(centre * centre, axis=-1, keepdims=True) + EPSILON)
    return centre * rs, rs


def norm_back(normed, rs, grad, gain):
    e = grad * gain
    return rs * (
        e
        - jnp.mean(e, axis=-1, keepdims=True)
        - normed * jnp.mean(e * normed, axis=-1, keepdims=True)
    )


def per_device_quad(tokens, params, out_grad, lengths):
    rows, width = tokens.shape
    hidden = FF
    sz = Sizes(width, hidden, HEADS, HEAD_DIM, params.shape[0])
    y, c, z, x = my_place()
    quarter = c * 2 + x
    bf16, f32 = jnp.bfloat16, jnp.float32

    def pick(value, index):
        return lax.dynamic_index_in_dim(value, index, 0, keepdims=False)

    def halves_of(value):
        half = value.shape[1] // 2
        first, second = value[:, :half], value[:, half:]
        return jnp.where(y == 0, first, second), jnp.where(y == 0, second, first)

    def to_other_y(sent):
        return over_y(sent.astype(bf16))

    def to_places(kept, got, turn=0):
        summed = kept.astype(f32) + got.astype(f32)
        summed = summed.reshape(4, summed.shape[0] // 4, -1)
        total = pick(summed, (z + 4 - turn) % 4)
        for d in (1, 2, 3):
            got = over_z(pick(summed, (z + d + 4 - turn) % 4).astype(bf16), d)
            total = total + got.astype(f32)
        return total

    w_qkv, w_out, w_fc, w_proj, vec, tok_all, cot_all = open_call(
        sz, params.reshape(sz.block, GRAIN, width), tokens, out_grad
    )
    flat = lambda value: value.reshape(-1, width)
    vectors = flat(vec).astype(f32)
    fc_bias = vectors[8 : 8 + hidden // width].reshape(hidden)
    w_qkv, cot_all = flat(w_qkv), flat(cot_all)
    normed_all, _ = norm_parts(flat(tok_all).astype(f32))
    act_one = (normed_all * vectors[0] + vectors[1]).astype(bf16)

    def quarter_of(vector):
        padded = jnp.pad(vector, (0, 4 * sz.part - width)).reshape(sz.quarter_heads, 4, sz.head_size)
        return lax.dynamic_index_in_dim(padded, quarter, 1, keepdims=False).reshape(sz.part)

    kv_bias = jnp.concatenate([jnp.zeros((sz.part,), f32), quarter_of(vectors[3])])
    kv = (dot_nt(act_one, w_qkv[sz.part :]) + kv_bias).astype(bf16)
    q = (dot_nt(act_one, w_qkv[: sz.part]) + quarter_of(vectors[2])).astype(bf16)
    mix, lse, before, mixed, _, w_fc, w_proj, w_out = forward_call(sz, q, kv, w_out, w_fc, w_proj)
    w_fc, w_out = flat(w_fc), flat(w_out)[:width]
    by_head = (sz.quarter_heads, sz.head_size)
    mixed = jnp.transpose(mixed.reshape((4, rows) + by_head), (1, 2, 0, 3)).reshape(rows, 4 * sz.part)[:, :width]
    inputs = tokens.astype(f32)
    residual = inputs + (dot_nt(mixed, w_out) + vectors[4])
    normed_two, rs_two = norm_parts(residual)
    act_two, w_proj = acts_call(sz, (normed_two * vectors[5] + vectors[6]).astype(bf16), w_proj)
    act_two, w_proj = flat(act_two), flat(w_proj)
    bias = lax.dynamic_index_in_dim(fc_bias.reshape(-1, 4, GRAIN), quarter, 1, keepdims=False)
    bias = bias.reshape(8, hidden // 32)[jnp.array(RANGES)].reshape(hidden // 4)
    pre_act = dot_nt(act_two, w_fc) + bias
    act_hidden, pull_gelu = jax.vjp(gelu_tanh, pre_act)
    act_hidden = act_hidden.astype(bf16)
    hid_mine, hid_other = halves_of(act_hidden)
    got_proj = to_other_y(dot_tn(hid_other, cot_all))
    grad_fc = pull_gelu(dot_nt(cot_all, w_proj))[0].astype(bf16)
    fc_mine, fc_other = halves_of(grad_fc)
    got_fc = to_other_y(dot_tn(fc_other, act_two))
    grad_two = quad_sum(rowwise(dot_nn(grad_fc, w_fc).astype(bf16)).reshape(2, 2, rows, width), 7)

    cot = out_grad.astype(f32)
    grad_res = cot + norm_back(normed_two, rs_two, grad_two, vectors[5])
    grad_attn = grad_res.astype(bf16)
    grad_mix = dot_nn(grad_attn, w_out).astype(bf16)
    grad_mix = jnp.pad(grad_mix, ((0, 0), (0, 4 * sz.part - width)))
    grad_mix = jnp.transpose(grad_mix.reshape(rows, sz.quarter_heads, 4, sz.head_size), (2, 0, 1, 3))
    grad_mix = grad_mix.reshape(4, rows, sz.part)
    grad_mix = swap_call(grad_mix, 3).reshape(4 * rows, sz.part)
    g_proj = to_places(dot_tn(hid_mine, cot_all), got_proj, sz.proj_turn)
    partial_out = rowwise(dot_nn(act_hidden, w_proj).astype(bf16)).reshape(2, 2, rows, width)
    dq_before, dkv_before, out_sum = attend_back(
        sz, False, q, before, grad_mix, mix, lse, None, partial_out, 4
    )
    output = (residual + out_sum + vectors[7]).astype(bf16)
    returned = permute(dkv_before.astype(bf16), lambda py, pc, pz, px: (py, pc, pz - 1, px) if pz % 2 == 1 else None)
    g_fc = to_places(dot_tn(fc_mine, act_two), got_fc, sz.fc_turn)
    g_out = rowwise(dot_tn(jnp.pad(grad_attn, ((0, 0), (0, 4 * sz.part - width))), mixed).astype(bf16))
    dq, dkv, g_out = attend_back(sz, True, q, kv, grad_mix, mix, lse, dq_before, g_out.reshape(2, 2, sz.part, width), 5)
    g_out = g_out.reshape(2, sz.part // 2, width)
    got_out = to_other_y(pick(g_out, 1 - y))
    grad_qkv = jnp.concatenate([dq, (dkv + returned.astype(f32)).astype(bf16)], axis=1)
    g_qkv = rowwise(dot_tn(grad_qkv, act_one).astype(bf16)).reshape(4, 2, 3 * sz.part // 8, width)
    half_qkv = lambda index: lax.dynamic_index_in_dim(g_qkv, index, 1, keepdims=False).reshape(-1, width)
    got_qkv = to_other_y(half_qkv(1 - y))
    grad_one = quad_sum(rowwise(dot_nn(grad_qkv, w_qkv).astype(bf16)).reshape(2, 2, rows, width), 6)
    g_out = to_places(pick(g_out, y), got_out)
    g_qkv = to_places(half_qkv(y), got_qkv)

    normed_one, rs_one = norm_parts(inputs)
    input_grad = (grad_res + norm_back(normed_one, rs_one, grad_one, vectors[0])).astype(bf16)

    def placed(vector):
        spread = jnp.zeros((sz.quarter_heads, 4, sz.head_size), f32)
        spread = lax.dynamic_update_slice_in_dim(spread, vector.reshape(-1, 1, sz.head_size), quarter, 1)
        return spread.reshape(4 * sz.part)[:width]

    sums = jnp.sum(grad_qkv.astype(f32), axis=0)
    bias_sum = jnp.sum(grad_fc.astype(f32), axis=0).reshape(8, hidden // 32)[jnp.array(SPOTS)]
    fc_rows = lax.dynamic_update_slice_in_dim(
        jnp.zeros((hidden // 4 // GRAIN, 4, GRAIN), f32), bias_sum.reshape(-1, 1, GRAIN), quarter, 1
    )
    grad_vectors = jnp.concatenate(
        [
            jnp.stack(
                [
                    jnp.sum(grad_one * normed_one, axis=0),
                    jnp.sum(grad_one, axis=0),
                    placed(sums[: sz.part]),
                    placed(sums[2 * sz.part :]),
                    jnp.sum(grad_attn.astype(f32), axis=0),
                    jnp.sum(grad_two * normed_two, axis=0),
                    jnp.sum(grad_two, axis=0),
                    jnp.sum(cot, axis=0),
                ]
            ),
            fc_rows.reshape(hidden // width, width),
        ]
    )
    count = grad_vectors.shape[0]
    grad_vectors = jnp.pad(grad_vectors, ((0, sz.vec * GRAIN - count), (0, 0)))
    grains = lambda value: value.astype(bf16).reshape(-1, GRAIN, width)
    table, all_vectors = collect(
        sz, grains(g_qkv), grains(g_out), grains(g_fc), grains(g_proj), grad_vectors.reshape(sz.vec, GRAIN, width)
    )
    grad_vectors = jnp.sum(all_vectors.reshape(32, sz.vec * GRAIN, width), axis=0)[:count]
    table = table.reshape(sz.block * GRAIN, width).astype(f32)
    used = (sz.vec_start % sz.block) * GRAIN
    tail = jnp.concatenate(
        [grad_vectors, jnp.zeros((sz.block * GRAIN - used - grad_vectors.shape[0], width), f32)]
    )
    last = flat_id(y, c, z, x) == sz.vec_start // sz.block
    tail = jnp.where(last, tail, table[used:])
    param_grad = jnp.concatenate([table[:used], tail])
    return (output, input_grad, param_grad)


def fits_quad(mesh, tokens, params, lengths):
    dp, cp = mesh.shape["dp"], mesh.shape["cp"]
    rows = tokens.shape[0] // (dp * cp)
    width = tokens.shape[1]
    blocks = params.shape[0] // (dp * cp)
    return (
        (dp, cp) == (4, 8)
        and lengths.shape[1] == 2
        and rows * cp == lengths.shape[1] * MIN_LEN
        and rows % 128 == 0
        and blocks % GRAIN == 0
        and (HEADS, HEAD_DIM, FF, width) == (25, 64, 6400, 1600)
    )


def solution(mesh):
    in_specs = (P(("dp", "cp"), None), P(("dp", "cp"), None), P(("dp", "cp"), None), P("dp", None))
    out_specs = (P(("dp", "cp"), None), P(("dp", "cp"), None), P(("dp", "cp"), None))

    def step(tokens, params, out_grad, lengths):
        body = per_device_quad if fits_quad(mesh, tokens, params, lengths) else per_device_general

        return jax.shard_map(
            body, mesh=mesh, in_specs=in_specs, out_specs=out_specs, check_vma=False
        )(tokens, params, out_grad, lengths)

    return step
```

```python
import functools

import jax
import jax.numpy as jnp
from jax import lax
from jax.experimental import pallas as pl
from jax.experimental.layout import Layout, with_layout_constraint
from jax.experimental.pallas import tpu as pltpu
from jax.sharding import PartitionSpec as P


HEADS = 25
FF = 6400
HEAD_DIM = 64
TILE = 128
MIN_LEN = 1024
MAX_LEN = 4096


EPSILON = 1e-05
MASKED = -1e30
GELU_SCALE = 0.7978845608028654


def from_behind(value, axis, by):
    length = lax.axis_size(axis)
    pairs = [(i, i + by) for i in range(length) if 0 <= i + by < length]
    return lax.ppermute(value, axis, pairs)


def layer_norm(values, gain_row, bias_row):
    centre = values - jnp.mean(values, axis=-1, keepdims=True)
    spread = jnp.mean(centre * centre, axis=-1, keepdims=True)
    return centre * lax.rsqrt(spread + EPSILON) * gain_row + bias_row


def gelu_tanh(values):
    return (
        0.5 * values * (1.0 + jnp.tanh(GELU_SCALE * (values + 0.044715 * values * values * values)))
    )


def segment_of(position, seq_ends):
    return jnp.sum((position[:, None] >= seq_ends[None, :]).astype(jnp.int32), axis=1)


def unpack(gathered, model_width, hidden):
    out_end = 4 * model_width
    fc_end = out_end + hidden
    proj_end = fc_end + hidden
    vec_end = proj_end + 8
    return (
        gathered[0 : 3 * model_width],
        gathered[3 * model_width : out_end],
        gathered[out_end:fc_end],
        gathered[fc_end:proj_end],
        gathered[proj_end:vec_end].astype(jnp.float32),
        gathered[vec_end : vec_end + hidden // model_width].astype(jnp.float32).reshape(hidden),
    )


def matmul_nt(left_mat, right_mat):
    return lax.dot_general(
        left_mat, right_mat, (((1,), (1,)), ((), ())), preferred_element_type=jnp.float32
    )


def matmul_tn(left_mat, right_mat):
    return lax.dot_general(
        left_mat, right_mat, (((0,), (0,)), ((), ())), preferred_element_type=jnp.float32
    )


def matmul_nn(left_mat, right_mat):
    return jnp.dot(left_mat, right_mat, preferred_element_type=jnp.float32)


def per_device_general(tokens, params, out_grad, lengths):
    tok_rows, model_width = tokens.shape
    hidden = FF
    head_count = HEADS
    head_size = HEAD_DIM
    cp_count = lax.axis_size("cp")
    group_rows = tok_rows * cp_count
    seq_count = lengths.shape[1]
    longest = min(MAX_LEN, group_rows - (seq_count - 1) * MIN_LEN)
    reach_back = min(cp_count - 1, (longest + tok_rows - TILE - 1) // tok_rows)
    pair_count = (reach_back + 2) // 2
    score_scale = head_size ** (-0.5)
    gathered = lax.all_gather(params, ("dp", "cp"), axis=0, tiled=True)
    w_attn, w_out, w_fc, w_proj, vectors, fc_bias = unpack(gathered, model_width, hidden)
    inputs = tokens.astype(jnp.float32)
    act_one = layer_norm(inputs, vectors[0], vectors[1]).astype(jnp.bfloat16)
    qkv_bias = jnp.concatenate([vectors[2], jnp.zeros_like(vectors[2]), vectors[3]])
    qkv = (matmul_nt(act_one, w_attn) + qkv_bias).astype(jnp.bfloat16)
    queries = qkv[:, :model_width].reshape(tok_rows, head_count, head_size)
    key_value = qkv[:, model_width:]
    device = lax.axis_index("cp")
    seq_ends = jnp.cumsum(lengths[0])
    query_pos = device * tok_rows + jnp.arange(tok_rows, dtype=jnp.int32)
    query_seg = segment_of(query_pos, seq_ends)
    store = jnp.zeros((2 * pair_count, tok_rows, 2 * model_width), jnp.bfloat16)
    store = store.at[0].set(key_value)

    def fetch(step_index, state_pair):
        moving, held_rows = state_pair
        moving = from_behind(moving, "cp", 1)
        return (moving, lax.dynamic_update_index_in_dim(held_rows, moving, step_index, 0))

    _, store = lax.fori_loop(1, reach_back + 1, fetch, (key_value, store))

    def pair_mask(pair_index):
        owners = 2 * pair_index + jnp.arange(2, dtype=jnp.int32)
        key_pos = (
            (device - owners)[:, None] * tok_rows + jnp.arange(tok_rows, dtype=jnp.int32)[None, :]
        ).reshape(2 * tok_rows)
        usable = jnp.broadcast_to((owners <= reach_back)[:, None], (2, tok_rows)).reshape(
            2 * tok_rows
        ) & (key_pos >= 0)
        key_seg = segment_of(key_pos, seq_ends)
        return (
            (key_seg[None, :] == query_seg[:, None])
            & (key_pos[None, :] <= query_pos[:, None])
            & usable[None, :]
        )

    def pair_rows(pair_index):
        block_rows = lax.dynamic_slice_in_dim(store, 2 * pair_index, 2, 0).reshape(
            2 * tok_rows, 2 * model_width
        )
        return (
            block_rows[:, :model_width].reshape(2 * tok_rows, head_count, head_size),
            block_rows[:, model_width:].reshape(2 * tok_rows, head_count, head_size),
        )

    def pair_scores(key_rows, allowed):
        raw_scores = (
            jnp.einsum("qhd,khd->hqk", queries, key_rows, preferred_element_type=jnp.float32)
            * score_scale
        )
        return jnp.where(allowed[None], raw_scores, MASKED)

    def visit(work):

        def step_pair(pair_index, running):
            allowed = pair_mask(pair_index)
            result = work(pair_index, allowed, running)
            return result

        return step_pair

    def add_total(pair_index, allowed, running):
        row_top, summed = running
        key_rows, _ = pair_rows(pair_index)
        scores = pair_scores(key_rows, allowed)
        new_top = jnp.maximum(row_top, jnp.max(scores, axis=-1, keepdims=True))
        summed = summed * jnp.exp(row_top - new_top) + jnp.sum(
            jnp.exp(scores - new_top), axis=-1, keepdims=True
        )
        return (new_top, summed)

    start_top = jnp.full((head_count, tok_rows, 1), MASKED, jnp.float32)
    start_sum = jnp.zeros((head_count, tok_rows, 1), jnp.float32)
    row_top, summed = lax.fori_loop(0, pair_count, visit(add_total), (start_top, start_sum))
    log_total = row_top + jnp.log(summed)

    def add_mix(pair_index, allowed, running):
        key_rows, value_rows = pair_rows(pair_index)
        prob_rows = jnp.exp(pair_scores(key_rows, allowed) - log_total).astype(jnp.bfloat16)
        return running + jnp.einsum(
            "hqk,khd->qhd", prob_rows, value_rows, preferred_element_type=jnp.float32
        )

    mixed_full = lax.fori_loop(
        0, pair_count, visit(add_mix), jnp.zeros((tok_rows, head_count, head_size), jnp.float32)
    )
    mixed = mixed_full.reshape(tok_rows, model_width).astype(jnp.bfloat16)
    attn_out = matmul_nt(mixed, w_out) + vectors[4]
    residual = inputs + attn_out
    act_two = layer_norm(residual, vectors[5], vectors[6]).astype(jnp.bfloat16)
    pre_act = matmul_nt(act_two, w_fc) + fc_bias
    act_hidden = gelu_tanh(pre_act).astype(jnp.bfloat16)
    output = (residual + matmul_nn(act_hidden, w_proj) + vectors[7]).astype(jnp.bfloat16)
    gathered = lax.all_gather(params, ("dp", "cp"), axis=0, tiled=True)
    w_attn, w_out, w_fc, w_proj, vectors, fc_bias = unpack(gathered, model_width, hidden)
    grad_out_f = out_grad.astype(jnp.float32)
    grad_hidden = matmul_nt(out_grad, w_proj)
    _, pull_gelu = jax.vjp(gelu_tanh, pre_act)
    grad_fc = pull_gelu(grad_hidden)[0].astype(jnp.bfloat16)
    grad_act_two = matmul_nn(grad_fc, w_fc)
    _, pull_two = jax.vjp(layer_norm, residual, vectors[5], vectors[6])
    grad_res_norm, grad_gain_two, grad_bias_two = pull_two(grad_act_two)
    grad_res = grad_out_f + grad_res_norm
    grad_attn = grad_res.astype(jnp.bfloat16)
    grad_mix = (
        matmul_nn(grad_attn, w_out).astype(jnp.bfloat16).reshape(tok_rows, head_count, head_size)
    )
    grad_dot = jnp.transpose(jnp.sum(grad_mix.astype(jnp.float32) * mixed_full, axis=-1), (1, 0))[
        :, :, None
    ]

    def add_grads(pair_index, allowed, running):
        grad_query, grad_store = running
        key_rows, value_rows = pair_rows(pair_index)
        prob_rows = jnp.exp(pair_scores(key_rows, allowed) - log_total)
        grad_probs = jnp.einsum(
            "qhd,khd->hqk", grad_mix, value_rows, preferred_element_type=jnp.float32
        )
        grad_scores = (prob_rows * (grad_probs - grad_dot)).astype(jnp.bfloat16)
        grad_query = (
            grad_query
            + jnp.einsum("hqk,khd->qhd", grad_scores, key_rows, preferred_element_type=jnp.float32)
            * score_scale
        )
        grad_keys = (
            jnp.einsum("hqk,qhd->khd", grad_scores, queries, preferred_element_type=jnp.float32)
            * score_scale
        )
        grad_values = jnp.einsum(
            "hqk,qhd->khd",
            prob_rows.astype(jnp.bfloat16),
            grad_mix,
            preferred_element_type=jnp.float32,
        )
        pair_grad = jnp.concatenate(
            [
                grad_keys.reshape(2 * tok_rows, model_width),
                grad_values.reshape(2 * tok_rows, model_width),
            ],
            axis=1,
        )
        pair_grad = pair_grad.reshape(2, tok_rows, 2 * model_width)
        grad_store = lax.dynamic_update_slice_in_dim(grad_store, pair_grad, 2 * pair_index, 0)
        return (grad_query, grad_store)

    start_query = jnp.zeros((tok_rows, head_count, head_size), jnp.float32)
    start_store = jnp.zeros((2 * pair_count, tok_rows, 2 * model_width), jnp.float32)
    grad_query, grad_store = lax.fori_loop(
        0, pair_count, visit(add_grads), (start_query, start_store)
    )

    def send_back(step_index, moving):
        moving = moving + lax.dynamic_index_in_dim(
            grad_store, reach_back - step_index, 0, keepdims=False
        )
        return from_behind(moving.astype(jnp.bfloat16), "cp", -1).astype(moving.dtype)

    returned = lax.fori_loop(
        0, reach_back, send_back, jnp.zeros((tok_rows, 2 * model_width), jnp.float32)
    )
    grad_kv = returned + grad_store[0]
    grad_qkv = jnp.concatenate([grad_query.reshape(tok_rows, model_width), grad_kv], axis=1).astype(
        jnp.bfloat16
    )
    grad_qkv_f = grad_qkv.astype(jnp.float32)
    grad_act_one = matmul_nn(grad_qkv, w_attn)
    _, pull_one = jax.vjp(layer_norm, inputs, vectors[0], vectors[1])
    grad_in_norm, grad_gain_one, grad_bias_one = pull_one(grad_act_one)
    input_grad = (grad_res + grad_in_norm).astype(jnp.bfloat16)
    grad_vectors = jnp.stack(
        [
            grad_gain_one,
            grad_bias_one,
            jnp.sum(grad_qkv_f[:, :model_width], axis=0),
            jnp.sum(grad_qkv_f[:, 2 * model_width :], axis=0),
            jnp.sum(grad_attn.astype(jnp.float32), axis=0),
            grad_gain_two,
            grad_bias_two,
            jnp.sum(grad_out_f, axis=0),
        ]
    )
    grad_fc_bias = jnp.sum(grad_fc.astype(jnp.float32), axis=0).reshape(
        hidden // model_width, model_width
    )
    used_rows = 4 * model_width + 2 * hidden + 8 + hidden // model_width
    total_rows = gathered.shape[0]
    local_grad = jnp.concatenate(
        [
            matmul_tn(grad_qkv, act_one),
            matmul_tn(grad_attn, mixed),
            matmul_tn(grad_fc, act_two),
            matmul_tn(act_hidden, out_grad),
            grad_vectors,
            grad_fc_bias,
            jnp.zeros((total_rows - used_rows, model_width), jnp.float32),
        ],
        axis=0,
    )
    dp_count = lax.axis_size("dp")
    device_count = dp_count * cp_count
    share_rows = total_rows // device_count
    spread_rows = local_grad.reshape(device_count, 1, share_rows, model_width)
    received = lax.all_to_all(
        spread_rows.astype(jnp.bfloat16), ("dp", "cp"), split_axis=0, concat_axis=1, tiled=True
    ).astype(spread_rows.dtype)
    param_grad = jnp.sum(received, axis=1).reshape(share_rows, model_width)
    return (output, input_grad, param_grad)


MESH = pl.DeviceIdType.MESH
GRAIN = 8
NT = (((1,), (1,)), ((), ()))
TN = (((0,), (0,)), ((), ()))


def dot_nt(a, b):
    return lax.dot_general(a, b, NT, preferred_element_type=jnp.float32)


def dot_tn(a, b):
    return lax.dot_general(a, b, TN, preferred_element_type=jnp.float32)


def dot_nn(a, b):
    return jnp.dot(a, b, preferred_element_type=jnp.float32)


def flat_id(y, c, z, x):
    return ((y * 2 + c) * 4 + z) * 2 + x


def permute(value, move):
    pairs = []
    for y in range(2):
        for c in range(2):
            for z in range(4):
                for x in range(2):
                    to = move(y, c, z, x)
                    if to is not None:
                        pairs.append((flat_id(y, c, z, x), flat_id(*to)))
    return lax.ppermute(value, ("dp", "cp"), pairs)


def over_y(value):
    return permute(value, lambda y, c, z, x: (1 - y, c, z, x))


def over_z(value, by):
    return permute(value, lambda y, c, z, x: (y, c, (z + by) % 4, x))


class Sizes:
    def __init__(self, width, hidden, heads, head_size, rows):
        self.heads = heads
        self.head_size = head_size
        self.quarter_heads = -(-heads // 4)
        self.part = self.quarter_heads * head_size
        self.part_grains = self.part // GRAIN
        self.width_grains = width // GRAIN
        self.spill = 4 * self.part_grains - self.width_grains
        self.qkv = 3 * self.part_grains // 8
        self.out = self.part_grains // 8
        self.mlp = hidden // 4 // 8 // GRAIN
        self.block = rows // GRAIN
        self.out_start = 3 * self.width_grains
        self.fc_start = 4 * self.width_grains
        self.proj_start = self.fc_start + hidden // GRAIN
        self.vec_start = self.proj_start + hidden // GRAIN
        self.vec = 2
        self.head_grains = head_size // GRAIN
        self.fc_turn = self.turn(self.fc_start)
        self.proj_turn = self.turn(self.proj_start)

    def turn(self, start):
        return start // (2 * self.block) % 4


def spot_of_range(r):
    y = r // 6 + (r % 2) * ((r // 3) % 2)
    u = (r - (r + 5) // 8 - (r + 3) // 8) % 4
    return y, u


def range_of_spot(y, u):
    first = u + u // 3
    second = (1 - u // 2) * (u + 6) + (u // 2) * (2 * u - 1)
    return (1 - y) * first + y * second


RANGES = (0, 1, 2, 4, 6, 7, 3, 5)
SPOTS = (0, 1, 2, 6, 3, 7, 4, 5)


def slot_qkv(y, z):
    return 2 * z + y


def slot_out(y, z):
    return 4 * y + z


def slot_turned(turn):
    return lambda y, z: 4 * y + (z + 4 - turn) % 4


def my_place():
    dp = lax.axis_index("dp")
    cp = lax.axis_index("cp")
    return dp // 2, dp % 2, cp // 2, cp % 2


def device_of(quarter, y, z):
    return y * 2 + quarter // 2, z * 2 + quarter % 2


class Wires:
    def __init__(self, send_sems, recv_sems):
        self.send_sems = send_sems
        self.recv_sems = recv_sems
        self.count = 0

    def to(self, src, dst, dp, cp):
        index = self.count
        self.count += 1
        return pltpu.make_async_remote_copy(
            src_ref=src,
            dst_ref=dst,
            send_sem=self.send_sems.at[index],
            recv_sem=self.recv_sems.at[index],
            device_id=(dp, cp),
            device_id_type=MESH,
        )


class PlaceGather:
    def __init__(self, wires, full, slot, along=True, over=True):
        self.full = full
        self.dp, self.cp = lax.axis_index("dp"), lax.axis_index("cp")
        self.y, self.z, self.x = self.dp // 2, self.cp // 2, self.cp % 2
        self.above = (self.dp, ((self.z + 1) % 4) * 2 + self.x)
        self.below = (self.dp, ((self.z + 3) % 4) * 2 + self.x)
        self.across = ((self.dp + 2) % 4, self.cp)

        def share(by, to):
            view = full.at[slot(self.y, (self.z + 4 + by) % 4)]
            return wires.to(view, view, *to)

        if along:
            self.up = [share(1 - k, self.above) for k in (1, 2, 3)]
            self.down = [share(k - 1, self.below) for k in (1, 2, 3)]
        self.own_over = share(0, self.across) if over else None
        self.over = [self.own_over] + [share(d, self.across) if along else None for d in (1, 2, 3)]

    def partners(self):
        return [self.above, self.below, self.across]

    def start_over(self):
        self.own_over.start()

    def start(self):
        @pl.when(self.z < 3)
        def _():
            self.up[0].start()

        @pl.when(self.z > 0)
        def _():
            self.down[0].start()

        if self.own_over is not None:
            self.start_over()

    def forward(self, steps=(1, 2, 3)):
        for k in steps:

            @pl.when(self.z >= k)
            def _():
                self.up[k - 1].wait_recv()
                if k < 3:

                    @pl.when(self.z < 3)
                    def _():
                        self.up[k].start()

                self.over[4 - k].start()

            @pl.when(self.z <= 3 - k)
            def _():
                self.down[k - 1].wait_recv()
                if k < 3:

                    @pl.when(self.z > 0)
                    def _():
                        self.down[k].start()

                self.over[k].start()

    def finish(self):
        sent_over = [copy for copy in self.over if copy is not None]
        for copy in sent_over:
            copy.wait_recv()
        for copy in sent_over:
            copy.wait_send()
        for k in (1, 2, 3):

            @pl.when(jnp.logical_and(self.z >= k - 1, self.z < 3))
            def _():
                self.up[k - 1].wait_send()

            @pl.when(jnp.logical_and(self.z <= 4 - k, self.z > 0))
            def _():
                self.down[k - 1].wait_send()


class QuadGather:
    def __init__(self, wires, block, full, local_sem):
        self.wires = wires
        self.block = block
        self.full = full
        self.dp, self.cp = lax.axis_index("dp"), lax.axis_index("cp")
        self.c, self.x = self.dp % 2, self.cp % 2
        self.over_x = (self.dp, self.cp + 1 - 2 * self.x)
        self.over_c = (self.dp + 1 - 2 * self.c, self.cp)
        self.local_sem = local_sem

    def start(self):
        spot = self.full.at[self.c, self.x]
        self.by_x = self.wires.to(self.block, spot, *self.over_x)
        self.by_c = self.wires.to(self.block, spot, *self.over_c)
        self.by_x.start()
        self.by_c.start()
        self.local = pltpu.make_async_copy(self.block, spot, self.local_sem)
        self.local.start()

    def forward(self):
        self.by_x.wait_recv()
        spot = self.full.at[self.c, 1 - self.x]
        self.pass_on = self.wires.to(spot, spot, *self.over_c)
        self.pass_on.start()

    def finish(self):
        self.by_c.wait_recv()
        self.pass_on.wait_recv()
        self.by_x.wait_send()
        self.by_c.wait_send()
        self.pass_on.wait_send()
        self.local.wait()


def open_kernel(
    sz, p_ref, tok_ref, cot_ref, qkv_ref, out_ref, fc_ref, proj_ref, vec_ref, tok_all, cot_all,
    spread_sems, kind_sems, send_sems, recv_sems, local_sems,
):
    y, c, z, x = my_place()
    me = flat_id(y, c, z, x)
    wires = Wires(send_sems, recv_sems)
    tok = QuadGather(wires, tok_ref, tok_all, local_sems.at[0])
    cot = QuadGather(wires, cot_ref, cot_all, local_sems.at[1])

    def send(grain, ref, spot, slot, quarter, py, pz, sem, recv):
        dp, cp = device_of(quarter, py, pz)
        mine = dp * 8 + cp == me

        @pl.when(mine)
        def _():
            pltpu.make_async_copy(p_ref.at[grain], ref.at[spot, slot], recv).start()

        @pl.when(jnp.logical_not(mine))
        def _():
            pltpu.make_async_remote_copy(
                src_ref=p_ref.at[grain],
                dst_ref=ref.at[spot, slot],
                send_sem=sem,
                recv_sem=recv,
                device_id=(dp, cp),
                device_id_type=MESH,
            ).start()

    def sent(grain, ref, spot, slot, quarter, py, pz, sem, recv):
        dp, cp = device_of(quarter, py, pz)

        @pl.when(dp * 8 + cp != me)
        def _():
            pltpu.make_async_copy(p_ref.at[grain], p_ref.at[grain], sem).wait()

    def headed(act, grain):
        table = me * sz.block + grain
        part = table // sz.width_grains
        inner = table % sz.width_grains
        head = inner // sz.head_grains
        rest = inner % sz.head_grains

        def one(quarter, sem):
            local = part * sz.part_grains + (head // 4) * sz.head_grains + rest
            spot = local // sz.qkv
            act(grain, qkv_ref, spot, local % sz.qkv, quarter, spot % 2, spot // 2, sem, kind_sems.at[0])

        @pl.when(table < sz.out_start)
        def _():
            one(head % 4, spread_sems.at[grain])

            @pl.when(head == sz.heads - 1)
            def _():
                for quarter in range(1, 4):
                    one(quarter, spread_sems.at[sz.block + (quarter - 1) * sz.head_grains + rest])

    def outward(act, grain):
        local = me * sz.block + grain - sz.out_start

        def one(quarter, inner, sem):
            spot = inner // sz.out
            act(grain, out_ref, spot, inner % sz.out, quarter, spot // 4, spot % 4, sem, kind_sems.at[1])

        @pl.when(jnp.logical_and(local >= 0, local < sz.width_grains))
        def _():
            one(local // sz.part_grains, local % sz.part_grains, spread_sems.at[grain])

            @pl.when(local < sz.spill)
            def _():
                one(3, sz.part_grains - sz.spill + local, spread_sems.at[sz.block + 3 * sz.head_grains + local])

    def plain(act, grain, base, turn, ref, recv):
        offset = me * sz.block + grain - base

        @pl.when(jnp.logical_and(offset >= 0, offset < 32 * sz.mlp))
        def _():
            local = offset // 4
            py, u = spot_of_range(local // sz.mlp)
            act(
                grain, ref, py * 4 + u, local % sz.mlp, offset % 4, py, (u + turn) % 4,
                spread_sems.at[grain], recv,
            )

    def heads(act):
        def one(grain, _):
            headed(act, grain)
            return 0

        lax.fori_loop(0, sz.block, one, 0)

    def others(act):
        def one(grain, _):
            outward(act, grain)
            plain(act, grain, sz.fc_start, sz.fc_turn, fc_ref, kind_sems.at[2])
            plain(act, grain, sz.proj_start, sz.proj_turn, proj_ref, kind_sems.at[3])
            return 0

        lax.fori_loop(0, sz.block, one, 0)

    owner = sz.vec_start // sz.block
    spot = sz.vec_start % sz.block

    def vector_sends(act):
        @pl.when(me == owner)
        def _():
            def to(device, _):
                @pl.when(device != me)
                def _():
                    act(
                        pltpu.make_async_remote_copy(
                            src_ref=p_ref.at[pl.ds(spot, sz.vec)],
                            dst_ref=vec_ref,
                            send_sem=spread_sems.at[sz.block + 3 * sz.head_grains + sz.spill + device],
                            recv_sem=kind_sems.at[4],
                            device_id=(device // 8, device % 8),
                            device_id_type=MESH,
                        )
                    )

                return 0

            lax.fori_loop(0, 32, to, 0)

    heads(send)
    tok.start()
    mine = slot_qkv(y, z)
    pltpu.make_async_copy(qkv_ref.at[mine], qkv_ref.at[mine], kind_sems.at[0]).wait()
    weights = PlaceGather(wires, qkv_ref, slot_qkv)
    weights.start()
    vector_sends(lambda copy: copy.start())

    @pl.when(me == owner)
    def _():
        pltpu.make_async_copy(p_ref.at[pl.ds(spot, sz.vec)], vec_ref, kind_sems.at[4]).start()

    others(send)
    cot.start()
    weights.forward()
    tok.forward()
    cot.forward()
    heads(sent)
    others(sent)
    vector_sends(lambda copy: copy.wait_send())
    for index, (ref, slot) in enumerate(
        ((out_ref, slot_out), (fc_ref, slot_turned(sz.fc_turn)), (proj_ref, slot_turned(sz.proj_turn)))
    ):
        view = ref.at[slot(y, z)]
        pltpu.make_async_copy(view, view, kind_sems.at[index + 1]).wait()
    pltpu.make_async_copy(vec_ref, vec_ref, kind_sems.at[4]).wait()
    tok.finish()
    cot.finish()
    weights.finish()


HBM = pl.BlockSpec(memory_space=pl.ANY)
VMEM = pl.BlockSpec(memory_space=pltpu.VMEM)
REMOTE = pltpu.CompilerParams(has_side_effects=True)


def remote_params(ident=None, vmem=None):
    return pltpu.CompilerParams(has_side_effects=True, collective_id=ident, vmem_limit_bytes=vmem)


def greet(partners):
    barrier = pltpu.get_barrier_semaphore()
    for dp, cp in partners:
        pl.semaphore_signal(barrier, inc=1, device_id=(dp, cp), device_id_type=MESH)
    pl.semaphore_wait(barrier, len(partners))


def cost(us):
    return pl.CostEstimate(flops=0, bytes_accessed=int(us * 3.0e6), transcendentals=0)


def wire_sems(count):
    return [pltpu.SemaphoreType.DMA((count,)), pltpu.SemaphoreType.DMA((count,))]


def open_call(sz, table, tokens, cotangent):
    rows, width = tokens.shape

    def like(*shape):
        return jax.ShapeDtypeStruct(shape + (width,), table.dtype)

    return pl.pallas_call(
        functools.partial(open_kernel, sz),
        out_shape=(
            like(8, sz.qkv, GRAIN),
            like(8, sz.out, GRAIN),
            like(8, sz.mlp, GRAIN),
            like(8, sz.mlp, GRAIN),
            like(sz.vec, GRAIN),
            like(2, 2, rows),
            like(2, 2, rows),
        ),
        in_specs=[HBM, VMEM, VMEM],
        out_specs=[HBM] * 7,
        scratch_shapes=[
            pltpu.SemaphoreType.DMA((sz.block + 3 * sz.head_grains + sz.spill + 32,)),
            pltpu.SemaphoreType.DMA((5,)),
            *wire_sems(16),
            pltpu.SemaphoreType.DMA((2,)),
        ],
        compiler_params=REMOTE,
        name="open",
    )(table, tokens, cotangent)


def forward_kernel(
    heads, size, fc_turn, proj_turn, q_ref, kv_ref, out_in, fc_in, proj_in,
    mix_ref, lse_ref, before_ref, mixed_ref, out_ref, fc_ref, proj_ref, out_all,
    stage, send_sems, recv_sems, local_sems,
):
    y, c, z, x = my_place()
    dp, cp = lax.axis_index("dp"), lax.axis_index("cp")
    wires = Wires(send_sems, recv_sems)
    part = heads * size
    rows = q_ref.shape[0] // 2
    blk = 128
    scale = size**-0.5
    odd = z % 2 == 1
    w_out = PlaceGather(wires, out_ref, slot_out)
    w_fc = PlaceGather(wires, fc_ref, slot_turned(fc_turn))
    w_proj = PlaceGather(wires, proj_ref, slot_turned(proj_turn), along=False)
    others = [(c, 1 - x), (1 - c, x), (1 - c, 1 - x)]
    quad = [(y * 2 + tc, z * 2 + tx) for tc, tx in others]
    greet(w_out.partners() + quad)
    keys = wires.to(kv_ref, before_ref, dp, (cp + 2) % 8)

    w_out.start()
    w_fc.start()

    def own(group, _):
        start = group * rows
        for i in range(rows // blk):
            here = pl.ds(pl.multiple_of(start + i * blk, blk), blk)
            seen = (i + 1) * blk
            keys_at = pl.ds(pl.multiple_of(start, rows), seen)
            lane = lax.broadcasted_iota(jnp.int32, (blk, seen), 1)
            line = lax.broadcasted_iota(jnp.int32, (blk, seen), 0)
            allowed = lane <= line + i * blk
            for h in range(heads):
                cols = slice(h * size, (h + 1) * size)
                vals = slice(part + h * size, part + (h + 1) * size)
                s = dot_nt(q_ref[here, cols], kv_ref[keys_at, cols]) * scale
                s = jnp.where(allowed, s, MASKED)
                top = jnp.max(s, axis=-1, keepdims=True)
                p = jnp.exp(s - top)
                total = jnp.sum(p, axis=-1, keepdims=True)
                mix_ref[here, cols] = dot_nn(p.astype(jnp.bfloat16), kv_ref[keys_at, vals]) / total
                lse_ref[here, h : h + 1] = top + jnp.log(total)
        return 0

    lax.fori_loop(0, 2, own, 0)
    w_out.forward()

    @pl.when(jnp.logical_not(odd))
    def _():
        keys.start()

    w_fc.forward((1,))

    def add_before(index, _):
        here = pl.ds(pl.multiple_of(index * blk, blk), blk)
        keys_at = pl.ds(pl.multiple_of((index * blk) // rows * rows, rows), rows)
        for h in range(heads):
            cols = slice(h * size, (h + 1) * size)
            vals = slice(part + h * size, part + (h + 1) * size)
            s = dot_nt(q_ref[here, cols], before_ref[keys_at, cols]) * scale
            lse = lse_ref[here, h : h + 1]
            top = jnp.maximum(lse, jnp.max(s, axis=-1, keepdims=True))
            p = jnp.exp(s - top)
            kept = jnp.exp(lse - top)
            total = kept + jnp.sum(p, axis=-1, keepdims=True)
            mix = mix_ref[here, cols] * kept + dot_nn(p.astype(jnp.bfloat16), before_ref[keys_at, vals])
            mix_ref[here, cols] = mix / total
            lse_ref[here, h : h + 1] = top + jnp.log(total)
        return 0

    w_out.finish()
    whole = QuadGather(wires, out_ref, out_all, local_sems.at[0])
    whole.start()

    @pl.when(z < 3)
    def _():
        w_fc.forward((2,))

    @pl.when(odd)
    def _():
        keys.wait_recv()
        lax.fori_loop(0, 2 * rows // blk, add_before, 0)

    def round_off(index, _):
        here = pl.ds(pl.multiple_of(index * blk, blk), blk)
        stage[here, :] = mix_ref[here, :].astype(stage.dtype)
        return 0

    lax.fori_loop(0, 2 * rows // blk, round_off, 0)

    @pl.when(z == 3)
    def _():
        w_fc.forward((2,))

    w_proj.start_over()
    mine = c * 2 + x
    each = rows // 2
    swaps = []
    for (tc, tx), (tdp, tcp) in zip(others, quad):
        block = stage.at[pl.ds(pl.multiple_of((tc * 2 + tx) * each, each), each)]
        swaps.append(wires.to(block, mixed_ref.at[mine], tdp, tcp))
    for copy in swaps:
        copy.start()
    local = pltpu.make_async_copy(
        stage.at[pl.ds(pl.multiple_of(mine * each, each), each)], mixed_ref.at[mine], local_sems.at[1]
    )
    local.start()
    w_fc.forward((3,))
    whole.forward()
    for copy in swaps:
        copy.wait_recv()
    whole.finish()
    w_fc.finish()
    w_proj.over[0].wait_recv()
    w_proj.over[0].wait_send()
    for copy in swaps:
        copy.wait_send()
    local.wait()

    @pl.when(jnp.logical_not(odd))
    def _():
        keys.wait_send()


def forward_call(sz, q, kv, w_out, w_fc, w_proj):
    part = sz.part
    rows = q.shape[0]

    def like(value, *lead):
        return jax.ShapeDtypeStruct(lead + value.shape, value.dtype)

    return pl.pallas_call(
        functools.partial(forward_kernel, sz.quarter_heads, sz.head_size, sz.fc_turn, sz.proj_turn),
        out_shape=(
            jax.ShapeDtypeStruct((rows, part), jnp.float32),
            jax.ShapeDtypeStruct((rows, 8), jnp.float32),
            like(kv),
            jax.ShapeDtypeStruct((4, rows // 4, part), jnp.bfloat16),
            like(w_out),
            like(w_fc),
            like(w_proj),
            like(w_out, 2, 2),
        ),
        in_specs=[VMEM, VMEM, HBM, HBM, HBM],
        out_specs=[VMEM] * 4 + [HBM] * 4,
        input_output_aliases={2: 4, 3: 5, 4: 6},
        scratch_shapes=[
            pltpu.VMEM((rows, part), jnp.bfloat16),
            *wire_sems(37),
            pltpu.SemaphoreType.DMA((2,)),
        ],
        cost_estimate=cost(120),
        compiler_params=remote_params(1, 56 << 20),
        name="forward",
    )(q, kv, w_out, w_fc, w_proj)


def acts_kernel(proj_turn, act_ref, proj_in, act_all, proj_ref, send_sems, recv_sems, local_sem):
    wires = Wires(send_sems, recv_sems)
    quad = QuadGather(wires, act_ref, act_all, local_sem)
    places = PlaceGather(wires, proj_ref, slot_turned(proj_turn), over=False)
    greet(places.partners() + [quad.over_x, quad.over_c])
    quad.start()
    places.start()
    quad.forward()
    places.forward()
    quad.finish()
    places.finish()


def grads_kernel(act_ref, act_all, send_sems, recv_sems, local_sem):
    wires = Wires(send_sems, recv_sems)
    quad = QuadGather(wires, act_ref, act_all, local_sem)
    greet([quad.over_x, quad.over_c])
    quad.start()
    quad.forward()
    quad.finish()


def grads_call(act, ident):
    return pl.pallas_call(
        grads_kernel,
        out_shape=jax.ShapeDtypeStruct((2, 2) + act.shape, act.dtype),
        in_specs=[VMEM],
        out_specs=HBM,
        scratch_shapes=[*wire_sems(3), pltpu.SemaphoreType.DMA],
        cost_estimate=cost(25),
        compiler_params=remote_params(ident),
        name="grads",
    )(act)


def acts_call(sz, act, w_proj):
    return pl.pallas_call(
        functools.partial(acts_kernel, sz.proj_turn),
        out_shape=(
            jax.ShapeDtypeStruct((2, 2) + act.shape, act.dtype),
            jax.ShapeDtypeStruct(w_proj.shape, w_proj.dtype),
        ),
        in_specs=[VMEM, HBM],
        out_specs=[HBM] * 2,
        input_output_aliases={1: 1},
        scratch_shapes=[*wire_sems(13), pltpu.SemaphoreType.DMA],
        cost_estimate=cost(60),
        compiler_params=remote_params(2),
        name="acts",
    )(act, w_proj)


class QuadSum:
    step = 32

    def __init__(self, in_ref, out_ref, got_c, stage, got_x, send_sems, recv_sems):
        self.y, self.c, self.z, self.x = my_place()
        dp, cp = lax.axis_index("dp"), lax.axis_index("cp")
        wires = Wires(send_sems, recv_sems)
        self.in_ref, self.out_ref, self.got_c, self.stage, self.got_x = in_ref, out_ref, got_c, stage, got_x
        self.partners = [(dp + 1 - 2 * self.c, cp), (dp, cp + 1 - 2 * self.x)]
        self.by_c = wires.to(in_ref.at[1 - self.c], got_c, *self.partners[0])
        self.by_x = wires.to(stage, got_x, *self.partners[1])

    def each(self, act):
        def one(index, _):
            act(pl.ds(pl.multiple_of(index * self.step, self.step), self.step))
            return 0

        lax.fori_loop(0, self.out_ref.shape[0] // self.step, one, 0)

    def start(self):
        greet(self.partners)
        self.by_c.start()

    def middle(self):
        c, x = self.c, self.x
        self.by_c.wait_recv()

        def to_send(span):
            self.stage[span, :] = (
                self.in_ref[c, 1 - x, span, :].astype(jnp.float32) + self.got_c[1 - x, span, :].astype(jnp.float32)
            ).astype(self.stage.dtype)

        self.each(to_send)
        self.by_x.start()

    def finish(self):
        c, x = self.c, self.x
        self.by_x.wait_recv()

        def to_add(span):
            self.out_ref[span, :] = (
                self.in_ref[c, x, span, :].astype(jnp.float32)
                + self.got_c[x, span, :].astype(jnp.float32)
                + self.got_x[span, :].astype(jnp.float32)
            )

        self.each(to_add)
        self.by_c.wait_send()
        self.by_x.wait_send()


def quad_sum_kernel(*refs):
    quad = QuadSum(*refs)
    quad.start()
    quad.middle()
    quad.finish()


def quad_scratch(partial):
    rows, width = partial.shape[2:]
    return [
        pltpu.VMEM((2, rows, width), partial.dtype),
        pltpu.VMEM((rows, width), partial.dtype),
        pltpu.VMEM((rows, width), partial.dtype),
        *wire_sems(2),
    ]


def quad_sum(partial, ident):
    return pl.pallas_call(
        quad_sum_kernel,
        out_shape=jax.ShapeDtypeStruct(partial.shape[2:], jnp.float32),
        in_specs=[VMEM],
        out_specs=VMEM,
        scratch_shapes=quad_scratch(partial),
        compiler_params=remote_params(ident),
        cost_estimate=cost(30),
        name="quad_sum",
    )(partial)


class Collector:
    def __init__(self, sz):
        self.sz = sz
        self.y, self.c, self.z, self.x = my_place()
        self.me = flat_id(self.y, self.c, self.z, self.x)
        self.quarter = self.c * 2 + self.x

    def send(self, src, dst, table, sem, recv):
        dest = table // self.sz.block

        @pl.when(dest == self.me)
        def _():
            pltpu.make_async_copy(src, dst, recv).start()

        @pl.when(dest != self.me)
        def _():
            pltpu.make_async_remote_copy(
                src_ref=src,
                dst_ref=dst,
                send_sem=sem,
                recv_sem=recv,
                device_id=(dest // 8, dest % 8),
                device_id_type=MESH,
            ).start()

    def sent(self, src, dst, table, sem, recv):
        @pl.when(table // self.sz.block != self.me)
        def _():
            pltpu.make_async_copy(src, src, sem).wait()

    def received(self, first, count, view, recv):
        block = self.sz.block
        for device in range(first // block, -(-(first + count) // block)):
            grains = min(first + count, (device + 1) * block) - max(first, device * block)

            @pl.when(self.me == device)
            def _():
                pltpu.make_async_copy(view(grains), view(grains), recv).wait()


def collect_mlp_kernel(sz, fc_ref, proj_ref, g_ref, send_sems, recv_sem):
    to = Collector(sz)

    def run(act):
        for ref, base, turn, first_sem in (
            (fc_ref, sz.fc_start, sz.fc_turn, 0), (proj_ref, sz.proj_start, sz.proj_turn, sz.mlp)
        ):
            r = range_of_spot(to.y, (to.z + 4 - turn) % 4)

            def one(slot, _):
                table = base + 4 * (r * sz.mlp + slot) + to.quarter
                act(ref.at[slot], g_ref.at[table % sz.block], table, send_sems.at[first_sem + slot], recv_sem)
                return 0

            lax.fori_loop(0, sz.mlp, one, 0)

    run(to.send)
    run(to.sent)
    to.received(sz.fc_start, 64 * sz.mlp, lambda n: g_ref.at[pl.ds(0, n)], recv_sem)


def collect_mlp(sz, fc, proj):
    return pl.pallas_call(
        functools.partial(collect_mlp_kernel, sz),
        out_shape=jax.ShapeDtypeStruct((sz.block, GRAIN, fc.shape[-1]), fc.dtype),
        in_specs=[HBM] * 2,
        out_specs=HBM,
        scratch_shapes=[pltpu.SemaphoreType.DMA((2 * sz.mlp,)), pltpu.SemaphoreType.DMA],
        cost_estimate=cost(30),
        compiler_params=REMOTE,
        name="collect_mlp",
    )(fc, proj)


def collect_rest_kernel(
    sz, qkv_ref, out_ref, vec_ref, g_ref, outs_ref, vecs_ref, qkv_sems, out_sems, vec_sems, recv_sems
):
    to = Collector(sz)
    out_share = out_ref.shape[0]

    def run(act):
        def heads(slot, _):
            local = slot_qkv(to.y, to.z) * sz.qkv + slot
            inner = local % sz.part_grains
            head = 4 * (inner // sz.head_grains) + to.quarter

            @pl.when(head < sz.heads)
            def _():
                table = (local // sz.part_grains) * sz.width_grains + head * sz.head_grains + inner % sz.head_grains
                act(qkv_ref.at[slot], g_ref.at[table % sz.block], table, qkv_sems.at[slot], recv_sems.at[0])

            return 0

        lax.fori_loop(0, sz.qkv, heads, 0)

        def outward(slot, _):
            table = sz.out_start + slot_out(to.y, to.z) * out_share + slot
            dst = outs_ref.at[to.quarter, table % sz.block]
            act(out_ref.at[slot], dst, table, out_sems.at[slot], recv_sems.at[1])
            return 0

        lax.fori_loop(0, out_share, outward, 0)

    last = sz.vec_start // sz.block
    vec_copy = pltpu.make_async_remote_copy(
        src_ref=vec_ref,
        dst_ref=vecs_ref.at[to.me],
        send_sem=vec_sems.at[0],
        recv_sem=vec_sems.at[1],
        device_id=(last // 8, last % 8),
        device_id_type=MESH,
    )

    @pl.when(to.me != last)
    def _():
        vec_copy.start()

    @pl.when(to.me == last)
    def _():
        pltpu.make_async_copy(vec_ref, vecs_ref.at[to.me], vec_sems.at[1]).start()

    run(to.send)
    run(to.sent)

    @pl.when(to.me != last)
    def _():
        vec_copy.wait_send()

    @pl.when(to.me == last)
    def _():
        pltpu.make_async_copy(vecs_ref, vecs_ref, vec_sems.at[1]).wait()

    to.received(0, 3 * sz.width_grains, lambda n: g_ref.at[pl.ds(0, n)], recv_sems.at[0])
    to.received(sz.out_start, sz.width_grains, lambda n: outs_ref.at[:, pl.ds(0, n)], recv_sems.at[1])


def collect_rest(sz, qkv, out, vectors):
    def like(value, *lead):
        return jax.ShapeDtypeStruct(lead + value.shape[-2:], value.dtype)

    return pl.pallas_call(
        functools.partial(collect_rest_kernel, sz),
        out_shape=(like(qkv, sz.block), like(out, 4, sz.block), like(vectors, 32, sz.vec)),
        in_specs=[HBM] * 3,
        out_specs=[HBM] * 3,
        scratch_shapes=[
            pltpu.SemaphoreType.DMA((sz.qkv,)),
            pltpu.SemaphoreType.DMA((out.shape[0],)),
            pltpu.SemaphoreType.DMA((2,)),
            pltpu.SemaphoreType.DMA((2,)),
        ],
        cost_estimate=cost(30),
        compiler_params=REMOTE,
        name="collect_rest",
    )(qkv, out, vectors)


def attend_back_kernel(heads, size, own, *refs):
    if own:
        q_ref, kv_ref, do_ref, mix_ref, lse_ref, seed_ref, dq_ref, dkv_ref = refs
    else:
        q_ref, kv_ref, do_ref, mix_ref, lse_ref, term_ref, dq_ref, dkv_ref, sum_ref = refs[:9]
        quad = QuadSum(term_ref, sum_ref, *refs[-5:])
        quad.start()
    _, _, z, _ = my_place()
    part = heads * size
    rows = q_ref.shape[0] // 2
    blk = 128
    scale = size**-0.5

    def visit(here, start, seen, allowed):
        keys_at = pl.ds(start, seen)
        for h in range(heads):
            cols = slice(h * size, (h + 1) * size)
            vals = slice(part + h * size, part + (h + 1) * size)
            q = q_ref[here, cols]
            k = kv_ref[keys_at, cols]
            do = do_ref[here, cols]
            s = dot_nt(q, k) * scale
            p = jnp.exp(s - lse_ref[here, h : h + 1])
            if own:
                p = jnp.where(allowed, p, 0.0)
            dp = dot_nt(do, kv_ref[keys_at, vals])
            delta = jnp.sum(do.astype(jnp.float32) * mix_ref[here, cols], axis=-1, keepdims=True)
            ds = (p * (dp - delta)).astype(jnp.bfloat16)
            dq = dot_nn(ds, k) * scale
            if own:
                dq = dq + seed_ref[here, cols]
            dq_ref[here, cols] = dq.astype(dq_ref.dtype)
            dkv_ref[keys_at, cols] += dot_tn(ds, q) * scale
            dkv_ref[keys_at, vals] += dot_tn(p.astype(jnp.bfloat16), do)

    def group(index):
        start = pl.multiple_of(index * rows, rows)
        if not own:

            def block(i, _):
                visit(pl.ds(pl.multiple_of(start + i * blk, blk), blk), start, rows, None)
                return 0

            lax.fori_loop(0, rows // blk, block, 0)
            return
        for i in range(rows // blk):
            seen = (i + 1) * blk
            lane = lax.broadcasted_iota(jnp.int32, (blk, seen), 1)
            line = lax.broadcasted_iota(jnp.int32, (blk, seen), 0)
            visit(pl.ds(pl.multiple_of(start + i * blk, blk), blk), start, seen, lane <= line + i * blk)

    def clear(index, _):
        here = pl.ds(pl.multiple_of(index * blk, blk), blk)
        dkv_ref[here, :] = jnp.zeros((blk, dkv_ref.shape[1]), dkv_ref.dtype)
        if not own:
            dq_ref[here, :] = jnp.zeros((blk, dq_ref.shape[1]), dq_ref.dtype)
        return 0

    lax.fori_loop(0, 2 * rows // blk, clear, 0)

    def one(index, _):
        if own:
            group(index)
        else:

            @pl.when(z % 2 == 1)
            def _():
                group(index)

            @pl.when(index == 0)
            def _():
                quad.middle()

        return 0

    lax.fori_loop(0, 2, one, 0)
    if not own:
        quad.finish()


def attend_back(sz, q, kv, grad_mix, mix, lse, seed=None, term=None, ident=None):
    own = term is None
    operands = [q, kv, grad_mix, mix, lse, seed if own else term]
    out_shape = [
        jax.ShapeDtypeStruct(q.shape, jnp.bfloat16 if own else jnp.float32),
        jax.ShapeDtypeStruct(kv.shape, jnp.float32),
    ]
    if not own:
        out_shape.append(jax.ShapeDtypeStruct(term.shape[2:], jnp.float32))
    params = pltpu.CompilerParams(vmem_limit_bytes=56 << 20) if own else remote_params(ident, 56 << 20)
    return pl.pallas_call(
        functools.partial(attend_back_kernel, sz.quarter_heads, sz.head_size, own),
        out_shape=out_shape,
        in_specs=[VMEM] * len(operands),
        out_specs=[VMEM] * len(out_shape),
        scratch_shapes=[] if own else quad_scratch(term),
        cost_estimate=cost(35),
        compiler_params=params,
        name="attend_back_own" if own else "attend_back_before",
    )(*operands)


def rowwise(value):
    return with_layout_constraint(value, Layout(major_to_minor=(0, 1)))


def norm_parts(values):
    mean = jnp.mean(values, axis=-1, keepdims=True)
    centre = values - mean
    rs = lax.rsqrt(jnp.mean(centre * centre, axis=-1, keepdims=True) + EPSILON)
    return centre * rs, rs


def norm_back(normed, rs, grad, gain):
    e = grad * gain
    return rs * (
        e
        - jnp.mean(e, axis=-1, keepdims=True)
        - normed * jnp.mean(e * normed, axis=-1, keepdims=True)
    )


def per_device_quad(tokens, params, out_grad, lengths):
    rows, width = tokens.shape
    hidden = FF
    sz = Sizes(width, hidden, HEADS, HEAD_DIM, params.shape[0])
    y, c, z, x = my_place()
    quarter = c * 2 + x
    bf16, f32 = jnp.bfloat16, jnp.float32

    def pick(value, index):
        return lax.dynamic_index_in_dim(value, index, 0, keepdims=False)

    def halves_of(value):
        half = value.shape[1] // 2
        first, second = value[:, :half], value[:, half:]
        return jnp.where(y == 0, first, second), jnp.where(y == 0, second, first)

    def to_other_y(sent):
        return over_y(sent.astype(bf16))

    def to_places(kept, got, turn=0):
        summed = kept.astype(f32) + got.astype(f32)
        summed = summed.reshape(4, summed.shape[0] // 4, -1)
        total = pick(summed, (z + 4 - turn) % 4)
        for d in (1, 2, 3):
            got = over_z(pick(summed, (z + d + 4 - turn) % 4).astype(bf16), d)
            total = total + got.astype(f32)
        return total

    w_qkv, w_out, w_fc, w_proj, vec, tok_all, cot_all = open_call(
        sz, params.reshape(sz.block, GRAIN, width), tokens, out_grad
    )
    flat = lambda value: value.reshape(-1, width)
    vectors = flat(vec).astype(f32)
    fc_bias = vectors[8 : 8 + hidden // width].reshape(hidden)
    w_qkv, cot_all = flat(w_qkv), flat(cot_all)
    normed_all, _ = norm_parts(flat(tok_all).astype(f32))
    act_one = (normed_all * vectors[0] + vectors[1]).astype(bf16)

    def quarter_of(vector):
        padded = jnp.pad(vector, (0, 4 * sz.part - width)).reshape(sz.quarter_heads, 4, sz.head_size)
        return lax.dynamic_index_in_dim(padded, quarter, 1, keepdims=False).reshape(sz.part)

    kv_bias = jnp.concatenate([jnp.zeros((sz.part,), f32), quarter_of(vectors[3])])
    kv = (dot_nt(act_one, w_qkv[sz.part :]) + kv_bias).astype(bf16)
    q = (dot_nt(act_one, w_qkv[: sz.part]) + quarter_of(vectors[2])).astype(bf16)
    mix, lse, before, mixed, _, w_fc, w_proj, w_out = forward_call(sz, q, kv, w_out, w_fc, w_proj)
    w_fc, w_out = flat(w_fc), flat(w_out)[:width]
    by_quarter = jnp.pad(w_out, ((0, 0), (0, 4 * sz.part - width)))
    by_quarter = by_quarter.reshape(width, sz.quarter_heads, 4, sz.head_size)
    w_out_own = lax.dynamic_index_in_dim(by_quarter, quarter, 2, keepdims=False).reshape(width, sz.part)
    by_head = (sz.quarter_heads, sz.head_size)
    mixed = jnp.transpose(mixed.reshape((4, rows) + by_head), (1, 2, 0, 3)).reshape(rows, 4 * sz.part)[:, :width]
    inputs = tokens.astype(f32)
    residual = inputs + (dot_nt(mixed, w_out) + vectors[4])
    normed_two, rs_two = norm_parts(residual)
    act_two, w_proj = acts_call(sz, (normed_two * vectors[5] + vectors[6]).astype(bf16), w_proj)
    act_two, w_proj = flat(act_two), flat(w_proj)
    bias = lax.dynamic_index_in_dim(fc_bias.reshape(-1, 4, GRAIN), quarter, 1, keepdims=False)
    bias = bias.reshape(8, hidden // 32)[jnp.array(RANGES)].reshape(hidden // 4)
    pre_act = dot_nt(act_two, w_fc) + bias
    act_hidden, pull_gelu = jax.vjp(gelu_tanh, pre_act)
    act_hidden = act_hidden.astype(bf16)
    hid_mine, hid_other = halves_of(act_hidden)
    got_proj = to_other_y(dot_tn(hid_other, cot_all))
    grad_fc = pull_gelu(dot_nt(cot_all, w_proj))[0].astype(bf16)
    fc_mine, fc_other = halves_of(grad_fc)
    got_fc = to_other_y(dot_tn(fc_other, act_two))
    grad_two = quad_sum(rowwise(dot_nn(grad_fc, w_fc).astype(bf16)).reshape(2, 2, rows, width), 7)

    cot = out_grad.astype(f32)
    grad_res = cot + norm_back(normed_two, rs_two, grad_two, vectors[5])
    grad_attn = grad_res.astype(bf16)
    attn_all = flat(grads_call(grad_attn, 3))
    grad_mix = rowwise(dot_nn(attn_all, w_out_own).astype(bf16))
    g_proj = to_places(dot_tn(hid_mine, cot_all), got_proj, sz.proj_turn)
    partial_out = rowwise(dot_nn(act_hidden, w_proj).astype(bf16)).reshape(2, 2, rows, width)
    dq_before, dkv_before, out_sum = attend_back(
        sz, q, before, grad_mix, mix, lse, term=partial_out, ident=4
    )
    output = (residual + out_sum + vectors[7]).astype(bf16)
    returned = permute(dkv_before.astype(bf16), lambda py, pc, pz, px: (py, pc, pz - 1, px) if pz % 2 == 1 else None)
    g_out = rowwise(dot_tn(attn_all, mix.astype(bf16)).astype(bf16)).reshape(2, width // 2, sz.part)
    got_out = to_other_y(pick(g_out, 1 - y))
    g_fc = to_places(dot_tn(fc_mine, act_two), got_fc, sz.fc_turn)
    dq, dkv = attend_back(sz, q, kv, grad_mix, mix, lse, seed=dq_before)
    grad_qkv = jnp.concatenate([dq, (dkv + returned.astype(f32)).astype(bf16)], axis=1)
    g_qkv = rowwise(dot_tn(grad_qkv, act_one).astype(bf16)).reshape(4, 2, 3 * sz.part // 8, width)
    half_qkv = lambda index: lax.dynamic_index_in_dim(g_qkv, index, 1, keepdims=False).reshape(-1, width)
    got_qkv = to_other_y(half_qkv(1 - y))
    partial_one = rowwise(dot_nn(grad_qkv, w_qkv).astype(bf16))
    grad_one = quad_sum(partial_one.reshape(2, 2, rows, width), 6)
    g_out = to_places(pick(g_out, y), got_out)
    g_qkv = to_places(half_qkv(y), got_qkv)
    grains = lambda value: value.astype(bf16).reshape(-1, GRAIN, value.shape[-1])
    table_mlp = collect_mlp(sz, grains(g_fc), grains(g_proj))

    normed_one, rs_one = norm_parts(inputs)
    input_grad = (grad_res + norm_back(normed_one, rs_one, grad_one, vectors[0])).astype(bf16)

    def placed(vector):
        spread = jnp.zeros((sz.quarter_heads, 4, sz.head_size), f32)
        spread = lax.dynamic_update_slice_in_dim(spread, vector.reshape(-1, 1, sz.head_size), quarter, 1)
        return spread.reshape(4 * sz.part)[:width]

    sums = jnp.sum(grad_qkv.astype(f32), axis=0)
    bias_sum = jnp.sum(grad_fc.astype(f32), axis=0).reshape(8, hidden // 32)[jnp.array(SPOTS)]
    fc_rows = lax.dynamic_update_slice_in_dim(
        jnp.zeros((hidden // 4 // GRAIN, 4, GRAIN), f32), bias_sum.reshape(-1, 1, GRAIN), quarter, 1
    )
    grad_vectors = jnp.concatenate(
        [
            jnp.stack(
                [
                    jnp.sum(grad_one * normed_one, axis=0),
                    jnp.sum(grad_one, axis=0),
                    placed(sums[: sz.part]),
                    placed(sums[2 * sz.part :]),
                    jnp.sum(grad_attn.astype(f32), axis=0),
                    jnp.sum(grad_two * normed_two, axis=0),
                    jnp.sum(grad_two, axis=0),
                    jnp.sum(cot, axis=0),
                ]
            ),
            fc_rows.reshape(hidden // width, width),
        ]
    )
    count = grad_vectors.shape[0]
    grad_vectors = jnp.pad(grad_vectors, ((0, sz.vec * GRAIN - count), (0, 0)))
    table_qkv, table_out, all_vectors = collect_rest(
        sz, grains(g_qkv), grains(g_out), grad_vectors.reshape(sz.vec, GRAIN, width)
    )
    grad_vectors = jnp.sum(all_vectors.reshape(32, sz.vec * GRAIN, width), axis=0)[:count]
    table_out = table_out.reshape((4, sz.block * GRAIN) + by_head)
    table_out = jnp.transpose(table_out, (1, 2, 0, 3)).reshape(sz.block * GRAIN, 4 * sz.part)[:, :width]
    me = flat_id(y, c, z, x)
    row = me * (sz.block * GRAIN) + lax.broadcasted_iota(jnp.int32, (sz.block * GRAIN, 1), 0)
    table = jnp.where(
        row < sz.out_start * GRAIN,
        flat(table_qkv),
        jnp.where(row < sz.fc_start * GRAIN, table_out, flat(table_mlp)),
    ).astype(f32)
    used = (sz.vec_start % sz.block) * GRAIN
    tail = jnp.concatenate([grad_vectors, jnp.zeros((sz.block * GRAIN - used - count, width), f32)])
    last = me == sz.vec_start // sz.block
    tail = jnp.where(last, tail, table[used:])
    param_grad = jnp.concatenate([table[:used], tail])
    return (output, input_grad, param_grad)


def fits_quad(mesh, tokens, params, lengths):
    dp, cp = mesh.shape["dp"], mesh.shape["cp"]
    rows = tokens.shape[0] // (dp * cp)
    width = tokens.shape[1]
    blocks = params.shape[0] // (dp * cp)
    return (
        (dp, cp) == (4, 8)
        and lengths.shape[1] == 2
        and rows * cp == lengths.shape[1] * MIN_LEN
        and rows % 128 == 0
        and blocks % GRAIN == 0
        and (HEADS, HEAD_DIM, FF, width) == (25, 64, 6400, 1600)
    )


def solution(mesh):
    in_specs = (P(("dp", "cp"), None), P(("dp", "cp"), None), P(("dp", "cp"), None), P("dp", None))
    out_specs = (P(("dp", "cp"), None), P(("dp", "cp"), None), P(("dp", "cp"), None))

    def step(tokens, params, out_grad, lengths):
        body = per_device_quad if fits_quad(mesh, tokens, params, lengths) else per_device_general

        return jax.shard_map(
            body, mesh=mesh, in_specs=in_specs, out_specs=out_specs, check_vma=False
        )(tokens, params, out_grad, lengths)

    return step
```

```python
import functools

import jax
import jax.numpy as jnp
from jax import lax
from jax.experimental import pallas as pl
from jax.experimental.layout import Layout, with_layout_constraint
from jax.experimental.pallas import tpu as pltpu
from jax.sharding import PartitionSpec as P


HEADS = 25
FF = 6400
HEAD_DIM = 64
TILE = 128
MIN_LEN = 1024
MAX_LEN = 4096


EPSILON = 1e-05
MASKED = -1e30
GELU_SCALE = 0.7978845608028654


def from_behind(value, axis, by):
    length = lax.axis_size(axis)
    pairs = [(i, i + by) for i in range(length) if 0 <= i + by < length]
    return lax.ppermute(value, axis, pairs)


def layer_norm(values, gain_row, bias_row):
    centre = values - jnp.mean(values, axis=-1, keepdims=True)
    spread = jnp.mean(centre * centre, axis=-1, keepdims=True)
    return centre * lax.rsqrt(spread + EPSILON) * gain_row + bias_row


def gelu_tanh(values):
    return (
        0.5 * values * (1.0 + jnp.tanh(GELU_SCALE * (values + 0.044715 * values * values * values)))
    )


def segment_of(position, seq_ends):
    return jnp.sum((position[:, None] >= seq_ends[None, :]).astype(jnp.int32), axis=1)


def unpack(gathered, model_width, hidden):
    out_end = 4 * model_width
    fc_end = out_end + hidden
    proj_end = fc_end + hidden
    vec_end = proj_end + 8
    return (
        gathered[0 : 3 * model_width],
        gathered[3 * model_width : out_end],
        gathered[out_end:fc_end],
        gathered[fc_end:proj_end],
        gathered[proj_end:vec_end].astype(jnp.float32),
        gathered[vec_end : vec_end + hidden // model_width].astype(jnp.float32).reshape(hidden),
    )


def matmul_nt(left_mat, right_mat):
    return lax.dot_general(
        left_mat, right_mat, (((1,), (1,)), ((), ())), preferred_element_type=jnp.float32
    )


def matmul_tn(left_mat, right_mat):
    return lax.dot_general(
        left_mat, right_mat, (((0,), (0,)), ((), ())), preferred_element_type=jnp.float32
    )


def matmul_nn(left_mat, right_mat):
    return jnp.dot(left_mat, right_mat, preferred_element_type=jnp.float32)


def per_device_general(tokens, params, out_grad, lengths):
    tok_rows, model_width = tokens.shape
    hidden = FF
    head_count = HEADS
    head_size = HEAD_DIM
    cp_count = lax.axis_size("cp")
    group_rows = tok_rows * cp_count
    seq_count = lengths.shape[1]
    longest = min(MAX_LEN, group_rows - (seq_count - 1) * MIN_LEN)
    reach_back = min(cp_count - 1, (longest + tok_rows - TILE - 1) // tok_rows)
    pair_count = (reach_back + 2) // 2
    score_scale = head_size ** (-0.5)
    gathered = lax.all_gather(params, ("dp", "cp"), axis=0, tiled=True)
    w_attn, w_out, w_fc, w_proj, vectors, fc_bias = unpack(gathered, model_width, hidden)
    inputs = tokens.astype(jnp.float32)
    act_one = layer_norm(inputs, vectors[0], vectors[1]).astype(jnp.bfloat16)
    qkv_bias = jnp.concatenate([vectors[2], jnp.zeros_like(vectors[2]), vectors[3]])
    qkv = (matmul_nt(act_one, w_attn) + qkv_bias).astype(jnp.bfloat16)
    queries = qkv[:, :model_width].reshape(tok_rows, head_count, head_size)
    key_value = qkv[:, model_width:]
    device = lax.axis_index("cp")
    seq_ends = jnp.cumsum(lengths[0])
    query_pos = device * tok_rows + jnp.arange(tok_rows, dtype=jnp.int32)
    query_seg = segment_of(query_pos, seq_ends)
    store = jnp.zeros((2 * pair_count, tok_rows, 2 * model_width), jnp.bfloat16)
    store = store.at[0].set(key_value)

    def fetch(step_index, state_pair):
        moving, held_rows = state_pair
        moving = from_behind(moving, "cp", 1)
        return (moving, lax.dynamic_update_index_in_dim(held_rows, moving, step_index, 0))

    _, store = lax.fori_loop(1, reach_back + 1, fetch, (key_value, store))

    def pair_mask(pair_index):
        owners = 2 * pair_index + jnp.arange(2, dtype=jnp.int32)
        key_pos = (
            (device - owners)[:, None] * tok_rows + jnp.arange(tok_rows, dtype=jnp.int32)[None, :]
        ).reshape(2 * tok_rows)
        usable = jnp.broadcast_to((owners <= reach_back)[:, None], (2, tok_rows)).reshape(
            2 * tok_rows
        ) & (key_pos >= 0)
        key_seg = segment_of(key_pos, seq_ends)
        return (
            (key_seg[None, :] == query_seg[:, None])
            & (key_pos[None, :] <= query_pos[:, None])
            & usable[None, :]
        )

    def pair_rows(pair_index):
        block_rows = lax.dynamic_slice_in_dim(store, 2 * pair_index, 2, 0).reshape(
            2 * tok_rows, 2 * model_width
        )
        return (
            block_rows[:, :model_width].reshape(2 * tok_rows, head_count, head_size),
            block_rows[:, model_width:].reshape(2 * tok_rows, head_count, head_size),
        )

    def pair_scores(key_rows, allowed):
        raw_scores = (
            jnp.einsum("qhd,khd->hqk", queries, key_rows, preferred_element_type=jnp.float32)
            * score_scale
        )
        return jnp.where(allowed[None], raw_scores, MASKED)

    def visit(work):

        def step_pair(pair_index, running):
            allowed = pair_mask(pair_index)
            result = work(pair_index, allowed, running)
            return result

        return step_pair

    def add_total(pair_index, allowed, running):
        row_top, summed = running
        key_rows, _ = pair_rows(pair_index)
        scores = pair_scores(key_rows, allowed)
        new_top = jnp.maximum(row_top, jnp.max(scores, axis=-1, keepdims=True))
        summed = summed * jnp.exp(row_top - new_top) + jnp.sum(
            jnp.exp(scores - new_top), axis=-1, keepdims=True
        )
        return (new_top, summed)

    start_top = jnp.full((head_count, tok_rows, 1), MASKED, jnp.float32)
    start_sum = jnp.zeros((head_count, tok_rows, 1), jnp.float32)
    row_top, summed = lax.fori_loop(0, pair_count, visit(add_total), (start_top, start_sum))
    log_total = row_top + jnp.log(summed)

    def add_mix(pair_index, allowed, running):
        key_rows, value_rows = pair_rows(pair_index)
        prob_rows = jnp.exp(pair_scores(key_rows, allowed) - log_total).astype(jnp.bfloat16)
        return running + jnp.einsum(
            "hqk,khd->qhd", prob_rows, value_rows, preferred_element_type=jnp.float32
        )

    mixed_full = lax.fori_loop(
        0, pair_count, visit(add_mix), jnp.zeros((tok_rows, head_count, head_size), jnp.float32)
    )
    mixed = mixed_full.reshape(tok_rows, model_width).astype(jnp.bfloat16)
    attn_out = matmul_nt(mixed, w_out) + vectors[4]
    residual = inputs + attn_out
    act_two = layer_norm(residual, vectors[5], vectors[6]).astype(jnp.bfloat16)
    pre_act = matmul_nt(act_two, w_fc) + fc_bias
    act_hidden = gelu_tanh(pre_act).astype(jnp.bfloat16)
    output = (residual + matmul_nn(act_hidden, w_proj) + vectors[7]).astype(jnp.bfloat16)
    gathered = lax.all_gather(params, ("dp", "cp"), axis=0, tiled=True)
    w_attn, w_out, w_fc, w_proj, vectors, fc_bias = unpack(gathered, model_width, hidden)
    grad_out_f = out_grad.astype(jnp.float32)
    grad_hidden = matmul_nt(out_grad, w_proj)
    _, pull_gelu = jax.vjp(gelu_tanh, pre_act)
    grad_fc = pull_gelu(grad_hidden)[0].astype(jnp.bfloat16)
    grad_act_two = matmul_nn(grad_fc, w_fc)
    _, pull_two = jax.vjp(layer_norm, residual, vectors[5], vectors[6])
    grad_res_norm, grad_gain_two, grad_bias_two = pull_two(grad_act_two)
    grad_res = grad_out_f + grad_res_norm
    grad_attn = grad_res.astype(jnp.bfloat16)
    grad_mix = (
        matmul_nn(grad_attn, w_out).astype(jnp.bfloat16).reshape(tok_rows, head_count, head_size)
    )
    grad_dot = jnp.transpose(jnp.sum(grad_mix.astype(jnp.float32) * mixed_full, axis=-1), (1, 0))[
        :, :, None
    ]

    def add_grads(pair_index, allowed, running):
        grad_query, grad_store = running
        key_rows, value_rows = pair_rows(pair_index)
        prob_rows = jnp.exp(pair_scores(key_rows, allowed) - log_total)
        grad_probs = jnp.einsum(
            "qhd,khd->hqk", grad_mix, value_rows, preferred_element_type=jnp.float32
        )
        grad_scores = (prob_rows * (grad_probs - grad_dot)).astype(jnp.bfloat16)
        grad_query = (
            grad_query
            + jnp.einsum("hqk,khd->qhd", grad_scores, key_rows, preferred_element_type=jnp.float32)
            * score_scale
        )
        grad_keys = (
            jnp.einsum("hqk,qhd->khd", grad_scores, queries, preferred_element_type=jnp.float32)
            * score_scale
        )
        grad_values = jnp.einsum(
            "hqk,qhd->khd",
            prob_rows.astype(jnp.bfloat16),
            grad_mix,
            preferred_element_type=jnp.float32,
        )
        pair_grad = jnp.concatenate(
            [
                grad_keys.reshape(2 * tok_rows, model_width),
                grad_values.reshape(2 * tok_rows, model_width),
            ],
            axis=1,
        )
        pair_grad = pair_grad.reshape(2, tok_rows, 2 * model_width)
        grad_store = lax.dynamic_update_slice_in_dim(grad_store, pair_grad, 2 * pair_index, 0)
        return (grad_query, grad_store)

    start_query = jnp.zeros((tok_rows, head_count, head_size), jnp.float32)
    start_store = jnp.zeros((2 * pair_count, tok_rows, 2 * model_width), jnp.float32)
    grad_query, grad_store = lax.fori_loop(
        0, pair_count, visit(add_grads), (start_query, start_store)
    )

    def send_back(step_index, moving):
        moving = moving + lax.dynamic_index_in_dim(
            grad_store, reach_back - step_index, 0, keepdims=False
        )
        return from_behind(moving.astype(jnp.bfloat16), "cp", -1).astype(moving.dtype)

    returned = lax.fori_loop(
        0, reach_back, send_back, jnp.zeros((tok_rows, 2 * model_width), jnp.float32)
    )
    grad_kv = returned + grad_store[0]
    grad_qkv = jnp.concatenate([grad_query.reshape(tok_rows, model_width), grad_kv], axis=1).astype(
        jnp.bfloat16
    )
    grad_qkv_f = grad_qkv.astype(jnp.float32)
    grad_act_one = matmul_nn(grad_qkv, w_attn)
    _, pull_one = jax.vjp(layer_norm, inputs, vectors[0], vectors[1])
    grad_in_norm, grad_gain_one, grad_bias_one = pull_one(grad_act_one)
    input_grad = (grad_res + grad_in_norm).astype(jnp.bfloat16)
    grad_vectors = jnp.stack(
        [
            grad_gain_one,
            grad_bias_one,
            jnp.sum(grad_qkv_f[:, :model_width], axis=0),
            jnp.sum(grad_qkv_f[:, 2 * model_width :], axis=0),
            jnp.sum(grad_attn.astype(jnp.float32), axis=0),
            grad_gain_two,
            grad_bias_two,
            jnp.sum(grad_out_f, axis=0),
        ]
    )
    grad_fc_bias = jnp.sum(grad_fc.astype(jnp.float32), axis=0).reshape(
        hidden // model_width, model_width
    )
    used_rows = 4 * model_width + 2 * hidden + 8 + hidden // model_width
    total_rows = gathered.shape[0]
    local_grad = jnp.concatenate(
        [
            matmul_tn(grad_qkv, act_one),
            matmul_tn(grad_attn, mixed),
            matmul_tn(grad_fc, act_two),
            matmul_tn(act_hidden, out_grad),
            grad_vectors,
            grad_fc_bias,
            jnp.zeros((total_rows - used_rows, model_width), jnp.float32),
        ],
        axis=0,
    )
    dp_count = lax.axis_size("dp")
    device_count = dp_count * cp_count
    share_rows = total_rows // device_count
    spread_rows = local_grad.reshape(device_count, 1, share_rows, model_width)
    received = lax.all_to_all(
        spread_rows.astype(jnp.bfloat16), ("dp", "cp"), split_axis=0, concat_axis=1, tiled=True
    ).astype(spread_rows.dtype)
    param_grad = jnp.sum(received, axis=1).reshape(share_rows, model_width)
    return (output, input_grad, param_grad)


MESH = pl.DeviceIdType.MESH
GRAIN = 8
NT = (((1,), (1,)), ((), ()))
TN = (((0,), (0,)), ((), ()))


def dot_nt(a, b):
    return lax.dot_general(a, b, NT, preferred_element_type=jnp.float32)


def dot_tn(a, b):
    return lax.dot_general(a, b, TN, preferred_element_type=jnp.float32)


def dot_nn(a, b):
    return jnp.dot(a, b, preferred_element_type=jnp.float32)


def flat_id(y, c, z, x):
    return ((y * 2 + c) * 4 + z) * 2 + x


def permute(value, move):
    pairs = []
    for y in range(2):
        for c in range(2):
            for z in range(4):
                for x in range(2):
                    to = move(y, c, z, x)
                    if to is not None:
                        pairs.append((flat_id(y, c, z, x), flat_id(*to)))
    return lax.ppermute(value, ("dp", "cp"), pairs)


def over_y(value):
    return permute(value, lambda y, c, z, x: (1 - y, c, z, x))


def over_z(value, by):
    return permute(value, lambda y, c, z, x: (y, c, (z + by) % 4, x))


class Sizes:
    def __init__(self, width, hidden, heads, head_size, rows):
        self.heads = heads
        self.head_size = head_size
        self.quarter_heads = -(-heads // 4)
        self.part = self.quarter_heads * head_size
        self.part_grains = self.part // GRAIN
        self.width_grains = width // GRAIN
        self.spill = 4 * self.part_grains - self.width_grains
        self.qkv = 3 * self.part_grains // 8
        self.out = self.part_grains // 8
        self.mlp = hidden // 4 // 8 // GRAIN
        self.block = rows // GRAIN
        self.out_start = 3 * self.width_grains
        self.fc_start = 4 * self.width_grains
        self.proj_start = self.fc_start + hidden // GRAIN
        self.vec_start = self.proj_start + hidden // GRAIN
        self.vec = 2
        self.head_grains = head_size // GRAIN
        self.fc_turn = self.turn(self.fc_start)
        self.proj_turn = self.turn(self.proj_start)

    def turn(self, start):
        return start // (2 * self.block) % 4


def spot_of_range(r):
    y = r // 6 + (r % 2) * ((r // 3) % 2)
    u = (r - (r + 5) // 8 - (r + 3) // 8) % 4
    return y, u


def range_of_spot(y, u):
    first = u + u // 3
    second = (1 - u // 2) * (u + 6) + (u // 2) * (2 * u - 1)
    return (1 - y) * first + y * second


RANGES = (0, 1, 2, 4, 6, 7, 3, 5)
SPOTS = (0, 1, 2, 6, 3, 7, 4, 5)


def slot_qkv(y, z):
    return 2 * z + y


def slot_out(y, z):
    return 4 * y + z


def slot_turned(turn):
    return lambda y, z: 4 * y + (z + 4 - turn) % 4


def my_place():
    dp = lax.axis_index("dp")
    cp = lax.axis_index("cp")
    return dp // 2, dp % 2, cp // 2, cp % 2


def device_of(quarter, y, z):
    return y * 2 + quarter // 2, z * 2 + quarter % 2


class Wires:
    def __init__(self, send_sems, recv_sems):
        self.send_sems = send_sems
        self.recv_sems = recv_sems
        self.count = 0

    def to(self, src, dst, dp, cp):
        index = self.count
        self.count += 1
        return pltpu.make_async_remote_copy(
            src_ref=src,
            dst_ref=dst,
            send_sem=self.send_sems.at[index],
            recv_sem=self.recv_sems.at[index],
            device_id=(dp, cp),
            device_id_type=MESH,
        )


class PlaceGather:
    def __init__(self, wires, full, slot, along=True, over=True):
        self.full = full
        self.dp, self.cp = lax.axis_index("dp"), lax.axis_index("cp")
        self.y, self.z, self.x = self.dp // 2, self.cp // 2, self.cp % 2
        self.above = (self.dp, ((self.z + 1) % 4) * 2 + self.x)
        self.below = (self.dp, ((self.z + 3) % 4) * 2 + self.x)
        self.across = ((self.dp + 2) % 4, self.cp)

        def share(by, to):
            view = full.at[slot(self.y, (self.z + 4 + by) % 4)]
            return wires.to(view, view, *to)

        if along:
            self.up = [share(1 - k, self.above) for k in (1, 2, 3)]
            self.down = [share(k - 1, self.below) for k in (1, 2, 3)]
        self.own_over = share(0, self.across) if over else None
        self.over = [self.own_over] + [share(d, self.across) if along else None for d in (1, 2, 3)]

    def partners(self):
        return [self.above, self.below, self.across]

    def start_over(self):
        self.own_over.start()

    def start(self):
        @pl.when(self.z < 3)
        def _():
            self.up[0].start()

        @pl.when(self.z > 0)
        def _():
            self.down[0].start()

        if self.own_over is not None:
            self.start_over()

    def forward(self, steps=(1, 2, 3)):
        for k in steps:

            @pl.when(self.z >= k)
            def _():
                self.up[k - 1].wait_recv()
                if k < 3:

                    @pl.when(self.z < 3)
                    def _():
                        self.up[k].start()

                self.over[4 - k].start()

            @pl.when(self.z <= 3 - k)
            def _():
                self.down[k - 1].wait_recv()
                if k < 3:

                    @pl.when(self.z > 0)
                    def _():
                        self.down[k].start()

                self.over[k].start()

    def finish(self):
        sent_over = [copy for copy in self.over if copy is not None]
        for copy in sent_over:
            copy.wait_recv()
        for copy in sent_over:
            copy.wait_send()
        for k in (1, 2, 3):

            @pl.when(jnp.logical_and(self.z >= k - 1, self.z < 3))
            def _():
                self.up[k - 1].wait_send()

            @pl.when(jnp.logical_and(self.z <= 4 - k, self.z > 0))
            def _():
                self.down[k - 1].wait_send()


class QuadGather:
    def __init__(self, wires, block, full, local_sem):
        self.wires = wires
        self.block = block
        self.full = full
        self.dp, self.cp = lax.axis_index("dp"), lax.axis_index("cp")
        self.c, self.x = self.dp % 2, self.cp % 2
        self.over_x = (self.dp, self.cp + 1 - 2 * self.x)
        self.over_c = (self.dp + 1 - 2 * self.c, self.cp)
        self.local_sem = local_sem

    def start(self):
        spot = self.full.at[self.c, self.x]
        self.by_x = self.wires.to(self.block, spot, *self.over_x)
        self.by_c = self.wires.to(self.block, spot, *self.over_c)
        self.by_x.start()
        self.by_c.start()
        self.local = pltpu.make_async_copy(self.block, spot, self.local_sem)
        self.local.start()

    def forward(self):
        self.by_x.wait_recv()
        spot = self.full.at[self.c, 1 - self.x]
        self.pass_on = self.wires.to(spot, spot, *self.over_c)
        self.pass_on.start()

    def finish(self):
        self.by_c.wait_recv()
        self.pass_on.wait_recv()
        self.by_x.wait_send()
        self.by_c.wait_send()
        self.pass_on.wait_send()
        self.local.wait()


def open_kernel(
    sz, p_ref, tok_ref, cot_ref, qkv_ref, out_ref, fc_ref, proj_ref, vec_ref, tok_all, cot_all,
    spread_sems, kind_sems, send_sems, recv_sems, local_sems,
):
    y, c, z, x = my_place()
    me = flat_id(y, c, z, x)
    wires = Wires(send_sems, recv_sems)
    tok = QuadGather(wires, tok_ref, tok_all, local_sems.at[0])
    cot = QuadGather(wires, cot_ref, cot_all, local_sems.at[1])

    def send(grain, ref, spot, slot, quarter, py, pz, sem, recv):
        dp, cp = device_of(quarter, py, pz)
        mine = dp * 8 + cp == me

        @pl.when(mine)
        def _():
            pltpu.make_async_copy(p_ref.at[grain], ref.at[spot, slot], recv).start()

        @pl.when(jnp.logical_not(mine))
        def _():
            pltpu.make_async_remote_copy(
                src_ref=p_ref.at[grain],
                dst_ref=ref.at[spot, slot],
                send_sem=sem,
                recv_sem=recv,
                device_id=(dp, cp),
                device_id_type=MESH,
            ).start()

    def sent(grain, ref, spot, slot, quarter, py, pz, sem, recv):
        dp, cp = device_of(quarter, py, pz)

        @pl.when(dp * 8 + cp != me)
        def _():
            pltpu.make_async_copy(p_ref.at[grain], p_ref.at[grain], sem).wait()

    def headed(act, grain):
        table = me * sz.block + grain
        part = table // sz.width_grains
        inner = table % sz.width_grains
        head = inner // sz.head_grains
        rest = inner % sz.head_grains

        def one(quarter, sem):
            local = part * sz.part_grains + (2 * (head // 8) + head % 2) * sz.head_grains + rest
            spot = local // sz.qkv
            act(grain, qkv_ref, spot, local % sz.qkv, quarter, spot % 2, spot // 2, sem, kind_sems.at[0])

        @pl.when(table < sz.out_start)
        def _():
            one((head // 2) % 4, spread_sems.at[grain])

            @pl.when(head == sz.heads - 1)
            def _():
                for quarter in range(1, 4):
                    one(quarter, spread_sems.at[sz.block + (quarter - 1) * sz.head_grains + rest])

    def outward(act, grain):
        local = me * sz.block + grain - sz.out_start

        def one(quarter, inner, sem):
            spot = inner // sz.out
            act(grain, out_ref, spot, inner % sz.out, quarter, spot // 4, spot % 4, sem, kind_sems.at[1])

        @pl.when(jnp.logical_and(local >= 0, local < sz.width_grains))
        def _():
            one(local // sz.part_grains, local % sz.part_grains, spread_sems.at[grain])

            @pl.when(local < sz.spill)
            def _():
                one(3, sz.part_grains - sz.spill + local, spread_sems.at[sz.block + 3 * sz.head_grains + local])

    def plain(act, grain, base, turn, ref, recv):
        offset = me * sz.block + grain - base

        @pl.when(jnp.logical_and(offset >= 0, offset < 32 * sz.mlp))
        def _():
            local = offset // 4
            py, u = spot_of_range(local // sz.mlp)
            act(
                grain, ref, py * 4 + u, local % sz.mlp, offset % 4, py, (u + turn) % 4,
                spread_sems.at[grain], recv,
            )

    def heads(act):
        def one(grain, _):
            headed(act, grain)
            return 0

        lax.fori_loop(0, sz.block, one, 0)

    def others(act):
        def one(grain, _):
            outward(act, grain)
            plain(act, grain, sz.fc_start, sz.fc_turn, fc_ref, kind_sems.at[2])
            plain(act, grain, sz.proj_start, sz.proj_turn, proj_ref, kind_sems.at[3])
            return 0

        lax.fori_loop(0, sz.block, one, 0)

    owner = sz.vec_start // sz.block
    spot = sz.vec_start % sz.block

    def vector_sends(act):
        @pl.when(me == owner)
        def _():
            def to(device, _):
                @pl.when(device != me)
                def _():
                    act(
                        pltpu.make_async_remote_copy(
                            src_ref=p_ref.at[pl.ds(spot, sz.vec)],
                            dst_ref=vec_ref,
                            send_sem=spread_sems.at[sz.block + 3 * sz.head_grains + sz.spill + device],
                            recv_sem=kind_sems.at[4],
                            device_id=(device // 8, device % 8),
                            device_id_type=MESH,
                        )
                    )

                return 0

            lax.fori_loop(0, 32, to, 0)

    heads(send)
    tok.start()
    mine = slot_qkv(y, z)
    pltpu.make_async_copy(qkv_ref.at[mine], qkv_ref.at[mine], kind_sems.at[0]).wait()
    weights = PlaceGather(wires, qkv_ref, slot_qkv)
    weights.start()
    vector_sends(lambda copy: copy.start())

    @pl.when(me == owner)
    def _():
        pltpu.make_async_copy(p_ref.at[pl.ds(spot, sz.vec)], vec_ref, kind_sems.at[4]).start()

    others(send)
    cot.start()
    weights.forward()
    tok.forward()
    cot.forward()
    heads(sent)
    others(sent)
    vector_sends(lambda copy: copy.wait_send())
    for index, (ref, slot) in enumerate(
        ((out_ref, slot_out), (fc_ref, slot_turned(sz.fc_turn)), (proj_ref, slot_turned(sz.proj_turn)))
    ):
        view = ref.at[slot(y, z)]
        pltpu.make_async_copy(view, view, kind_sems.at[index + 1]).wait()
    pltpu.make_async_copy(vec_ref, vec_ref, kind_sems.at[4]).wait()
    tok.finish()
    cot.finish()
    weights.finish()


HBM = pl.BlockSpec(memory_space=pl.ANY)
VMEM = pl.BlockSpec(memory_space=pltpu.VMEM)
REMOTE = pltpu.CompilerParams(has_side_effects=True)


def remote_params(ident=None, vmem=None):
    return pltpu.CompilerParams(has_side_effects=True, collective_id=ident, vmem_limit_bytes=vmem)


def greet(partners):
    barrier = pltpu.get_barrier_semaphore()
    for dp, cp in partners:
        pl.semaphore_signal(barrier, inc=1, device_id=(dp, cp), device_id_type=MESH)
    pl.semaphore_wait(barrier, len(partners))


def cost(us):
    return pl.CostEstimate(flops=0, bytes_accessed=int(us * 3.0e6), transcendentals=0)


def wire_sems(count):
    return [pltpu.SemaphoreType.DMA((count,)), pltpu.SemaphoreType.DMA((count,))]


def open_call(sz, table, tokens, cotangent):
    rows, width = tokens.shape

    def like(*shape):
        return jax.ShapeDtypeStruct(shape + (width,), table.dtype)

    return pl.pallas_call(
        functools.partial(open_kernel, sz),
        out_shape=(
            like(8, sz.qkv, GRAIN),
            like(8, sz.out, GRAIN),
            like(8, sz.mlp, GRAIN),
            like(8, sz.mlp, GRAIN),
            like(sz.vec, GRAIN),
            like(2, 2, rows),
            like(2, 2, rows),
        ),
        in_specs=[HBM, VMEM, VMEM],
        out_specs=[HBM] * 7,
        scratch_shapes=[
            pltpu.SemaphoreType.DMA((sz.block + 3 * sz.head_grains + sz.spill + 32,)),
            pltpu.SemaphoreType.DMA((5,)),
            *wire_sems(16),
            pltpu.SemaphoreType.DMA((2,)),
        ],
        compiler_params=REMOTE,
        name="open",
    )(table, tokens, cotangent)


def forward_kernel(
    heads, size, fc_turn, proj_turn, q_ref, kv_ref, out_in, fc_in, proj_in,
    mix_ref, lse_ref, before_ref, mixed_ref, out_ref, fc_ref, proj_ref, out_all,
    stage, send_sems, recv_sems, local_sems,
):
    y, c, z, x = my_place()
    dp, cp = lax.axis_index("dp"), lax.axis_index("cp")
    wires = Wires(send_sems, recv_sems)
    part = heads * size
    rows = q_ref.shape[0] // 2
    blk = 128
    scale = size**-0.5
    odd = z % 2 == 1
    w_out = PlaceGather(wires, out_ref, slot_out)
    w_fc = PlaceGather(wires, fc_ref, slot_turned(fc_turn))
    w_proj = PlaceGather(wires, proj_ref, slot_turned(proj_turn), along=False)
    others = [(c, 1 - x), (1 - c, x), (1 - c, 1 - x)]
    quad = [(y * 2 + tc, z * 2 + tx) for tc, tx in others]
    greet(w_out.partners() + quad)
    keys = wires.to(kv_ref, before_ref, dp, (cp + 2) % 8)

    w_out.start()
    w_fc.start()

    def own(group, _):
        start = group * rows
        for i in range(rows // blk):
            here = pl.ds(pl.multiple_of(start + i * blk, blk), blk)
            seen = (i + 1) * blk
            keys_at = pl.ds(pl.multiple_of(start, rows), seen)
            lane = lax.broadcasted_iota(jnp.int32, (blk, seen), 1)
            line = lax.broadcasted_iota(jnp.int32, (blk, seen), 0)
            allowed = lane <= line + i * blk
            for h in range(heads):
                cols = slice(h * size, (h + 1) * size)
                vals = slice(part + h * size, part + (h + 1) * size)
                s = dot_nt(q_ref[here, cols], kv_ref[keys_at, cols]) * scale
                s = jnp.where(allowed, s, MASKED)
                top = jnp.max(s, axis=-1, keepdims=True)
                p = jnp.exp(s - top)
                total = jnp.sum(p, axis=-1, keepdims=True)
                mix_ref[here, cols] = dot_nn(p.astype(jnp.bfloat16), kv_ref[keys_at, vals]) / total
                lse_ref[here, h : h + 1] = top + jnp.log(total)
        return 0

    lax.fori_loop(0, 2, own, 0)
    w_out.forward()

    @pl.when(jnp.logical_not(odd))
    def _():
        keys.start()

    w_fc.forward((1,))

    def add_before(index, _):
        here = pl.ds(pl.multiple_of(index * blk, blk), blk)
        keys_at = pl.ds(pl.multiple_of((index * blk) // rows * rows, rows), rows)
        for h in range(heads):
            cols = slice(h * size, (h + 1) * size)
            vals = slice(part + h * size, part + (h + 1) * size)
            s = dot_nt(q_ref[here, cols], before_ref[keys_at, cols]) * scale
            lse = lse_ref[here, h : h + 1]
            top = jnp.maximum(lse, jnp.max(s, axis=-1, keepdims=True))
            p = jnp.exp(s - top)
            kept = jnp.exp(lse - top)
            total = kept + jnp.sum(p, axis=-1, keepdims=True)
            mix = mix_ref[here, cols] * kept + dot_nn(p.astype(jnp.bfloat16), before_ref[keys_at, vals])
            mix_ref[here, cols] = mix / total
            lse_ref[here, h : h + 1] = top + jnp.log(total)
        return 0

    w_out.finish()
    whole = QuadGather(wires, out_ref, out_all, local_sems.at[0])
    whole.start()

    @pl.when(z < 3)
    def _():
        w_fc.forward((2,))

    @pl.when(odd)
    def _():
        keys.wait_recv()
        lax.fori_loop(0, 2 * rows // blk, add_before, 0)

    def round_off(index, _):
        here = pl.ds(pl.multiple_of(index * blk, blk), blk)
        stage[here, :] = mix_ref[here, :].astype(stage.dtype)
        return 0

    lax.fori_loop(0, 2 * rows // blk, round_off, 0)

    @pl.when(z == 3)
    def _():
        w_fc.forward((2,))

    w_proj.start_over()
    mine = c * 2 + x
    each = rows // 2
    swaps = []
    for (tc, tx), (tdp, tcp) in zip(others, quad):
        block = stage.at[pl.ds(pl.multiple_of((tc * 2 + tx) * each, each), each)]
        swaps.append(wires.to(block, mixed_ref.at[mine], tdp, tcp))
    for copy in swaps:
        copy.start()
    local = pltpu.make_async_copy(
        stage.at[pl.ds(pl.multiple_of(mine * each, each), each)], mixed_ref.at[mine], local_sems.at[1]
    )
    local.start()
    w_fc.forward((3,))
    whole.forward()
    for copy in swaps:
        copy.wait_recv()
    whole.finish()
    w_fc.finish()
    w_proj.over[0].wait_recv()
    w_proj.over[0].wait_send()
    for copy in swaps:
        copy.wait_send()
    local.wait()

    @pl.when(jnp.logical_not(odd))
    def _():
        keys.wait_send()


def forward_call(sz, q, kv, w_out, w_fc, w_proj):
    part = sz.part
    rows = q.shape[0]

    def like(value, *lead):
        return jax.ShapeDtypeStruct(lead + value.shape, value.dtype)

    return pl.pallas_call(
        functools.partial(forward_kernel, sz.quarter_heads, sz.head_size, sz.fc_turn, sz.proj_turn),
        out_shape=(
            jax.ShapeDtypeStruct((rows, part), jnp.float32),
            jax.ShapeDtypeStruct((rows, 8), jnp.float32),
            like(kv),
            jax.ShapeDtypeStruct((4, rows // 4, part), jnp.bfloat16),
            like(w_out),
            like(w_fc),
            like(w_proj),
            like(w_out, 2, 2),
        ),
        in_specs=[VMEM, VMEM, HBM, HBM, HBM],
        out_specs=[VMEM] * 4 + [HBM] * 4,
        input_output_aliases={2: 4, 3: 5, 4: 6},
        scratch_shapes=[
            pltpu.VMEM((rows, part), jnp.bfloat16),
            *wire_sems(37),
            pltpu.SemaphoreType.DMA((2,)),
        ],
        cost_estimate=cost(120),
        compiler_params=remote_params(1, 56 << 20),
        name="forward",
    )(q, kv, w_out, w_fc, w_proj)


def acts_kernel(proj_turn, act_ref, proj_in, act_all, proj_ref, send_sems, recv_sems, local_sem):
    wires = Wires(send_sems, recv_sems)
    quad = QuadGather(wires, act_ref, act_all, local_sem)
    places = PlaceGather(wires, proj_ref, slot_turned(proj_turn), over=False)
    greet(places.partners() + [quad.over_x, quad.over_c])
    quad.start()
    places.start()
    quad.forward()
    places.forward()
    quad.finish()
    places.finish()


def grads_kernel(act_ref, act_all, send_sems, recv_sems, local_sem):
    wires = Wires(send_sems, recv_sems)
    quad = QuadGather(wires, act_ref, act_all, local_sem)
    greet([quad.over_x, quad.over_c])
    quad.start()
    quad.forward()
    quad.finish()


def grads_call(act, ident):
    return pl.pallas_call(
        grads_kernel,
        out_shape=jax.ShapeDtypeStruct((2, 2) + act.shape, act.dtype),
        in_specs=[VMEM],
        out_specs=HBM,
        scratch_shapes=[*wire_sems(3), pltpu.SemaphoreType.DMA],
        cost_estimate=cost(25),
        compiler_params=remote_params(ident),
        name="grads",
    )(act)


def acts_call(sz, act, w_proj):
    return pl.pallas_call(
        functools.partial(acts_kernel, sz.proj_turn),
        out_shape=(
            jax.ShapeDtypeStruct((2, 2) + act.shape, act.dtype),
            jax.ShapeDtypeStruct(w_proj.shape, w_proj.dtype),
        ),
        in_specs=[VMEM, HBM],
        out_specs=[HBM] * 2,
        input_output_aliases={1: 1},
        scratch_shapes=[*wire_sems(13), pltpu.SemaphoreType.DMA],
        cost_estimate=cost(60),
        compiler_params=remote_params(2),
        name="acts",
    )(act, w_proj)


class QuadSum:
    step = 32

    def __init__(self, in_ref, out_ref, got_c, stage, got_x, send_sems, recv_sems):
        self.y, self.c, self.z, self.x = my_place()
        dp, cp = lax.axis_index("dp"), lax.axis_index("cp")
        wires = Wires(send_sems, recv_sems)
        self.in_ref, self.out_ref, self.got_c, self.stage, self.got_x = in_ref, out_ref, got_c, stage, got_x
        self.partners = [(dp + 1 - 2 * self.c, cp), (dp, cp + 1 - 2 * self.x)]
        self.by_c = wires.to(in_ref.at[1 - self.c], got_c, *self.partners[0])
        self.by_x = wires.to(stage, got_x, *self.partners[1])

    def each(self, act):
        def one(index, _):
            act(pl.ds(pl.multiple_of(index * self.step, self.step), self.step))
            return 0

        lax.fori_loop(0, self.out_ref.shape[0] // self.step, one, 0)

    def start(self):
        greet(self.partners)
        self.by_c.start()

    def middle(self):
        c, x = self.c, self.x
        self.by_c.wait_recv()

        def to_send(span):
            self.stage[span, :] = (
                self.in_ref[c, 1 - x, span, :].astype(jnp.float32) + self.got_c[1 - x, span, :].astype(jnp.float32)
            ).astype(self.stage.dtype)

        self.each(to_send)
        self.by_x.start()

    def finish(self):
        c, x = self.c, self.x
        self.by_x.wait_recv()

        def to_add(span):
            self.out_ref[span, :] = (
                self.in_ref[c, x, span, :].astype(jnp.float32)
                + self.got_c[x, span, :].astype(jnp.float32)
                + self.got_x[span, :].astype(jnp.float32)
            )

        self.each(to_add)
        self.by_c.wait_send()
        self.by_x.wait_send()


def quad_sum_kernel(*refs):
    quad = QuadSum(*refs)
    quad.start()
    quad.middle()
    quad.finish()


def quad_scratch(partial):
    rows, width = partial.shape[2:]
    return [
        pltpu.VMEM((2, rows, width), partial.dtype),
        pltpu.VMEM((rows, width), partial.dtype),
        pltpu.VMEM((rows, width), partial.dtype),
        *wire_sems(2),
    ]


def quad_sum(partial, ident):
    return pl.pallas_call(
        quad_sum_kernel,
        out_shape=jax.ShapeDtypeStruct(partial.shape[2:], jnp.float32),
        in_specs=[VMEM],
        out_specs=VMEM,
        scratch_shapes=quad_scratch(partial),
        compiler_params=remote_params(ident),
        cost_estimate=cost(30),
        name="quad_sum",
    )(partial)


class Collector:
    def __init__(self, sz):
        self.sz = sz
        self.y, self.c, self.z, self.x = my_place()
        self.me = flat_id(self.y, self.c, self.z, self.x)
        self.quarter = self.c * 2 + self.x

    def send(self, src, dst, table, sem, recv):
        dest = table // self.sz.block

        @pl.when(dest == self.me)
        def _():
            pltpu.make_async_copy(src, dst, recv).start()

        @pl.when(dest != self.me)
        def _():
            pltpu.make_async_remote_copy(
                src_ref=src,
                dst_ref=dst,
                send_sem=sem,
                recv_sem=recv,
                device_id=(dest // 8, dest % 8),
                device_id_type=MESH,
            ).start()

    def sent(self, src, dst, table, sem, recv):
        @pl.when(table // self.sz.block != self.me)
        def _():
            pltpu.make_async_copy(src, src, sem).wait()

    def received(self, first, count, view, recv):
        block = self.sz.block
        for device in range(first // block, -(-(first + count) // block)):
            grains = min(first + count, (device + 1) * block) - max(first, device * block)

            @pl.when(self.me == device)
            def _():
                pltpu.make_async_copy(view(grains), view(grains), recv).wait()


def collect_mlp_kernel(sz, fc_ref, proj_ref, out_ref, g_ref, outs_ref, send_sems, out_sems, recv_sems):
    to = Collector(sz)
    recv_sem = recv_sems.at[0]
    out_share = out_ref.shape[0]

    def run(act):
        for ref, base, turn, first_sem in (
            (fc_ref, sz.fc_start, sz.fc_turn, 0), (proj_ref, sz.proj_start, sz.proj_turn, sz.mlp)
        ):
            r = range_of_spot(to.y, (to.z + 4 - turn) % 4)

            def one(slot, _):
                table = base + 4 * (r * sz.mlp + slot) + to.quarter
                act(ref.at[slot], g_ref.at[table % sz.block], table, send_sems.at[first_sem + slot], recv_sem)
                return 0

            lax.fori_loop(0, sz.mlp, one, 0)

        def outward(slot, _):
            table = sz.out_start + slot_out(to.y, to.z) * out_share + slot
            dst = outs_ref.at[to.quarter, table % sz.block]
            act(out_ref.at[slot], dst, table, out_sems.at[slot], recv_sems.at[1])
            return 0

        lax.fori_loop(0, out_share, outward, 0)

    run(to.send)
    run(to.sent)
    to.received(sz.fc_start, 64 * sz.mlp, lambda n: g_ref.at[pl.ds(0, n)], recv_sem)
    to.received(sz.out_start, sz.width_grains, lambda n: outs_ref.at[:, pl.ds(0, n)], recv_sems.at[1])


def collect_mlp(sz, fc, proj, out):
    return pl.pallas_call(
        functools.partial(collect_mlp_kernel, sz),
        out_shape=(
            jax.ShapeDtypeStruct((sz.block, GRAIN, fc.shape[-1]), fc.dtype),
            jax.ShapeDtypeStruct((4, sz.block, GRAIN, out.shape[-1]), out.dtype),
        ),
        in_specs=[HBM] * 3,
        out_specs=[HBM] * 2,
        scratch_shapes=[
            pltpu.SemaphoreType.DMA((2 * sz.mlp,)),
            pltpu.SemaphoreType.DMA((out.shape[0],)),
            pltpu.SemaphoreType.DMA((2,)),
        ],
        cost_estimate=cost(30),
        compiler_params=REMOTE,
        name="collect_mlp",
    )(fc, proj, out)


def collect_rest_kernel(
    sz, qkv_ref, vec_ref, g_ref, vecs_ref, qkv_sems, vec_sems, recv_sem
):
    to = Collector(sz)

    def run(act):
        def heads(slot, _):
            local = slot_qkv(to.y, to.z) * sz.qkv + slot
            inner = local % sz.part_grains
            index = inner // sz.head_grains
            head = 8 * (index // 2) + 2 * to.quarter + index % 2

            @pl.when(head < sz.heads)
            def _():
                table = (local // sz.part_grains) * sz.width_grains + head * sz.head_grains + inner % sz.head_grains
                act(qkv_ref.at[slot], g_ref.at[table % sz.block], table, qkv_sems.at[slot], recv_sem)

            return 0

        lax.fori_loop(0, sz.qkv, heads, 0)

    last = sz.vec_start // sz.block
    vec_copy = pltpu.make_async_remote_copy(
        src_ref=vec_ref,
        dst_ref=vecs_ref.at[to.me],
        send_sem=vec_sems.at[0],
        recv_sem=vec_sems.at[1],
        device_id=(last // 8, last % 8),
        device_id_type=MESH,
    )

    @pl.when(to.me != last)
    def _():
        vec_copy.start()

    @pl.when(to.me == last)
    def _():
        pltpu.make_async_copy(vec_ref, vecs_ref.at[to.me], vec_sems.at[1]).start()

    run(to.send)
    run(to.sent)

    @pl.when(to.me != last)
    def _():
        vec_copy.wait_send()

    @pl.when(to.me == last)
    def _():
        pltpu.make_async_copy(vecs_ref, vecs_ref, vec_sems.at[1]).wait()

    to.received(0, 3 * sz.width_grains, lambda n: g_ref.at[pl.ds(0, n)], recv_sem)


def collect_rest(sz, qkv, vectors):
    def like(value, *lead):
        return jax.ShapeDtypeStruct(lead + value.shape[-2:], value.dtype)

    return pl.pallas_call(
        functools.partial(collect_rest_kernel, sz),
        out_shape=(like(qkv, sz.block), like(vectors, 32, sz.vec)),
        in_specs=[HBM] * 2,
        out_specs=[HBM] * 2,
        scratch_shapes=[
            pltpu.SemaphoreType.DMA((sz.qkv,)),
            pltpu.SemaphoreType.DMA((2,)),
            pltpu.SemaphoreType.DMA,
        ],
        cost_estimate=cost(30),
        compiler_params=REMOTE,
        name="collect_rest",
    )(qkv, vectors)


def attend_back_kernel(heads, size, own, *refs):
    if own:
        q_ref, kv_ref, do_ref, mix_ref, lse_ref, seed_ref, dq_ref, dkv_ref = refs
    else:
        q_ref, kv_ref, do_ref, mix_ref, lse_ref, term_ref, dq_ref, dkv_ref, sum_ref = refs[:9]
        quad = QuadSum(term_ref, sum_ref, *refs[-5:])
        quad.start()
    _, _, z, _ = my_place()
    part = heads * size
    rows = q_ref.shape[0] // 2
    blk = 128
    scale = size**-0.5

    def visit(here, start, seen, allowed):
        keys_at = pl.ds(start, seen)
        for h in range(heads):
            cols = slice(h * size, (h + 1) * size)
            vals = slice(part + h * size, part + (h + 1) * size)
            q = q_ref[here, cols]
            k = kv_ref[keys_at, cols]
            do = do_ref[here, cols]
            s = dot_nt(q, k) * scale
            p = jnp.exp(s - lse_ref[here, h : h + 1])
            if own:
                p = jnp.where(allowed, p, 0.0)
            dp = dot_nt(do, kv_ref[keys_at, vals])
            delta = jnp.sum(do.astype(jnp.float32) * mix_ref[here, cols], axis=-1, keepdims=True)
            ds = (p * (dp - delta)).astype(jnp.bfloat16)
            dq = dot_nn(ds, k) * scale
            if own:
                dq = dq + seed_ref[here, cols]
            dq_ref[here, cols] = dq.astype(dq_ref.dtype)
            dkv_ref[keys_at, cols] += dot_tn(ds, q) * scale
            dkv_ref[keys_at, vals] += dot_tn(p.astype(jnp.bfloat16), do)

    def group(index):
        start = pl.multiple_of(index * rows, rows)
        if not own:

            def block(i, _):
                visit(pl.ds(pl.multiple_of(start + i * blk, blk), blk), start, rows, None)
                return 0

            lax.fori_loop(0, rows // blk, block, 0)
            return
        for i in range(rows // blk):
            seen = (i + 1) * blk
            lane = lax.broadcasted_iota(jnp.int32, (blk, seen), 1)
            line = lax.broadcasted_iota(jnp.int32, (blk, seen), 0)
            visit(pl.ds(pl.multiple_of(start + i * blk, blk), blk), start, seen, lane <= line + i * blk)

    def clear(index, _):
        here = pl.ds(pl.multiple_of(index * blk, blk), blk)
        dkv_ref[here, :] = jnp.zeros((blk, dkv_ref.shape[1]), dkv_ref.dtype)
        if not own:
            dq_ref[here, :] = jnp.zeros((blk, dq_ref.shape[1]), dq_ref.dtype)
        return 0

    lax.fori_loop(0, 2 * rows // blk, clear, 0)

    def one(index, _):
        if own:
            group(index)
        else:

            @pl.when(z % 2 == 1)
            def _():
                group(index)

            @pl.when(index == 0)
            def _():
                quad.middle()

        return 0

    lax.fori_loop(0, 2, one, 0)
    if not own:
        quad.finish()


def attend_back(sz, q, kv, grad_mix, mix, lse, seed=None, term=None, ident=None):
    own = term is None
    operands = [q, kv, grad_mix, mix, lse, seed if own else term]
    out_shape = [
        jax.ShapeDtypeStruct(q.shape, jnp.bfloat16 if own else jnp.float32),
        jax.ShapeDtypeStruct(kv.shape, jnp.float32),
    ]
    if not own:
        out_shape.append(jax.ShapeDtypeStruct(term.shape[2:], jnp.float32))
    params = pltpu.CompilerParams(vmem_limit_bytes=56 << 20) if own else remote_params(ident, 56 << 20)
    return pl.pallas_call(
        functools.partial(attend_back_kernel, sz.quarter_heads, sz.head_size, own),
        out_shape=out_shape,
        in_specs=[VMEM] * len(operands),
        out_specs=[VMEM] * len(out_shape),
        scratch_shapes=[] if own else quad_scratch(term),
        cost_estimate=cost(35),
        compiler_params=params,
        name="attend_back_own" if own else "attend_back_before",
    )(*operands)


def rowwise(value):
    return with_layout_constraint(value, Layout(major_to_minor=(0, 1)))


def norm_parts(values):
    mean = jnp.mean(values, axis=-1, keepdims=True)
    centre = values - mean
    rs = lax.rsqrt(jnp.mean(centre * centre, axis=-1, keepdims=True) + EPSILON)
    return centre * rs, rs


def norm_back(normed, rs, grad, gain):
    e = grad * gain
    return rs * (
        e
        - jnp.mean(e, axis=-1, keepdims=True)
        - normed * jnp.mean(e * normed, axis=-1, keepdims=True)
    )


def per_device_quad(tokens, params, out_grad, lengths):
    rows, width = tokens.shape
    hidden = FF
    sz = Sizes(width, hidden, HEADS, HEAD_DIM, params.shape[0])
    y, c, z, x = my_place()
    quarter = c * 2 + x
    bf16, f32 = jnp.bfloat16, jnp.float32

    def pick(value, index):
        return lax.dynamic_index_in_dim(value, index, 0, keepdims=False)

    def halves_of(value):
        half = value.shape[1] // 2
        first, second = value[:, :half], value[:, half:]
        return jnp.where(y == 0, first, second), jnp.where(y == 0, second, first)

    def to_other_y(sent):
        return over_y(sent.astype(bf16))

    def to_places(kept, got, turn=0):
        summed = kept.astype(f32) + got.astype(f32)
        summed = summed.reshape(4, summed.shape[0] // 4, -1)
        total = pick(summed, (z + 4 - turn) % 4)
        for d in (1, 2, 3):
            got = over_z(pick(summed, (z + d + 4 - turn) % 4).astype(bf16), d)
            total = total + got.astype(f32)
        return total

    w_qkv, w_out, w_fc, w_proj, vec, tok_all, cot_all = open_call(
        sz, params.reshape(sz.block, GRAIN, width), tokens, out_grad
    )
    flat = lambda value: value.reshape(-1, width)
    vectors = flat(vec).astype(f32)
    fc_bias = vectors[8 : 8 + hidden // width].reshape(hidden)
    w_qkv, cot_all = flat(w_qkv), flat(cot_all)
    normed_all, _ = norm_parts(flat(tok_all).astype(f32))
    act_one = (normed_all * vectors[0] + vectors[1]).astype(bf16)

    pair = 2 * sz.head_size
    turns = width // (4 * pair)
    rest = width - 4 * turns * pair

    def quarter_of(value):
        blocks = [lax.dynamic_slice_in_dim(value, (4 * j + quarter) * pair, pair, 1) for j in range(turns)]
        end = value[:, width - rest :]
        return jnp.concatenate(blocks + [jnp.where(quarter == 0, end, jnp.zeros_like(end))], axis=1)

    def by_head(quarters):
        blocks = [quarters[k][:, j * pair : (j + 1) * pair] for j in range(turns) for k in range(4)]
        return jnp.concatenate(blocks + [quarters[0][:, turns * pair : turns * pair + rest]], axis=1)

    biases = quarter_of(vectors[2:4])
    kv_bias = jnp.concatenate([jnp.zeros((sz.part,), f32), biases[1]])
    kv = (dot_nt(act_one, w_qkv[sz.part :]) + kv_bias).astype(bf16)
    q = (dot_nt(act_one, w_qkv[: sz.part]) + biases[0]).astype(bf16)
    mix, lse, before, mixed, _, w_fc, w_proj, w_out = forward_call(sz, q, kv, w_out, w_fc, w_proj)
    w_fc, w_out = flat(w_fc), flat(w_out)[:width]
    mixed = by_head(mixed)
    inputs = tokens.astype(f32)
    residual = inputs + (dot_nt(mixed, w_out) + vectors[4])
    normed_two, rs_two = norm_parts(residual)
    act_two, w_proj = acts_call(sz, (normed_two * vectors[5] + vectors[6]).astype(bf16), w_proj)
    act_two, w_proj = flat(act_two), flat(w_proj)
    bias = lax.dynamic_index_in_dim(fc_bias.reshape(-1, 4, GRAIN), quarter, 1, keepdims=False)
    bias = bias.reshape(8, hidden // 32)[jnp.array(RANGES)].reshape(hidden // 4)
    pre_act = dot_nt(act_two, w_fc) + bias
    act_hidden, pull_gelu = jax.vjp(gelu_tanh, pre_act)
    act_hidden = act_hidden.astype(bf16)
    hid_mine, hid_other = halves_of(act_hidden)
    got_proj = to_other_y(dot_tn(hid_other, cot_all))
    grad_fc = pull_gelu(dot_nt(cot_all, w_proj))[0].astype(bf16)
    fc_mine, fc_other = halves_of(grad_fc)
    got_fc = to_other_y(dot_tn(fc_other, act_two))
    grad_two = quad_sum(rowwise(dot_nn(grad_fc, w_fc).astype(bf16)).reshape(2, 2, rows, width), 7)

    cot = out_grad.astype(f32)
    grad_res = cot + norm_back(normed_two, rs_two, grad_two, vectors[5])
    grad_attn = grad_res.astype(bf16)
    attn_all = flat(grads_call(grad_attn, 3))
    grad_mix = rowwise(dot_nn(attn_all, w_out).astype(bf16))
    grad_mix = rowwise(quarter_of(grad_mix))
    g_proj = to_places(dot_tn(hid_mine, cot_all), got_proj, sz.proj_turn)
    partial_out = rowwise(dot_nn(act_hidden, w_proj).astype(bf16)).reshape(2, 2, rows, width)
    dq_before, dkv_before, out_sum = attend_back(
        sz, q, before, grad_mix, mix, lse, term=partial_out, ident=4
    )
    output = (residual + out_sum + vectors[7]).astype(bf16)
    returned = permute(
        dkv_before.astype(bf16), lambda py, pc, pz, px: (py, pc, pz - 1, px) if pz % 2 == 1 else None
    )
    g_out = rowwise(dot_tn(attn_all, mix.astype(bf16)).astype(bf16)).reshape(2, width // 2, sz.part)
    got_out = to_other_y(pick(g_out, 1 - y))
    g_fc = to_places(dot_tn(fc_mine, act_two), got_fc, sz.fc_turn)
    dq, dkv = attend_back(sz, q, kv, grad_mix, mix, lse, seed=dq_before)
    grad_qkv = jnp.concatenate([dq, (dkv + returned.astype(f32)).astype(bf16)], axis=1)
    g_qkv = rowwise(dot_tn(grad_qkv, act_one).astype(bf16)).reshape(4, 2, 3 * sz.part // 8, width)
    half_qkv = lambda index: lax.dynamic_index_in_dim(g_qkv, index, 1, keepdims=False).reshape(-1, width)
    got_qkv = to_other_y(half_qkv(1 - y))
    partial_one = rowwise(dot_nn(grad_qkv, w_qkv).astype(bf16))
    grad_one = quad_sum(partial_one.reshape(2, 2, rows, width), 6)
    g_out = to_places(pick(g_out, y), got_out)
    g_qkv = to_places(half_qkv(y), got_qkv)
    grains = lambda value: value.astype(bf16).reshape(-1, GRAIN, value.shape[-1])
    table_mlp, table_out = collect_mlp(sz, grains(g_fc), grains(g_proj), grains(g_out))
    table_out = by_head(table_out.reshape(4, -1, sz.part))

    normed_one, rs_one = norm_parts(inputs)
    input_grad = (grad_res + norm_back(normed_one, rs_one, grad_one, vectors[0])).astype(bf16)

    def placed(vector):
        spread = jnp.zeros((1, width), f32)
        for j in range(turns):
            block = vector[None, j * pair : (j + 1) * pair]
            spread = lax.dynamic_update_slice_in_dim(spread, block, (4 * j + quarter) * pair, 1)
        end = jnp.where(quarter == 0, vector[turns * pair : turns * pair + rest], 0.0)
        return jnp.concatenate([spread[0, : width - rest], end])

    sums = jnp.sum(grad_qkv.astype(f32), axis=0)
    bias_sum = jnp.sum(grad_fc.astype(f32), axis=0).reshape(8, hidden // 32)[jnp.array(SPOTS)]
    fc_rows = lax.dynamic_update_slice_in_dim(
        jnp.zeros((hidden // 4 // GRAIN, 4, GRAIN), f32), bias_sum.reshape(-1, 1, GRAIN), quarter, 1
    )
    grad_vectors = jnp.concatenate(
        [
            jnp.stack(
                [
                    jnp.sum(grad_one * normed_one, axis=0),
                    jnp.sum(grad_one, axis=0),
                    placed(sums[: sz.part]),
                    placed(sums[2 * sz.part :]),
                    jnp.sum(grad_attn.astype(f32), axis=0),
                    jnp.sum(grad_two * normed_two, axis=0),
                    jnp.sum(grad_two, axis=0),
                    jnp.sum(cot, axis=0),
                ]
            ),
            fc_rows.reshape(hidden // width, width),
        ]
    )
    count = grad_vectors.shape[0]
    grad_vectors = jnp.pad(grad_vectors, ((0, sz.vec * GRAIN - count), (0, 0)))
    table_qkv, all_vectors = collect_rest(sz, grains(g_qkv), grad_vectors.reshape(sz.vec, GRAIN, width))
    grad_vectors = jnp.sum(all_vectors.reshape(32, sz.vec * GRAIN, width), axis=0)[:count]
    me = flat_id(y, c, z, x)
    row = me * (sz.block * GRAIN) + lax.broadcasted_iota(jnp.int32, (sz.block * GRAIN, 1), 0)
    table = jnp.where(
        row < sz.out_start * GRAIN,
        flat(table_qkv),
        jnp.where(row < sz.fc_start * GRAIN, table_out, flat(table_mlp)),
    ).astype(f32)
    used = (sz.vec_start % sz.block) * GRAIN
    tail = jnp.concatenate([grad_vectors, jnp.zeros((sz.block * GRAIN - used - count, width), f32)])
    last = me == sz.vec_start // sz.block
    tail = jnp.where(last, tail, table[used:])
    param_grad = jnp.concatenate([table[:used], tail])
    return (output, input_grad, param_grad)


def fits_quad(mesh, tokens, params, lengths):
    dp, cp = mesh.shape["dp"], mesh.shape["cp"]
    rows = tokens.shape[0] // (dp * cp)
    width = tokens.shape[1]
    blocks = params.shape[0] // (dp * cp)
    return (
        (dp, cp) == (4, 8)
        and lengths.shape[1] == 2
        and rows * cp == lengths.shape[1] * MIN_LEN
        and rows % 128 == 0
        and blocks % GRAIN == 0
        and (HEADS, HEAD_DIM, FF, width) == (25, 64, 6400, 1600)
    )


def solution(mesh):
    in_specs = (P(("dp", "cp"), None), P(("dp", "cp"), None), P(("dp", "cp"), None), P("dp", None))
    out_specs = (P(("dp", "cp"), None), P(("dp", "cp"), None), P(("dp", "cp"), None))

    def step(tokens, params, out_grad, lengths):
        body = per_device_quad if fits_quad(mesh, tokens, params, lengths) else per_device_general

        return jax.shard_map(
            body, mesh=mesh, in_specs=in_specs, out_specs=out_specs, check_vma=False
        )(tokens, params, out_grad, lengths)

    return step
```

```python
import functools

import jax
import jax.numpy as jnp
from jax import lax
from jax.experimental import pallas as pl
from jax.experimental.layout import Layout, with_layout_constraint
from jax.experimental.pallas import tpu as pltpu
from jax.sharding import PartitionSpec as P


HEADS = 25
FF = 6400
HEAD_DIM = 64
TILE = 128
MIN_LEN = 1024
MAX_LEN = 4096


EPSILON = 1e-05
MASKED = -1e30
GELU_SCALE = 0.7978845608028654


def from_behind(value, axis, by):
    length = lax.axis_size(axis)
    pairs = [(i, i + by) for i in range(length) if 0 <= i + by < length]
    return lax.ppermute(value, axis, pairs)


def layer_norm(values, gain_row, bias_row):
    centre = values - jnp.mean(values, axis=-1, keepdims=True)
    spread = jnp.mean(centre * centre, axis=-1, keepdims=True)
    return centre * lax.rsqrt(spread + EPSILON) * gain_row + bias_row


def gelu_tanh(values):
    return (
        0.5 * values * (1.0 + jnp.tanh(GELU_SCALE * (values + 0.044715 * values * values * values)))
    )


def segment_of(position, seq_ends):
    return jnp.sum((position[:, None] >= seq_ends[None, :]).astype(jnp.int32), axis=1)


def unpack(gathered, model_width, hidden):
    out_end = 4 * model_width
    fc_end = out_end + hidden
    proj_end = fc_end + hidden
    vec_end = proj_end + 8
    return (
        gathered[0 : 3 * model_width],
        gathered[3 * model_width : out_end],
        gathered[out_end:fc_end],
        gathered[fc_end:proj_end],
        gathered[proj_end:vec_end].astype(jnp.float32),
        gathered[vec_end : vec_end + hidden // model_width].astype(jnp.float32).reshape(hidden),
    )


def matmul_nt(left_mat, right_mat):
    return lax.dot_general(
        left_mat, right_mat, (((1,), (1,)), ((), ())), preferred_element_type=jnp.float32
    )


def matmul_tn(left_mat, right_mat):
    return lax.dot_general(
        left_mat, right_mat, (((0,), (0,)), ((), ())), preferred_element_type=jnp.float32
    )


def matmul_nn(left_mat, right_mat):
    return jnp.dot(left_mat, right_mat, preferred_element_type=jnp.float32)


def per_device_general(tokens, params, out_grad, lengths):
    tok_rows, model_width = tokens.shape
    hidden = FF
    head_count = HEADS
    head_size = HEAD_DIM
    cp_count = lax.axis_size("cp")
    group_rows = tok_rows * cp_count
    seq_count = lengths.shape[1]
    longest = min(MAX_LEN, group_rows - (seq_count - 1) * MIN_LEN)
    reach_back = min(cp_count - 1, (longest + tok_rows - TILE - 1) // tok_rows)
    pair_count = (reach_back + 2) // 2
    score_scale = head_size ** (-0.5)
    gathered = lax.all_gather(params, ("dp", "cp"), axis=0, tiled=True)
    w_attn, w_out, w_fc, w_proj, vectors, fc_bias = unpack(gathered, model_width, hidden)
    inputs = tokens.astype(jnp.float32)
    act_one = layer_norm(inputs, vectors[0], vectors[1]).astype(jnp.bfloat16)
    qkv_bias = jnp.concatenate([vectors[2], jnp.zeros_like(vectors[2]), vectors[3]])
    qkv = (matmul_nt(act_one, w_attn) + qkv_bias).astype(jnp.bfloat16)
    queries = qkv[:, :model_width].reshape(tok_rows, head_count, head_size)
    key_value = qkv[:, model_width:]
    device = lax.axis_index("cp")
    seq_ends = jnp.cumsum(lengths[0])
    query_pos = device * tok_rows + jnp.arange(tok_rows, dtype=jnp.int32)
    query_seg = segment_of(query_pos, seq_ends)
    store = jnp.zeros((2 * pair_count, tok_rows, 2 * model_width), jnp.bfloat16)
    store = store.at[0].set(key_value)

    def fetch(step_index, state_pair):
        moving, held_rows = state_pair
        moving = from_behind(moving, "cp", 1)
        return (moving, lax.dynamic_update_index_in_dim(held_rows, moving, step_index, 0))

    _, store = lax.fori_loop(1, reach_back + 1, fetch, (key_value, store))

    def pair_mask(pair_index):
        owners = 2 * pair_index + jnp.arange(2, dtype=jnp.int32)
        key_pos = (
            (device - owners)[:, None] * tok_rows + jnp.arange(tok_rows, dtype=jnp.int32)[None, :]
        ).reshape(2 * tok_rows)
        usable = jnp.broadcast_to((owners <= reach_back)[:, None], (2, tok_rows)).reshape(
            2 * tok_rows
        ) & (key_pos >= 0)
        key_seg = segment_of(key_pos, seq_ends)
        return (
            (key_seg[None, :] == query_seg[:, None])
            & (key_pos[None, :] <= query_pos[:, None])
            & usable[None, :]
        )

    def pair_rows(pair_index):
        block_rows = lax.dynamic_slice_in_dim(store, 2 * pair_index, 2, 0).reshape(
            2 * tok_rows, 2 * model_width
        )
        return (
            block_rows[:, :model_width].reshape(2 * tok_rows, head_count, head_size),
            block_rows[:, model_width:].reshape(2 * tok_rows, head_count, head_size),
        )

    def pair_scores(key_rows, allowed):
        raw_scores = (
            jnp.einsum("qhd,khd->hqk", queries, key_rows, preferred_element_type=jnp.float32)
            * score_scale
        )
        return jnp.where(allowed[None], raw_scores, MASKED)

    def visit(work):

        def step_pair(pair_index, running):
            allowed = pair_mask(pair_index)
            result = work(pair_index, allowed, running)
            return result

        return step_pair

    def add_total(pair_index, allowed, running):
        row_top, summed = running
        key_rows, _ = pair_rows(pair_index)
        scores = pair_scores(key_rows, allowed)
        new_top = jnp.maximum(row_top, jnp.max(scores, axis=-1, keepdims=True))
        summed = summed * jnp.exp(row_top - new_top) + jnp.sum(
            jnp.exp(scores - new_top), axis=-1, keepdims=True
        )
        return (new_top, summed)

    start_top = jnp.full((head_count, tok_rows, 1), MASKED, jnp.float32)
    start_sum = jnp.zeros((head_count, tok_rows, 1), jnp.float32)
    row_top, summed = lax.fori_loop(0, pair_count, visit(add_total), (start_top, start_sum))
    log_total = row_top + jnp.log(summed)

    def add_mix(pair_index, allowed, running):
        key_rows, value_rows = pair_rows(pair_index)
        prob_rows = jnp.exp(pair_scores(key_rows, allowed) - log_total).astype(jnp.bfloat16)
        return running + jnp.einsum(
            "hqk,khd->qhd", prob_rows, value_rows, preferred_element_type=jnp.float32
        )

    mixed_full = lax.fori_loop(
        0, pair_count, visit(add_mix), jnp.zeros((tok_rows, head_count, head_size), jnp.float32)
    )
    mixed = mixed_full.reshape(tok_rows, model_width).astype(jnp.bfloat16)
    attn_out = matmul_nt(mixed, w_out) + vectors[4]
    residual = inputs + attn_out
    act_two = layer_norm(residual, vectors[5], vectors[6]).astype(jnp.bfloat16)
    pre_act = matmul_nt(act_two, w_fc) + fc_bias
    act_hidden = gelu_tanh(pre_act).astype(jnp.bfloat16)
    output = (residual + matmul_nn(act_hidden, w_proj) + vectors[7]).astype(jnp.bfloat16)
    gathered = lax.all_gather(params, ("dp", "cp"), axis=0, tiled=True)
    w_attn, w_out, w_fc, w_proj, vectors, fc_bias = unpack(gathered, model_width, hidden)
    grad_out_f = out_grad.astype(jnp.float32)
    grad_hidden = matmul_nt(out_grad, w_proj)
    _, pull_gelu = jax.vjp(gelu_tanh, pre_act)
    grad_fc = pull_gelu(grad_hidden)[0].astype(jnp.bfloat16)
    grad_act_two = matmul_nn(grad_fc, w_fc)
    _, pull_two = jax.vjp(layer_norm, residual, vectors[5], vectors[6])
    grad_res_norm, grad_gain_two, grad_bias_two = pull_two(grad_act_two)
    grad_res = grad_out_f + grad_res_norm
    grad_attn = grad_res.astype(jnp.bfloat16)
    grad_mix = (
        matmul_nn(grad_attn, w_out).astype(jnp.bfloat16).reshape(tok_rows, head_count, head_size)
    )
    grad_dot = jnp.transpose(jnp.sum(grad_mix.astype(jnp.float32) * mixed_full, axis=-1), (1, 0))[
        :, :, None
    ]

    def add_grads(pair_index, allowed, running):
        grad_query, grad_store = running
        key_rows, value_rows = pair_rows(pair_index)
        prob_rows = jnp.exp(pair_scores(key_rows, allowed) - log_total)
        grad_probs = jnp.einsum(
            "qhd,khd->hqk", grad_mix, value_rows, preferred_element_type=jnp.float32
        )
        grad_scores = (prob_rows * (grad_probs - grad_dot)).astype(jnp.bfloat16)
        grad_query = (
            grad_query
            + jnp.einsum("hqk,khd->qhd", grad_scores, key_rows, preferred_element_type=jnp.float32)
            * score_scale
        )
        grad_keys = (
            jnp.einsum("hqk,qhd->khd", grad_scores, queries, preferred_element_type=jnp.float32)
            * score_scale
        )
        grad_values = jnp.einsum(
            "hqk,qhd->khd",
            prob_rows.astype(jnp.bfloat16),
            grad_mix,
            preferred_element_type=jnp.float32,
        )
        pair_grad = jnp.concatenate(
            [
                grad_keys.reshape(2 * tok_rows, model_width),
                grad_values.reshape(2 * tok_rows, model_width),
            ],
            axis=1,
        )
        pair_grad = pair_grad.reshape(2, tok_rows, 2 * model_width)
        grad_store = lax.dynamic_update_slice_in_dim(grad_store, pair_grad, 2 * pair_index, 0)
        return (grad_query, grad_store)

    start_query = jnp.zeros((tok_rows, head_count, head_size), jnp.float32)
    start_store = jnp.zeros((2 * pair_count, tok_rows, 2 * model_width), jnp.float32)
    grad_query, grad_store = lax.fori_loop(
        0, pair_count, visit(add_grads), (start_query, start_store)
    )

    def send_back(step_index, moving):
        moving = moving + lax.dynamic_index_in_dim(
            grad_store, reach_back - step_index, 0, keepdims=False
        )
        return from_behind(moving.astype(jnp.bfloat16), "cp", -1).astype(moving.dtype)

    returned = lax.fori_loop(
        0, reach_back, send_back, jnp.zeros((tok_rows, 2 * model_width), jnp.float32)
    )
    grad_kv = returned + grad_store[0]
    grad_qkv = jnp.concatenate([grad_query.reshape(tok_rows, model_width), grad_kv], axis=1).astype(
        jnp.bfloat16
    )
    grad_qkv_f = grad_qkv.astype(jnp.float32)
    grad_act_one = matmul_nn(grad_qkv, w_attn)
    _, pull_one = jax.vjp(layer_norm, inputs, vectors[0], vectors[1])
    grad_in_norm, grad_gain_one, grad_bias_one = pull_one(grad_act_one)
    input_grad = (grad_res + grad_in_norm).astype(jnp.bfloat16)
    grad_vectors = jnp.stack(
        [
            grad_gain_one,
            grad_bias_one,
            jnp.sum(grad_qkv_f[:, :model_width], axis=0),
            jnp.sum(grad_qkv_f[:, 2 * model_width :], axis=0),
            jnp.sum(grad_attn.astype(jnp.float32), axis=0),
            grad_gain_two,
            grad_bias_two,
            jnp.sum(grad_out_f, axis=0),
        ]
    )
    grad_fc_bias = jnp.sum(grad_fc.astype(jnp.float32), axis=0).reshape(
        hidden // model_width, model_width
    )
    used_rows = 4 * model_width + 2 * hidden + 8 + hidden // model_width
    total_rows = gathered.shape[0]
    local_grad = jnp.concatenate(
        [
            matmul_tn(grad_qkv, act_one),
            matmul_tn(grad_attn, mixed),
            matmul_tn(grad_fc, act_two),
            matmul_tn(act_hidden, out_grad),
            grad_vectors,
            grad_fc_bias,
            jnp.zeros((total_rows - used_rows, model_width), jnp.float32),
        ],
        axis=0,
    )
    dp_count = lax.axis_size("dp")
    device_count = dp_count * cp_count
    share_rows = total_rows // device_count
    spread_rows = local_grad.reshape(device_count, 1, share_rows, model_width)
    received = lax.all_to_all(
        spread_rows.astype(jnp.bfloat16), ("dp", "cp"), split_axis=0, concat_axis=1, tiled=True
    ).astype(spread_rows.dtype)
    param_grad = jnp.sum(received, axis=1).reshape(share_rows, model_width)
    return (output, input_grad, param_grad)


MESH = pl.DeviceIdType.MESH
GRAIN = 8
NT = (((1,), (1,)), ((), ()))
TN = (((0,), (0,)), ((), ()))


def dot_nt(a, b):
    return lax.dot_general(a, b, NT, preferred_element_type=jnp.float32)


def dot_tn(a, b):
    return lax.dot_general(a, b, TN, preferred_element_type=jnp.float32)


def dot_nn(a, b):
    return jnp.dot(a, b, preferred_element_type=jnp.float32)


def flat_id(y, c, z, x):
    return ((y * 2 + c) * 4 + z) * 2 + x


def permute(value, move):
    pairs = []
    for y in range(2):
        for c in range(2):
            for z in range(4):
                for x in range(2):
                    to = move(y, c, z, x)
                    if to is not None:
                        pairs.append((flat_id(y, c, z, x), flat_id(*to)))
    return lax.ppermute(value, ("dp", "cp"), pairs)


def over_y(value):
    return permute(value, lambda y, c, z, x: (1 - y, c, z, x))


def over_z(value, by):
    return permute(value, lambda y, c, z, x: (y, c, (z + by) % 4, x))


class Sizes:
    def __init__(self, width, hidden, heads, head_size, rows):
        self.heads = heads
        self.head_size = head_size
        self.quarter_heads = -(-heads // 4)
        self.part = self.quarter_heads * head_size
        self.part_grains = self.part // GRAIN
        self.width_grains = width // GRAIN
        self.spill = 4 * self.part_grains - self.width_grains
        self.qkv = 3 * self.part_grains // 8
        self.out = self.part_grains // 8
        self.mlp = hidden // 4 // 8 // GRAIN
        self.block = rows // GRAIN
        self.out_start = 3 * self.width_grains
        self.fc_start = 4 * self.width_grains
        self.proj_start = self.fc_start + hidden // GRAIN
        self.vec_start = self.proj_start + hidden // GRAIN
        self.vec = 2
        self.head_grains = head_size // GRAIN
        self.fc_turn = self.turn(self.fc_start)
        self.proj_turn = self.turn(self.proj_start)

    def turn(self, start):
        return start // (2 * self.block) % 4


def spot_of_range(r):
    y = r // 6 + (r % 2) * ((r // 3) % 2)
    u = (r - (r + 5) // 8 - (r + 3) // 8) % 4
    return y, u


def range_of_spot(y, u):
    first = u + u // 3
    second = (1 - u // 2) * (u + 6) + (u // 2) * (2 * u - 1)
    return (1 - y) * first + y * second


RANGES = (0, 1, 2, 4, 6, 7, 3, 5)
SPOTS = (0, 1, 2, 6, 3, 7, 4, 5)


def slot_qkv(y, z):
    return 2 * z + y


def slot_out(y, z):
    return 4 * y + z


def slot_turned(turn):
    return lambda y, z: 4 * y + (z + 4 - turn) % 4


def my_place():
    dp = lax.axis_index("dp")
    cp = lax.axis_index("cp")
    return dp // 2, dp % 2, cp // 2, cp % 2


def device_of(quarter, y, z):
    return y * 2 + quarter // 2, z * 2 + quarter % 2


class Wires:
    def __init__(self, send_sems, recv_sems):
        self.send_sems = send_sems
        self.recv_sems = recv_sems
        self.count = 0

    def to(self, src, dst, dp, cp):
        index = self.count
        self.count += 1
        return pltpu.make_async_remote_copy(
            src_ref=src,
            dst_ref=dst,
            send_sem=self.send_sems.at[index],
            recv_sem=self.recv_sems.at[index],
            device_id=(dp, cp),
            device_id_type=MESH,
        )


class PlaceGather:
    def __init__(self, wires, full, slot, steps=(1, 2, 3), over=(0, 1, 2, 3)):
        self.full = full
        self.dp, self.cp = lax.axis_index("dp"), lax.axis_index("cp")
        self.y, self.z, self.x = self.dp // 2, self.cp // 2, self.cp % 2
        self.above = (self.dp, ((self.z + 1) % 4) * 2 + self.x)
        self.below = (self.dp, ((self.z + 3) % 4) * 2 + self.x)
        self.across = ((self.dp + 2) % 4, self.cp)

        def share(by, to):
            view = full.at[slot(self.y, (self.z + 4 + by) % 4)]
            return wires.to(view, view, *to)

        self.steps = steps
        self.up = {k: share(1 - k, self.above) for k in steps}
        self.down = {k: share(k - 1, self.below) for k in steps}
        self.over = {d: share(d, self.across) for d in over}

    def partners(self):
        return [self.above, self.below, self.across]

    def start(self):
        if 1 in self.steps:

            @pl.when(self.z < 3)
            def _():
                self.up[1].start()

            @pl.when(self.z > 0)
            def _():
                self.down[1].start()

        if 0 in self.over:
            self.over[0].start()

    def forward(self, steps=(1, 2, 3)):
        for k in steps:

            @pl.when(self.z >= k)
            def _():
                if k in self.steps:
                    self.up[k].wait_recv()
                if k + 1 in self.steps:

                    @pl.when(self.z < 3)
                    def _():
                        self.up[k + 1].start()

                if 4 - k in self.over:
                    self.over[4 - k].start()

            @pl.when(self.z <= 3 - k)
            def _():
                if k in self.steps:
                    self.down[k].wait_recv()
                if k + 1 in self.steps:

                    @pl.when(self.z > 0)
                    def _():
                        self.down[k + 1].start()

                if k in self.over:
                    self.over[k].start()

    def finish(self):
        for copy in self.over.values():
            copy.wait_recv()
        for copy in self.over.values():
            copy.wait_send()
        for k in self.steps:

            @pl.when(jnp.logical_and(self.z >= k - 1, self.z < 3))
            def _():
                self.up[k].wait_send()

            @pl.when(jnp.logical_and(self.z <= 4 - k, self.z > 0))
            def _():
                self.down[k].wait_send()


class QuadGather:
    def __init__(self, wires, block, full, local_sem):
        self.wires = wires
        self.block = block
        self.full = full
        self.dp, self.cp = lax.axis_index("dp"), lax.axis_index("cp")
        self.c, self.x = self.dp % 2, self.cp % 2
        self.over_x = (self.dp, self.cp + 1 - 2 * self.x)
        self.over_c = (self.dp + 1 - 2 * self.c, self.cp)
        self.local_sem = local_sem

    def start(self):
        spot = self.full.at[self.c, self.x]
        self.by_x = self.wires.to(self.block, spot, *self.over_x)
        self.by_c = self.wires.to(self.block, spot, *self.over_c)
        self.by_x.start()
        self.by_c.start()
        self.local = pltpu.make_async_copy(self.block, spot, self.local_sem)
        self.local.start()

    def forward(self):
        self.by_x.wait_recv()
        spot = self.full.at[self.c, 1 - self.x]
        self.pass_on = self.wires.to(spot, spot, *self.over_c)
        self.pass_on.start()

    def finish(self):
        self.by_c.wait_recv()
        self.pass_on.wait_recv()
        self.by_x.wait_send()
        self.by_c.wait_send()
        self.pass_on.wait_send()
        self.local.wait()


def open_kernel(
    sz, p_ref, tok_ref, cot_ref, qkv_ref, out_ref, fc_ref, proj_ref, vec_ref, tok_all, cot_all,
    spread_sems, kind_sems, send_sems, recv_sems, local_sems,
):
    y, c, z, x = my_place()
    me = flat_id(y, c, z, x)
    wires = Wires(send_sems, recv_sems)
    tok = QuadGather(wires, tok_ref, tok_all, local_sems.at[0])
    cot = QuadGather(wires, cot_ref, cot_all, local_sems.at[1])

    def send(grain, ref, spot, slot, quarter, py, pz, sem, recv):
        dp, cp = device_of(quarter, py, pz)
        mine = dp * 8 + cp == me

        @pl.when(mine)
        def _():
            pltpu.make_async_copy(p_ref.at[grain], ref.at[spot, slot], recv).start()

        @pl.when(jnp.logical_not(mine))
        def _():
            pltpu.make_async_remote_copy(
                src_ref=p_ref.at[grain],
                dst_ref=ref.at[spot, slot],
                send_sem=sem,
                recv_sem=recv,
                device_id=(dp, cp),
                device_id_type=MESH,
            ).start()

    def sent(grain, ref, spot, slot, quarter, py, pz, sem, recv):
        dp, cp = device_of(quarter, py, pz)

        @pl.when(dp * 8 + cp != me)
        def _():
            pltpu.make_async_copy(p_ref.at[grain], p_ref.at[grain], sem).wait()

    def headed(act, grain):
        table = me * sz.block + grain
        part = table // sz.width_grains
        inner = table % sz.width_grains
        head = inner // sz.head_grains
        rest = inner % sz.head_grains

        def one(quarter, sem):
            local = part * sz.part_grains + (2 * (head // 8) + head % 2) * sz.head_grains + rest
            spot = local // sz.qkv
            act(grain, qkv_ref, spot, local % sz.qkv, quarter, spot % 2, spot // 2, sem, kind_sems.at[0])

        @pl.when(table < sz.out_start)
        def _():
            one((head // 2) % 4, spread_sems.at[grain])

            @pl.when(head == sz.heads - 1)
            def _():
                for quarter in range(1, 4):
                    one(quarter, spread_sems.at[sz.block + (quarter - 1) * sz.head_grains + rest])

    def outward(act, grain):
        local = me * sz.block + grain - sz.out_start

        def one(quarter, inner, sem):
            spot = inner // sz.out
            act(grain, out_ref, spot, inner % sz.out, quarter, spot // 4, spot % 4, sem, kind_sems.at[1])

        @pl.when(jnp.logical_and(local >= 0, local < sz.width_grains))
        def _():
            one(local // sz.part_grains, local % sz.part_grains, spread_sems.at[grain])

            @pl.when(local < sz.spill)
            def _():
                one(3, sz.part_grains - sz.spill + local, spread_sems.at[sz.block + 3 * sz.head_grains + local])

    def plain(act, grain, base, turn, ref, recv):
        offset = me * sz.block + grain - base

        @pl.when(jnp.logical_and(offset >= 0, offset < 32 * sz.mlp))
        def _():
            local = offset // 4
            py, u = spot_of_range(local // sz.mlp)
            act(
                grain, ref, py * 4 + u, local % sz.mlp, offset % 4, py, (u + turn) % 4,
                spread_sems.at[grain], recv,
            )

    def heads(act):
        def one(grain, _):
            headed(act, grain)
            return 0

        lax.fori_loop(0, sz.block, one, 0)

    def others(act):
        def one(grain, _):
            outward(act, grain)
            plain(act, grain, sz.fc_start, sz.fc_turn, fc_ref, kind_sems.at[2])
            plain(act, grain, sz.proj_start, sz.proj_turn, proj_ref, kind_sems.at[3])
            return 0

        lax.fori_loop(0, sz.block, one, 0)

    owner = sz.vec_start // sz.block
    spot = sz.vec_start % sz.block

    def vector_sends(act):
        @pl.when(me == owner)
        def _():
            def to(device, _):
                @pl.when(device != me)
                def _():
                    act(
                        pltpu.make_async_remote_copy(
                            src_ref=p_ref.at[pl.ds(spot, sz.vec)],
                            dst_ref=vec_ref,
                            send_sem=spread_sems.at[sz.block + 3 * sz.head_grains + sz.spill + device],
                            recv_sem=kind_sems.at[4],
                            device_id=(device // 8, device % 8),
                            device_id_type=MESH,
                        )
                    )

                return 0

            lax.fori_loop(0, 32, to, 0)

    heads(send)
    tok.start()
    mine = slot_qkv(y, z)
    pltpu.make_async_copy(qkv_ref.at[mine], qkv_ref.at[mine], kind_sems.at[0]).wait()
    weights = PlaceGather(wires, qkv_ref, slot_qkv)
    weights.start()
    vector_sends(lambda copy: copy.start())

    @pl.when(me == owner)
    def _():
        pltpu.make_async_copy(p_ref.at[pl.ds(spot, sz.vec)], vec_ref, kind_sems.at[4]).start()

    others(send)
    cot.start()
    tok.forward()
    weights.forward()
    early = []
    for index, (ref, slot) in enumerate(((out_ref, slot_out), (fc_ref, slot_turned(sz.fc_turn)))):
        view = ref.at[slot(y, z)]
        pltpu.make_async_copy(view, view, kind_sems.at[index + 1]).wait()
        early.append(PlaceGather(wires, ref, slot, steps=(1,), over=(0,)))
        early[-1].start()
    cot.forward()
    heads(sent)
    others(sent)
    vector_sends(lambda copy: copy.wait_send())
    view = proj_ref.at[slot_turned(sz.proj_turn)(y, z)]
    pltpu.make_async_copy(view, view, kind_sems.at[3]).wait()
    pltpu.make_async_copy(vec_ref, vec_ref, kind_sems.at[4]).wait()
    tok.finish()
    cot.finish()
    weights.finish()
    for first in early:
        first.forward((1,))
        first.finish()


HBM = pl.BlockSpec(memory_space=pl.ANY)
VMEM = pl.BlockSpec(memory_space=pltpu.VMEM)
REMOTE = pltpu.CompilerParams(has_side_effects=True)


def remote_params(ident=None, vmem=None):
    return pltpu.CompilerParams(has_side_effects=True, collective_id=ident, vmem_limit_bytes=vmem)


def greet(partners):
    barrier = pltpu.get_barrier_semaphore()
    for dp, cp in partners:
        pl.semaphore_signal(barrier, inc=1, device_id=(dp, cp), device_id_type=MESH)
    pl.semaphore_wait(barrier, len(partners))


def cost(us):
    return pl.CostEstimate(flops=0, bytes_accessed=int(us * 3.0e6), transcendentals=0)


def wire_sems(count):
    return [pltpu.SemaphoreType.DMA((count,)), pltpu.SemaphoreType.DMA((count,))]


def open_call(sz, table, tokens, cotangent):
    rows, width = tokens.shape

    def like(*shape):
        return jax.ShapeDtypeStruct(shape + (width,), table.dtype)

    return pl.pallas_call(
        functools.partial(open_kernel, sz),
        out_shape=(
            like(8, sz.qkv, GRAIN),
            like(8, sz.out, GRAIN),
            like(8, sz.mlp, GRAIN),
            like(8, sz.mlp, GRAIN),
            like(sz.vec, GRAIN),
            like(2, 2, rows),
            like(2, 2, rows),
        ),
        in_specs=[HBM, VMEM, VMEM],
        out_specs=[HBM] * 7,
        scratch_shapes=[
            pltpu.SemaphoreType.DMA((sz.block + 3 * sz.head_grains + sz.spill + 32,)),
            pltpu.SemaphoreType.DMA((5,)),
            *wire_sems(22),
            pltpu.SemaphoreType.DMA((2,)),
        ],
        compiler_params=REMOTE,
        name="open",
    )(table, tokens, cotangent)


def forward_kernel(
    heads, size, fc_turn, proj_turn, q_ref, kv_ref, out_in, fc_in, proj_in,
    mix_ref, lse_ref, before_ref, mixed_ref, out_ref, fc_ref, proj_ref, out_all,
    stage, send_sems, recv_sems, local_sems,
):
    y, c, z, x = my_place()
    dp, cp = lax.axis_index("dp"), lax.axis_index("cp")
    wires = Wires(send_sems, recv_sems)
    part = heads * size
    rows = q_ref.shape[0] // 2
    blk = 256
    scale = size**-0.5
    odd = z % 2 == 1
    w_out = PlaceGather(wires, out_ref, slot_out, steps=(2, 3), over=(1, 2, 3))
    w_fc = PlaceGather(wires, fc_ref, slot_turned(fc_turn), steps=(2, 3), over=(1, 2, 3))
    w_proj = PlaceGather(wires, proj_ref, slot_turned(proj_turn), steps=(1,), over=(0,))
    others = [(c, 1 - x), (1 - c, x), (1 - c, 1 - x)]
    quad = [(y * 2 + tc, z * 2 + tx) for tc, tx in others]
    greet(w_out.partners() + quad)
    keys = wires.to(kv_ref, before_ref, dp, (cp + 2) % 8)

    w_out.forward()

    @pl.when(jnp.logical_not(odd))
    def _():
        keys.start()

    w_fc.forward((1,))

    def own(group, _):
        start = group * rows
        for i in range(rows // blk):
            here = pl.ds(pl.multiple_of(start + i * blk, blk), blk)
            seen = (i + 1) * blk
            keys_at = pl.ds(pl.multiple_of(start, rows), seen)
            lane = lax.broadcasted_iota(jnp.int32, (blk, seen), 1)
            line = lax.broadcasted_iota(jnp.int32, (blk, seen), 0)
            allowed = lane <= line + i * blk
            for h in range(heads):
                cols = slice(h * size, (h + 1) * size)
                vals = slice(part + h * size, part + (h + 1) * size)
                s = dot_nt(q_ref[here, cols], kv_ref[keys_at, cols]) * scale
                s = jnp.where(allowed, s, MASKED)
                top = jnp.max(s, axis=-1, keepdims=True)
                p = jnp.exp(s - top)
                total = jnp.sum(p, axis=-1, keepdims=True)
                mix_ref[here, cols] = dot_nn(p.astype(jnp.bfloat16), kv_ref[keys_at, vals]) / total
                lse_ref[here, h : h + 1] = top + jnp.log(total)
        return 0

    lax.fori_loop(0, 2, own, 0)

    def add_before(index, _):
        here = pl.ds(pl.multiple_of(index * blk, blk), blk)
        keys_at = pl.ds(pl.multiple_of((index * blk) // rows * rows, rows), rows)
        for h in range(heads):
            cols = slice(h * size, (h + 1) * size)
            vals = slice(part + h * size, part + (h + 1) * size)
            s = dot_nt(q_ref[here, cols], before_ref[keys_at, cols]) * scale
            lse = lse_ref[here, h : h + 1]
            top = jnp.maximum(lse, jnp.max(s, axis=-1, keepdims=True))
            p = jnp.exp(s - top)
            kept = jnp.exp(lse - top)
            total = kept + jnp.sum(p, axis=-1, keepdims=True)
            mix = mix_ref[here, cols] * kept + dot_nn(p.astype(jnp.bfloat16), before_ref[keys_at, vals])
            mix_ref[here, cols] = mix / total
            lse_ref[here, h : h + 1] = top + jnp.log(total)
        return 0

    w_out.finish()
    whole = QuadGather(wires, out_ref, out_all, local_sems.at[0])
    whole.start()

    @pl.when(z < 3)
    def _():
        w_fc.forward((2,))

    @pl.when(odd)
    def _():
        keys.wait_recv()
        lax.fori_loop(0, 2 * rows // blk, add_before, 0)

    def round_off(index, _):
        here = pl.ds(pl.multiple_of(index * blk, blk), blk)
        stage[here, :] = mix_ref[here, :].astype(stage.dtype)
        return 0

    lax.fori_loop(0, 2 * rows // blk, round_off, 0)

    @pl.when(z == 3)
    def _():
        w_fc.forward((2,))

    mine = c * 2 + x
    each = rows // 2
    swaps = []
    for (tc, tx), (tdp, tcp) in zip(others, quad):
        block = stage.at[pl.ds(pl.multiple_of((tc * 2 + tx) * each, each), each)]
        swaps.append(wires.to(block, mixed_ref.at[mine], tdp, tcp))
    for copy in swaps:
        copy.start()
    local = pltpu.make_async_copy(
        stage.at[pl.ds(pl.multiple_of(mine * each, each), each)], mixed_ref.at[mine], local_sems.at[1]
    )
    local.start()
    whole.forward()
    w_fc.forward((3,))
    w_proj.start()
    for copy in swaps:
        copy.wait_recv()
    whole.finish()
    w_fc.finish()
    w_proj.forward((1,))
    w_proj.finish()
    for copy in swaps:
        copy.wait_send()
    local.wait()

    @pl.when(jnp.logical_not(odd))
    def _():
        keys.wait_send()


def forward_call(sz, q, kv, w_out, w_fc, w_proj):
    part = sz.part
    rows = q.shape[0]

    def like(value, *lead):
        return jax.ShapeDtypeStruct(lead + value.shape, value.dtype)

    return pl.pallas_call(
        functools.partial(forward_kernel, sz.quarter_heads, sz.head_size, sz.fc_turn, sz.proj_turn),
        out_shape=(
            jax.ShapeDtypeStruct((rows, part), jnp.float32),
            jax.ShapeDtypeStruct((rows, 8), jnp.float32),
            like(kv),
            jax.ShapeDtypeStruct((4, rows // 4, part), jnp.bfloat16),
            like(w_out),
            like(w_fc),
            like(w_proj),
            like(w_out, 2, 2),
        ),
        in_specs=[VMEM, VMEM, HBM, HBM, HBM],
        out_specs=[VMEM] * 4 + [HBM] * 4,
        input_output_aliases={2: 4, 3: 5, 4: 6},
        scratch_shapes=[
            pltpu.VMEM((rows, part), jnp.bfloat16),
            *wire_sems(37),
            pltpu.SemaphoreType.DMA((2,)),
        ],
        cost_estimate=cost(120),
        compiler_params=remote_params(1, 56 << 20),
        name="forward",
    )(q, kv, w_out, w_fc, w_proj)


def acts_kernel(proj_turn, act_ref, proj_in, act_all, proj_ref, send_sems, recv_sems, local_sem):
    wires = Wires(send_sems, recv_sems)
    quad = QuadGather(wires, act_ref, act_all, local_sem)
    places = PlaceGather(wires, proj_ref, slot_turned(proj_turn), steps=(2, 3), over=(1, 2, 3))
    greet(places.partners() + [quad.over_x, quad.over_c])
    quad.start()
    places.forward((1, 2))
    quad.forward()
    places.forward((3,))
    quad.finish()
    places.finish()


def grads_kernel(act_ref, act_all, send_sems, recv_sems, local_sem):
    wires = Wires(send_sems, recv_sems)
    quad = QuadGather(wires, act_ref, act_all, local_sem)
    greet([quad.over_x, quad.over_c])
    quad.start()
    quad.forward()
    quad.finish()


def grads_call(act, ident):
    return pl.pallas_call(
        grads_kernel,
        out_shape=jax.ShapeDtypeStruct((2, 2) + act.shape, act.dtype),
        in_specs=[VMEM],
        out_specs=HBM,
        scratch_shapes=[*wire_sems(3), pltpu.SemaphoreType.DMA],
        cost_estimate=cost(25),
        compiler_params=remote_params(ident),
        name="grads",
    )(act)


def acts_call(sz, act, w_proj):
    return pl.pallas_call(
        functools.partial(acts_kernel, sz.proj_turn),
        out_shape=(
            jax.ShapeDtypeStruct((2, 2) + act.shape, act.dtype),
            jax.ShapeDtypeStruct(w_proj.shape, w_proj.dtype),
        ),
        in_specs=[VMEM, HBM],
        out_specs=[HBM] * 2,
        input_output_aliases={1: 1},
        scratch_shapes=[*wire_sems(13), pltpu.SemaphoreType.DMA],
        cost_estimate=cost(60),
        compiler_params=remote_params(2),
        name="acts",
    )(act, w_proj)


class QuadSum:
    step = 32

    def __init__(self, in_ref, out_ref, got_c, stage, got_x, send_sems, recv_sems):
        self.y, self.c, self.z, self.x = my_place()
        dp, cp = lax.axis_index("dp"), lax.axis_index("cp")
        wires = Wires(send_sems, recv_sems)
        self.in_ref, self.out_ref, self.got_c, self.stage, self.got_x = in_ref, out_ref, got_c, stage, got_x
        self.partners = [(dp + 1 - 2 * self.c, cp), (dp, cp + 1 - 2 * self.x)]
        self.by_c = wires.to(in_ref.at[1 - self.c], got_c, *self.partners[0])
        self.by_x = wires.to(stage, got_x, *self.partners[1])

    def each(self, act):
        def one(index, _):
            act(pl.ds(pl.multiple_of(index * self.step, self.step), self.step))
            return 0

        lax.fori_loop(0, self.out_ref.shape[0] // self.step, one, 0)

    def start(self):
        greet(self.partners)
        self.by_c.start()

    def middle(self):
        c, x = self.c, self.x
        self.by_c.wait_recv()

        def to_send(span):
            self.stage[span, :] = (
                self.in_ref[c, 1 - x, span, :].astype(jnp.float32) + self.got_c[1 - x, span, :].astype(jnp.float32)
            ).astype(self.stage.dtype)

        self.each(to_send)
        self.by_x.start()

    def finish(self):
        c, x = self.c, self.x
        self.by_x.wait_recv()

        def to_add(span):
            self.out_ref[span, :] = (
                self.in_ref[c, x, span, :].astype(jnp.float32)
                + self.got_c[x, span, :].astype(jnp.float32)
                + self.got_x[span, :].astype(jnp.float32)
            )

        self.each(to_add)
        self.by_c.wait_send()
        self.by_x.wait_send()


def quad_sum_kernel(*refs):
    quad = QuadSum(*refs)
    quad.start()
    quad.middle()
    quad.finish()


def quad_scratch(partial):
    rows, width = partial.shape[2:]
    return [
        pltpu.VMEM((2, rows, width), partial.dtype),
        pltpu.VMEM((rows, width), partial.dtype),
        pltpu.VMEM((rows, width), partial.dtype),
        *wire_sems(2),
    ]


def quad_sum(partial, ident):
    return pl.pallas_call(
        quad_sum_kernel,
        out_shape=jax.ShapeDtypeStruct(partial.shape[2:], jnp.float32),
        in_specs=[VMEM],
        out_specs=VMEM,
        scratch_shapes=quad_scratch(partial),
        compiler_params=remote_params(ident),
        cost_estimate=cost(30),
        name="quad_sum",
    )(partial)


class Collector:
    def __init__(self, sz):
        self.sz = sz
        self.y, self.c, self.z, self.x = my_place()
        self.me = flat_id(self.y, self.c, self.z, self.x)
        self.quarter = self.c * 2 + self.x

    def send(self, src, dst, table, sem, recv):
        dest = table // self.sz.block

        @pl.when(dest == self.me)
        def _():
            pltpu.make_async_copy(src, dst, recv).start()

        @pl.when(dest != self.me)
        def _():
            pltpu.make_async_remote_copy(
                src_ref=src,
                dst_ref=dst,
                send_sem=sem,
                recv_sem=recv,
                device_id=(dest // 8, dest % 8),
                device_id_type=MESH,
            ).start()

    def sent(self, src, dst, table, sem, recv):
        @pl.when(table // self.sz.block != self.me)
        def _():
            pltpu.make_async_copy(src, src, sem).wait()

    def received(self, first, count, view, recv):
        block = self.sz.block
        for device in range(first // block, -(-(first + count) // block)):
            grains = min(first + count, (device + 1) * block) - max(first, device * block)

            @pl.when(self.me == device)
            def _():
                pltpu.make_async_copy(view(grains), view(grains), recv).wait()


def collect_mlp_kernel(sz, fc_ref, proj_ref, out_ref, g_ref, outs_ref, send_sems, out_sems, recv_sems):
    to = Collector(sz)
    recv_sem = recv_sems.at[0]
    out_share = out_ref.shape[0]

    def run(act):
        for ref, base, turn, first_sem in (
            (fc_ref, sz.fc_start, sz.fc_turn, 0), (proj_ref, sz.proj_start, sz.proj_turn, sz.mlp)
        ):
            r = range_of_spot(to.y, (to.z + 4 - turn) % 4)

            def one(slot, _):
                table = base + 4 * (r * sz.mlp + slot) + to.quarter
                act(ref.at[slot], g_ref.at[table % sz.block], table, send_sems.at[first_sem + slot], recv_sem)
                return 0

            lax.fori_loop(0, sz.mlp, one, 0)

        def outward(slot, _):
            table = sz.out_start + slot_out(to.y, to.z) * out_share + slot
            dst = outs_ref.at[to.quarter, table % sz.block]
            act(out_ref.at[slot], dst, table, out_sems.at[slot], recv_sems.at[1])
            return 0

        lax.fori_loop(0, out_share, outward, 0)

    run(to.send)
    run(to.sent)
    to.received(sz.fc_start, 64 * sz.mlp, lambda n: g_ref.at[pl.ds(0, n)], recv_sem)
    to.received(sz.out_start, sz.width_grains, lambda n: outs_ref.at[:, pl.ds(0, n)], recv_sems.at[1])


def collect_mlp(sz, fc, proj, out):
    return pl.pallas_call(
        functools.partial(collect_mlp_kernel, sz),
        out_shape=(
            jax.ShapeDtypeStruct((sz.block, GRAIN, fc.shape[-1]), fc.dtype),
            jax.ShapeDtypeStruct((4, sz.block, GRAIN, out.shape[-1]), out.dtype),
        ),
        in_specs=[HBM] * 3,
        out_specs=[HBM] * 2,
        scratch_shapes=[
            pltpu.SemaphoreType.DMA((2 * sz.mlp,)),
            pltpu.SemaphoreType.DMA((out.shape[0],)),
            pltpu.SemaphoreType.DMA((2,)),
        ],
        cost_estimate=cost(30),
        compiler_params=REMOTE,
        name="collect_mlp",
    )(fc, proj, out)


def collect_rest_kernel(
    sz, qkv_ref, vec_ref, g_ref, vecs_ref, qkv_sems, vec_sems, recv_sem
):
    to = Collector(sz)

    def run(act):
        def heads(slot, _):
            local = slot_qkv(to.y, to.z) * sz.qkv + slot
            inner = local % sz.part_grains
            index = inner // sz.head_grains
            head = 8 * (index // 2) + 2 * to.quarter + index % 2

            @pl.when(head < sz.heads)
            def _():
                table = (local // sz.part_grains) * sz.width_grains + head * sz.head_grains + inner % sz.head_grains
                act(qkv_ref.at[slot], g_ref.at[table % sz.block], table, qkv_sems.at[slot], recv_sem)

            return 0

        lax.fori_loop(0, sz.qkv, heads, 0)

    last = sz.vec_start // sz.block
    vec_copy = pltpu.make_async_remote_copy(
        src_ref=vec_ref,
        dst_ref=vecs_ref.at[to.me],
        send_sem=vec_sems.at[0],
        recv_sem=vec_sems.at[1],
        device_id=(last // 8, last % 8),
        device_id_type=MESH,
    )

    @pl.when(to.me != last)
    def _():
        vec_copy.start()

    @pl.when(to.me == last)
    def _():
        pltpu.make_async_copy(vec_ref, vecs_ref.at[to.me], vec_sems.at[1]).start()

    run(to.send)
    run(to.sent)

    @pl.when(to.me != last)
    def _():
        vec_copy.wait_send()

    @pl.when(to.me == last)
    def _():
        pltpu.make_async_copy(vecs_ref, vecs_ref, vec_sems.at[1]).wait()

    to.received(0, 3 * sz.width_grains, lambda n: g_ref.at[pl.ds(0, n)], recv_sem)


def collect_rest(sz, qkv, vectors):
    def like(value, *lead):
        return jax.ShapeDtypeStruct(lead + value.shape[-2:], value.dtype)

    return pl.pallas_call(
        functools.partial(collect_rest_kernel, sz),
        out_shape=(like(qkv, sz.block), like(vectors, 32, sz.vec)),
        in_specs=[HBM] * 2,
        out_specs=[HBM] * 2,
        scratch_shapes=[
            pltpu.SemaphoreType.DMA((sz.qkv,)),
            pltpu.SemaphoreType.DMA((2,)),
            pltpu.SemaphoreType.DMA,
        ],
        cost_estimate=cost(30),
        compiler_params=REMOTE,
        name="collect_rest",
    )(qkv, vectors)


def attend_back_kernel(heads, size, own, *refs):
    if own:
        q_ref, kv_ref, do_ref, mix_ref, lse_ref, seed_ref, dq_ref, dkv_ref = refs
    else:
        q_ref, kv_ref, do_ref, mix_ref, lse_ref, term_ref, dq_ref, dkv_ref, sum_ref = refs[:9]
        quad = QuadSum(term_ref, sum_ref, *refs[-5:])
        quad.start()
    _, _, z, _ = my_place()
    part = heads * size
    rows = q_ref.shape[0] // 2
    blk = 256
    scale = size**-0.5

    def visit(here, start, seen, allowed):
        keys_at = pl.ds(start, seen)
        for h in range(heads):
            cols = slice(h * size, (h + 1) * size)
            vals = slice(part + h * size, part + (h + 1) * size)
            q = q_ref[here, cols]
            k = kv_ref[keys_at, cols]
            do = do_ref[here, cols]
            s = dot_nt(q, k) * scale
            p = jnp.exp(s - lse_ref[here, h : h + 1])
            if own:
                p = jnp.where(allowed, p, 0.0)
            dp = dot_nt(do, kv_ref[keys_at, vals])
            delta = jnp.sum(do.astype(jnp.float32) * mix_ref[here, cols], axis=-1, keepdims=True)
            ds = (p * (dp - delta)).astype(jnp.bfloat16)
            dq = dot_nn(ds, k) * scale
            if own:
                dq = dq + seed_ref[here, cols]
            dq_ref[here, cols] = dq.astype(dq_ref.dtype)
            dkv_ref[keys_at, cols] += dot_tn(ds, q) * scale
            dkv_ref[keys_at, vals] += dot_tn(p.astype(jnp.bfloat16), do)

    def group(index):
        start = pl.multiple_of(index * rows, rows)
        if not own:

            def block(i, _):
                visit(pl.ds(pl.multiple_of(start + i * blk, blk), blk), start, rows, None)
                return 0

            lax.fori_loop(0, rows // blk, block, 0)
            return
        for i in range(rows // blk):
            seen = (i + 1) * blk
            lane = lax.broadcasted_iota(jnp.int32, (blk, seen), 1)
            line = lax.broadcasted_iota(jnp.int32, (blk, seen), 0)
            visit(pl.ds(pl.multiple_of(start + i * blk, blk), blk), start, seen, lane <= line + i * blk)

    def clear(index, _):
        here = pl.ds(pl.multiple_of(index * blk, blk), blk)
        dkv_ref[here, :] = jnp.zeros((blk, dkv_ref.shape[1]), dkv_ref.dtype)
        if not own:
            dq_ref[here, :] = jnp.zeros((blk, dq_ref.shape[1]), dq_ref.dtype)
        return 0

    lax.fori_loop(0, 2 * rows // blk, clear, 0)

    def one(index, _):
        if own:
            group(index)
        else:

            @pl.when(z % 2 == 1)
            def _():
                group(index)

            @pl.when(index == 0)
            def _():
                quad.middle()

        return 0

    lax.fori_loop(0, 2, one, 0)
    if not own:
        quad.finish()


def attend_back(sz, q, kv, grad_mix, mix, lse, seed=None, term=None, ident=None):
    own = term is None
    operands = [q, kv, grad_mix, mix, lse, seed if own else term]
    out_shape = [
        jax.ShapeDtypeStruct(q.shape, jnp.bfloat16 if own else jnp.float32),
        jax.ShapeDtypeStruct(kv.shape, jnp.float32),
    ]
    if not own:
        out_shape.append(jax.ShapeDtypeStruct(term.shape[2:], jnp.float32))
    params = pltpu.CompilerParams(vmem_limit_bytes=56 << 20) if own else remote_params(ident, 56 << 20)
    return pl.pallas_call(
        functools.partial(attend_back_kernel, sz.quarter_heads, sz.head_size, own),
        out_shape=out_shape,
        in_specs=[VMEM] * len(operands),
        out_specs=[VMEM] * len(out_shape),
        scratch_shapes=[] if own else quad_scratch(term),
        cost_estimate=cost(35),
        compiler_params=params,
        name="attend_back_own" if own else "attend_back_before",
    )(*operands)


def rowwise(value):
    return with_layout_constraint(value, Layout(major_to_minor=(0, 1)))


def norm_parts(values):
    mean = jnp.mean(values, axis=-1, keepdims=True)
    centre = values - mean
    rs = lax.rsqrt(jnp.mean(centre * centre, axis=-1, keepdims=True) + EPSILON)
    return centre * rs, rs


def norm_back(normed, rs, grad, gain):
    e = grad * gain
    return rs * (
        e
        - jnp.mean(e, axis=-1, keepdims=True)
        - normed * jnp.mean(e * normed, axis=-1, keepdims=True)
    )


def per_device_quad(tokens, params, out_grad, lengths):
    rows, width = tokens.shape
    hidden = FF
    sz = Sizes(width, hidden, HEADS, HEAD_DIM, params.shape[0])
    y, c, z, x = my_place()
    quarter = c * 2 + x
    bf16, f32 = jnp.bfloat16, jnp.float32

    def pick(value, index):
        return lax.dynamic_index_in_dim(value, index, 0, keepdims=False)

    def halves_of(value):
        half = value.shape[1] // 2
        first, second = value[:, :half], value[:, half:]
        return jnp.where(y == 0, first, second), jnp.where(y == 0, second, first)

    def to_other_y(sent):
        return over_y(sent.astype(bf16))

    def to_places(kept, got, turn=0):
        summed = kept.astype(f32) + got.astype(f32)
        summed = summed.reshape(4, summed.shape[0] // 4, -1)
        total = pick(summed, (z + 4 - turn) % 4)
        for d in (1, 2, 3):
            got = over_z(pick(summed, (z + d + 4 - turn) % 4).astype(bf16), d)
            total = total + got.astype(f32)
        return total

    w_qkv, w_out, w_fc, w_proj, vec, tok_all, cot_all = open_call(
        sz, params.reshape(sz.block, GRAIN, width), tokens, out_grad
    )
    flat = lambda value: value.reshape(-1, width)
    vectors = flat(vec).astype(f32)
    fc_bias = vectors[8 : 8 + hidden // width].reshape(hidden)
    w_qkv, cot_all = flat(w_qkv), flat(cot_all)
    normed_all, _ = norm_parts(flat(tok_all).astype(f32))
    act_one = (normed_all * vectors[0] + vectors[1]).astype(bf16)

    pair = 2 * sz.head_size
    turns = width // (4 * pair)
    rest = width - 4 * turns * pair

    def quarter_of(value):
        blocks = [lax.dynamic_slice_in_dim(value, (4 * j + quarter) * pair, pair, 1) for j in range(turns)]
        end = value[:, width - rest :]
        return jnp.concatenate(blocks + [jnp.where(quarter == 0, end, jnp.zeros_like(end))], axis=1)

    def by_head(quarters):
        blocks = [quarters[k][:, j * pair : (j + 1) * pair] for j in range(turns) for k in range(4)]
        return jnp.concatenate(blocks + [quarters[0][:, turns * pair : turns * pair + rest]], axis=1)

    biases = quarter_of(vectors[2:4])
    kv_bias = jnp.concatenate([jnp.zeros((sz.part,), f32), biases[1]])
    kv = (dot_nt(act_one, w_qkv[sz.part :]) + kv_bias).astype(bf16)
    q = (dot_nt(act_one, w_qkv[: sz.part]) + biases[0]).astype(bf16)
    mix, lse, before, mixed, _, w_fc, w_proj, w_out = forward_call(sz, q, kv, w_out, w_fc, w_proj)
    w_fc, w_out = flat(w_fc), flat(w_out)[:width]
    mixed = by_head(mixed)
    inputs = tokens.astype(f32)
    residual = inputs + (dot_nt(mixed, w_out) + vectors[4])
    normed_two, rs_two = norm_parts(residual)
    act_two, w_proj = acts_call(sz, (normed_two * vectors[5] + vectors[6]).astype(bf16), w_proj)
    act_two, w_proj = flat(act_two), flat(w_proj)
    bias = lax.dynamic_index_in_dim(fc_bias.reshape(-1, 4, GRAIN), quarter, 1, keepdims=False)
    bias = bias.reshape(8, hidden // 32)[jnp.array(RANGES)].reshape(hidden // 4)
    pre_act = dot_nt(act_two, w_fc) + bias
    act_hidden, pull_gelu = jax.vjp(gelu_tanh, pre_act)
    act_hidden = act_hidden.astype(bf16)
    hid_mine, hid_other = halves_of(act_hidden)
    got_proj = to_other_y(dot_tn(hid_other, cot_all))
    grad_fc = pull_gelu(dot_nt(cot_all, w_proj))[0].astype(bf16)
    fc_mine, fc_other = halves_of(grad_fc)
    got_fc = to_other_y(dot_tn(fc_other, act_two))
    grad_two = quad_sum(rowwise(dot_nn(grad_fc, w_fc).astype(bf16)).reshape(2, 2, rows, width), 7)

    cot = out_grad.astype(f32)
    grad_res = cot + norm_back(normed_two, rs_two, grad_two, vectors[5])
    grad_attn = grad_res.astype(bf16)
    attn_all = flat(grads_call(grad_attn, 3))
    grad_mix = rowwise(dot_nn(attn_all, w_out).astype(bf16))
    grad_mix = rowwise(quarter_of(grad_mix))
    g_proj = to_places(dot_tn(hid_mine, cot_all), got_proj, sz.proj_turn)
    partial_out = rowwise(dot_nn(act_hidden, w_proj).astype(bf16)).reshape(2, 2, rows, width)
    dq_before, dkv_before, out_sum = attend_back(
        sz, q, before, grad_mix, mix, lse, term=partial_out, ident=4
    )
    output = (residual + out_sum + vectors[7]).astype(bf16)
    returned = permute(
        dkv_before.astype(bf16), lambda py, pc, pz, px: (py, pc, pz - 1, px) if pz % 2 == 1 else None
    )
    g_out = rowwise(dot_tn(attn_all, mix.astype(bf16)).astype(bf16)).reshape(2, width // 2, sz.part)
    got_out = to_other_y(pick(g_out, 1 - y))
    g_fc = to_places(dot_tn(fc_mine, act_two), got_fc, sz.fc_turn)
    dq, dkv = attend_back(sz, q, kv, grad_mix, mix, lse, seed=dq_before)
    grad_qkv = jnp.concatenate([dq, (dkv + returned.astype(f32)).astype(bf16)], axis=1)
    g_qkv = rowwise(dot_tn(grad_qkv, act_one).astype(bf16)).reshape(4, 2, 3 * sz.part // 8, width)
    half_qkv = lambda index: lax.dynamic_index_in_dim(g_qkv, index, 1, keepdims=False).reshape(-1, width)
    got_qkv = to_other_y(half_qkv(1 - y))
    partial_one = rowwise(dot_nn(grad_qkv, w_qkv).astype(bf16))
    grad_one = quad_sum(partial_one.reshape(2, 2, rows, width), 6)
    g_out = to_places(pick(g_out, y), got_out)
    g_qkv = to_places(half_qkv(y), got_qkv)
    grains = lambda value: value.astype(bf16).reshape(-1, GRAIN, value.shape[-1])
    table_mlp, table_out = collect_mlp(sz, grains(g_fc), grains(g_proj), grains(g_out))
    table_out = by_head(table_out.reshape(4, -1, sz.part))

    normed_one, rs_one = norm_parts(inputs)
    input_grad = (grad_res + norm_back(normed_one, rs_one, grad_one, vectors[0])).astype(bf16)

    def placed(vector):
        spread = jnp.zeros((1, width), f32)
        for j in range(turns):
            block = vector[None, j * pair : (j + 1) * pair]
            spread = lax.dynamic_update_slice_in_dim(spread, block, (4 * j + quarter) * pair, 1)
        end = jnp.where(quarter == 0, vector[turns * pair : turns * pair + rest], 0.0)
        return jnp.concatenate([spread[0, : width - rest], end])

    sums = jnp.sum(grad_qkv.astype(f32), axis=0)
    bias_sum = jnp.sum(grad_fc.astype(f32), axis=0).reshape(8, hidden // 32)[jnp.array(SPOTS)]
    fc_rows = lax.dynamic_update_slice_in_dim(
        jnp.zeros((hidden // 4 // GRAIN, 4, GRAIN), f32), bias_sum.reshape(-1, 1, GRAIN), quarter, 1
    )
    grad_vectors = jnp.concatenate(
        [
            jnp.stack(
                [
                    jnp.sum(grad_one * normed_one, axis=0),
                    jnp.sum(grad_one, axis=0),
                    placed(sums[: sz.part]),
                    placed(sums[2 * sz.part :]),
                    jnp.sum(grad_attn.astype(f32), axis=0),
                    jnp.sum(grad_two * normed_two, axis=0),
                    jnp.sum(grad_two, axis=0),
                    jnp.sum(cot, axis=0),
                ]
            ),
            fc_rows.reshape(hidden // width, width),
        ]
    )
    count = grad_vectors.shape[0]
    grad_vectors = jnp.pad(grad_vectors, ((0, sz.vec * GRAIN - count), (0, 0)))
    table_qkv, all_vectors = collect_rest(sz, grains(g_qkv), grad_vectors.reshape(sz.vec, GRAIN, width))
    grad_vectors = jnp.sum(all_vectors.reshape(32, sz.vec * GRAIN, width), axis=0)[:count]
    me = flat_id(y, c, z, x)
    row = me * (sz.block * GRAIN) + lax.broadcasted_iota(jnp.int32, (sz.block * GRAIN, 1), 0)
    used = (sz.vec_start % sz.block) * GRAIN
    tail = jnp.pad(grad_vectors, ((used, sz.block * GRAIN - used - count), (0, 0)))
    param_grad = jnp.where(
        row < sz.out_start * GRAIN,
        flat(table_qkv).astype(f32),
        jnp.where(
            row < sz.fc_start * GRAIN,
            table_out.astype(f32),
            jnp.where(row < sz.vec_start * GRAIN, flat(table_mlp).astype(f32), tail),
        ),
    )
    return (output, input_grad, param_grad)


def fits_quad(mesh, tokens, params, lengths):
    dp, cp = mesh.shape["dp"], mesh.shape["cp"]
    rows = tokens.shape[0] // (dp * cp)
    width = tokens.shape[1]
    blocks = params.shape[0] // (dp * cp)
    return (
        (dp, cp) == (4, 8)
        and lengths.shape[1] == 2
        and rows * cp == lengths.shape[1] * MIN_LEN
        and rows % 128 == 0
        and blocks % GRAIN == 0
        and (HEADS, HEAD_DIM, FF, width) == (25, 64, 6400, 1600)
    )


def solution(mesh):
    in_specs = (P(("dp", "cp"), None), P(("dp", "cp"), None), P(("dp", "cp"), None), P("dp", None))
    out_specs = (P(("dp", "cp"), None), P(("dp", "cp"), None), P(("dp", "cp"), None))

    def step(tokens, params, out_grad, lengths):
        body = per_device_quad if fits_quad(mesh, tokens, params, lengths) else per_device_general

        return jax.shard_map(
            body, mesh=mesh, in_specs=in_specs, out_specs=out_specs, check_vma=False
        )(tokens, params, out_grad, lengths)

    return step
```

```python
import functools

import jax
import jax.numpy as jnp
from jax import lax
from jax.experimental import pallas as pl
from jax.experimental.layout import Layout, with_layout_constraint
from jax.experimental.pallas import tpu as pltpu
from jax.sharding import PartitionSpec as P


HEADS = 25
FF = 6400
HEAD_DIM = 64
TILE = 128
MIN_LEN = 1024
MAX_LEN = 4096


EPSILON = 1e-05
MASKED = -1e30
GELU_SCALE = 0.7978845608028654


def from_behind(value, axis, by):
    length = lax.axis_size(axis)
    pairs = [(i, i + by) for i in range(length) if 0 <= i + by < length]
    return lax.ppermute(value, axis, pairs)


def layer_norm(values, gain_row, bias_row):
    centre = values - jnp.mean(values, axis=-1, keepdims=True)
    spread = jnp.mean(centre * centre, axis=-1, keepdims=True)
    return centre * lax.rsqrt(spread + EPSILON) * gain_row + bias_row


def gelu_tanh(values):
    return (
        0.5 * values * (1.0 + jnp.tanh(GELU_SCALE * (values + 0.044715 * values * values * values)))
    )


def segment_of(position, seq_ends):
    return jnp.sum((position[:, None] >= seq_ends[None, :]).astype(jnp.int32), axis=1)


def unpack(gathered, model_width, hidden):
    out_end = 4 * model_width
    fc_end = out_end + hidden
    proj_end = fc_end + hidden
    vec_end = proj_end + 8
    return (
        gathered[0 : 3 * model_width],
        gathered[3 * model_width : out_end],
        gathered[out_end:fc_end],
        gathered[fc_end:proj_end],
        gathered[proj_end:vec_end].astype(jnp.float32),
        gathered[vec_end : vec_end + hidden // model_width].astype(jnp.float32).reshape(hidden),
    )


def matmul_nt(left_mat, right_mat):
    return lax.dot_general(
        left_mat, right_mat, (((1,), (1,)), ((), ())), preferred_element_type=jnp.float32
    )


def matmul_tn(left_mat, right_mat):
    return lax.dot_general(
        left_mat, right_mat, (((0,), (0,)), ((), ())), preferred_element_type=jnp.float32
    )


def matmul_nn(left_mat, right_mat):
    return jnp.dot(left_mat, right_mat, preferred_element_type=jnp.float32)


def per_device_general(tokens, params, out_grad, lengths):
    tok_rows, model_width = tokens.shape
    hidden = FF
    head_count = HEADS
    head_size = HEAD_DIM
    cp_count = lax.axis_size("cp")
    group_rows = tok_rows * cp_count
    seq_count = lengths.shape[1]
    longest = min(MAX_LEN, group_rows - (seq_count - 1) * MIN_LEN)
    reach_back = min(cp_count - 1, (longest + tok_rows - TILE - 1) // tok_rows)
    pair_count = (reach_back + 2) // 2
    score_scale = head_size ** (-0.5)
    gathered = lax.all_gather(params, ("dp", "cp"), axis=0, tiled=True)
    w_attn, w_out, w_fc, w_proj, vectors, fc_bias = unpack(gathered, model_width, hidden)
    inputs = tokens.astype(jnp.float32)
    act_one = layer_norm(inputs, vectors[0], vectors[1]).astype(jnp.bfloat16)
    qkv_bias = jnp.concatenate([vectors[2], jnp.zeros_like(vectors[2]), vectors[3]])
    qkv = (matmul_nt(act_one, w_attn) + qkv_bias).astype(jnp.bfloat16)
    queries = qkv[:, :model_width].reshape(tok_rows, head_count, head_size)
    key_value = qkv[:, model_width:]
    device = lax.axis_index("cp")
    seq_ends = jnp.cumsum(lengths[0])
    query_pos = device * tok_rows + jnp.arange(tok_rows, dtype=jnp.int32)
    query_seg = segment_of(query_pos, seq_ends)
    store = jnp.zeros((2 * pair_count, tok_rows, 2 * model_width), jnp.bfloat16)
    store = store.at[0].set(key_value)

    def fetch(step_index, state_pair):
        moving, held_rows = state_pair
        moving = from_behind(moving, "cp", 1)
        return (moving, lax.dynamic_update_index_in_dim(held_rows, moving, step_index, 0))

    _, store = lax.fori_loop(1, reach_back + 1, fetch, (key_value, store))

    def pair_mask(pair_index):
        owners = 2 * pair_index + jnp.arange(2, dtype=jnp.int32)
        key_pos = (
            (device - owners)[:, None] * tok_rows + jnp.arange(tok_rows, dtype=jnp.int32)[None, :]
        ).reshape(2 * tok_rows)
        usable = jnp.broadcast_to((owners <= reach_back)[:, None], (2, tok_rows)).reshape(
            2 * tok_rows
        ) & (key_pos >= 0)
        key_seg = segment_of(key_pos, seq_ends)
        return (
            (key_seg[None, :] == query_seg[:, None])
            & (key_pos[None, :] <= query_pos[:, None])
            & usable[None, :]
        )

    def pair_rows(pair_index):
        block_rows = lax.dynamic_slice_in_dim(store, 2 * pair_index, 2, 0).reshape(
            2 * tok_rows, 2 * model_width
        )
        return (
            block_rows[:, :model_width].reshape(2 * tok_rows, head_count, head_size),
            block_rows[:, model_width:].reshape(2 * tok_rows, head_count, head_size),
        )

    def pair_scores(key_rows, allowed):
        raw_scores = (
            jnp.einsum("qhd,khd->hqk", queries, key_rows, preferred_element_type=jnp.float32)
            * score_scale
        )
        return jnp.where(allowed[None], raw_scores, MASKED)

    def visit(work):

        def step_pair(pair_index, running):
            allowed = pair_mask(pair_index)
            result = work(pair_index, allowed, running)
            return result

        return step_pair

    def add_total(pair_index, allowed, running):
        row_top, summed = running
        key_rows, _ = pair_rows(pair_index)
        scores = pair_scores(key_rows, allowed)
        new_top = jnp.maximum(row_top, jnp.max(scores, axis=-1, keepdims=True))
        summed = summed * jnp.exp(row_top - new_top) + jnp.sum(
            jnp.exp(scores - new_top), axis=-1, keepdims=True
        )
        return (new_top, summed)

    start_top = jnp.full((head_count, tok_rows, 1), MASKED, jnp.float32)
    start_sum = jnp.zeros((head_count, tok_rows, 1), jnp.float32)
    row_top, summed = lax.fori_loop(0, pair_count, visit(add_total), (start_top, start_sum))
    log_total = row_top + jnp.log(summed)

    def add_mix(pair_index, allowed, running):
        key_rows, value_rows = pair_rows(pair_index)
        prob_rows = jnp.exp(pair_scores(key_rows, allowed) - log_total).astype(jnp.bfloat16)
        return running + jnp.einsum(
            "hqk,khd->qhd", prob_rows, value_rows, preferred_element_type=jnp.float32
        )

    mixed_full = lax.fori_loop(
        0, pair_count, visit(add_mix), jnp.zeros((tok_rows, head_count, head_size), jnp.float32)
    )
    mixed = mixed_full.reshape(tok_rows, model_width).astype(jnp.bfloat16)
    attn_out = matmul_nt(mixed, w_out) + vectors[4]
    residual = inputs + attn_out
    act_two = layer_norm(residual, vectors[5], vectors[6]).astype(jnp.bfloat16)
    pre_act = matmul_nt(act_two, w_fc) + fc_bias
    act_hidden = gelu_tanh(pre_act).astype(jnp.bfloat16)
    output = (residual + matmul_nn(act_hidden, w_proj) + vectors[7]).astype(jnp.bfloat16)
    gathered = lax.all_gather(params, ("dp", "cp"), axis=0, tiled=True)
    w_attn, w_out, w_fc, w_proj, vectors, fc_bias = unpack(gathered, model_width, hidden)
    grad_out_f = out_grad.astype(jnp.float32)
    grad_hidden = matmul_nt(out_grad, w_proj)
    _, pull_gelu = jax.vjp(gelu_tanh, pre_act)
    grad_fc = pull_gelu(grad_hidden)[0].astype(jnp.bfloat16)
    grad_act_two = matmul_nn(grad_fc, w_fc)
    _, pull_two = jax.vjp(layer_norm, residual, vectors[5], vectors[6])
    grad_res_norm, grad_gain_two, grad_bias_two = pull_two(grad_act_two)
    grad_res = grad_out_f + grad_res_norm
    grad_attn = grad_res.astype(jnp.bfloat16)
    grad_mix = (
        matmul_nn(grad_attn, w_out).astype(jnp.bfloat16).reshape(tok_rows, head_count, head_size)
    )
    grad_dot = jnp.transpose(jnp.sum(grad_mix.astype(jnp.float32) * mixed_full, axis=-1), (1, 0))[
        :, :, None
    ]

    def add_grads(pair_index, allowed, running):
        grad_query, grad_store = running
        key_rows, value_rows = pair_rows(pair_index)
        prob_rows = jnp.exp(pair_scores(key_rows, allowed) - log_total)
        grad_probs = jnp.einsum(
            "qhd,khd->hqk", grad_mix, value_rows, preferred_element_type=jnp.float32
        )
        grad_scores = (prob_rows * (grad_probs - grad_dot)).astype(jnp.bfloat16)
        grad_query = (
            grad_query
            + jnp.einsum("hqk,khd->qhd", grad_scores, key_rows, preferred_element_type=jnp.float32)
            * score_scale
        )
        grad_keys = (
            jnp.einsum("hqk,qhd->khd", grad_scores, queries, preferred_element_type=jnp.float32)
            * score_scale
        )
        grad_values = jnp.einsum(
            "hqk,qhd->khd",
            prob_rows.astype(jnp.bfloat16),
            grad_mix,
            preferred_element_type=jnp.float32,
        )
        pair_grad = jnp.concatenate(
            [
                grad_keys.reshape(2 * tok_rows, model_width),
                grad_values.reshape(2 * tok_rows, model_width),
            ],
            axis=1,
        )
        pair_grad = pair_grad.reshape(2, tok_rows, 2 * model_width)
        grad_store = lax.dynamic_update_slice_in_dim(grad_store, pair_grad, 2 * pair_index, 0)
        return (grad_query, grad_store)

    start_query = jnp.zeros((tok_rows, head_count, head_size), jnp.float32)
    start_store = jnp.zeros((2 * pair_count, tok_rows, 2 * model_width), jnp.float32)
    grad_query, grad_store = lax.fori_loop(
        0, pair_count, visit(add_grads), (start_query, start_store)
    )

    def send_back(step_index, moving):
        moving = moving + lax.dynamic_index_in_dim(
            grad_store, reach_back - step_index, 0, keepdims=False
        )
        return from_behind(moving.astype(jnp.bfloat16), "cp", -1).astype(moving.dtype)

    returned = lax.fori_loop(
        0, reach_back, send_back, jnp.zeros((tok_rows, 2 * model_width), jnp.float32)
    )
    grad_kv = returned + grad_store[0]
    grad_qkv = jnp.concatenate([grad_query.reshape(tok_rows, model_width), grad_kv], axis=1).astype(
        jnp.bfloat16
    )
    grad_qkv_f = grad_qkv.astype(jnp.float32)
    grad_act_one = matmul_nn(grad_qkv, w_attn)
    _, pull_one = jax.vjp(layer_norm, inputs, vectors[0], vectors[1])
    grad_in_norm, grad_gain_one, grad_bias_one = pull_one(grad_act_one)
    input_grad = (grad_res + grad_in_norm).astype(jnp.bfloat16)
    grad_vectors = jnp.stack(
        [
            grad_gain_one,
            grad_bias_one,
            jnp.sum(grad_qkv_f[:, :model_width], axis=0),
            jnp.sum(grad_qkv_f[:, 2 * model_width :], axis=0),
            jnp.sum(grad_attn.astype(jnp.float32), axis=0),
            grad_gain_two,
            grad_bias_two,
            jnp.sum(grad_out_f, axis=0),
        ]
    )
    grad_fc_bias = jnp.sum(grad_fc.astype(jnp.float32), axis=0).reshape(
        hidden // model_width, model_width
    )
    used_rows = 4 * model_width + 2 * hidden + 8 + hidden // model_width
    total_rows = gathered.shape[0]
    local_grad = jnp.concatenate(
        [
            matmul_tn(grad_qkv, act_one),
            matmul_tn(grad_attn, mixed),
            matmul_tn(grad_fc, act_two),
            matmul_tn(act_hidden, out_grad),
            grad_vectors,
            grad_fc_bias,
            jnp.zeros((total_rows - used_rows, model_width), jnp.float32),
        ],
        axis=0,
    )
    dp_count = lax.axis_size("dp")
    device_count = dp_count * cp_count
    share_rows = total_rows // device_count
    spread_rows = local_grad.reshape(device_count, 1, share_rows, model_width)
    received = lax.all_to_all(
        spread_rows.astype(jnp.bfloat16), ("dp", "cp"), split_axis=0, concat_axis=1, tiled=True
    ).astype(spread_rows.dtype)
    param_grad = jnp.sum(received, axis=1).reshape(share_rows, model_width)
    return (output, input_grad, param_grad)


MESH = pl.DeviceIdType.MESH
GRAIN = 8
NT = (((1,), (1,)), ((), ()))
TN = (((0,), (0,)), ((), ()))


def dot_nt(a, b):
    return lax.dot_general(a, b, NT, preferred_element_type=jnp.float32)


def dot_tn(a, b):
    return lax.dot_general(a, b, TN, preferred_element_type=jnp.float32)


def dot_nn(a, b):
    return jnp.dot(a, b, preferred_element_type=jnp.float32)


def flat_id(y, c, z, x):
    return ((y * 2 + c) * 4 + z) * 2 + x


def permute(value, move):
    pairs = []
    for y in range(2):
        for c in range(2):
            for z in range(4):
                for x in range(2):
                    to = move(y, c, z, x)
                    if to is not None:
                        pairs.append((flat_id(y, c, z, x), flat_id(*to)))
    return lax.ppermute(value, ("dp", "cp"), pairs)


def over_y(value):
    return permute(value, lambda y, c, z, x: (1 - y, c, z, x))


def over_z(value, by):
    return permute(value, lambda y, c, z, x: (y, c, (z + by) % 4, x))


class Sizes:
    def __init__(self, width, hidden, heads, head_size, rows):
        self.heads = heads
        self.head_size = head_size
        self.quarter_heads = -(-heads // 4)
        self.part = self.quarter_heads * head_size
        self.part_grains = self.part // GRAIN
        self.width_grains = width // GRAIN
        self.spill = 4 * self.part_grains - self.width_grains
        self.qkv = 3 * self.part_grains // 8
        self.out = self.part_grains // 8
        self.mlp = hidden // 4 // 8 // GRAIN
        self.block = rows // GRAIN
        self.out_start = 3 * self.width_grains
        self.fc_start = 4 * self.width_grains
        self.proj_start = self.fc_start + hidden // GRAIN
        self.vec_start = self.proj_start + hidden // GRAIN
        self.vec = 2
        self.head_grains = head_size // GRAIN
        self.fc_turn = self.turn(self.fc_start)
        self.proj_turn = self.turn(self.proj_start)

    def turn(self, start):
        return start // (2 * self.block) % 4


def spot_of_range(r):
    y = r // 6 + (r % 2) * ((r // 3) % 2)
    u = (r - (r + 5) // 8 - (r + 3) // 8) % 4
    return y, u


def range_of_spot(y, u):
    first = u + u // 3
    second = (1 - u // 2) * (u + 6) + (u // 2) * (2 * u - 1)
    return (1 - y) * first + y * second


RANGES = (0, 1, 2, 4, 6, 7, 3, 5)
SPOTS = (0, 1, 2, 6, 3, 7, 4, 5)


def slot_qkv(y, z):
    return 2 * z + y


def slot_out(y, z):
    return 4 * y + z


def slot_turned(turn):
    return lambda y, z: 4 * y + (z + 4 - turn) % 4


def my_place():
    dp = lax.axis_index("dp")
    cp = lax.axis_index("cp")
    return dp // 2, dp % 2, cp // 2, cp % 2


def device_of(quarter, y, z):
    return y * 2 + quarter // 2, z * 2 + quarter % 2


class Wires:
    def __init__(self, send_sems, recv_sems):
        self.send_sems = send_sems
        self.recv_sems = recv_sems
        self.count = 0

    def to(self, src, dst, dp, cp):
        index = self.count
        self.count += 1
        return pltpu.make_async_remote_copy(
            src_ref=src,
            dst_ref=dst,
            send_sem=self.send_sems.at[index],
            recv_sem=self.recv_sems.at[index],
            device_id=(dp, cp),
            device_id_type=MESH,
        )


class PlaceGather:
    def __init__(self, wires, full, slot, steps=(1, 2, 3), over=(0, 1, 2, 3), rows=None):
        self.full = full
        self.dp, self.cp = lax.axis_index("dp"), lax.axis_index("cp")
        self.y, self.z, self.x = self.dp // 2, self.cp // 2, self.cp % 2
        self.above = (self.dp, ((self.z + 1) % 4) * 2 + self.x)
        self.below = (self.dp, ((self.z + 3) % 4) * 2 + self.x)
        self.across = ((self.dp + 2) % 4, self.cp)

        def share(by, to):
            spot = slot(self.y, (self.z + 4 + by) % 4)
            view = full.at[spot] if rows is None else full.at[pl.ds(pl.multiple_of(spot * rows, GRAIN), rows)]
            return wires.to(view, view, *to)

        self.steps = steps
        self.up = {k: share(1 - k, self.above) for k in steps}
        self.down = {k: share(k - 1, self.below) for k in steps}
        self.over = {d: share(d, self.across) for d in over}

    def partners(self):
        return [self.above, self.below, self.across]

    def start(self):
        if 1 in self.steps:

            @pl.when(self.z < 3)
            def _():
                self.up[1].start()

            @pl.when(self.z > 0)
            def _():
                self.down[1].start()

        if 0 in self.over:
            self.over[0].start()

    def forward(self, steps=(1, 2, 3)):
        for k in steps:

            @pl.when(self.z >= k)
            def _():
                if k in self.steps:
                    self.up[k].wait_recv()
                if k + 1 in self.steps:

                    @pl.when(self.z < 3)
                    def _():
                        self.up[k + 1].start()

                if 4 - k in self.over:
                    self.over[4 - k].start()

            @pl.when(self.z <= 3 - k)
            def _():
                if k in self.steps:
                    self.down[k].wait_recv()
                if k + 1 in self.steps:

                    @pl.when(self.z > 0)
                    def _():
                        self.down[k + 1].start()

                if k in self.over:
                    self.over[k].start()

    def finish(self):
        for copy in self.over.values():
            copy.wait_recv()
        for copy in self.over.values():
            copy.wait_send()
        for k in self.steps:

            @pl.when(jnp.logical_and(self.z >= k - 1, self.z < 3))
            def _():
                self.up[k].wait_send()

            @pl.when(jnp.logical_and(self.z <= 4 - k, self.z > 0))
            def _():
                self.down[k].wait_send()


class QuadGather:
    def __init__(self, wires, block, full, local_sem):
        self.wires = wires
        self.block = block
        self.full = full
        self.dp, self.cp = lax.axis_index("dp"), lax.axis_index("cp")
        self.c, self.x = self.dp % 2, self.cp % 2
        self.over_x = (self.dp, self.cp + 1 - 2 * self.x)
        self.over_c = (self.dp + 1 - 2 * self.c, self.cp)
        self.local_sem = local_sem

    def spot(self, c, x):
        if len(self.full.shape) > len(self.block.shape):
            return self.full.at[c, x]
        rows = self.block.shape[0]
        return self.full.at[pl.ds(pl.multiple_of((c * 2 + x) * rows, rows), rows)]

    def start(self):
        spot = self.spot(self.c, self.x)
        self.by_x = self.wires.to(self.block, spot, *self.over_x)
        self.by_c = self.wires.to(self.block, spot, *self.over_c)
        self.by_x.start()
        self.by_c.start()
        self.local = pltpu.make_async_copy(self.block, spot, self.local_sem)
        self.local.start()

    def forward(self):
        self.by_x.wait_recv()
        spot = self.spot(self.c, 1 - self.x)
        self.pass_on = self.wires.to(spot, spot, *self.over_c)
        self.pass_on.start()

    def finish(self):
        self.by_c.wait_recv()
        self.pass_on.wait_recv()
        self.by_x.wait_send()
        self.by_c.wait_send()
        self.pass_on.wait_send()
        self.local.wait()


def open_kernel(
    sz, p_ref, tok_ref, cot_ref, qkv_ref, out_ref, fc_ref, proj_ref, vec_ref, tok_all, cot_all,
    spread_sems, kind_sems, send_sems, recv_sems, local_sems,
):
    y, c, z, x = my_place()
    me = flat_id(y, c, z, x)
    wires = Wires(send_sems, recv_sems)
    tok = QuadGather(wires, tok_ref, tok_all, local_sems.at[0])
    cot = QuadGather(wires, cot_ref, cot_all, local_sems.at[1])

    def send(grain, ref, spot, slot, quarter, py, pz, sem, recv):
        dp, cp = device_of(quarter, py, pz)
        mine = dp * 8 + cp == me

        @pl.when(mine)
        def _():
            pltpu.make_async_copy(p_ref.at[grain], ref.at[spot, slot], recv).start()

        @pl.when(jnp.logical_not(mine))
        def _():
            pltpu.make_async_remote_copy(
                src_ref=p_ref.at[grain],
                dst_ref=ref.at[spot, slot],
                send_sem=sem,
                recv_sem=recv,
                device_id=(dp, cp),
                device_id_type=MESH,
            ).start()

    def sent(grain, ref, spot, slot, quarter, py, pz, sem, recv):
        dp, cp = device_of(quarter, py, pz)

        @pl.when(dp * 8 + cp != me)
        def _():
            pltpu.make_async_copy(p_ref.at[grain], p_ref.at[grain], sem).wait()

    def headed(act, grain):
        table = me * sz.block + grain
        part = table // sz.width_grains
        inner = table % sz.width_grains
        head = inner // sz.head_grains
        rest = inner % sz.head_grains

        def one(quarter, sem):
            local = part * sz.part_grains + (2 * (head // 8) + head % 2) * sz.head_grains + rest
            spot = local // sz.qkv
            act(grain, qkv_ref, spot, local % sz.qkv, quarter, spot % 2, spot // 2, sem, kind_sems.at[0])

        @pl.when(table < sz.out_start)
        def _():
            one((head // 2) % 4, spread_sems.at[grain])

            @pl.when(head == sz.heads - 1)
            def _():
                for quarter in range(1, 4):
                    one(quarter, spread_sems.at[sz.block + (quarter - 1) * sz.head_grains + rest])

    def outward(act, grain):
        local = me * sz.block + grain - sz.out_start

        def one(quarter, inner, sem):
            spot = inner // sz.out
            act(grain, out_ref, spot, inner % sz.out, quarter, spot // 4, spot % 4, sem, kind_sems.at[1])

        @pl.when(jnp.logical_and(local >= 0, local < sz.width_grains))
        def _():
            one(local // sz.part_grains, local % sz.part_grains, spread_sems.at[grain])

            @pl.when(local < sz.spill)
            def _():
                one(3, sz.part_grains - sz.spill + local, spread_sems.at[sz.block + 3 * sz.head_grains + local])

    def plain(act, grain, base, turn, ref, recv):
        offset = me * sz.block + grain - base

        @pl.when(jnp.logical_and(offset >= 0, offset < 32 * sz.mlp))
        def _():
            local = offset // 4
            py, u = spot_of_range(local // sz.mlp)
            act(
                grain, ref, py * 4 + u, local % sz.mlp, offset % 4, py, (u + turn) % 4,
                spread_sems.at[grain], recv,
            )

    def heads(act):
        def one(grain, _):
            headed(act, grain)
            return 0

        lax.fori_loop(0, sz.block, one, 0)

    def others(act):
        def one(grain, _):
            outward(act, grain)
            plain(act, grain, sz.fc_start, sz.fc_turn, fc_ref, kind_sems.at[2])
            plain(act, grain, sz.proj_start, sz.proj_turn, proj_ref, kind_sems.at[3])
            return 0

        lax.fori_loop(0, sz.block, one, 0)

    owner = sz.vec_start // sz.block
    spot = sz.vec_start % sz.block

    def vector_sends(act):
        @pl.when(me == owner)
        def _():
            def to(device, _):
                @pl.when(device != me)
                def _():
                    act(
                        pltpu.make_async_remote_copy(
                            src_ref=p_ref.at[pl.ds(spot, sz.vec)],
                            dst_ref=vec_ref,
                            send_sem=spread_sems.at[sz.block + 3 * sz.head_grains + sz.spill + device],
                            recv_sem=kind_sems.at[4],
                            device_id=(device // 8, device % 8),
                            device_id_type=MESH,
                        )
                    )

                return 0

            lax.fori_loop(0, 32, to, 0)

    heads(send)
    tok.start()
    mine = slot_qkv(y, z)
    pltpu.make_async_copy(qkv_ref.at[mine], qkv_ref.at[mine], kind_sems.at[0]).wait()
    weights = PlaceGather(wires, qkv_ref, slot_qkv)
    weights.start()
    vector_sends(lambda copy: copy.start())

    @pl.when(me == owner)
    def _():
        pltpu.make_async_copy(p_ref.at[pl.ds(spot, sz.vec)], vec_ref, kind_sems.at[4]).start()

    others(send)
    cot.start()
    tok.forward()
    weights.forward()
    early = []
    for index, (ref, slot) in enumerate(((out_ref, slot_out), (fc_ref, slot_turned(sz.fc_turn)))):
        view = ref.at[slot(y, z)]
        pltpu.make_async_copy(view, view, kind_sems.at[index + 1]).wait()
        early.append(PlaceGather(wires, ref, slot, steps=(1,), over=(0,)))
        early[-1].start()
    cot.forward()
    heads(sent)
    others(sent)
    vector_sends(lambda copy: copy.wait_send())
    view = proj_ref.at[slot_turned(sz.proj_turn)(y, z)]
    pltpu.make_async_copy(view, view, kind_sems.at[3]).wait()
    pltpu.make_async_copy(vec_ref, vec_ref, kind_sems.at[4]).wait()
    tok.finish()
    cot.finish()
    weights.finish()
    for first in early:
        first.forward((1,))
        first.finish()


HBM = pl.BlockSpec(memory_space=pl.ANY)
VMEM = pl.BlockSpec(memory_space=pltpu.VMEM)
REMOTE = pltpu.CompilerParams(has_side_effects=True)


def remote_params(ident=None, vmem=None):
    return pltpu.CompilerParams(has_side_effects=True, collective_id=ident, vmem_limit_bytes=vmem)


def greet(partners):
    barrier = pltpu.get_barrier_semaphore()
    for dp, cp in partners:
        pl.semaphore_signal(barrier, inc=1, device_id=(dp, cp), device_id_type=MESH)
    pl.semaphore_wait(barrier, len(partners))


def cost(us):
    return pl.CostEstimate(flops=0, bytes_accessed=int(us * 3.0e6), transcendentals=0)


def wire_sems(count):
    return [pltpu.SemaphoreType.DMA((count,)), pltpu.SemaphoreType.DMA((count,))]


def open_call(sz, table, tokens, cotangent):
    rows, width = tokens.shape

    def like(*shape):
        return jax.ShapeDtypeStruct(shape + (width,), table.dtype)

    return pl.pallas_call(
        functools.partial(open_kernel, sz),
        out_shape=(
            like(8, sz.qkv, GRAIN),
            like(8, sz.out, GRAIN),
            like(8, sz.mlp, GRAIN),
            like(8, sz.mlp, GRAIN),
            like(sz.vec, GRAIN),
            like(2, 2, rows),
            like(2, 2, rows),
        ),
        in_specs=[HBM, VMEM, VMEM],
        out_specs=[HBM] * 7,
        scratch_shapes=[
            pltpu.SemaphoreType.DMA((sz.block + 3 * sz.head_grains + sz.spill + 32,)),
            pltpu.SemaphoreType.DMA((5,)),
            *wire_sems(22),
            pltpu.SemaphoreType.DMA((2,)),
        ],
        compiler_params=REMOTE,
        name="open",
    )(table, tokens, cotangent)


def forward_kernel(
    heads, size, fc_turn, proj_turn, q_ref, kv_ref, out_in, fc_in, proj_in,
    mix_ref, lse_ref, before_ref, mixed_ref, out_ref, fc_ref, proj_ref, out_all,
    stage, send_sems, recv_sems, local_sems,
):
    y, c, z, x = my_place()
    dp, cp = lax.axis_index("dp"), lax.axis_index("cp")
    wires = Wires(send_sems, recv_sems)
    part = heads * size
    rows = q_ref.shape[0] // 2
    blk = 256
    scale = size**-0.5
    odd = z % 2 == 1
    w_out = PlaceGather(wires, out_ref, slot_out, steps=(2, 3), over=(1, 2, 3))
    w_fc = PlaceGather(wires, fc_ref, slot_turned(fc_turn), steps=(2, 3), over=(1, 2, 3))
    w_proj = PlaceGather(wires, proj_ref, slot_turned(proj_turn), steps=(1,), over=(0,))
    others = [(c, 1 - x), (1 - c, x), (1 - c, 1 - x)]
    quad = [(y * 2 + tc, z * 2 + tx) for tc, tx in others]
    greet(w_out.partners() + quad)
    keys = wires.to(kv_ref, before_ref, dp, (cp + 2) % 8)

    w_out.forward()

    @pl.when(jnp.logical_not(odd))
    def _():
        keys.start()

    w_fc.forward((1,))

    def own(group, _):
        start = group * rows
        for i in range(rows // blk):
            here = pl.ds(pl.multiple_of(start + i * blk, blk), blk)
            seen = (i + 1) * blk
            keys_at = pl.ds(pl.multiple_of(start, rows), seen)
            lane = lax.broadcasted_iota(jnp.int32, (blk, seen), 1)
            line = lax.broadcasted_iota(jnp.int32, (blk, seen), 0)
            allowed = lane <= line + i * blk
            for h in range(heads):
                cols = slice(h * size, (h + 1) * size)
                vals = slice(part + h * size, part + (h + 1) * size)
                s = dot_nt(q_ref[here, cols], kv_ref[keys_at, cols]) * scale
                s = jnp.where(allowed, s, MASKED)
                top = jnp.max(s, axis=-1, keepdims=True)
                p = jnp.exp(s - top)
                total = jnp.sum(p, axis=-1, keepdims=True)
                mix_ref[here, cols] = dot_nn(p.astype(jnp.bfloat16), kv_ref[keys_at, vals]) / total
                lse_ref[here, h : h + 1] = top + jnp.log(total)
        return 0

    lax.fori_loop(0, 2, own, 0)

    def add_before(index, _):
        here = pl.ds(pl.multiple_of(index * blk, blk), blk)
        keys_at = pl.ds(pl.multiple_of((index * blk) // rows * rows, rows), rows)
        for h in range(heads):
            cols = slice(h * size, (h + 1) * size)
            vals = slice(part + h * size, part + (h + 1) * size)
            s = dot_nt(q_ref[here, cols], before_ref[keys_at, cols]) * scale
            lse = lse_ref[here, h : h + 1]
            top = jnp.maximum(lse, jnp.max(s, axis=-1, keepdims=True))
            p = jnp.exp(s - top)
            kept = jnp.exp(lse - top)
            total = kept + jnp.sum(p, axis=-1, keepdims=True)
            mix = mix_ref[here, cols] * kept + dot_nn(p.astype(jnp.bfloat16), before_ref[keys_at, vals])
            mix_ref[here, cols] = mix / total
            lse_ref[here, h : h + 1] = top + jnp.log(total)
        return 0

    w_out.finish()
    whole = QuadGather(wires, out_ref, out_all, local_sems.at[0])
    whole.start()

    @pl.when(z < 3)
    def _():
        w_fc.forward((2,))

    @pl.when(odd)
    def _():
        keys.wait_recv()
        lax.fori_loop(0, 2 * rows // blk, add_before, 0)

    def round_off(index, _):
        here = pl.ds(pl.multiple_of(index * blk, blk), blk)
        stage[here, :] = mix_ref[here, :].astype(stage.dtype)
        return 0

    lax.fori_loop(0, 2 * rows // blk, round_off, 0)

    @pl.when(z == 3)
    def _():
        w_fc.forward((2,))

    mine = c * 2 + x
    each = rows // 2
    swaps = []
    for (tc, tx), (tdp, tcp) in zip(others, quad):
        block = stage.at[pl.ds(pl.multiple_of((tc * 2 + tx) * each, each), each)]
        swaps.append(wires.to(block, mixed_ref.at[mine], tdp, tcp))
    for copy in swaps:
        copy.start()
    local = pltpu.make_async_copy(
        stage.at[pl.ds(pl.multiple_of(mine * each, each), each)], mixed_ref.at[mine], local_sems.at[1]
    )
    local.start()
    whole.forward()
    w_fc.forward((3,))
    w_proj.start()
    for copy in swaps:
        copy.wait_recv()
    whole.finish()
    w_fc.finish()
    w_proj.forward((1,))
    w_proj.finish()
    for copy in swaps:
        copy.wait_send()
    local.wait()

    @pl.when(jnp.logical_not(odd))
    def _():
        keys.wait_send()


def forward_call(sz, q, kv, w_out, w_fc, w_proj):
    part = sz.part
    rows = q.shape[0]

    def like(value, *lead):
        return jax.ShapeDtypeStruct(lead + value.shape, value.dtype)

    return pl.pallas_call(
        functools.partial(forward_kernel, sz.quarter_heads, sz.head_size, sz.fc_turn, sz.proj_turn),
        out_shape=(
            jax.ShapeDtypeStruct((rows, part), jnp.float32),
            jax.ShapeDtypeStruct((rows, 8), jnp.float32),
            like(kv),
            jax.ShapeDtypeStruct((4, rows // 4, part), jnp.bfloat16),
            like(w_out),
            like(w_fc),
            like(w_proj),
            like(w_out, 2, 2),
        ),
        in_specs=[VMEM, VMEM, HBM, HBM, HBM],
        out_specs=[VMEM] * 4 + [HBM] * 4,
        input_output_aliases={2: 4, 3: 5, 4: 6},
        scratch_shapes=[
            pltpu.VMEM((rows, part), jnp.bfloat16),
            *wire_sems(37),
            pltpu.SemaphoreType.DMA((2,)),
        ],
        cost_estimate=cost(120),
        compiler_params=remote_params(1, 56 << 20),
        name="forward",
    )(q, kv, w_out, w_fc, w_proj)


class QuadSum:
    step = 32

    def __init__(self, in_ref, out_ref, got_c, stage, got_x, send_sems, recv_sems):
        self.y, self.c, self.z, self.x = my_place()
        dp, cp = lax.axis_index("dp"), lax.axis_index("cp")
        wires = Wires(send_sems, recv_sems)
        self.in_ref, self.out_ref, self.got_c, self.stage, self.got_x = in_ref, out_ref, got_c, stage, got_x
        self.partners = [(dp + 1 - 2 * self.c, cp), (dp, cp + 1 - 2 * self.x)]
        self.by_c = wires.to(in_ref.at[1 - self.c], got_c, *self.partners[0])
        self.by_x = wires.to(stage, got_x, *self.partners[1])

    def each(self, act):
        def one(index, _):
            act(pl.ds(pl.multiple_of(index * self.step, self.step), self.step))
            return 0

        lax.fori_loop(0, self.out_ref.shape[0] // self.step, one, 0)

    def start(self, greeting=True):
        if greeting:
            greet(self.partners)
        self.by_c.start()

    def middle(self):
        c, x = self.c, self.x
        self.by_c.wait_recv()

        def to_send(span):
            self.stage[span, :] = (
                self.in_ref[c, 1 - x, span, :].astype(jnp.float32) + self.got_c[1 - x, span, :].astype(jnp.float32)
            ).astype(self.stage.dtype)

        self.each(to_send)
        self.by_x.start()

    def finish(self):
        c, x = self.c, self.x
        self.by_x.wait_recv()

        def to_add(span):
            self.out_ref[span, :] = (
                self.in_ref[c, x, span, :].astype(jnp.float32)
                + self.got_c[x, span, :].astype(jnp.float32)
                + self.got_x[span, :].astype(jnp.float32)
            )

        self.each(to_add)
        self.by_c.wait_send()
        self.by_x.wait_send()


def quad_scratch(partial):
    rows, width = partial.shape[2:]
    return [
        pltpu.VMEM((2, rows, width), partial.dtype),
        pltpu.VMEM((rows, width), partial.dtype),
        pltpu.VMEM((rows, width), partial.dtype),
        *wire_sems(2),
    ]


def fill_rows(left, first, right, out, step=160):
    def one(index, _):
        here = pl.ds(pl.multiple_of(index * step, step), step)
        rows = pl.ds(pl.multiple_of(first + index * step, 32), step)
        out[here, :] = dot_nn(left[rows, :], right[...]).astype(out.dtype)
        return 0

    lax.fori_loop(0, out.shape[0] // step, one, 0)


def fill_columns(left, right, out, step=256):
    def one(index, _):
        here = pl.ds(pl.multiple_of(index * step, step), step)
        out[here, :] = dot_tn(left[:, here], right[...]).astype(out.dtype)
        return 0

    lax.fori_loop(0, out.shape[0] // step, one, 0)


def gelu_parts(f):
    t = jnp.tanh(GELU_SCALE * (f + 0.044715 * f * f * f))
    return t, 0.5 * f * (1.0 + t)


def gelu_slope(f, t):
    return 0.5 * (1.0 + t) + 0.5 * f * (1.0 - t * t) * GELU_SCALE * (1.0 + 3.0 * 0.044715 * f * f)


def middle_kernel(
    proj_turn, act_ref, cot, w_fc, bias, proj_in,
    total, act_all, hid_t, proj_sum, fc_sent, fc_kept, bias_grad, proj_ref,
    f_all, df_t, w_proj, proj_sent, proj_got, term, got_c, stage, got_x,
    send_sems, recv_sems, sum_send, sum_recv, local_sems,
):
    y, c, _, _ = my_place()
    wires = Wires(send_sems, recv_sems)
    hidden = w_fc.shape[0]
    half = hidden // 2
    step = 160
    quad = QuadGather(wires, act_ref, act_all, local_sems.at[0])
    places = PlaceGather(
        wires, proj_ref, slot_turned(proj_turn), steps=(2, 3), over=(1, 2, 3), rows=hidden // 8
    )
    across = wires.to(proj_sent, proj_got, *places.across)
    summed = QuadSum(term, total, got_c, stage, got_x, sum_send, sum_recv)
    greet(places.partners() + [quad.over_x, quad.over_c])
    quad.start()
    places.forward((1, 2))
    quad.forward()
    quad.finish()

    def hidden_rows(first):
        def one(index, _):
            rows = pl.ds(pl.multiple_of(first + index * step, 32), step)
            f = dot_nt(w_fc[rows, :], act_all[...]) + bias[rows, :]
            f_all[rows, :] = f
            hid_t[rows, :] = gelu_parts(f)[1].astype(hid_t.dtype)
            return 0

        lax.fori_loop(0, half // step, one, 0)

    hidden_rows((1 - y) * half)
    places.forward((3,))
    fill_rows(hid_t, (1 - y) * half, cot, proj_sent)
    across.start()
    hidden_rows(y * half)
    fill_rows(hid_t, y * half, cot, proj_sum)
    places.finish()
    load = pltpu.make_async_copy(proj_ref, w_proj, local_sems.at[1])
    load.start()
    load.wait()

    def back_rows(index, _):
        rows = pl.ds(pl.multiple_of(index * step, 32), step)
        f = f_all[rows, :]
        grad = dot_nt(w_proj[rows, :], cot[...])
        df = (grad * gelu_slope(f, gelu_parts(f)[0])).astype(df_t.dtype)
        df_t[rows, :] = df
        bias_grad[rows, :] = jnp.sum(df.astype(jnp.float32), axis=1, keepdims=True)
        return 0

    lax.fori_loop(0, hidden // step, back_rows, 0)
    block = term.shape[2]

    def tokens_of(core):
        for side in range(2):
            columns = pl.ds(pl.multiple_of((core * 2 + side) * block, block), block)
            term[core, side, :, :] = dot_tn(df_t[:, columns], w_fc[...]).astype(term.dtype)

    tokens_of(1 - c)
    summed.start(greeting=False)
    tokens_of(c)
    summed.middle()
    fill_rows(df_t, (1 - y) * half, act_all, fc_sent)
    fill_rows(df_t, y * half, act_all, fc_kept)
    across.wait_recv()

    def add(index, _):
        rows = pl.ds(pl.multiple_of(index * step, 32), step)
        proj_sum[rows, :] = (
            proj_sum[rows, :].astype(jnp.float32) + proj_got[rows, :].astype(jnp.float32)
        ).astype(proj_sum.dtype)
        return 0

    lax.fori_loop(0, half // step, add, 0)
    summed.finish()
    across.wait_send()


def middle_call(sz, act, cot, w_fc, bias, w_proj):
    rows, width = act.shape
    hidden = w_fc.shape[0]
    bf16, f32 = act.dtype, jnp.float32
    half = jax.ShapeDtypeStruct((hidden // 2, width), bf16)
    return pl.pallas_call(
        functools.partial(middle_kernel, sz.proj_turn),
        out_shape=(
            jax.ShapeDtypeStruct((rows, width), f32),
            jax.ShapeDtypeStruct((4 * rows, width), bf16),
            jax.ShapeDtypeStruct((hidden, 4 * rows), bf16),
            half,
            half,
            half,
            jax.ShapeDtypeStruct((hidden, 1), f32),
            jax.ShapeDtypeStruct((hidden, width), bf16),
        ),
        in_specs=[VMEM] * 4 + [HBM],
        out_specs=[VMEM] * 7 + [HBM],
        input_output_aliases={4: 7},
        scratch_shapes=[
            pltpu.VMEM((hidden, 4 * rows), f32),
            pltpu.VMEM((hidden, 4 * rows), bf16),
            pltpu.VMEM((hidden, width), bf16),
            pltpu.VMEM((hidden // 2, width), bf16),
            pltpu.VMEM((hidden // 2, width), bf16),
            pltpu.VMEM((2, 2, rows, width), bf16),
            pltpu.VMEM((2, rows, width), bf16),
            pltpu.VMEM((rows, width), bf16),
            pltpu.VMEM((rows, width), bf16),
            *wire_sems(11),
            *wire_sems(2),
            pltpu.SemaphoreType.DMA((2,)),
        ],
        cost_estimate=cost(110),
        compiler_params=remote_params(2, 63 << 20),
        name="middle",
    )(act, cot, w_fc, bias, w_proj)


def grads_kernel(act_ref, hid_t, w_proj, act_all, partial_out, send_sems, recv_sems, local_sem):
    wires = Wires(send_sems, recv_sems)
    quad = QuadGather(wires, act_ref, act_all, local_sem)
    greet([quad.over_x, quad.over_c])
    quad.start()
    fill_columns(hid_t, w_proj, partial_out)
    quad.forward()
    quad.finish()


def grads_call(act, hid_t, w_proj, ident):
    width = w_proj.shape[1]
    return pl.pallas_call(
        grads_kernel,
        out_shape=(
            jax.ShapeDtypeStruct((2, 2) + act.shape, act.dtype),
            jax.ShapeDtypeStruct((hid_t.shape[1], width), jnp.bfloat16),
        ),
        in_specs=[VMEM] * 3,
        out_specs=[HBM, VMEM],
        scratch_shapes=[*wire_sems(3), pltpu.SemaphoreType.DMA],
        cost_estimate=cost(25),
        compiler_params=remote_params(ident, 60 << 20),
        name="grads",
    )(act, hid_t, w_proj)


def row_steps(rows, step=64):
    return [slice(start, min(start + step, rows)) for start in range(0, rows, step)]


class PlaceSum:
    def __init__(self, out, got, turn, send_sems, recv_sems, filled=False):
        self.y, self.c, self.z, self.x = my_place()
        self.dp = lax.axis_index("dp")
        self.filled = filled
        self.out, self.got, self.turn = out, got, turn
        self.send_sems, self.recv_sems = send_sems, recv_sems

    def place(self, k):
        return (k + self.turn) % 4

    def put(self, k, store):
        @pl.when(self.z == self.place(k))
        def _():
            store(self.got.at[self.place(k)])

        @pl.when(self.z != self.place(k))
        def _():
            if not self.filled:
                store(self.out.at[k])
            pltpu.make_async_remote_copy(
                src_ref=self.out.at[k],
                dst_ref=self.got.at[self.z],
                send_sem=self.send_sems.at[k],
                recv_sem=self.recv_sems.at[self.z],
                device_id=(self.dp, self.place(k) * 2 + self.x),
                device_id_type=MESH,
            ).start()

    def total(self, into):
        for s in range(4):

            @pl.when(self.z != s)
            def _():
                pltpu.make_async_copy(self.got.at[s], self.got.at[s], self.recv_sems.at[s]).wait()

        for rows in row_steps(self.got.shape[1]):
            terms = [self.got[s, rows, :].astype(jnp.float32) for s in range(4)]
            into[rows, :] = (terms[0] + terms[1] + (terms[2] + terms[3])).astype(into.dtype)

    def finish(self):
        for k in range(4):

            @pl.when(self.z != self.place(k))
            def _():
                pltpu.make_async_copy(self.out.at[k], self.out.at[k], self.send_sems.at[k]).wait()


class Collector:
    def __init__(self, sz):
        self.sz = sz
        self.y, self.c, self.z, self.x = my_place()
        self.me = flat_id(self.y, self.c, self.z, self.x)
        self.quarter = self.c * 2 + self.x

    def send(self, src, dst, table, sem, recv):
        dest = table // self.sz.block

        @pl.when(dest == self.me)
        def _():
            pltpu.make_async_copy(src, dst, recv).start()

        @pl.when(dest != self.me)
        def _():
            pltpu.make_async_remote_copy(
                src_ref=src,
                dst_ref=dst,
                send_sem=sem,
                recv_sem=recv,
                device_id=(dest // 8, dest % 8),
                device_id_type=MESH,
            ).start()

    def sent(self, src, dst, table, sem, recv):
        @pl.when(table // self.sz.block != self.me)
        def _():
            pltpu.make_async_copy(src, src, sem).wait()

    def received(self, first, count, view, recv):
        block = self.sz.block
        for device in range(first // block, -(-(first + count) // block)):
            grains = min(first + count, (device + 1) * block) - max(first, device * block)

            @pl.when(self.me == device)
            def _():
                pltpu.make_async_copy(view(grains), view(grains), recv).wait()


def close_kernel(
    sz, dqkv, act, w_qkv, normed, vec_in, fc_sum, out_sum, proj_share,
    total, g_qkv, g_mlp, g_outs, vecs, qkv_share, fc_share, out_share,
    grads, got_y, qkv_out, qkv_got, fc_got, out_got, share_v, out_v, vec_v, term, got_c, stage, got_x,
    y_send, y_recv, z_send, z_recv, sum_send, sum_recv, grain_sems, kind_sems, local_sems, vec_sems,
):
    to = Collector(sz)
    y, c, z = to.y, to.c, to.z
    dp, cp = lax.axis_index("dp"), lax.axis_index("cp")
    rows = got_y.shape[1]
    block = term.shape[2]
    fc = PlaceSum(fc_sum, fc_got, sz.fc_turn, z_send.at[0], z_recv.at[0], True)
    out = PlaceSum(out_sum, out_got, 0, z_send.at[1], z_recv.at[1], True)
    qkv = PlaceSum(qkv_out, qkv_got, 0, z_send.at[2], z_recv.at[2])
    summed = QuadSum(term, total, got_c, stage, got_x, sum_send, sum_recv)

    for part in (out, fc):
        for k in range(4):
            part.put(k, lambda ref, k=k, part=part: store_same(part.out.at[k], ref, local_sems.at[0]))

    def mlp_grains(act_on, ref, base, turn, first_sem):
        r = range_of_spot(y, (z + 4 - turn) % 4)

        def one(slot, _):
            table = base + 4 * (r * sz.mlp + slot) + to.quarter
            act_on(ref(slot), g_mlp.at[table % sz.block], table, grain_sems.at[first_sem + slot], kind_sems.at[0])
            return 0

        lax.fori_loop(0, sz.mlp, one, 0)

    def grain_of(ref):
        return lambda slot: ref.at[pl.ds(pl.multiple_of(slot * GRAIN, GRAIN), GRAIN)]

    def out_grains(act_on, first_sem):
        count = out_share.shape[0] // GRAIN

        def one(slot, _):
            table = sz.out_start + slot_out(y, z) * count + slot
            dst = g_outs.at[to.quarter, table % sz.block]
            act_on(grain_of(out_share)(slot), dst, table, grain_sems.at[first_sem + slot], kind_sems.at[1])
            return 0

        lax.fori_loop(0, count, one, 0)

    def head_grains(act_on, first_sem):
        def one(slot, _):
            local = slot_qkv(y, z) * sz.qkv + slot
            inner = local % sz.part_grains
            index = inner // sz.head_grains
            head = 8 * (index // 2) + 2 * to.quarter + index % 2

            @pl.when(head < sz.heads)
            def _():
                table = (local // sz.part_grains) * sz.width_grains + head * sz.head_grains + inner % sz.head_grains
                act_on(
                    grain_of(qkv_share)(slot), g_qkv.at[table % sz.block], table,
                    grain_sems.at[first_sem + slot], kind_sems.at[2],
                )

            return 0

        lax.fori_loop(0, sz.qkv, one, 0)

    counts = (0, sz.mlp, 2 * sz.mlp, 3 * sz.mlp)
    mlp_grains(to.send, lambda slot: proj_share.at[slot], sz.proj_start, sz.proj_turn, counts[0])

    across = []
    for k in range(4):
        for s in (2 * k, 2 * k + 1):
            grads[s, :, :] = dot_tn(dqkv[:, s * rows : (s + 1) * rows], act[...]).astype(grads.dtype)
        copy = pltpu.make_async_remote_copy(
            src_ref=grads.at[2 * k + 1 - y],
            dst_ref=got_y.at[k],
            send_sem=y_send.at[k],
            recv_sem=y_recv.at[k],
            device_id=((dp + 2) % 4, cp),
            device_id_type=MESH,
        )
        copy.start()
        across.append(copy)

    def tokens_of(core):
        for side in range(2):
            here = pl.ds(pl.multiple_of((core * 2 + side) * block, block), block)
            term[core, side, :, :] = dot_nn(dqkv[here, :], w_qkv[...]).astype(term.dtype)

    tokens_of(1 - c)
    summed.start(greeting=False)
    tokens_of(c)
    summed.middle()

    def share_sum(k):
        def store(ref):
            for step in row_steps(rows):
                ref[step, :] = (
                    grads[2 * k + y, step, :].astype(jnp.float32) + got_y[k, step, :].astype(jnp.float32)
                ).astype(ref.dtype)

        return store

    def settle(part, value, share):
        part.total(value)
        copy = pltpu.make_async_copy(value, share, local_sems.at[1])
        copy.start()
        copy.wait()

    settle(out, out_v, out_share)
    out_grains(to.send, counts[2])
    for k in range(2):
        across[k].wait_recv()
        qkv.put(k, share_sum(k))
    settle(fc, share_v, fc_share)
    mlp_grains(to.send, grain_of(fc_share), sz.fc_start, sz.fc_turn, counts[1])
    for k in range(2, 4):
        across[k].wait_recv()
        qkv.put(k, share_sum(k))
    summed.finish()

    vec_v[...] = vec_in[...]
    vec_v[0:1, :] = jnp.sum(total[...] * normed[...], axis=0, keepdims=True)
    vec_v[1:2, :] = jnp.sum(total[...], axis=0, keepdims=True)
    last = sz.vec_start // sz.block
    vec_copy = pltpu.make_async_remote_copy(
        src_ref=vec_v,
        dst_ref=vecs.at[to.me],
        send_sem=vec_sems.at[0],
        recv_sem=vec_sems.at[1],
        device_id=(last // 8, last % 8),
        device_id_type=MESH,
    )

    @pl.when(to.me != last)
    def _():
        vec_copy.start()

    @pl.when(to.me == last)
    def _():
        pltpu.make_async_copy(vec_v, vecs.at[to.me], vec_sems.at[1]).start()

    settle(qkv, share_v.at[0:rows], qkv_share)
    head_grains(to.send, counts[3])

    for copy in across:
        copy.wait_send()
    for part in (out, fc, qkv):
        part.finish()
    mlp_grains(to.sent, lambda slot: proj_share.at[slot], sz.proj_start, sz.proj_turn, counts[0])
    mlp_grains(to.sent, grain_of(fc_share), sz.fc_start, sz.fc_turn, counts[1])
    out_grains(to.sent, counts[2])
    head_grains(to.sent, counts[3])

    @pl.when(to.me != last)
    def _():
        vec_copy.wait_send()

    @pl.when(to.me == last)
    def _():
        pltpu.make_async_copy(vecs, vecs, vec_sems.at[1]).wait()

    to.received(sz.fc_start, 64 * sz.mlp, lambda n: g_mlp.at[pl.ds(0, n)], kind_sems.at[0])
    to.received(sz.out_start, sz.width_grains, lambda n: g_outs.at[:, pl.ds(0, n)], kind_sems.at[1])
    to.received(0, 3 * sz.width_grains, lambda n: g_qkv.at[pl.ds(0, n)], kind_sems.at[2])


def store_same(src, ref, sem):
    copy = pltpu.make_async_copy(src, ref, sem)
    copy.start()
    copy.wait()


def close_call(sz, dqkv, act, w_qkv, normed, vectors, fc_sum, out_sum, proj_share):
    rows, width = normed.shape
    bf16, f32 = act.dtype, jnp.float32
    qkv_rows, out_rows, mlp_rows = sz.qkv * GRAIN, out_sum.shape[1], fc_sum.shape[1]

    def like(*shape, dtype=bf16):
        return jax.ShapeDtypeStruct(shape, dtype)

    def vmem(*shape):
        return pltpu.VMEM(shape, bf16)

    return pl.pallas_call(
        functools.partial(close_kernel, sz),
        out_shape=(
            like(rows, width, dtype=f32),
            like(sz.block, GRAIN, width),
            like(sz.block, GRAIN, width),
            like(4, sz.block, GRAIN, sz.part),
            like(32, *vectors.shape, dtype=f32),
            like(qkv_rows, width),
            like(mlp_rows, width),
            like(out_rows, sz.part),
        ),
        in_specs=[VMEM] * 7 + [HBM],
        out_specs=[VMEM] + [HBM] * 7,
        scratch_shapes=[
            vmem(8, qkv_rows, width),
            vmem(4, qkv_rows, width),
            vmem(4, qkv_rows, width),
            vmem(4, qkv_rows, width),
            vmem(4, mlp_rows, width),
            vmem(4, out_rows, sz.part),
            vmem(mlp_rows, width),
            vmem(out_rows, sz.part),
            pltpu.VMEM(vectors.shape, f32),
            vmem(2, 2, rows, width),
            vmem(2, rows, width),
            vmem(rows, width),
            vmem(rows, width),
            *wire_sems(4),
            pltpu.SemaphoreType.DMA((3, 4)),
            pltpu.SemaphoreType.DMA((3, 4)),
            *wire_sems(2),
            pltpu.SemaphoreType.DMA((3 * sz.mlp + sz.qkv,)),
            pltpu.SemaphoreType.DMA((3,)),
            pltpu.SemaphoreType.DMA((2,)),
            pltpu.SemaphoreType.DMA((2,)),
        ],
        cost_estimate=cost(120),
        compiler_params=remote_params(None, 62 << 20),
        name="close",
    )(dqkv, act, w_qkv, normed, vectors, fc_sum, out_sum, proj_share)


def attend_back_kernel(heads, size, own, *refs):
    if own:
        q_ref, kv_ref, do_ref, mix_ref, lse_ref, seed_ref, dq_ref, dkv_ref = refs
    else:
        q_ref, kv_ref, do_ref, mix_ref, lse_ref, term_ref, dq_ref, dkv_ref, sum_ref = refs[:9]
        quad = QuadSum(term_ref, sum_ref, *refs[-5:])
        quad.start()
    _, _, z, _ = my_place()
    part = heads * size
    rows = q_ref.shape[0] // 2
    blk = 256
    scale = size**-0.5

    def visit(here, start, seen, allowed):
        keys_at = pl.ds(start, seen)
        for h in range(heads):
            cols = slice(h * size, (h + 1) * size)
            vals = slice(part + h * size, part + (h + 1) * size)
            q = q_ref[here, cols]
            k = kv_ref[keys_at, cols]
            do = do_ref[here, cols]
            s = dot_nt(q, k) * scale
            p = jnp.exp(s - lse_ref[here, h : h + 1])
            if own:
                p = jnp.where(allowed, p, 0.0)
            dp = dot_nt(do, kv_ref[keys_at, vals])
            delta = jnp.sum(do.astype(jnp.float32) * mix_ref[here, cols], axis=-1, keepdims=True)
            ds = (p * (dp - delta)).astype(jnp.bfloat16)
            dq = dot_nn(ds, k) * scale
            if own:
                dq = dq + seed_ref[here, cols]
            dq_ref[here, cols] = dq.astype(dq_ref.dtype)
            dkv_ref[keys_at, cols] += dot_tn(ds, q) * scale
            dkv_ref[keys_at, vals] += dot_tn(p.astype(jnp.bfloat16), do)

    def group(index):
        start = pl.multiple_of(index * rows, rows)
        if not own:

            def block(i, _):
                visit(pl.ds(pl.multiple_of(start + i * blk, blk), blk), start, rows, None)
                return 0

            lax.fori_loop(0, rows // blk, block, 0)
            return
        for i in range(rows // blk):
            seen = (i + 1) * blk
            lane = lax.broadcasted_iota(jnp.int32, (blk, seen), 1)
            line = lax.broadcasted_iota(jnp.int32, (blk, seen), 0)
            visit(pl.ds(pl.multiple_of(start + i * blk, blk), blk), start, seen, lane <= line + i * blk)

    def clear(index, _):
        here = pl.ds(pl.multiple_of(index * blk, blk), blk)
        dkv_ref[here, :] = jnp.zeros((blk, dkv_ref.shape[1]), dkv_ref.dtype)
        if not own:
            dq_ref[here, :] = jnp.zeros((blk, dq_ref.shape[1]), dq_ref.dtype)
        return 0

    lax.fori_loop(0, 2 * rows // blk, clear, 0)

    def one(index, _):
        if own:
            group(index)
        else:

            @pl.when(z % 2 == 1)
            def _():
                group(index)

            @pl.when(index == 0)
            def _():
                quad.middle()

        return 0

    lax.fori_loop(0, 2, one, 0)
    if not own:
        quad.finish()


def attend_back(sz, q, kv, grad_mix, mix, lse, seed=None, term=None, ident=None):
    own = term is None
    operands = [q, kv, grad_mix, mix, lse, seed if own else term]
    out_shape = [
        jax.ShapeDtypeStruct(q.shape, jnp.bfloat16 if own else jnp.float32),
        jax.ShapeDtypeStruct(kv.shape, jnp.float32),
    ]
    if not own:
        out_shape.append(jax.ShapeDtypeStruct(term.shape[2:], jnp.float32))
    params = pltpu.CompilerParams(vmem_limit_bytes=56 << 20) if own else remote_params(ident, 56 << 20)
    return pl.pallas_call(
        functools.partial(attend_back_kernel, sz.quarter_heads, sz.head_size, own),
        out_shape=out_shape,
        in_specs=[VMEM] * len(operands),
        out_specs=[VMEM] * len(out_shape),
        scratch_shapes=[] if own else quad_scratch(term),
        cost_estimate=cost(35),
        compiler_params=params,
        name="attend_back_own" if own else "attend_back_before",
    )(*operands)


def rowwise(value):
    return with_layout_constraint(value, Layout(major_to_minor=(0, 1)))


def norm_parts(values):
    mean = jnp.mean(values, axis=-1, keepdims=True)
    centre = values - mean
    rs = lax.rsqrt(jnp.mean(centre * centre, axis=-1, keepdims=True) + EPSILON)
    return centre * rs, rs


def norm_back(normed, rs, grad, gain):
    e = grad * gain
    return rs * (
        e
        - jnp.mean(e, axis=-1, keepdims=True)
        - normed * jnp.mean(e * normed, axis=-1, keepdims=True)
    )


def per_device_quad(tokens, params, out_grad, lengths):
    rows, width = tokens.shape
    hidden = FF
    sz = Sizes(width, hidden, HEADS, HEAD_DIM, params.shape[0])
    y, c, z, x = my_place()
    quarter = c * 2 + x
    bf16, f32 = jnp.bfloat16, jnp.float32

    def pick(value, index):
        return lax.dynamic_index_in_dim(value, index, 0, keepdims=False)

    def to_other_y(sent):
        return over_y(sent.astype(bf16))

    def to_places(kept, got, turn=0):
        summed = kept.astype(f32) if got is None else kept.astype(f32) + got.astype(f32)
        summed = summed.reshape(4, summed.shape[0] // 4, -1)
        total = pick(summed, (z + 4 - turn) % 4)
        for d in (1, 2, 3):
            got = over_z(pick(summed, (z + d + 4 - turn) % 4).astype(bf16), d)
            total = total + got.astype(f32)
        return total

    w_qkv, w_out, w_fc, w_proj, vec, tok_all, cot_all = open_call(
        sz, params.reshape(sz.block, GRAIN, width), tokens, out_grad
    )
    flat = lambda value: value.reshape(-1, width)
    vectors = flat(vec).astype(f32)
    fc_bias = vectors[8 : 8 + hidden // width].reshape(hidden)
    w_qkv, cot_all = flat(w_qkv), flat(cot_all)
    normed_all, _ = norm_parts(flat(tok_all).astype(f32))
    act_one = (normed_all * vectors[0] + vectors[1]).astype(bf16)

    pair = 2 * sz.head_size
    turns = width // (4 * pair)
    rest = width - 4 * turns * pair

    def quarter_of(value):
        blocks = [lax.dynamic_slice_in_dim(value, (4 * j + quarter) * pair, pair, 1) for j in range(turns)]
        end = value[:, width - rest :]
        return jnp.concatenate(blocks + [jnp.where(quarter == 0, end, jnp.zeros_like(end))], axis=1)

    def by_head(quarters):
        blocks = [quarters[k][:, j * pair : (j + 1) * pair] for j in range(turns) for k in range(4)]
        return jnp.concatenate(blocks + [quarters[0][:, turns * pair : turns * pair + rest]], axis=1)

    biases = quarter_of(vectors[2:4])
    kv_bias = jnp.concatenate([jnp.zeros((sz.part,), f32), biases[1]])
    kv = (dot_nt(act_one, w_qkv[sz.part :]) + kv_bias).astype(bf16)
    q = (dot_nt(act_one, w_qkv[: sz.part]) + biases[0]).astype(bf16)
    mix, lse, before, mixed, _, w_fc, w_proj, w_out = forward_call(sz, q, kv, w_out, w_fc, w_proj)
    w_fc, w_out = flat(w_fc), flat(w_out)[:width]
    mixed = by_head(mixed)
    inputs = tokens.astype(f32)
    residual = inputs + (dot_nt(mixed, w_out) + vectors[4])
    normed_two, rs_two = norm_parts(residual)
    act_two = (normed_two * vectors[5] + vectors[6]).astype(bf16)
    bias = lax.dynamic_index_in_dim(fc_bias.reshape(-1, 4, GRAIN), quarter, 1, keepdims=False)
    bias = bias.reshape(8, hidden // 32)[jnp.array(RANGES)].reshape(hidden // 4, 1)
    grad_two, act_two, hid_t, proj_sum, fc_sent, fc_kept, bias_sum, w_proj = middle_call(
        sz, act_two, cot_all, w_fc, bias, flat(w_proj)
    )
    got_fc = to_other_y(fc_sent)

    cot = out_grad.astype(f32)
    grad_res = cot + norm_back(normed_two, rs_two, grad_two, vectors[5])
    grad_attn = grad_res.astype(bf16)
    attn_all, partial_out = grads_call(grad_attn, hid_t, w_proj, 3)
    attn_all = flat(attn_all)
    grad_mix = rowwise(dot_nn(attn_all, w_out).astype(bf16))
    grad_mix = rowwise(quarter_of(grad_mix))
    g_proj = to_places(proj_sum, None, sz.proj_turn)
    partial_out = partial_out.reshape(2, 2, rows, width)
    dq_before, dkv_before, out_sum = attend_back(
        sz, q, before, grad_mix, mix, lse, term=partial_out, ident=4
    )
    output = (residual + out_sum + vectors[7]).astype(bf16)
    returned = permute(
        dkv_before.astype(bf16), lambda py, pc, pz, px: (py, pc, pz - 1, px) if pz % 2 == 1 else None
    )
    g_out = rowwise(dot_tn(attn_all, mix.astype(bf16)).astype(bf16)).reshape(2, width // 2, sz.part)
    got_out = to_other_y(pick(g_out, 1 - y))
    fc_sum = (fc_kept.astype(f32) + got_fc.astype(f32)).astype(bf16).reshape(4, hidden // 32, width)
    out_sum = (pick(g_out, y).astype(f32) + got_out.astype(f32)).astype(bf16).reshape(4, width // 8, sz.part)
    dq, dkv = attend_back(sz, q, kv, grad_mix, mix, lse, seed=dq_before)
    grad_qkv = jnp.concatenate([dq, (dkv + returned.astype(f32)).astype(bf16)], axis=1)
    normed_one, rs_one = norm_parts(inputs)
    grains = lambda value: value.astype(bf16).reshape(-1, GRAIN, value.shape[-1])

    def placed(vector):
        spread = jnp.zeros((1, width), f32)
        for j in range(turns):
            block = vector[None, j * pair : (j + 1) * pair]
            spread = lax.dynamic_update_slice_in_dim(spread, block, (4 * j + quarter) * pair, 1)
        end = jnp.where(quarter == 0, vector[turns * pair : turns * pair + rest], 0.0)
        return jnp.concatenate([spread[0, : width - rest], end])

    sums = jnp.sum(grad_qkv.astype(f32), axis=0)
    bias_sum = bias_sum.reshape(8, hidden // 32)[jnp.array(SPOTS)]
    fc_rows = lax.dynamic_update_slice_in_dim(
        jnp.zeros((hidden // 4 // GRAIN, 4, GRAIN), f32), bias_sum.reshape(-1, 1, GRAIN), quarter, 1
    )
    grad_vectors = jnp.concatenate(
        [
            jnp.stack(
                [
                    jnp.zeros((width,), f32),
                    jnp.zeros((width,), f32),
                    placed(sums[: sz.part]),
                    placed(sums[2 * sz.part :]),
                    jnp.sum(grad_attn.astype(f32), axis=0),
                    jnp.sum(grad_two * normed_two, axis=0),
                    jnp.sum(grad_two, axis=0),
                    jnp.sum(cot, axis=0),
                ]
            ),
            fc_rows.reshape(hidden // width, width),
        ]
    )
    count = grad_vectors.shape[0]
    grad_vectors = jnp.pad(grad_vectors, ((0, sz.vec * GRAIN - count), (0, 0)))
    grad_one, table_qkv, table_mlp, table_out, all_vectors = close_call(
        sz, grad_qkv, act_one, w_qkv, normed_one, grad_vectors, fc_sum, out_sum, grains(g_proj)
    )[:5]
    input_grad = (grad_res + norm_back(normed_one, rs_one, grad_one, vectors[0])).astype(bf16)
    grad_vectors = jnp.sum(all_vectors, axis=0)[:count]
    table_out = by_head(table_out.reshape(4, -1, sz.part))
    me = flat_id(y, c, z, x)
    row = me * (sz.block * GRAIN) + lax.broadcasted_iota(jnp.int32, (sz.block * GRAIN, 1), 0)
    used = (sz.vec_start % sz.block) * GRAIN
    tail = jnp.pad(grad_vectors, ((used, sz.block * GRAIN - used - count), (0, 0)))
    param_grad = jnp.where(
        row < sz.out_start * GRAIN,
        flat(table_qkv).astype(f32),
        jnp.where(
            row < sz.fc_start * GRAIN,
            table_out.astype(f32),
            jnp.where(row < sz.vec_start * GRAIN, flat(table_mlp).astype(f32), tail),
        ),
    )
    return (output, input_grad, param_grad)


def fits_quad(mesh, tokens, params, lengths):
    dp, cp = mesh.shape["dp"], mesh.shape["cp"]
    rows = tokens.shape[0] // (dp * cp)
    width = tokens.shape[1]
    blocks = params.shape[0] // (dp * cp)
    return (
        (dp, cp) == (4, 8)
        and lengths.shape[1] == 2
        and rows * cp == lengths.shape[1] * MIN_LEN
        and rows % 128 == 0
        and blocks % GRAIN == 0
        and (HEADS, HEAD_DIM, FF, width) == (25, 64, 6400, 1600)
    )


def solution(mesh):
    in_specs = (P(("dp", "cp"), None), P(("dp", "cp"), None), P(("dp", "cp"), None), P("dp", None))
    out_specs = (P(("dp", "cp"), None), P(("dp", "cp"), None), P(("dp", "cp"), None))

    def step(tokens, params, out_grad, lengths):
        body = per_device_quad if fits_quad(mesh, tokens, params, lengths) else per_device_general

        return jax.shard_map(
            body, mesh=mesh, in_specs=in_specs, out_specs=out_specs, check_vma=False
        )(tokens, params, out_grad, lengths)

    return step
```

```python
import functools

import jax
import jax.numpy as jnp
from jax import lax
from jax.experimental import pallas as pl
from jax.experimental.layout import Layout, with_layout_constraint
from jax.experimental.pallas import tpu as pltpu
from jax.sharding import PartitionSpec as P


HEADS = 25
FF = 6400
HEAD_DIM = 64
TILE = 128
MIN_LEN = 1024
MAX_LEN = 4096


EPSILON = 1e-05
MASKED = -1e30
GELU_SCALE = 0.7978845608028654


def from_behind(value, axis, by):
    length = lax.axis_size(axis)
    pairs = [(i, i + by) for i in range(length) if 0 <= i + by < length]
    return lax.ppermute(value, axis, pairs)


def layer_norm(values, gain_row, bias_row):
    centre = values - jnp.mean(values, axis=-1, keepdims=True)
    spread = jnp.mean(centre * centre, axis=-1, keepdims=True)
    return centre * lax.rsqrt(spread + EPSILON) * gain_row + bias_row


def gelu_tanh(values):
    return (
        0.5 * values * (1.0 + jnp.tanh(GELU_SCALE * (values + 0.044715 * values * values * values)))
    )


def segment_of(position, seq_ends):
    return jnp.sum((position[:, None] >= seq_ends[None, :]).astype(jnp.int32), axis=1)


def unpack(gathered, model_width, hidden):
    out_end = 4 * model_width
    fc_end = out_end + hidden
    proj_end = fc_end + hidden
    vec_end = proj_end + 8
    return (
        gathered[0 : 3 * model_width],
        gathered[3 * model_width : out_end],
        gathered[out_end:fc_end],
        gathered[fc_end:proj_end],
        gathered[proj_end:vec_end].astype(jnp.float32),
        gathered[vec_end : vec_end + hidden // model_width].astype(jnp.float32).reshape(hidden),
    )


def matmul_nt(left_mat, right_mat):
    return lax.dot_general(
        left_mat, right_mat, (((1,), (1,)), ((), ())), preferred_element_type=jnp.float32
    )


def matmul_tn(left_mat, right_mat):
    return lax.dot_general(
        left_mat, right_mat, (((0,), (0,)), ((), ())), preferred_element_type=jnp.float32
    )


def matmul_nn(left_mat, right_mat):
    return jnp.dot(left_mat, right_mat, preferred_element_type=jnp.float32)


def per_device_general(tokens, params, out_grad, lengths):
    tok_rows, model_width = tokens.shape
    hidden = FF
    head_count = HEADS
    head_size = HEAD_DIM
    cp_count = lax.axis_size("cp")
    group_rows = tok_rows * cp_count
    seq_count = lengths.shape[1]
    longest = min(MAX_LEN, group_rows - (seq_count - 1) * MIN_LEN)
    reach_back = min(cp_count - 1, (longest + tok_rows - TILE - 1) // tok_rows)
    pair_count = (reach_back + 2) // 2
    score_scale = head_size ** (-0.5)
    gathered = lax.all_gather(params, ("dp", "cp"), axis=0, tiled=True)
    w_attn, w_out, w_fc, w_proj, vectors, fc_bias = unpack(gathered, model_width, hidden)
    inputs = tokens.astype(jnp.float32)
    act_one = layer_norm(inputs, vectors[0], vectors[1]).astype(jnp.bfloat16)
    qkv_bias = jnp.concatenate([vectors[2], jnp.zeros_like(vectors[2]), vectors[3]])
    qkv = (matmul_nt(act_one, w_attn) + qkv_bias).astype(jnp.bfloat16)
    queries = qkv[:, :model_width].reshape(tok_rows, head_count, head_size)
    key_value = qkv[:, model_width:]
    device = lax.axis_index("cp")
    seq_ends = jnp.cumsum(lengths[0])
    query_pos = device * tok_rows + jnp.arange(tok_rows, dtype=jnp.int32)
    query_seg = segment_of(query_pos, seq_ends)
    store = jnp.zeros((2 * pair_count, tok_rows, 2 * model_width), jnp.bfloat16)
    store = store.at[0].set(key_value)

    def fetch(step_index, state_pair):
        moving, held_rows = state_pair
        moving = from_behind(moving, "cp", 1)
        return (moving, lax.dynamic_update_index_in_dim(held_rows, moving, step_index, 0))

    _, store = lax.fori_loop(1, reach_back + 1, fetch, (key_value, store))

    def pair_mask(pair_index):
        owners = 2 * pair_index + jnp.arange(2, dtype=jnp.int32)
        key_pos = (
            (device - owners)[:, None] * tok_rows + jnp.arange(tok_rows, dtype=jnp.int32)[None, :]
        ).reshape(2 * tok_rows)
        usable = jnp.broadcast_to((owners <= reach_back)[:, None], (2, tok_rows)).reshape(
            2 * tok_rows
        ) & (key_pos >= 0)
        key_seg = segment_of(key_pos, seq_ends)
        return (
            (key_seg[None, :] == query_seg[:, None])
            & (key_pos[None, :] <= query_pos[:, None])
            & usable[None, :]
        )

    def pair_rows(pair_index):
        block_rows = lax.dynamic_slice_in_dim(store, 2 * pair_index, 2, 0).reshape(
            2 * tok_rows, 2 * model_width
        )
        return (
            block_rows[:, :model_width].reshape(2 * tok_rows, head_count, head_size),
            block_rows[:, model_width:].reshape(2 * tok_rows, head_count, head_size),
        )

    def pair_scores(key_rows, allowed):
        raw_scores = (
            jnp.einsum("qhd,khd->hqk", queries, key_rows, preferred_element_type=jnp.float32)
            * score_scale
        )
        return jnp.where(allowed[None], raw_scores, MASKED)

    def visit(work):

        def step_pair(pair_index, running):
            allowed = pair_mask(pair_index)
            result = work(pair_index, allowed, running)
            return result

        return step_pair

    def add_total(pair_index, allowed, running):
        row_top, summed = running
        key_rows, _ = pair_rows(pair_index)
        scores = pair_scores(key_rows, allowed)
        new_top = jnp.maximum(row_top, jnp.max(scores, axis=-1, keepdims=True))
        summed = summed * jnp.exp(row_top - new_top) + jnp.sum(
            jnp.exp(scores - new_top), axis=-1, keepdims=True
        )
        return (new_top, summed)

    start_top = jnp.full((head_count, tok_rows, 1), MASKED, jnp.float32)
    start_sum = jnp.zeros((head_count, tok_rows, 1), jnp.float32)
    row_top, summed = lax.fori_loop(0, pair_count, visit(add_total), (start_top, start_sum))
    log_total = row_top + jnp.log(summed)

    def add_mix(pair_index, allowed, running):
        key_rows, value_rows = pair_rows(pair_index)
        prob_rows = jnp.exp(pair_scores(key_rows, allowed) - log_total).astype(jnp.bfloat16)
        return running + jnp.einsum(
            "hqk,khd->qhd", prob_rows, value_rows, preferred_element_type=jnp.float32
        )

    mixed_full = lax.fori_loop(
        0, pair_count, visit(add_mix), jnp.zeros((tok_rows, head_count, head_size), jnp.float32)
    )
    mixed = mixed_full.reshape(tok_rows, model_width).astype(jnp.bfloat16)
    attn_out = matmul_nt(mixed, w_out) + vectors[4]
    residual = inputs + attn_out
    act_two = layer_norm(residual, vectors[5], vectors[6]).astype(jnp.bfloat16)
    pre_act = matmul_nt(act_two, w_fc) + fc_bias
    act_hidden = gelu_tanh(pre_act).astype(jnp.bfloat16)
    output = (residual + matmul_nn(act_hidden, w_proj) + vectors[7]).astype(jnp.bfloat16)
    gathered = lax.all_gather(params, ("dp", "cp"), axis=0, tiled=True)
    w_attn, w_out, w_fc, w_proj, vectors, fc_bias = unpack(gathered, model_width, hidden)
    grad_out_f = out_grad.astype(jnp.float32)
    grad_hidden = matmul_nt(out_grad, w_proj)
    _, pull_gelu = jax.vjp(gelu_tanh, pre_act)
    grad_fc = pull_gelu(grad_hidden)[0].astype(jnp.bfloat16)
    grad_act_two = matmul_nn(grad_fc, w_fc)
    _, pull_two = jax.vjp(layer_norm, residual, vectors[5], vectors[6])
    grad_res_norm, grad_gain_two, grad_bias_two = pull_two(grad_act_two)
    grad_res = grad_out_f + grad_res_norm
    grad_attn = grad_res.astype(jnp.bfloat16)
    grad_mix = (
        matmul_nn(grad_attn, w_out).astype(jnp.bfloat16).reshape(tok_rows, head_count, head_size)
    )
    grad_dot = jnp.transpose(jnp.sum(grad_mix.astype(jnp.float32) * mixed_full, axis=-1), (1, 0))[
        :, :, None
    ]

    def add_grads(pair_index, allowed, running):
        grad_query, grad_store = running
        key_rows, value_rows = pair_rows(pair_index)
        prob_rows = jnp.exp(pair_scores(key_rows, allowed) - log_total)
        grad_probs = jnp.einsum(
            "qhd,khd->hqk", grad_mix, value_rows, preferred_element_type=jnp.float32
        )
        grad_scores = (prob_rows * (grad_probs - grad_dot)).astype(jnp.bfloat16)
        grad_query = (
            grad_query
            + jnp.einsum("hqk,khd->qhd", grad_scores, key_rows, preferred_element_type=jnp.float32)
            * score_scale
        )
        grad_keys = (
            jnp.einsum("hqk,qhd->khd", grad_scores, queries, preferred_element_type=jnp.float32)
            * score_scale
        )
        grad_values = jnp.einsum(
            "hqk,qhd->khd",
            prob_rows.astype(jnp.bfloat16),
            grad_mix,
            preferred_element_type=jnp.float32,
        )
        pair_grad = jnp.concatenate(
            [
                grad_keys.reshape(2 * tok_rows, model_width),
                grad_values.reshape(2 * tok_rows, model_width),
            ],
            axis=1,
        )
        pair_grad = pair_grad.reshape(2, tok_rows, 2 * model_width)
        grad_store = lax.dynamic_update_slice_in_dim(grad_store, pair_grad, 2 * pair_index, 0)
        return (grad_query, grad_store)

    start_query = jnp.zeros((tok_rows, head_count, head_size), jnp.float32)
    start_store = jnp.zeros((2 * pair_count, tok_rows, 2 * model_width), jnp.float32)
    grad_query, grad_store = lax.fori_loop(
        0, pair_count, visit(add_grads), (start_query, start_store)
    )

    def send_back(step_index, moving):
        moving = moving + lax.dynamic_index_in_dim(
            grad_store, reach_back - step_index, 0, keepdims=False
        )
        return from_behind(moving.astype(jnp.bfloat16), "cp", -1).astype(moving.dtype)

    returned = lax.fori_loop(
        0, reach_back, send_back, jnp.zeros((tok_rows, 2 * model_width), jnp.float32)
    )
    grad_kv = returned + grad_store[0]
    grad_qkv = jnp.concatenate([grad_query.reshape(tok_rows, model_width), grad_kv], axis=1).astype(
        jnp.bfloat16
    )
    grad_qkv_f = grad_qkv.astype(jnp.float32)
    grad_act_one = matmul_nn(grad_qkv, w_attn)
    _, pull_one = jax.vjp(layer_norm, inputs, vectors[0], vectors[1])
    grad_in_norm, grad_gain_one, grad_bias_one = pull_one(grad_act_one)
    input_grad = (grad_res + grad_in_norm).astype(jnp.bfloat16)
    grad_vectors = jnp.stack(
        [
            grad_gain_one,
            grad_bias_one,
            jnp.sum(grad_qkv_f[:, :model_width], axis=0),
            jnp.sum(grad_qkv_f[:, 2 * model_width :], axis=0),
            jnp.sum(grad_attn.astype(jnp.float32), axis=0),
            grad_gain_two,
            grad_bias_two,
            jnp.sum(grad_out_f, axis=0),
        ]
    )
    grad_fc_bias = jnp.sum(grad_fc.astype(jnp.float32), axis=0).reshape(
        hidden // model_width, model_width
    )
    used_rows = 4 * model_width + 2 * hidden + 8 + hidden // model_width
    total_rows = gathered.shape[0]
    local_grad = jnp.concatenate(
        [
            matmul_tn(grad_qkv, act_one),
            matmul_tn(grad_attn, mixed),
            matmul_tn(grad_fc, act_two),
            matmul_tn(act_hidden, out_grad),
            grad_vectors,
            grad_fc_bias,
            jnp.zeros((total_rows - used_rows, model_width), jnp.float32),
        ],
        axis=0,
    )
    dp_count = lax.axis_size("dp")
    device_count = dp_count * cp_count
    share_rows = total_rows // device_count
    spread_rows = local_grad.reshape(device_count, 1, share_rows, model_width)
    received = lax.all_to_all(
        spread_rows.astype(jnp.bfloat16), ("dp", "cp"), split_axis=0, concat_axis=1, tiled=True
    ).astype(spread_rows.dtype)
    param_grad = jnp.sum(received, axis=1).reshape(share_rows, model_width)
    return (output, input_grad, param_grad)


MESH = pl.DeviceIdType.MESH
GRAIN = 8
NT = (((1,), (1,)), ((), ()))
TN = (((0,), (0,)), ((), ()))


def dot_nt(a, b):
    return lax.dot_general(a, b, NT, preferred_element_type=jnp.float32)


def dot_tn(a, b):
    return lax.dot_general(a, b, TN, preferred_element_type=jnp.float32)


def dot_nn(a, b):
    return jnp.dot(a, b, preferred_element_type=jnp.float32)


def flat_id(y, c, z, x):
    return ((y * 2 + c) * 4 + z) * 2 + x


def permute(value, move):
    pairs = []
    for y in range(2):
        for c in range(2):
            for z in range(4):
                for x in range(2):
                    to = move(y, c, z, x)
                    if to is not None:
                        pairs.append((flat_id(y, c, z, x), flat_id(*to)))
    return lax.ppermute(value, ("dp", "cp"), pairs)


def over_y(value):
    return permute(value, lambda y, c, z, x: (1 - y, c, z, x))


class Sizes:
    def __init__(self, width, hidden, heads, head_size, rows):
        self.heads = heads
        self.head_size = head_size
        self.quarter_heads = -(-heads // 4)
        self.part = self.quarter_heads * head_size
        self.part_grains = self.part // GRAIN
        self.width_grains = width // GRAIN
        self.spill = 4 * self.part_grains - self.width_grains
        self.qkv = 3 * self.part_grains // 8
        self.out = self.part_grains // 8
        self.mlp = hidden // 4 // 8 // GRAIN
        self.block = rows // GRAIN
        self.out_start = 3 * self.width_grains
        self.fc_start = 4 * self.width_grains
        self.proj_start = self.fc_start + hidden // GRAIN
        self.vec_start = self.proj_start + hidden // GRAIN
        self.vec = 2
        self.head_grains = head_size // GRAIN
        self.fc_turn = self.turn(self.fc_start)
        self.proj_turn = self.turn(self.proj_start)

    def turn(self, start):
        return start // (2 * self.block) % 4


def spot_of_range(r):
    y = r // 6 + (r % 2) * ((r // 3) % 2)
    u = (r - (r + 5) // 8 - (r + 3) // 8) % 4
    return y, u


def range_of_spot(y, u):
    first = u + u // 3
    second = (1 - u // 2) * (u + 6) + (u // 2) * (2 * u - 1)
    return (1 - y) * first + y * second


RANGES = (0, 1, 2, 4, 6, 7, 3, 5)
SPOTS = (0, 1, 2, 6, 3, 7, 4, 5)


def slot_qkv(y, z):
    return 2 * z + y


def slot_out(y, z):
    return 4 * y + z


def slot_turned(turn):
    return lambda y, z: 4 * y + (z + 4 - turn) % 4


def my_place():
    dp = lax.axis_index("dp")
    cp = lax.axis_index("cp")
    return dp // 2, dp % 2, cp // 2, cp % 2


def device_of(quarter, y, z):
    return y * 2 + quarter // 2, z * 2 + quarter % 2


class Wires:
    def __init__(self, send_sems, recv_sems):
        self.send_sems = send_sems
        self.recv_sems = recv_sems
        self.count = 0

    def to(self, src, dst, dp, cp):
        index = self.count
        self.count += 1
        return pltpu.make_async_remote_copy(
            src_ref=src,
            dst_ref=dst,
            send_sem=self.send_sems.at[index],
            recv_sem=self.recv_sems.at[index],
            device_id=(dp, cp),
            device_id_type=MESH,
        )


class PlaceGather:
    def __init__(self, wires, full, slot, steps=(1, 2, 3), over=(0, 1, 2, 3)):
        self.full = full
        self.dp, self.cp = lax.axis_index("dp"), lax.axis_index("cp")
        self.y, self.z, self.x = self.dp // 2, self.cp // 2, self.cp % 2
        self.above = (self.dp, ((self.z + 1) % 4) * 2 + self.x)
        self.below = (self.dp, ((self.z + 3) % 4) * 2 + self.x)
        self.across = ((self.dp + 2) % 4, self.cp)

        def share(by, to):
            spot = slot(self.y, (self.z + 4 + by) % 4)
            view = full.at[spot]
            return wires.to(view, view, *to)

        self.steps = steps
        self.up = {k: share(1 - k, self.above) for k in steps}
        self.down = {k: share(k - 1, self.below) for k in steps}
        self.over = {d: share(d, self.across) for d in over}

    def partners(self):
        return [self.above, self.below, self.across]

    def start(self):
        if 1 in self.steps:

            @pl.when(self.z < 3)
            def _():
                self.up[1].start()

            @pl.when(self.z > 0)
            def _():
                self.down[1].start()

        if 0 in self.over:
            self.over[0].start()

    def forward(self, steps=(1, 2, 3)):
        for k in steps:

            @pl.when(self.z >= k)
            def _():
                if k in self.steps:
                    self.up[k].wait_recv()
                if k + 1 in self.steps:

                    @pl.when(self.z < 3)
                    def _():
                        self.up[k + 1].start()

                if 4 - k in self.over:
                    self.over[4 - k].start()

            @pl.when(self.z <= 3 - k)
            def _():
                if k in self.steps:
                    self.down[k].wait_recv()
                if k + 1 in self.steps:

                    @pl.when(self.z > 0)
                    def _():
                        self.down[k + 1].start()

                if k in self.over:
                    self.over[k].start()

    def finish(self):
        for copy in self.over.values():
            copy.wait_recv()
        for copy in self.over.values():
            copy.wait_send()
        for k in self.steps:

            @pl.when(jnp.logical_and(self.z >= k - 1, self.z < 3))
            def _():
                self.up[k].wait_send()

            @pl.when(jnp.logical_and(self.z <= 4 - k, self.z > 0))
            def _():
                self.down[k].wait_send()


class QuadGather:
    def __init__(self, wires, block, full, local_sem):
        self.wires = wires
        self.block = block
        self.full = full
        self.dp, self.cp = lax.axis_index("dp"), lax.axis_index("cp")
        self.c, self.x = self.dp % 2, self.cp % 2
        self.over_x = (self.dp, self.cp + 1 - 2 * self.x)
        self.over_c = (self.dp + 1 - 2 * self.c, self.cp)
        self.local_sem = local_sem

    def spot(self, c, x):
        if len(self.full.shape) > len(self.block.shape):
            return self.full.at[c, x]
        rows = self.block.shape[0]
        return self.full.at[pl.ds(pl.multiple_of((c * 2 + x) * rows, rows), rows)]

    def start(self):
        spot = self.spot(self.c, self.x)
        self.by_x = self.wires.to(self.block, spot, *self.over_x)
        self.by_c = self.wires.to(self.block, spot, *self.over_c)
        self.by_x.start()
        self.by_c.start()
        self.local = pltpu.make_async_copy(self.block, spot, self.local_sem)
        self.local.start()

    def forward(self):
        self.by_x.wait_recv()
        spot = self.spot(self.c, 1 - self.x)
        self.pass_on = self.wires.to(spot, spot, *self.over_c)
        self.pass_on.start()

    def finish(self):
        self.by_c.wait_recv()
        self.pass_on.wait_recv()
        self.by_x.wait_send()
        self.by_c.wait_send()
        self.pass_on.wait_send()
        self.local.wait()


def open_kernel(
    sz, p_ref, tok_ref, cot_ref, qkv_ref, out_ref, fc_ref, proj_ref, vec_ref, tok_all, cot_all,
    spread_sems, kind_sems, send_sems, recv_sems, local_sems,
):
    y, c, z, x = my_place()
    me = flat_id(y, c, z, x)
    wires = Wires(send_sems, recv_sems)
    tok = QuadGather(wires, tok_ref, tok_all, local_sems.at[0])
    cot = QuadGather(wires, cot_ref, cot_all, local_sems.at[1])

    def send(grain, ref, spot, slot, quarter, py, pz, sem, recv):
        dp, cp = device_of(quarter, py, pz)
        mine = dp * 8 + cp == me

        @pl.when(mine)
        def _():
            pltpu.make_async_copy(p_ref.at[grain], ref.at[spot, slot], recv).start()

        @pl.when(jnp.logical_not(mine))
        def _():
            pltpu.make_async_remote_copy(
                src_ref=p_ref.at[grain],
                dst_ref=ref.at[spot, slot],
                send_sem=sem,
                recv_sem=recv,
                device_id=(dp, cp),
                device_id_type=MESH,
            ).start()

    def sent(grain, ref, spot, slot, quarter, py, pz, sem, recv):
        dp, cp = device_of(quarter, py, pz)

        @pl.when(dp * 8 + cp != me)
        def _():
            pltpu.make_async_copy(p_ref.at[grain], p_ref.at[grain], sem).wait()

    def headed(act, grain):
        table = me * sz.block + grain
        part = table // sz.width_grains
        inner = table % sz.width_grains
        head = inner // sz.head_grains
        rest = inner % sz.head_grains

        def one(quarter, sem):
            local = part * sz.part_grains + (2 * (head // 8) + head % 2) * sz.head_grains + rest
            spot = local // sz.qkv
            act(grain, qkv_ref, spot, local % sz.qkv, quarter, spot % 2, spot // 2, sem, kind_sems.at[0])

        @pl.when(table < sz.out_start)
        def _():
            one((head // 2) % 4, spread_sems.at[grain])

            @pl.when(head == sz.heads - 1)
            def _():
                for quarter in range(1, 4):
                    one(quarter, spread_sems.at[sz.block + (quarter - 1) * sz.head_grains + rest])

    def outward(act, grain):
        local = me * sz.block + grain - sz.out_start

        def one(quarter, inner, sem):
            spot = inner // sz.out
            act(grain, out_ref, spot, inner % sz.out, quarter, spot // 4, spot % 4, sem, kind_sems.at[1])

        @pl.when(jnp.logical_and(local >= 0, local < sz.width_grains))
        def _():
            one(local // sz.part_grains, local % sz.part_grains, spread_sems.at[grain])

            @pl.when(local < sz.spill)
            def _():
                one(3, sz.part_grains - sz.spill + local, spread_sems.at[sz.block + 3 * sz.head_grains + local])

    def plain(act, grain, base, turn, ref, recv):
        offset = me * sz.block + grain - base

        @pl.when(jnp.logical_and(offset >= 0, offset < 32 * sz.mlp))
        def _():
            local = offset // 4
            py, u = spot_of_range(local // sz.mlp)
            act(
                grain, ref, py * 4 + u, local % sz.mlp, offset % 4, py, (u + turn) % 4,
                spread_sems.at[grain], recv,
            )

    def heads(act):
        def one(grain, _):
            headed(act, grain)
            return 0

        lax.fori_loop(0, sz.block, one, 0)

    def others(act):
        def one(grain, _):
            outward(act, grain)
            plain(act, grain, sz.fc_start, sz.fc_turn, fc_ref, kind_sems.at[2])
            plain(act, grain, sz.proj_start, sz.proj_turn, proj_ref, kind_sems.at[3])
            return 0

        lax.fori_loop(0, sz.block, one, 0)

    owner = sz.vec_start // sz.block
    spot = sz.vec_start % sz.block

    def vector_sends(act):
        @pl.when(me == owner)
        def _():
            def to(device, _):
                @pl.when(device != me)
                def _():
                    act(
                        pltpu.make_async_remote_copy(
                            src_ref=p_ref.at[pl.ds(spot, sz.vec)],
                            dst_ref=vec_ref,
                            send_sem=spread_sems.at[sz.block + 3 * sz.head_grains + sz.spill + device],
                            recv_sem=kind_sems.at[4],
                            device_id=(device // 8, device % 8),
                            device_id_type=MESH,
                        )
                    )

                return 0

            lax.fori_loop(0, 32, to, 0)

    heads(send)
    tok.start()
    mine = slot_qkv(y, z)
    pltpu.make_async_copy(qkv_ref.at[mine], qkv_ref.at[mine], kind_sems.at[0]).wait()
    weights = PlaceGather(wires, qkv_ref, slot_qkv)
    weights.start()
    vector_sends(lambda copy: copy.start())

    @pl.when(me == owner)
    def _():
        pltpu.make_async_copy(p_ref.at[pl.ds(spot, sz.vec)], vec_ref, kind_sems.at[4]).start()

    others(send)
    cot.start()
    tok.forward()
    weights.forward()
    early = []
    for index, (ref, slot) in enumerate(((out_ref, slot_out), (fc_ref, slot_turned(sz.fc_turn)))):
        view = ref.at[slot(y, z)]
        pltpu.make_async_copy(view, view, kind_sems.at[index + 1]).wait()
        early.append(PlaceGather(wires, ref, slot, steps=(1,), over=(0,)))
        early[-1].start()
    cot.forward()
    heads(sent)
    others(sent)
    vector_sends(lambda copy: copy.wait_send())
    view = proj_ref.at[slot_turned(sz.proj_turn)(y, z)]
    pltpu.make_async_copy(view, view, kind_sems.at[3]).wait()
    pltpu.make_async_copy(vec_ref, vec_ref, kind_sems.at[4]).wait()
    tok.finish()
    cot.finish()
    weights.finish()
    for first in early:
        first.forward((1,))
        first.finish()


HBM = pl.BlockSpec(memory_space=pl.ANY)
VMEM = pl.BlockSpec(memory_space=pltpu.VMEM)
REMOTE = pltpu.CompilerParams(has_side_effects=True)


def remote_params(ident=None, vmem=None):
    return pltpu.CompilerParams(has_side_effects=True, collective_id=ident, vmem_limit_bytes=vmem)


def greet(partners):
    barrier = pltpu.get_barrier_semaphore()
    for dp, cp in partners:
        pl.semaphore_signal(barrier, inc=1, device_id=(dp, cp), device_id_type=MESH)
    pl.semaphore_wait(barrier, len(partners))


def cost(us):
    return pl.CostEstimate(flops=0, bytes_accessed=int(us * 3.0e6), transcendentals=0)


def wire_sems(count):
    return [pltpu.SemaphoreType.DMA((count,)), pltpu.SemaphoreType.DMA((count,))]


def open_call(sz, table, tokens, cotangent):
    rows, width = tokens.shape

    def like(*shape):
        return jax.ShapeDtypeStruct(shape + (width,), table.dtype)

    return pl.pallas_call(
        functools.partial(open_kernel, sz),
        out_shape=(
            like(8, sz.qkv, GRAIN),
            like(8, sz.out, GRAIN),
            like(8, sz.mlp, GRAIN),
            like(8, sz.mlp, GRAIN),
            like(sz.vec, GRAIN),
            like(2, 2, rows),
            like(2, 2, rows),
        ),
        in_specs=[HBM, VMEM, VMEM],
        out_specs=[HBM] * 7,
        scratch_shapes=[
            pltpu.SemaphoreType.DMA((sz.block + 3 * sz.head_grains + sz.spill + 32,)),
            pltpu.SemaphoreType.DMA((5,)),
            *wire_sems(22),
            pltpu.SemaphoreType.DMA((2,)),
        ],
        compiler_params=REMOTE,
        name="open",
    )(table, tokens, cotangent)


def forward_kernel(
    heads, size, fc_turn, proj_turn, q_ref, kv_ref, out_in, fc_in, proj_in,
    mix_ref, lse_ref, before_ref, mixed_ref, out_ref, fc_ref, proj_ref, out_all,
    stage, send_sems, recv_sems, local_sems,
):
    y, c, z, x = my_place()
    dp, cp = lax.axis_index("dp"), lax.axis_index("cp")
    wires = Wires(send_sems, recv_sems)
    part = heads * size
    rows = q_ref.shape[0] // 2
    blk = 256
    scale = size**-0.5
    odd = z % 2 == 1
    w_out = PlaceGather(wires, out_ref, slot_out, steps=(2, 3), over=(1, 2, 3))
    w_fc = PlaceGather(wires, fc_ref, slot_turned(fc_turn), steps=(2, 3), over=(1, 2, 3))
    w_proj = PlaceGather(wires, proj_ref, slot_turned(proj_turn), steps=(1,), over=(0,))
    others = [(c, 1 - x), (1 - c, x), (1 - c, 1 - x)]
    quad = [(y * 2 + tc, z * 2 + tx) for tc, tx in others]
    greet(w_out.partners() + quad)
    keys = wires.to(kv_ref, before_ref, dp, (cp + 2) % 8)

    w_out.forward()

    @pl.when(jnp.logical_not(odd))
    def _():
        keys.start()

    w_fc.forward((1,))

    def own(group, _):
        start = group * rows
        for i in range(rows // blk):
            here = pl.ds(pl.multiple_of(start + i * blk, blk), blk)
            seen = (i + 1) * blk
            keys_at = pl.ds(pl.multiple_of(start, rows), seen)
            lane = lax.broadcasted_iota(jnp.int32, (blk, seen), 1)
            line = lax.broadcasted_iota(jnp.int32, (blk, seen), 0)
            allowed = lane <= line + i * blk
            for h in range(heads):
                cols = slice(h * size, (h + 1) * size)
                vals = slice(part + h * size, part + (h + 1) * size)
                s = dot_nt(q_ref[here, cols], kv_ref[keys_at, cols]) * scale
                s = jnp.where(allowed, s, MASKED)
                top = jnp.max(s, axis=-1, keepdims=True)
                p = jnp.exp(s - top)
                total = jnp.sum(p, axis=-1, keepdims=True)
                mix_ref[here, cols] = dot_nn(p.astype(jnp.bfloat16), kv_ref[keys_at, vals]) / total
                lse_ref[here, h : h + 1] = top + jnp.log(total)
        return 0

    lax.fori_loop(0, 2, own, 0)

    def add_before(index, _):
        here = pl.ds(pl.multiple_of(index * blk, blk), blk)
        keys_at = pl.ds(pl.multiple_of((index * blk) // rows * rows, rows), rows)
        for h in range(heads):
            cols = slice(h * size, (h + 1) * size)
            vals = slice(part + h * size, part + (h + 1) * size)
            s = dot_nt(q_ref[here, cols], before_ref[keys_at, cols]) * scale
            lse = lse_ref[here, h : h + 1]
            top = jnp.maximum(lse, jnp.max(s, axis=-1, keepdims=True))
            p = jnp.exp(s - top)
            kept = jnp.exp(lse - top)
            total = kept + jnp.sum(p, axis=-1, keepdims=True)
            mix = mix_ref[here, cols] * kept + dot_nn(p.astype(jnp.bfloat16), before_ref[keys_at, vals])
            mix_ref[here, cols] = mix / total
            lse_ref[here, h : h + 1] = top + jnp.log(total)
        return 0

    w_out.finish()
    whole = QuadGather(wires, out_ref, out_all, local_sems.at[0])
    whole.start()

    @pl.when(z < 3)
    def _():
        w_fc.forward((2,))

    @pl.when(odd)
    def _():
        keys.wait_recv()
        lax.fori_loop(0, 2 * rows // blk, add_before, 0)

    def round_off(index, _):
        here = pl.ds(pl.multiple_of(index * blk, blk), blk)
        stage[here, :] = mix_ref[here, :].astype(stage.dtype)
        return 0

    lax.fori_loop(0, 2 * rows // blk, round_off, 0)

    @pl.when(z == 3)
    def _():
        w_fc.forward((2,))

    mine = c * 2 + x
    each = rows // 2
    swaps = []
    for (tc, tx), (tdp, tcp) in zip(others, quad):
        block = stage.at[pl.ds(pl.multiple_of((tc * 2 + tx) * each, each), each)]
        swaps.append(wires.to(block, mixed_ref.at[mine], tdp, tcp))
    for copy in swaps:
        copy.start()
    local = pltpu.make_async_copy(
        stage.at[pl.ds(pl.multiple_of(mine * each, each), each)], mixed_ref.at[mine], local_sems.at[1]
    )
    local.start()
    whole.forward()
    w_fc.forward((3,))
    w_proj.start()
    for copy in swaps:
        copy.wait_recv()
    whole.finish()
    w_fc.finish()
    w_proj.forward((1,))
    w_proj.finish()
    for copy in swaps:
        copy.wait_send()
    local.wait()

    @pl.when(jnp.logical_not(odd))
    def _():
        keys.wait_send()


def forward_call(sz, q, kv, w_out, w_fc, w_proj):
    part = sz.part
    rows = q.shape[0]

    def like(value, *lead):
        return jax.ShapeDtypeStruct(lead + value.shape, value.dtype)

    return pl.pallas_call(
        functools.partial(forward_kernel, sz.quarter_heads, sz.head_size, sz.fc_turn, sz.proj_turn),
        out_shape=(
            jax.ShapeDtypeStruct((rows, part), jnp.float32),
            jax.ShapeDtypeStruct((rows, 8), jnp.float32),
            like(kv),
            jax.ShapeDtypeStruct((4, rows // 4, part), jnp.bfloat16),
            like(w_out),
            like(w_fc),
            like(w_proj),
            like(w_out, 2, 2),
        ),
        in_specs=[VMEM, VMEM, HBM, HBM, HBM],
        out_specs=[VMEM] * 4 + [HBM] * 4,
        input_output_aliases={2: 4, 3: 5, 4: 6},
        scratch_shapes=[
            pltpu.VMEM((rows, part), jnp.bfloat16),
            *wire_sems(37),
            pltpu.SemaphoreType.DMA((2,)),
        ],
        cost_estimate=cost(120),
        compiler_params=remote_params(1, 56 << 20),
        name="forward",
    )(q, kv, w_out, w_fc, w_proj)


class QuadSum:
    step = 32

    def __init__(self, in_ref, out_ref, got_c, stage, got_x, send_sems, recv_sems):
        self.y, self.c, self.z, self.x = my_place()
        dp, cp = lax.axis_index("dp"), lax.axis_index("cp")
        wires = Wires(send_sems, recv_sems)
        self.in_ref, self.out_ref, self.got_c, self.stage, self.got_x = in_ref, out_ref, got_c, stage, got_x
        self.partners = [(dp + 1 - 2 * self.c, cp), (dp, cp + 1 - 2 * self.x)]
        self.by_c = wires.to(in_ref.at[1 - self.c], got_c, *self.partners[0])
        self.by_x = wires.to(stage, got_x, *self.partners[1])

    def each(self, act):
        def one(index, _):
            act(pl.ds(pl.multiple_of(index * self.step, self.step), self.step))
            return 0

        lax.fori_loop(0, self.out_ref.shape[0] // self.step, one, 0)

    def start(self, greeting=True):
        if greeting:
            greet(self.partners)
        self.by_c.start()

    def middle(self):
        c, x = self.c, self.x
        self.by_c.wait_recv()

        def to_send(span):
            self.stage[span, :] = (
                self.in_ref[c, 1 - x, span, :].astype(jnp.float32) + self.got_c[1 - x, span, :].astype(jnp.float32)
            ).astype(self.stage.dtype)

        self.each(to_send)
        self.by_x.start()

    def finish(self):
        c, x = self.c, self.x
        self.by_x.wait_recv()

        def to_add(span):
            self.out_ref[span, :] = (
                self.in_ref[c, x, span, :].astype(jnp.float32)
                + self.got_c[x, span, :].astype(jnp.float32)
                + self.got_x[span, :].astype(jnp.float32)
            )

        self.each(to_add)
        self.by_c.wait_send()
        self.by_x.wait_send()


def row_steps(rows, step=64):
    return [slice(start, min(start + step, rows)) for start in range(0, rows, step)]


class PlaceSum:
    def __init__(self, out, got, turn, send_sems, recv_sems, filled=False):
        self.y, self.c, self.z, self.x = my_place()
        self.dp = lax.axis_index("dp")
        self.out, self.got, self.turn, self.filled = out, got, turn, filled
        self.send_sems, self.recv_sems = send_sems, recv_sems

    def chunk(self, i):
        return (self.z + 5 + i - self.turn) % 4

    def put(self, i, store):
        if i == 3:
            store(self.got.at[self.z])
            return
        k = self.chunk(i)
        if not self.filled:
            store(self.out.at[k])
        pltpu.make_async_remote_copy(
            src_ref=self.out.at[k],
            dst_ref=self.got.at[self.z],
            send_sem=self.send_sems.at[i],
            recv_sem=self.recv_sems.at[self.z],
            device_id=(self.dp, ((self.z + 1 + i) % 4) * 2 + self.x),
            device_id_type=MESH,
        ).start()

    def total(self, into):
        for s in range(4):

            @pl.when(self.z != s)
            def _():
                pltpu.make_async_copy(self.got.at[s], self.got.at[s], self.recv_sems.at[s]).wait()

        for rows in row_steps(self.got.shape[1]):
            terms = [self.got[s, rows, :].astype(jnp.float32) for s in range(4)]
            into[rows, :] = (terms[0] + terms[1] + (terms[2] + terms[3])).astype(into.dtype)

    def finish(self):
        for i in range(3):
            view = self.out.at[self.chunk(i)]
            pltpu.make_async_copy(view, view, self.send_sems.at[i]).wait()


def copy_and_wait(src, dst, sem):
    copy = pltpu.make_async_copy(src, dst, sem)
    copy.start()
    copy.wait()


def gelu_parts(f):
    t = jnp.tanh(GELU_SCALE * (f + 0.044715 * f * f * f))
    return t, 0.5 * f * (1.0 + t)


def gelu_slope(f, t):
    return 0.5 * (1.0 + t) + 0.5 * f * (1.0 - t * t) * GELU_SCALE * (1.0 + 3.0 * 0.044715 * f * f)


class Crossing:
    def __init__(self, sent, kept, got_y, got_z, turn, y_sems, z_sems, out=None):
        dp, cp = lax.axis_index("dp"), lax.axis_index("cp")
        self.kept, self.got_y = kept, got_y
        self.places = PlaceSum(out, got_z, turn, *z_sems)
        self.copies = []
        for i in range(4):
            k = self.places.chunk(i)
            self.copies.append(
                pltpu.make_async_remote_copy(
                    src_ref=sent(k),
                    dst_ref=got_y.at[k],
                    send_sem=y_sems[0].at[i],
                    recv_sem=y_sems[1].at[i],
                    device_id=((dp + 2) % 4, cp),
                    device_id_type=MESH,
                )
            )

    def partners(self):
        dp, cp = lax.axis_index("dp"), lax.axis_index("cp")
        z, x = cp // 2, cp % 2
        return [((dp + 2) % 4, cp)] + [(dp, ((z + d) % 4) * 2 + x) for d in (1, 2, 3)]

    def start(self, i):
        self.copies[i].start()

    def settle(self, i):
        self.copies[i].wait_recv()
        k = self.places.chunk(i)
        kept = self.kept(k)

        def store(ref):
            for rows in row_steps(self.got_y.shape[1]):
                ref[rows, :] = (
                    kept[rows, :].astype(jnp.float32) + self.got_y[k, rows, :].astype(jnp.float32)
                ).astype(ref.dtype)

        self.places.put(i, store)

    def finish(self, value, share, sem):
        self.places.total(value)
        copy_and_wait(value, share, sem)

    def close(self):
        for copy in self.copies:
            copy.wait_send()
        self.places.finish()


def middle_kernel(
    proj_turn, act_ref, cot, w_fc, bias, proj_in,
    total, act_all, hid_t, fc_sent, fc_kept, bias_grad, proj_ref, proj_share,
    f_all, df_t, w_proj, proj_sent, proj_kept, got_y, got_z, share_v, term, got_c, stage, got_x,
    send_sems, recv_sems, y_send, y_recv, z_send, z_recv, sum_send, sum_recv, local_sems,
):
    y, c, _, _ = my_place()
    wires = Wires(send_sems, recv_sems)
    quad = QuadGather(wires, act_ref, act_all, local_sems.at[0])
    places = PlaceGather(wires, proj_ref, slot_turned(proj_turn), steps=(2, 3), over=(1, 2, 3))
    cross = Crossing(
        lambda k: proj_sent.at[k], lambda k: proj_kept.at[k], got_y, got_z, proj_turn,
        (y_send, y_recv), (z_send, z_recv), proj_kept,
    )
    summed = QuadSum(term, total, got_c, stage, got_x, sum_send, sum_recv)
    greet(cross.partners() + [quad.over_x, quad.over_c])
    quad.start()
    places.forward((1, 2))
    quad.forward()
    quad.finish()

    def hidden_of(side):
        def one(k, _):
            at = side * 4 + k
            f = dot_nt(w_fc[at], act_all[...]) + bias[at]
            f_all[at] = f.astype(f_all.dtype)
            hid_t[at] = gelu_parts(f)[1].astype(hid_t.dtype)
            return 0

        lax.fori_loop(0, 4, one, 0)

    hidden_of(1 - y)
    places.forward((3,))

    for i in range(4):
        k = cross.places.chunk(i)
        proj_sent[k] = dot_nn(hid_t[(1 - y) * 4 + k], cot[...]).astype(proj_sent.dtype)
        cross.start(i)
    hidden_of(y)

    def keep(k, _):
        proj_kept[k] = dot_nn(hid_t[y * 4 + k], cot[...]).astype(proj_kept.dtype)
        return 0

    lax.fori_loop(0, 4, keep, 0)
    places.finish()
    copy_and_wait(proj_ref, w_proj, local_sems.at[1])

    def back(at, _):
        f = f_all[at].astype(jnp.float32)
        grad = dot_nt(w_proj[at], cot[...])
        df = (grad * gelu_slope(f, gelu_parts(f)[0])).astype(df_t.dtype)
        df_t[at] = df
        bias_grad[at] = jnp.sum(df.astype(jnp.float32), axis=1, keepdims=True)
        return 0

    lax.fori_loop(0, 8, back, 0)
    cross.settle(0)
    block = term.shape[2]

    def tokens_of(core):
        for side in range(2):
            columns = pl.ds(pl.multiple_of((core * 2 + side) * block, block), block)
            value = dot_tn(df_t[0, :, columns], w_fc[0])
            for at in range(1, 8):
                value = value + dot_tn(df_t[at, :, columns], w_fc[at])
            term[core, side, :, :] = value.astype(term.dtype)

    tokens_of(1 - c)
    summed.start(greeting=False)
    tokens_of(c)
    summed.middle()
    cross.settle(1)

    def fc_terms(k, _):
        fc_sent[k] = dot_nn(df_t[(1 - y) * 4 + k], act_all[...]).astype(fc_sent.dtype)
        fc_kept[k] = dot_nn(df_t[y * 4 + k], act_all[...]).astype(fc_kept.dtype)
        return 0

    lax.fori_loop(0, 4, fc_terms, 0)
    cross.settle(2)
    summed.finish()
    cross.settle(3)
    cross.finish(share_v, proj_share, local_sems.at[1])
    cross.close()


def middle_call(sz, act, cot, w_fc, bias, w_proj):
    rows, width = act.shape
    share = w_fc.shape[1]
    bf16, f32 = act.dtype, jnp.float32

    def like(*shape, dtype=bf16):
        return jax.ShapeDtypeStruct(shape, dtype)

    def vmem(*shape):
        return pltpu.VMEM(shape, bf16)

    return pl.pallas_call(
        functools.partial(middle_kernel, sz.proj_turn),
        out_shape=(
            like(rows, width, dtype=f32),
            like(4 * rows, width),
            like(8, share, 4 * rows),
            like(4, share, width),
            like(4, share, width),
            like(8, share, 1, dtype=f32),
            like(8, share, width),
            like(share, width),
        ),
        in_specs=[VMEM] * 4 + [HBM],
        out_specs=[VMEM] * 6 + [HBM] * 2,
        input_output_aliases={4: 6},
        scratch_shapes=[
            vmem(8, share, 4 * rows),
            vmem(8, share, 4 * rows),
            vmem(8, share, width),
            vmem(4, share, width),
            vmem(4, share, width),
            vmem(4, share, width),
            vmem(4, share, width),
            vmem(share, width),
            vmem(2, 2, rows, width),
            vmem(2, rows, width),
            vmem(rows, width),
            vmem(rows, width),
            *wire_sems(10),
            *wire_sems(4),
            *wire_sems(4),
            *wire_sems(2),
            pltpu.SemaphoreType.DMA((2,)),
        ],
        cost_estimate=cost(110),
        compiler_params=remote_params(2, 63 << 20),
        name="middle",
    )(act, cot, w_fc, bias, w_proj)


def turn_kernel(
    heads, size, fc_turn, act_ref, w_out, hid_t, w_proj, fc_sent, fc_kept, q_ref, kv_ref, mix_ref, lse_ref,
    act_all, do_ref, dq_ref, dkv_ref, total, fc_share,
    dkv_sum, got_y, got_z, share_v, term, got_c, stage, got_x,
    send_sems, recv_sems, y_send, y_recv, z_send, z_recv, sum_send, sum_recv, local_sems,
):
    _, c, z, x = my_place()
    wires = Wires(send_sems, recv_sems)
    quad = QuadGather(wires, act_ref, act_all, local_sems.at[0])
    cross = Crossing(
        lambda k: fc_sent.at[k], lambda k: fc_kept.at[k], got_y, got_z, fc_turn,
        (y_send, y_recv), (z_send, z_recv), fc_kept,
    )
    summed = QuadSum(term, total, got_c, stage, got_x, sum_send, sum_recv)
    greet(cross.partners() + [quad.over_x, quad.over_c])
    quad.start()
    for k in range(4):
        cross.start(k)
    block = term.shape[2]

    def tokens_of(core):
        for side in range(2):
            columns = pl.ds(pl.multiple_of((core * 2 + side) * block, block), block)
            value = dot_tn(hid_t[0, :, columns], w_proj[0])
            for at in range(1, 8):
                value = value + dot_tn(hid_t[at, :, columns], w_proj[at])
            term[core, side, :, :] = value.astype(term.dtype)

    tokens_of(1 - c)
    summed.start(greeting=False)
    tokens_of(c)
    quad.forward()
    cross.settle(0)
    quad.finish()
    summed.middle()
    pair = 2 * size
    turns = heads * size // pair
    quarter = c * 2 + x

    def mix_rows(index, _):
        here = pl.ds(pl.multiple_of(index * block, block), block)
        for j in range(turns):
            columns = pl.ds(pl.multiple_of((4 * j + quarter) * pair, pair), pair)
            do_ref[here, j * pair : (j + 1) * pair] = dot_nn(act_all[here, :], w_out[:, columns]).astype(do_ref.dtype)

        @pl.when(quarter == 0)
        def _():
            last = w_out.shape[1] - size
            do_ref[here, turns * pair :] = dot_nn(act_all[here, :], w_out[:, last:]).astype(do_ref.dtype)

        @pl.when(quarter != 0)
        def _():
            do_ref[here, turns * pair :] = jnp.zeros((block, size), do_ref.dtype)

        return 0

    lax.fori_loop(0, 4, mix_rows, 0)
    part = heads * size
    rows = q_ref.shape[0] // 2
    blk = 256
    scale = size**-0.5
    odd = z % 2 == 1

    def group(index):
        start = pl.multiple_of(index * rows, rows)
        keys_at = pl.ds(start, rows)
        dkv_sum[...] = jnp.zeros_like(dkv_sum)

        def one(i, _):
            here = pl.ds(pl.multiple_of(start + i * blk, blk), blk)
            for h in range(heads):
                cols = slice(h * size, (h + 1) * size)
                vals = slice(part + h * size, part + (h + 1) * size)
                q = q_ref[here, cols]
                k = kv_ref[keys_at, cols]
                do = do_ref[here, cols]
                p = jnp.exp(dot_nt(q, k) * scale - lse_ref[here, h : h + 1])
                dp = dot_nt(do, kv_ref[keys_at, vals])
                delta = jnp.sum(do.astype(jnp.float32) * mix_ref[here, cols], axis=-1, keepdims=True)
                ds = (p * (dp - delta)).astype(jnp.bfloat16)
                dq_ref[here, cols] = dot_nn(ds, k) * scale
                dkv_sum[:, cols] += dot_tn(ds, q) * scale
                dkv_sum[:, vals] += dot_tn(p.astype(jnp.bfloat16), do)
            return 0

        lax.fori_loop(0, rows // blk, one, 0)
        dkv_ref[keys_at, :] = dkv_sum[...].astype(dkv_ref.dtype)

    @pl.when(jnp.logical_not(odd))
    def _():
        dq_ref[...] = jnp.zeros_like(dq_ref)

    def one_group(index, _):
        @pl.when(odd)
        def _():
            group(index)

        return 0

    lax.fori_loop(0, 1, one_group, 0)
    cross.settle(1)
    cross.settle(2)
    summed.finish()
    lax.fori_loop(1, 2, one_group, 0)
    cross.settle(3)
    cross.finish(share_v, fc_share, local_sems.at[1])
    cross.close()


def turn_call(sz, act, w_out, hid_t, w_proj, fc_sent, fc_kept, q, before, mix, lse):
    rows, width = act.shape
    share = w_proj.shape[1]
    bf16, f32 = act.dtype, jnp.float32

    def like(*shape, dtype=bf16):
        return jax.ShapeDtypeStruct(shape, dtype)

    def vmem(*shape):
        return pltpu.VMEM(shape, bf16)

    return pl.pallas_call(
        functools.partial(turn_kernel, sz.quarter_heads, sz.head_size, sz.fc_turn),
        out_shape=(
            like(4 * rows, width),
            like(4 * rows, sz.part),
            like(4 * rows, sz.part, dtype=f32),
            like(4 * rows, 2 * sz.part),
            like(rows, width, dtype=f32),
            like(share, width),
        ),
        in_specs=[VMEM] * 4 + [HBM] + [VMEM] * 5,
        out_specs=[VMEM] * 5 + [HBM],
        scratch_shapes=[
            pltpu.VMEM((2 * rows, 2 * sz.part), f32),
            vmem(4, share, width),
            vmem(4, share, width),
            vmem(share, width),
            vmem(2, 2, rows, width),
            vmem(2, rows, width),
            vmem(rows, width),
            vmem(rows, width),
            *wire_sems(3),
            *wire_sems(4),
            *wire_sems(4),
            *wire_sems(2),
            pltpu.SemaphoreType.DMA((2,)),
        ],
        cost_estimate=cost(80),
        compiler_params=remote_params(3, 62 << 20),
        name="turn",
    )(act, w_out, hid_t, w_proj, fc_sent, fc_kept, q, before, mix, lse)


class Collector:
    def __init__(self, sz):
        self.sz = sz
        self.y, self.c, self.z, self.x = my_place()
        self.me = flat_id(self.y, self.c, self.z, self.x)
        self.quarter = self.c * 2 + self.x

    def send(self, src, dst, table, sem, recv):
        dest = table // self.sz.block

        @pl.when(dest == self.me)
        def _():
            pltpu.make_async_copy(src, dst, recv).start()

        @pl.when(dest != self.me)
        def _():
            pltpu.make_async_remote_copy(
                src_ref=src,
                dst_ref=dst,
                send_sem=sem,
                recv_sem=recv,
                device_id=(dest // 8, dest % 8),
                device_id_type=MESH,
            ).start()

    def sent(self, src, dst, table, sem, recv):
        @pl.when(table // self.sz.block != self.me)
        def _():
            pltpu.make_async_copy(src, src, sem).wait()

    def received(self, first, count, view, recv):
        block = self.sz.block
        for device in range(first // block, -(-(first + count) // block)):
            grains = min(first + count, (device + 1) * block) - max(first, device * block)

            @pl.when(self.me == device)
            def _():
                pltpu.make_async_copy(view(grains), view(grains), recv).wait()


def close_kernel(
    sz, dqkv, act, w_qkv, normed, vec_in, out_sum, fc_share, proj_share,
    total, g_qkv, g_mlp, g_outs, vecs, qkv_share, out_share,
    grads, got_y, qkv_out, qkv_got, out_got, share_v, out_v, vec_v, term, got_c, stage, got_x,
    y_send, y_recv, z_send, z_recv, sum_send, sum_recv, grain_sems, kind_sems, local_sems, vec_sems,
):
    to = Collector(sz)
    y, c, z = to.y, to.c, to.z
    rows = got_y.shape[1]
    block = term.shape[2]
    out = PlaceSum(out_sum, out_got, 0, z_send.at[1], z_recv.at[1], True)
    cross = Crossing(
        lambda k: grads.at[2 * k + 1 - y], lambda k: grads.at[2 * k + y], got_y, qkv_got, 0,
        (y_send, y_recv), (z_send.at[2], z_recv.at[2]), qkv_out,
    )
    summed = QuadSum(term, total, got_c, stage, got_x, sum_send, sum_recv)

    for i in range(4):
        out.put(i, lambda ref, i=i: copy_and_wait(out_sum.at[out.chunk(i)], ref, local_sems.at[0]))

    def mlp_grains(act_on, ref, base, turn, first_sem):
        r = range_of_spot(y, (z + 4 - turn) % 4)

        def one(slot, _):
            table = base + 4 * (r * sz.mlp + slot) + to.quarter
            act_on(ref(slot), g_mlp.at[table % sz.block], table, grain_sems.at[first_sem + slot], kind_sems.at[0])
            return 0

        lax.fori_loop(0, sz.mlp, one, 0)

    def grain_of(ref):
        return lambda slot: ref.at[pl.ds(pl.multiple_of(slot * GRAIN, GRAIN), GRAIN)]

    def out_grains(act_on, first_sem):
        count = out_share.shape[0] // GRAIN

        def one(slot, _):
            table = sz.out_start + slot_out(y, z) * count + slot
            dst = g_outs.at[to.quarter, table % sz.block]
            act_on(grain_of(out_share)(slot), dst, table, grain_sems.at[first_sem + slot], kind_sems.at[1])
            return 0

        lax.fori_loop(0, count, one, 0)

    def head_grains(act_on, first_sem):
        def one(slot, _):
            local = slot_qkv(y, z) * sz.qkv + slot
            inner = local % sz.part_grains
            index = inner // sz.head_grains
            head = 8 * (index // 2) + 2 * to.quarter + index % 2

            @pl.when(head < sz.heads)
            def _():
                table = (local // sz.part_grains) * sz.width_grains + head * sz.head_grains + inner % sz.head_grains
                act_on(
                    grain_of(qkv_share)(slot), g_qkv.at[table % sz.block], table,
                    grain_sems.at[first_sem + slot], kind_sems.at[2],
                )

            return 0

        lax.fori_loop(0, sz.qkv, one, 0)

    counts = (0, sz.mlp, 2 * sz.mlp, 3 * sz.mlp)
    mlp_grains(to.send, grain_of(proj_share), sz.proj_start, sz.proj_turn, counts[0])
    mlp_grains(to.send, grain_of(fc_share), sz.fc_start, sz.fc_turn, counts[1])

    for s in range(8):
        grads[s, :, :] = dot_tn(dqkv[:, s * rows : (s + 1) * rows], act[...]).astype(grads.dtype)
    for i in range(4):
        cross.start(i)

    def tokens_of(core):
        for side in range(2):
            here = pl.ds(pl.multiple_of((core * 2 + side) * block, block), block)
            term[core, side, :, :] = dot_nn(dqkv[here, :], w_qkv[...]).astype(term.dtype)

    tokens_of(1 - c)
    summed.start(greeting=False)
    tokens_of(c)
    summed.middle()

    def settle(part, value, share):
        part.total(value)
        copy_and_wait(value, share, local_sems.at[1])

    settle(out, out_v, out_share)
    out_grains(to.send, counts[2])
    for i in range(4):
        cross.settle(i)
    summed.finish()

    vec_v[...] = vec_in[...]
    vec_v[0:1, :] = jnp.sum(total[...] * normed[...], axis=0, keepdims=True)
    vec_v[1:2, :] = jnp.sum(total[...], axis=0, keepdims=True)
    last = sz.vec_start // sz.block
    vec_copy = pltpu.make_async_remote_copy(
        src_ref=vec_v,
        dst_ref=vecs.at[to.me],
        send_sem=vec_sems.at[0],
        recv_sem=vec_sems.at[1],
        device_id=(last // 8, last % 8),
        device_id_type=MESH,
    )

    @pl.when(to.me != last)
    def _():
        vec_copy.start()

    @pl.when(to.me == last)
    def _():
        pltpu.make_async_copy(vec_v, vecs.at[to.me], vec_sems.at[1]).start()

    cross.finish(share_v, qkv_share, local_sems.at[1])
    head_grains(to.send, counts[3])

    cross.close()
    out.finish()
    mlp_grains(to.sent, grain_of(proj_share), sz.proj_start, sz.proj_turn, counts[0])
    mlp_grains(to.sent, grain_of(fc_share), sz.fc_start, sz.fc_turn, counts[1])
    out_grains(to.sent, counts[2])
    head_grains(to.sent, counts[3])

    @pl.when(to.me != last)
    def _():
        vec_copy.wait_send()

    @pl.when(to.me == last)
    def _():
        pltpu.make_async_copy(vecs, vecs, vec_sems.at[1]).wait()

    to.received(sz.fc_start, 64 * sz.mlp, lambda n: g_mlp.at[pl.ds(0, n)], kind_sems.at[0])
    to.received(sz.out_start, sz.width_grains, lambda n: g_outs.at[:, pl.ds(0, n)], kind_sems.at[1])
    to.received(0, 3 * sz.width_grains, lambda n: g_qkv.at[pl.ds(0, n)], kind_sems.at[2])


def close_call(sz, dqkv, act, w_qkv, normed, vectors, out_sum, fc_share, proj_share):
    rows, width = normed.shape
    bf16, f32 = act.dtype, jnp.float32
    qkv_rows, out_rows = sz.qkv * GRAIN, out_sum.shape[1]

    def like(*shape, dtype=bf16):
        return jax.ShapeDtypeStruct(shape, dtype)

    def vmem(*shape):
        return pltpu.VMEM(shape, bf16)

    return pl.pallas_call(
        functools.partial(close_kernel, sz),
        out_shape=(
            like(rows, width, dtype=f32),
            like(sz.block, GRAIN, width),
            like(sz.block, GRAIN, width),
            like(4, sz.block, GRAIN, sz.part),
            like(32, *vectors.shape, dtype=f32),
            like(qkv_rows, width),
            like(out_rows, sz.part),
        ),
        in_specs=[VMEM] * 6 + [HBM] * 2,
        out_specs=[VMEM] + [HBM] * 6,
        scratch_shapes=[
            vmem(8, qkv_rows, width),
            vmem(4, qkv_rows, width),
            vmem(4, qkv_rows, width),
            vmem(4, qkv_rows, width),
            vmem(4, out_rows, sz.part),
            vmem(qkv_rows, width),
            vmem(out_rows, sz.part),
            pltpu.VMEM(vectors.shape, f32),
            vmem(2, 2, rows, width),
            vmem(2, rows, width),
            vmem(rows, width),
            vmem(rows, width),
            *wire_sems(4),
            pltpu.SemaphoreType.DMA((3, 4)),
            pltpu.SemaphoreType.DMA((3, 4)),
            *wire_sems(2),
            pltpu.SemaphoreType.DMA((3 * sz.mlp + sz.qkv,)),
            pltpu.SemaphoreType.DMA((3,)),
            pltpu.SemaphoreType.DMA((2,)),
            pltpu.SemaphoreType.DMA((2,)),
        ],
        cost_estimate=cost(120),
        compiler_params=remote_params(None, 62 << 20),
        name="close",
    )(dqkv, act, w_qkv, normed, vectors, out_sum, fc_share, proj_share)


def attend_back_kernel(heads, size, q_ref, kv_ref, do_ref, mix_ref, lse_ref, seed_ref, dq_ref, dkv_ref):
    part = heads * size
    rows = q_ref.shape[0] // 2
    blk = 256
    scale = size**-0.5

    def group(index, _):
        start = pl.multiple_of(index * rows, rows)
        dkv_ref[pl.ds(start, rows), :] = jnp.zeros((rows, 2 * part), dkv_ref.dtype)
        for i in range(rows // blk):
            seen = (i + 1) * blk
            here = pl.ds(pl.multiple_of(start + i * blk, blk), blk)
            keys_at = pl.ds(start, seen)
            lane = lax.broadcasted_iota(jnp.int32, (blk, seen), 1)
            line = lax.broadcasted_iota(jnp.int32, (blk, seen), 0)
            allowed = lane <= line + i * blk
            for h in range(heads):
                cols = slice(h * size, (h + 1) * size)
                vals = slice(part + h * size, part + (h + 1) * size)
                q = q_ref[here, cols]
                k = kv_ref[keys_at, cols]
                do = do_ref[here, cols]
                p = jnp.exp(dot_nt(q, k) * scale - lse_ref[here, h : h + 1])
                p = jnp.where(allowed, p, 0.0)
                dp = dot_nt(do, kv_ref[keys_at, vals])
                delta = jnp.sum(do.astype(jnp.float32) * mix_ref[here, cols], axis=-1, keepdims=True)
                ds = (p * (dp - delta)).astype(jnp.bfloat16)
                dq_ref[here, cols] = (dot_nn(ds, k) * scale + seed_ref[here, cols]).astype(dq_ref.dtype)
                dkv_ref[keys_at, cols] += dot_tn(ds, q) * scale
                dkv_ref[keys_at, vals] += dot_tn(p.astype(jnp.bfloat16), do)
        return 0

    lax.fori_loop(0, 2, group, 0)


def attend_back(sz, q, kv, grad_mix, mix, lse, seed):
    return pl.pallas_call(
        functools.partial(attend_back_kernel, sz.quarter_heads, sz.head_size),
        out_shape=(
            jax.ShapeDtypeStruct(q.shape, jnp.bfloat16),
            jax.ShapeDtypeStruct(kv.shape, jnp.float32),
        ),
        in_specs=[VMEM] * 6,
        out_specs=[VMEM] * 2,
        cost_estimate=cost(35),
        compiler_params=pltpu.CompilerParams(vmem_limit_bytes=56 << 20),
        name="attend_back",
    )(q, kv, grad_mix, mix, lse, seed)


def rowwise(value):
    return with_layout_constraint(value, Layout(major_to_minor=(0, 1)))


def norm_parts(values):
    mean = jnp.mean(values, axis=-1, keepdims=True)
    centre = values - mean
    rs = lax.rsqrt(jnp.mean(centre * centre, axis=-1, keepdims=True) + EPSILON)
    return centre * rs, rs


def norm_back(normed, rs, grad, gain):
    e = grad * gain
    return rs * (
        e
        - jnp.mean(e, axis=-1, keepdims=True)
        - normed * jnp.mean(e * normed, axis=-1, keepdims=True)
    )


def per_device_quad(tokens, params, out_grad, lengths):
    _, width = tokens.shape
    hidden = FF
    sz = Sizes(width, hidden, HEADS, HEAD_DIM, params.shape[0])
    y, c, z, x = my_place()
    quarter = c * 2 + x
    bf16, f32 = jnp.bfloat16, jnp.float32

    def pick(value, index):
        return lax.dynamic_index_in_dim(value, index, 0, keepdims=False)

    def to_other_y(sent):
        return over_y(sent.astype(bf16))

    w_qkv, w_out, w_fc, w_proj, vec, tok_all, cot_all = open_call(
        sz, params.reshape(sz.block, GRAIN, width), tokens, out_grad
    )
    flat = lambda value: value.reshape(-1, width)
    vectors = flat(vec).astype(f32)
    fc_bias = vectors[8 : 8 + hidden // width].reshape(hidden)
    w_qkv, cot_all = flat(w_qkv), flat(cot_all)
    normed_all, _ = norm_parts(flat(tok_all).astype(f32))
    act_one = (normed_all * vectors[0] + vectors[1]).astype(bf16)

    pair = 2 * sz.head_size
    turns = width // (4 * pair)
    rest = width - 4 * turns * pair

    def quarter_of(value):
        blocks = [lax.dynamic_slice_in_dim(value, (4 * j + quarter) * pair, pair, 1) for j in range(turns)]
        end = value[:, width - rest :]
        return jnp.concatenate(blocks + [jnp.where(quarter == 0, end, jnp.zeros_like(end))], axis=1)

    def by_head(quarters):
        blocks = [quarters[k][:, j * pair : (j + 1) * pair] for j in range(turns) for k in range(4)]
        return jnp.concatenate(blocks + [quarters[0][:, turns * pair : turns * pair + rest]], axis=1)

    biases = quarter_of(vectors[2:4])
    kv_bias = jnp.concatenate([jnp.zeros((sz.part,), f32), biases[1]])
    kv = (dot_nt(act_one, w_qkv[sz.part :]) + kv_bias).astype(bf16)
    q = (dot_nt(act_one, w_qkv[: sz.part]) + biases[0]).astype(bf16)
    mix, lse, before, mixed, _, w_fc, w_proj, w_out = forward_call(sz, q, kv, w_out, w_fc, w_proj)
    w_fc, w_out = flat(w_fc), flat(w_out)[:width]
    mixed = by_head(mixed)
    inputs = tokens.astype(f32)
    residual = inputs + (dot_nt(mixed, w_out) + vectors[4])
    normed_two, rs_two = norm_parts(residual)
    act_two = (normed_two * vectors[5] + vectors[6]).astype(bf16)
    bias = lax.dynamic_index_in_dim(fc_bias.reshape(-1, 4, GRAIN), quarter, 1, keepdims=False)
    bias = bias.reshape(8, hidden // 32)[jnp.array(RANGES)][:, :, None]
    shares = lambda value: value.reshape(8, hidden // 32, width)
    grad_two, _, hid_t, fc_sent, fc_kept, bias_sum, w_proj, proj_share = middle_call(
        sz, act_two, cot_all, shares(w_fc), bias, shares(w_proj)
    )

    cot = out_grad.astype(f32)
    grad_res = cot + norm_back(normed_two, rs_two, grad_two, vectors[5])
    grad_attn = grad_res.astype(bf16)
    attn_all, grad_mix, dq_before, dkv_before, out_sum, fc_share = turn_call(
        sz, grad_attn, w_out, hid_t, w_proj, fc_sent, fc_kept, q, before, mix, lse
    )
    output = (residual + out_sum + vectors[7]).astype(bf16)
    returned = permute(
        dkv_before, lambda py, pc, pz, px: (py, pc, pz - 1, px) if pz % 2 == 1 else None
    )
    g_out = rowwise(dot_tn(attn_all, mix.astype(bf16)).astype(bf16)).reshape(2, width // 2, sz.part)
    got_out = to_other_y(pick(g_out, 1 - y))
    out_sum = (pick(g_out, y).astype(f32) + got_out.astype(f32)).astype(bf16).reshape(4, width // 8, sz.part)
    dq, dkv = attend_back(sz, q, kv, grad_mix, mix, lse, dq_before)
    grad_qkv = jnp.concatenate([dq, (dkv + returned.astype(f32)).astype(bf16)], axis=1)
    normed_one, rs_one = norm_parts(inputs)

    def placed(vector):
        spread = jnp.zeros((1, width), f32)
        for j in range(turns):
            block = vector[None, j * pair : (j + 1) * pair]
            spread = lax.dynamic_update_slice_in_dim(spread, block, (4 * j + quarter) * pair, 1)
        end = jnp.where(quarter == 0, vector[turns * pair : turns * pair + rest], 0.0)
        return jnp.concatenate([spread[0, : width - rest], end])

    sums = jnp.sum(grad_qkv.astype(f32), axis=0)
    bias_sum = bias_sum.reshape(8, hidden // 32)[jnp.array(SPOTS)]
    fc_rows = lax.dynamic_update_slice_in_dim(
        jnp.zeros((hidden // 4 // GRAIN, 4, GRAIN), f32), bias_sum.reshape(-1, 1, GRAIN), quarter, 1
    )
    grad_vectors = jnp.concatenate(
        [
            jnp.stack(
                [
                    jnp.zeros((width,), f32),
                    jnp.zeros((width,), f32),
                    placed(sums[: sz.part]),
                    placed(sums[2 * sz.part :]),
                    jnp.sum(grad_attn.astype(f32), axis=0),
                    jnp.sum(grad_two * normed_two, axis=0),
                    jnp.sum(grad_two, axis=0),
                    jnp.sum(cot, axis=0),
                ]
            ),
            fc_rows.reshape(hidden // width, width),
        ]
    )
    count = grad_vectors.shape[0]
    grad_vectors = jnp.pad(grad_vectors, ((0, sz.vec * GRAIN - count), (0, 0)))
    grad_one, table_qkv, table_mlp, table_out, all_vectors = close_call(
        sz, grad_qkv, act_one, w_qkv, normed_one, grad_vectors, out_sum, fc_share, proj_share
    )[:5]
    input_grad = (grad_res + norm_back(normed_one, rs_one, grad_one, vectors[0])).astype(bf16)
    grad_vectors = jnp.sum(all_vectors, axis=0)[:count]
    table_out = by_head(table_out.reshape(4, -1, sz.part))
    me = flat_id(y, c, z, x)
    row = me * (sz.block * GRAIN) + lax.broadcasted_iota(jnp.int32, (sz.block * GRAIN, 1), 0)
    used = (sz.vec_start % sz.block) * GRAIN
    tail = jnp.pad(grad_vectors, ((used, sz.block * GRAIN - used - count), (0, 0)))
    param_grad = jnp.where(
        row < sz.out_start * GRAIN,
        flat(table_qkv).astype(f32),
        jnp.where(
            row < sz.fc_start * GRAIN,
            table_out.astype(f32),
            jnp.where(row < sz.vec_start * GRAIN, flat(table_mlp).astype(f32), tail),
        ),
    )
    return (output, input_grad, param_grad)


def fits_quad(mesh, tokens, params, lengths):
    dp, cp = mesh.shape["dp"], mesh.shape["cp"]
    rows = tokens.shape[0] // (dp * cp)
    width = tokens.shape[1]
    blocks = params.shape[0] // (dp * cp)
    return (
        (dp, cp) == (4, 8)
        and lengths.shape[1] == 2
        and rows * cp == lengths.shape[1] * MIN_LEN
        and rows % 128 == 0
        and blocks % GRAIN == 0
        and (HEADS, HEAD_DIM, FF, width) == (25, 64, 6400, 1600)
    )


def solution(mesh):
    in_specs = (P(("dp", "cp"), None), P(("dp", "cp"), None), P(("dp", "cp"), None), P("dp", None))
    out_specs = (P(("dp", "cp"), None), P(("dp", "cp"), None), P(("dp", "cp"), None))

    def step(tokens, params, out_grad, lengths):
        body = per_device_quad if fits_quad(mesh, tokens, params, lengths) else per_device_general

        return jax.shard_map(
            body, mesh=mesh, in_specs=in_specs, out_specs=out_specs, check_vma=False
        )(tokens, params, out_grad, lengths)

    return step
```
